32 devices in a mesh: rep: 8 (over y, x, core), grp: 4 (over z).
Axes of the slice: x: 2, y: 2, z: 4, core: 2. Of those that a mesh axis runs over, the one named last changes fastest.
Arguments:
- frames: bfloat16 [8192, 768], P(('rep', 'grp')), may hold values from -6 to 6
- cotangent: bfloat16 [8192, 768], P(('rep', 'grp')), may hold values from -6 to 6
- params: bfloat16 [4, 1771776], P('grp'), may hold values from -8 to 8, as said below
- first_moment: float32 [4, 1771776], P('grp'), as said below
- second_moment: float32 [4, 1771776], P('grp'), as said below
Outputs:
- out_frames: bfloat16 [8192, 768], P(('rep', 'grp'))
- frames_grad: bfloat16 [8192, 768], P(('rep', 'grp'))
- param_grad: float32 [4, 1771776], P('grp')
- new_params: float32 [4, 1771776], P('grp')
- new_first: float32 [4, 1771776], P('grp')
- new_second: float32 [4, 1771776], P('grp')
The draws below stay inside these ranges and needn't reach their ends.
Inputs may be any that keep to these rules, and one draw needn't show every extreme that they name: `params`: laid out as the first step says; gains lie between 0.5 and 1.5. `first_moment`: laid out as the first step says. `second_moment`: Positive; laid out as the first step says.
All inputs are finite; a program needn't handle non-finite values.
Results may differ from the reference program's by a relative error of at most 0.012.
The reference program's roundings to bfloat16 on the way count: a program that leaves them out, or rounds other values in their place, can miss the bound.
Values may be sent and summed in bfloat16 or wider, within the bound.
A program may use at most 256 MiB of HBM per device.

```python
import math
import jax
import jax.numpy as jnp
from jax import lax

D = 768
FF = 3072
HDIM = 64
CLIP = 1024
TOKENS = 8192
N_REP = 8
N_GRP = 4


def tensor_shapes_drawn():
    return [(D, 1), (D, 1), (D, 3 * D), (2 * D, 1), (D, D), (D, 1), (D, 1), (D, 1), (D, FF), (FF, 1), (FF, D), (D, 1)]


def tensor_factors():
    return [1.5, 1.5, 1.0, 1.0, 0.3, 1.0, 0.6, 0.6, 0.3, 0.3, 0.7, 1.0]


def pack_rows(tensors):
    return jnp.concatenate([item.reshape(N_GRP, -1) for item in tensors], axis=1)


def bounded(key, shape):
    return jax.random.truncated_normal(key, -4.0, 4.0, shape, jnp.float32)


def draw_params(key, part):
    keys = jax.random.split(key, 16)
    root = 1.0 / math.sqrt(D)
    gain_one = jax.random.uniform(keys[0], (D, 1), jnp.float32, 0.5, 1.5)
    shift_one = 0.3 * bounded(keys[1], (D, 1))
    query_weight = bounded(keys[2], (D, D)) * root
    key_weight = bounded(keys[3], (D, D)) * root
    value_weight = bounded(keys[4], (D, D)) * root
    qkv_weight = jnp.concatenate([query_weight, key_weight, value_weight], axis=1)
    qv_bias = 0.3 * bounded(keys[7], (2 * D, 1))
    out_weight = bounded(keys[8], (D, D)) * root * math.sqrt(CLIP) * 0.5
    out_bias = 0.3 * bounded(keys[9], (D, 1))
    gain_two = jax.random.uniform(keys[10], (D, 1), jnp.float32, 0.5, 1.5)
    shift_two = 0.3 * bounded(keys[11], (D, 1))
    up_weight = bounded(keys[12], (D, FF)) * root
    up_bias = 0.3 * bounded(keys[13], (FF, 1))
    down_weight = bounded(keys[14], (FF, D)) / math.sqrt(FF)
    down_bias = 0.3 * bounded(keys[15], (D, 1))
    tensors = [gain_one, shift_one, qkv_weight, qv_bias, out_weight, out_bias, gain_two, shift_two, up_weight, up_bias, down_weight, down_bias]
    return pack_rows(tensors).astype(jnp.bfloat16)


def segment_scales():
    pieces = []
    base = math.sqrt(CLIP / N_REP)
    for height, breadth in tensor_shapes_drawn():
        factor = 0.3 if breadth > 1 else 1.0
        pieces.append(jnp.full((height, breadth), base * factor, jnp.float32))
    return pack_rows(pieces)


def moment_scales():
    pieces = []
    base = math.sqrt(CLIP / N_REP)
    for shape, factor in zip(tensor_shapes_drawn(), tensor_factors()):
        pieces.append(jnp.full(shape, base * factor, jnp.float32))
    return pack_rows(pieces)


def draw_first_moment(key, part):
    scales = segment_scales()
    return 0.15 * scales * bounded(key, scales.shape)


def draw_second_moment(key, part):
    scales = moment_scales()
    lowest = 0.02
    highest = 12.0
    spread = jnp.exp(jax.random.uniform(key, scales.shape, jnp.float32, math.log(lowest), math.log(highest)))
    return 0.02 * scales * scales * spread


def shard_levels(stream_key, extent, shards, low, largest):
    def one(position, parts):
        steps = jax.random.uniform(jax.random.fold_in(jax.random.fold_in(stream_key, 6), position), (parts,), jnp.float32, low / len(shards), largest / len(shards))
        return jnp.repeat(jnp.exp(steps), extent[position] // parts).reshape((-1,) + (1,) * (len(extent) - position - 1))

    level = one(*shards[0])
    for cut in shards[1:]:
        level = level * one(*cut)
    return level


def gaussian(key, dims, scale, bound, cuts=(), held_as=jnp.bfloat16):
    loudness = shard_levels(key, dims, cuts, -0.22, 0.18) if cuts else 1.0
    array = jax.random.normal(key, dims, jnp.float32) * scale * loudness
    return jnp.minimum(jnp.maximum(array, -bound), bound).astype(held_as)


def setup_inputs(seed: int = 0) -> dict:
    splits = jax.random.split(jax.random.key(seed), 6)
    return {
        "frames": gaussian(splits[0], (TOKENS, D), 1.0, 6.0, ((0, 32),)),
        "cotangent": gaussian(splits[1], (TOKENS, D), 1.0, 6.0, ((0, 32),)),
        "params": draw_params(jax.random.fold_in(splits[5], 71), 0),
        "first_moment": draw_first_moment(jax.random.fold_in(splits[5], 71), 0),
        "second_moment": draw_second_moment(jax.random.fold_in(splits[5], 71), 0),
    }


EPS_NORM = 1e-05
BETA_ONE = 0.9
BETA_TWO = 0.98
ADAM_EPS = 1e-06
LEARN_RATE = 0.006
DECAY = 0.01
adam_step = 4
HIGHEST = lax.Precision.HIGHEST

def tensor_shapes():
    return [(D, 1), (D, 1), (D, 3 * D), (2 * D, 1), (D, D), (D, 1), (D, 1), (D, 1), (D, FF), (FF, 1), (FF, D), (D, 1)]

def unpack(flat):
    groups = flat.shape[0]
    result = []
    offset = 0
    for height, breadth in tensor_shapes():
        length = height * breadth // groups
        block = flat[:, offset:offset + length]
        if breadth > 1:
            result.append(block.reshape(height, breadth))
        else:
            result.append(block.reshape(height))
        offset += length
    return tuple(result)

def pack(tensors, groups):
    return jnp.concatenate([item.reshape(groups, -1) for item in tensors], axis=1)

def norm_forward(values):
    center = values - lax.optimization_barrier(jnp.mean(values, axis=-1, keepdims=True))
    inverse = lax.rsqrt(lax.optimization_barrier(jnp.mean(center * center, axis=-1, keepdims=True)) + EPS_NORM)
    return (center * inverse, inverse)

def norm_backward(upstream, normalized, inverse, gain):
    scaled = upstream * gain
    return inverse * (scaled - lax.optimization_barrier(jnp.mean(scaled, axis=-1, keepdims=True)) - normalized * lax.optimization_barrier(jnp.mean(scaled * normalized, axis=-1, keepdims=True)))

def gelu(values):
    return 0.5 * values * (1.0 + lax.erf(values * 0.7071067811865476))

def gelu_slope(values):
    return 0.5 * (1.0 + lax.erf(values * 0.7071067811865476)) + values * jnp.exp(-0.5 * values * values) * 0.3989422804014327

def to_pairs(matrix):
    heads = matrix.shape[1] // HDIM
    return matrix.reshape(matrix.shape[0], heads // 2, 2, HDIM).transpose(1, 0, 2, 3)

def from_pairs(stacked):
    return stacked.transpose(1, 0, 2, 3).reshape(stacked.shape[1], -1)

def attend(query, keys, values):
    scale = HDIM ** (-0.5)

    def one_pair(items):
        query_pair, key_pair, value_pair = items
        scores = jnp.einsum('qhd,khd->hqk', query_pair.astype(jnp.float32), key_pair.astype(jnp.float32), precision=HIGHEST) * scale
        highest = lax.optimization_barrier(jnp.max(scores, axis=-1, keepdims=True))
        log_total = highest + jnp.log(lax.optimization_barrier(jnp.sum(jnp.exp(scores - highest), axis=-1, keepdims=True)))
        shares = jnp.exp(scores - log_total).astype(jnp.bfloat16)
        mixed = jnp.einsum('hqk,khd->qhd', shares.astype(jnp.float32), value_pair.astype(jnp.float32), precision=HIGHEST)
        return (mixed, log_total[..., 0])
    mixed, log_total = lax.map(one_pair, (to_pairs(query), to_pairs(keys), to_pairs(values)))
    return (from_pairs(mixed).astype(jnp.bfloat16), log_total)

def attend_back(query, keys, values, attended, upstream, log_total):
    scale = HDIM ** (-0.5)

    def one_pair(items):
        query_pair, key_pair, value_pair, attended_pair, upstream_pair, log_pair = items
        query_wide = query_pair.astype(jnp.float32)
        key_wide = key_pair.astype(jnp.float32)
        upstream_wide = upstream_pair.astype(jnp.float32)
        scores = jnp.einsum('qhd,khd->hqk', query_wide, key_wide, precision=HIGHEST) * scale
        shares = jnp.exp(scores - log_pair[..., None])
        value_grad = jnp.einsum('hqk,qhd->khd', shares.astype(jnp.bfloat16).astype(jnp.float32), upstream_wide, precision=HIGHEST)
        share_grad = jnp.einsum('qhd,khd->hqk', upstream_wide, value_pair.astype(jnp.float32), precision=HIGHEST)
        centre = lax.optimization_barrier(jnp.sum(upstream_wide * attended_pair.astype(jnp.float32), axis=-1)).transpose(1, 0)
        score_grad = (shares * (share_grad - centre[..., None]) * scale).astype(jnp.bfloat16).astype(jnp.float32)
        query_grad = jnp.einsum('hqk,khd->qhd', score_grad, key_wide, precision=HIGHEST)
        key_grad = jnp.einsum('hqk,qhd->khd', score_grad, query_wide, precision=HIGHEST)
        return (query_grad, key_grad, value_grad)
    stacked = (to_pairs(query), to_pairs(keys), to_pairs(values), to_pairs(attended), to_pairs(upstream), log_total)
    query_grad, key_grad, value_grad = lax.map(one_pair, stacked)
    return (from_pairs(query_grad), from_pairs(key_grad), from_pairs(value_grad))

def clip_pass(frames, cotangent, weights):
    gain_one, shift_one, qkv_weight, qv_bias, out_weight, out_bias, gain_two, shift_two, up_weight, up_bias, down_weight, down_bias = weights
    width = frames.shape[1]
    inputs = frames.astype(jnp.float32)
    normal_one, inverse_one = norm_forward(inputs)
    normed_one = (normal_one * gain_one.astype(jnp.float32) + shift_one.astype(jnp.float32)).astype(jnp.bfloat16)
    bias_three = jnp.concatenate([qv_bias[:width].astype(jnp.float32), jnp.zeros((width,), jnp.float32), qv_bias[width:].astype(jnp.float32)])
    projected = (jnp.dot(normed_one, qkv_weight, preferred_element_type=jnp.float32) + bias_three).astype(jnp.bfloat16)
    query = projected[:, :width]
    keys = projected[:, width:2 * width]
    values = projected[:, 2 * width:]
    attended, log_total = attend(query, keys, values)
    middle = jnp.dot(attended, out_weight, preferred_element_type=jnp.float32) + out_bias.astype(jnp.float32) + inputs
    normal_two, inverse_two = norm_forward(middle)
    normed_two = (normal_two * gain_two.astype(jnp.float32) + shift_two.astype(jnp.float32)).astype(jnp.bfloat16)
    hidden_pre = jnp.dot(normed_two, up_weight, preferred_element_type=jnp.float32) + up_bias.astype(jnp.float32)
    activated = gelu(hidden_pre).astype(jnp.bfloat16)
    out_frames = (jnp.dot(activated, down_weight, preferred_element_type=jnp.float32) + down_bias.astype(jnp.float32) + middle).astype(jnp.bfloat16)
    upstream = cotangent.astype(jnp.float32)
    pre_grad = jnp.dot(cotangent, down_weight.T, preferred_element_type=jnp.float32) * gelu_slope(hidden_pre)
    pre_grad_half = pre_grad.astype(jnp.bfloat16)
    normed_two_grad = jnp.dot(pre_grad_half, up_weight.T, preferred_element_type=jnp.float32)
    middle_grad = upstream + norm_backward(normed_two_grad, normal_two, inverse_two, gain_two.astype(jnp.float32))
    middle_half = middle_grad.astype(jnp.bfloat16)
    attended_grad = jnp.dot(middle_half, out_weight.T, preferred_element_type=jnp.float32).astype(jnp.bfloat16)
    query_grad, key_grad, value_grad = attend_back(query, keys, values, attended, attended_grad, log_total)
    projected_grad = jnp.concatenate([query_grad, key_grad, value_grad], axis=1).astype(jnp.bfloat16)
    normed_one_grad = jnp.dot(projected_grad, qkv_weight.T, preferred_element_type=jnp.float32)
    frames_grad = (middle_grad + norm_backward(normed_one_grad, normal_one, inverse_one, gain_one.astype(jnp.float32))).astype(jnp.bfloat16)
    grads = (lax.optimization_barrier(jnp.sum(normed_one_grad * normal_one, axis=0)), lax.optimization_barrier(jnp.sum(normed_one_grad, axis=0)), jnp.dot(normed_one.T, projected_grad, preferred_element_type=jnp.float32), jnp.concatenate([lax.optimization_barrier(jnp.sum(query_grad, axis=0)), lax.optimization_barrier(jnp.sum(value_grad, axis=0))]), jnp.dot(attended.T, middle_half, preferred_element_type=jnp.float32), lax.optimization_barrier(jnp.sum(middle_grad, axis=0)), lax.optimization_barrier(jnp.sum(normed_two_grad * normal_two, axis=0)), lax.optimization_barrier(jnp.sum(normed_two_grad, axis=0)), jnp.dot(normed_two.T, pre_grad_half, preferred_element_type=jnp.float32), lax.optimization_barrier(jnp.sum(pre_grad, axis=0)), jnp.dot(activated.T, cotangent, preferred_element_type=jnp.float32), lax.optimization_barrier(jnp.sum(upstream, axis=0)))
    return (out_frames, frames_grad, grads)

def adam_update(params, grad, first, second):
    new_first = BETA_ONE * first + (1.0 - BETA_ONE) * grad
    new_second = BETA_TWO * second + (1.0 - BETA_TWO) * grad * grad
    first_hat = new_first / (1.0 - BETA_ONE ** adam_step)
    second_hat = new_second / (1.0 - BETA_TWO ** adam_step)
    current = params.astype(jnp.float32)
    new_params = current - LEARN_RATE * (first_hat / (jnp.sqrt(second_hat) + ADAM_EPS) + DECAY * current)
    return (new_first, new_second, new_params)

def reference(frames, cotangent, params, first_moment, second_moment):
    weights = unpack(params)
    clips = frames.reshape(N_REP, CLIP, D)
    cotangents = cotangent.reshape(N_REP, CLIP, D)
    initial = tuple((jnp.zeros(item.shape, jnp.float32) for item in weights))

    def one_clip(totals, pair):
        out_frames, frames_grad, grads = clip_pass(pair[0], pair[1], weights)
        return (tuple((left + right for left, right in zip(totals, grads))), (out_frames, frames_grad))
    totals, (outputs, inputs_grad) = lax.scan(one_clip, initial, (clips, cotangents))
    param_grad = pack(totals, N_GRP) / N_REP
    new_first, new_second, new_params = adam_update(params, param_grad, first_moment, second_moment)
    return (outputs.reshape(TOKENS, D), inputs_grad.reshape(TOKENS, D), param_grad, new_params, new_first, new_second)
```

```python
import functools
import jax
import jax.numpy as jnp
from jax import lax
from jax.sharding import PartitionSpec as P
from jax.experimental import pallas as pl
from jax.experimental.pallas import tpu as pltpu

MESH = pl.DeviceIdType.MESH
BF = jnp.bfloat16
F32 = jnp.float32
D = 768
FF = 3072
HDIM = 64
LANE = 128
FLAT = 1771776
FROWS = FLAT // LANE


class Mat:
    def __init__(self, offset, block, cols, suba, subb):
        self.offset, self.block, self.cols = offset, block, cols
        self.tiles = cols // LANE
        self.row0 = offset // LANE
        self.shifted = offset % LANE != 0
        self.quarter = block // 4
        self.half = cols // 2
        self.sub = (suba, subb)


QKV = Mat(384, 192, 2304, (0, 48, 0, 640), (0, 48, 640, 512))
OUT = Mat(443136, 192, 768, (0, 48, 0, 128), (0, 48, 128, 256))
UP = Mat(591168, 192, 3072, (0, 48, 0, 768), (0, 48, 768, 768))
DOWN = Mat(1181760, 768, 768, (0, 96, 0, 384), (96, 96, 0, 384))
MATS = (QKV, OUT, UP, DOWN)
SMALL = ((0, 3), (3459, 3), (4614, 5), (9226, 7), (13840, 2))
SROWS = 24


def flip(index, bit):
    return index + bit - 2 * bit * ((index // bit) % 2)


def mo(value, by):
    return pl.multiple_of(value, by)


def part(ref, m, r, k, h, sub=None):
    r0, rn, c0, cn = m.sub[sub] if sub is not None else (0, m.quarter, 0, m.half)
    row = mo(r * m.block + k * m.quarter + r0, 16)
    col = mo(h * m.half + c0, LANE)
    return ref.at[pl.ds(row, rn), pl.ds(col, cn)]


def slab(ref, m, r, h):
    return ref.at[pl.ds(mo(r * m.block, 16), m.block), pl.ds(mo(h * m.half, LANE), m.half)]


def remote(src, dst, send, recv, rep, grp):
    return pltpu.make_async_remote_copy(
        src_ref=src, dst_ref=dst, send_sem=send, recv_sem=recv,
        device_id={"rep": rep, "grp": grp}, device_id_type=MESH)


def greet(rep, g, groups, everyone=False):
    barrier = pltpu.get_barrier_semaphore()
    peers = [(flip(rep, b), g) for b in (1, 2, 4)]
    peers += [(rep, lax.rem(g + i, groups)) for i in range(1, groups)]
    return barrier, peers


def do_barrier(barrier, peers):
    for r, gg in peers:
        pl.semaphore_signal(barrier, inc=1, device_id={"rep": r, "grp": gg}, device_id_type=MESH)
    pl.semaphore_wait(barrier, len(peers))


def relayout(m, k, pbuf, fbuf, out):
    nrows = m.quarter * m.tiles
    extra = 8 if m.shifted else 0
    start = mo((m.row0 + k * nrows) * LANE, LANE)
    piece = pbuf[:, pl.ds(start, (nrows + extra) * LANE)]
    fbuf[0:nrows + extra, :] = piece.astype(F32).reshape(nrows + extra, LANE)
    low = lax.broadcasted_iota(jnp.int32, (m.quarter, LANE), 1) < 64
    for c in range(m.tiles):
        a = fbuf[pl.ds(c, m.quarter, stride=m.tiles), :]
        if m.shifted:
            b = fbuf[pl.ds(c + 1, m.quarter, stride=m.tiles), :]
            a = pltpu.roll(jnp.where(low, b, a), 64, 1)
        out[pl.ds(mo(k * m.quarter, 16), m.quarter), c * LANE:(c + 1) * LANE] = a.astype(BF)


def gather_kernel(groups, p_ref, fr_ref, wq, wo, wu, wd, fa, sm, pbuf, fbuf, sq, so, su, sd, smb,
                  lsem, osem, zs, zr, xs, xr, ys, yr, fas, far, fbs, fbr, cs, cr, ms, mr):
    rep, g = lax.axis_index("rep"), lax.axis_index("grp")
    s = lax.rem(rep, 8)
    h = lax.rem(s, 2)
    k = s // 2
    kx, ky, kd = flip(k, 1), flip(k, 2), 3 - k
    full = (wq, wo, wu, wd)
    blocks = (sq, so, su, sd)
    tokens = fr_ref.shape[0]
    barrier, peers = greet(rep, g, groups)
    bounds = [0]
    for m in MATS[1:]:
        bounds.append(m.offset // LANE * LANE)
    bounds.append(FLAT)
    loads = []
    for i in range(4):
        view = (slice(None), pl.ds(bounds[i], bounds[i + 1] - bounds[i]))
        cp = pltpu.make_async_copy(p_ref.at[view], pbuf.at[view], lsem.at[i])
        cp.start()
        loads.append(cp)
    do_barrier(barrier, peers)

    def zcopy(t, d, step, src, dst):
        target = lax.rem(g + (1 if d == 0 else groups - 1), groups)
        return remote(src, dst, zs.at[t, d, step], zr.at[t, d, step], rep, target)

    def has_next(d):
        return g < groups - 1 if d == 0 else g > 0

    def own_send(t):
        for d in range(2):
            @pl.when(has_next(d))
            def _():
                if t == 4:
                    zcopy(t, d, 0, fr_ref, fa.at[pl.ds(mo(g * tokens, 16), tokens), :]).start()
                else:
                    m = MATS[t]
                    src = blocks[t].at[pl.ds(mo(k * m.quarter, 16), m.quarter), pl.ds(mo(h * m.half, LANE), m.half)]
                    zcopy(t, d, 0, src, part(full[t], m, g, k, h)).start()

    def rest(t):
        def body(i, c):
            relayout(MATS[t], lax.rem(k + i, 4), pbuf, fbuf, blocks[t])
            return c
        lax.fori_loop(1, 4, body, 0)
        pltpu.make_async_copy(blocks[t], full[t].at[pl.ds(mo(g * MATS[t].block, 16), MATS[t].block), :], osem.at[t]).start()

    def row_of(d, step):
        return g - 1 - step if d == 0 else g + 1 + step

    def valid(d, step):
        return g - 1 - step >= 0 if d == 0 else g + 1 + step <= groups - 1

    slots = [(d, step) for step in range(groups - 1) for d in range(2)]

    def zregion(t, r):
        if t == 4:
            return fa.at[pl.ds(mo(r * tokens, 16), tokens), :]
        return part(full[t], MATS[t], r, k, h)

    def stage0(t, d, step):
        @pl.when(valid(d, step))
        def _():
            r = row_of(d, step)
            reg = zregion(t, r)
            zcopy(t, d, step, reg, reg).wait_recv()
            if step < groups - 2:
                @pl.when(has_next(d))
                def _():
                    zcopy(t, d, step + 1, reg, reg).start()
            if t < 4:
                i = d * (groups - 1) + step
                remote(reg, reg, xs.at[t, i], xr.at[t, i], flip(rep, 2), g).start()
                remote(reg, reg, ys.at[t, i], yr.at[t, i], flip(rep, 4), g).start()

    def stage1(t, d, step):
        @pl.when(valid(d, step))
        def _():
            r, i, m = row_of(d, step), d * (groups - 1) + step, MATS[t]
            reg = part(full[t], m, r, kx, h)
            remote(reg, reg, xs.at[t, i], xr.at[t, i], flip(rep, 2), g).wait_recv()
            a = part(full[t], m, r, kx, h, 0)
            remote(a, a, fas.at[t, i], far.at[t, i], flip(rep, 4), g).start()
            reg = part(full[t], m, r, ky, h)
            remote(reg, reg, ys.at[t, i], yr.at[t, i], flip(rep, 4), g).wait_recv()
            b = part(full[t], m, r, ky, h, 1)
            remote(b, b, fbs.at[t, i], fbr.at[t, i], flip(rep, 2), g).start()

    def stage2(t, d, step):
        @pl.when(valid(d, step))
        def _():
            r, i, m = row_of(d, step), d * (groups - 1) + step, MATS[t]
            a, b = part(full[t], m, r, kd, h, 0), part(full[t], m, r, kd, h, 1)
            remote(a, a, fas.at[t, i], far.at[t, i], flip(rep, 4), g).wait_recv()
            remote(b, b, fbs.at[t, i], fbr.at[t, i], flip(rep, 2), g).wait_recv()
            c = slab(full[t], m, r, h)
            remote(c, c, cs.at[t, i], cr.at[t, i], flip(rep, 1), g).start()

    def stage3(t, d, step):
        @pl.when(valid(d, step))
        def _():
            r, i, m = row_of(d, step), d * (groups - 1) + step, MATS[t]
            c = slab(full[t], m, r, 1 - h)
            remote(c, c, cs.at[t, i], cr.at[t, i], flip(rep, 1), g).wait_recv()

    loads[0].wait()
    relayout(QKV, k, pbuf, fbuf, sq)
    own_send(0)
    own_send(4)
    loads[1].wait()
    relayout(OUT, k, pbuf, fbuf, so)
    own_send(1)
    loads[2].wait()
    loads[3].wait()
    relayout(UP, k, pbuf, fbuf, su)
    own_send(2)
    relayout(DOWN, k, pbuf, fbuf, sd)
    own_send(3)
    row = 0
    for first, count in SMALL:
        smb[row:row + count, :] = pbuf[:, first * LANE:(first + count) * LANE].astype(F32).reshape(count, LANE)
        row += count
    smb[row:SROWS, :] = jnp.zeros((SROWS - row, LANE), F32)
    for i in range(1, groups):
        remote(smb, sm.at[g], ms.at[i - 1], mr.at[i - 1], rep, lax.rem(g + i, groups)).start()
    pltpu.make_async_copy(smb, sm.at[g], osem.at[4]).start()
    pltpu.make_async_copy(fr_ref, fa.at[pl.ds(mo(g * tokens, 16), tokens), :], osem.at[5]).start()

    items = [(t, d, step) for step in range(groups - 1) for t in (0, 4, 1, 2, 3) for d in range(2)]
    mats = [it for it in items if it[0] < 4]
    fillers = {1: 0, 3: 1, 5: 2, 7: 3}
    lag = 2
    n1 = n2 = n3 = 0
    count = 0
    for n, it in enumerate(items):
        stage0(*it)
        if it[0] < 4:
            count += 1
        if n in fillers:
            rest(fillers[n])
        while n1 < count - lag:
            stage1(*mats[n1])
            n1 += 1
        while n2 < n1 - lag:
            stage2(*mats[n2])
            n2 += 1
    while n1 < len(mats):
        stage1(*mats[n1])
        n1 += 1
        if n2 < n1 - lag:
            stage2(*mats[n2])
            n2 += 1
    while n2 < len(mats):
        stage2(*mats[n2])
        n2 += 1
    for it in mats:
        stage3(*it)
    for t in (0, 4, 1, 2, 3):
        reg = zregion(t, g)
        for d in range(2):
            @pl.when(has_next(d))
            def _():
                zcopy(t, d, 0, reg, reg).wait_send()
        for (d, step) in slots:
            i = d * (groups - 1) + step

            @pl.when(valid(d, step))
            def _():
                r = row_of(d, step)
                if step < groups - 2:
                    @pl.when(has_next(d))
                    def _():
                        zcopy(t, d, step + 1, reg, reg).wait_send()
                if t < 4:
                    m = MATS[t]
                    remote(reg, reg, xs.at[t, i], xr.at[t, i], flip(rep, 2), g).wait_send()
                    remote(reg, reg, ys.at[t, i], yr.at[t, i], flip(rep, 4), g).wait_send()
                    a, b = part(full[t], m, r, kx, h, 0), part(full[t], m, r, ky, h, 1)
                    remote(a, a, fas.at[t, i], far.at[t, i], flip(rep, 4), g).wait_send()
                    remote(b, b, fbs.at[t, i], fbr.at[t, i], flip(rep, 2), g).wait_send()
                    c = slab(full[t], m, r, h)
                    remote(c, c, cs.at[t, i], cr.at[t, i], flip(rep, 1), g).wait_send()
        if t < 4:
            pltpu.make_async_copy(blocks[t], full[t].at[pl.ds(mo(g * MATS[t].block, 16), MATS[t].block), :], osem.at[t]).wait()
    for i in range(1, groups):
        cp = remote(smb, sm.at[lax.rem(g + groups - i, groups)], ms.at[i - 1], mr.at[i - 1], rep, lax.rem(g + i, groups))
        cp.wait_send()
        cp.wait_recv()
    pltpu.make_async_copy(smb, sm.at[g], osem.at[4]).wait()
    pltpu.make_async_copy(fr_ref, fa.at[pl.ds(mo(g * tokens, 16), tokens), :], osem.at[5]).wait()


def gather(params, frames, groups):
    dma = pltpu.SemaphoreType.DMA
    n = 2 * (groups - 1)
    tokens = frames.shape[0]
    shapes = [jax.ShapeDtypeStruct((m.block * groups, m.cols), BF) for m in MATS]
    shapes += [jax.ShapeDtypeStruct((tokens * groups, D), BF), jax.ShapeDtypeStruct((groups, SROWS, LANE), F32)]
    return pl.pallas_call(
        functools.partial(gather_kernel, groups),
        out_shape=shapes,
        in_specs=[pl.BlockSpec(memory_space=pl.ANY), pl.BlockSpec(memory_space=pltpu.VMEM)],
        out_specs=[pl.BlockSpec(memory_space=pl.ANY)] * 6,
        scratch_shapes=[
            pltpu.VMEM((1, FLAT + 8 * LANE), BF),
            pltpu.VMEM((48 * 24 + 16, LANE), F32),
        ] + [pltpu.VMEM((m.block, m.cols), BF) for m in MATS] + [
            pltpu.VMEM((SROWS, LANE), F32),
            dma((4,)), dma((6,)), dma((5, 2, groups)), dma((5, 2, groups)),
            dma((4, n)), dma((4, n)), dma((4, n)), dma((4, n)), dma((4, n)), dma((4, n)), dma((4, n)), dma((4, n)),
            dma((4, n)), dma((4, n)), dma((groups,)), dma((groups,)),
        ],
        compiler_params=pltpu.CompilerParams(collective_id=0, has_side_effects=True, vmem_limit_bytes=40 << 20),
        name="gather",
    )(params, frames)


def add_rows(dst, a, b, rows, step=16):
    def body(i, c):
        at = pl.ds(mo(i * step, 16), step)
        dst[at, :] = (a[at, :].astype(F32) + b[at, :].astype(F32)).astype(dst.dtype)
        return c
    lax.fori_loop(0, rows // step, body, 0)


def cell(ref, m, r, kk, sub=None):
    r0, rn, c0, cn = m.sub[sub] if sub is not None else (0, m.quarter, 0, m.half)
    return ref.at[pl.ds(mo(r * m.block + kk * m.quarter + r0, 16), rn), pl.ds(c0, cn)]


ORDER = (2, 3, 0, 1)


def reduce_kernel(groups, highs, gq, go, gu, gd, sm_ref, oq, oo, ou, od, osm, *scratch):
    own, scratch = scratch[:4], scratch[4:]
    buf1, scratch = scratch[:4], scratch[4:]
    buf2, scratch = scratch[:4], scratch[4:]
    buf3, scratch = scratch[:4], scratch[4:]
    zbuf, scratch = scratch[:4], scratch[4:]
    fin, scratch = scratch[:4], scratch[4:]
    (smacc, smin, lsem, c1s, c1r, a1s, a1r, b1s, b1r, a2s, a2r, b2s, b2r, zs, zr, fxs, fxr, os, xs, xr, ys, yr,
     fas, far, fbs, fbr, cs, cr, sms, smr) = scratch
    rep, g = lax.axis_index("rep"), lax.axis_index("grp")
    s = lax.rem(rep, 8)
    h = lax.rem(s, 2)
    k = s // 2
    x, y = lax.rem(k, 2), k // 2
    kx, ky, kd = flip(k, 1), flip(k, 2), 3 - k
    core, xn, yn = flip(rep, 1), flip(rep, 2), flip(rep, 4)
    grads = (gq, go, gu, gd)
    outs = (oq, oo, ou, od)
    barrier, peers = greet(rep, g, groups)
    peers += [(flip(rep, 8 << b), g) for b in range(highs)]
    do_barrier(barrier, peers)

    def row(i):
        return lax.rem(g + 1 + i, groups)

    def load(t, i):
        m = MATS[t]
        at = pl.ds(mo(row(i) * m.block, 16), m.block)
        return pltpu.make_async_copy(grads[t].at[at, pl.ds(mo(h * m.half, LANE), m.half)], own[t].at[at, :], lsem.at[t, i])

    def first(t, i):
        m = MATS[t]
        at = pl.ds(mo(row(i) * m.block, 16), m.block)
        return remote(grads[t].at[at, pl.ds(mo((1 - h) * m.half, LANE), m.half)], buf1[t].at[at, :],
                      c1s.at[t, i], c1r.at[t, i], core, g)

    def acopy(t, i, j, kk):
        return remote(cell(buf1[t], MATS[t], row(i), kk, 0), cell(buf2[t], MATS[t], row(i), kk, 0),
                      a1s.at[t, i, j], a1r.at[t, i, j], xn, g)

    def bcopy(t, i, j, kk):
        return remote(cell(buf1[t], MATS[t], row(i), kk, 1), cell(buf2[t], MATS[t], row(i), kk, 1),
                      b1s.at[t, i, j], b1r.at[t, i, j], yn, g)

    def a2copy(t, i, kk):
        return remote(cell(buf2[t], MATS[t], row(i), kk, 0), cell(buf3[t], MATS[t], row(i), kk, 0),
                      a2s.at[t, i], a2r.at[t, i], yn, g)

    def b2copy(t, i, kk):
        return remote(cell(buf2[t], MATS[t], row(i), kk, 1), cell(buf3[t], MATS[t], row(i), kk, 1),
                      b2s.at[t, i], b2r.at[t, i], xn, g)

    def zcopy(t, i):
        return remote(cell(buf3[t], MATS[t], row(i), k), zbuf[t].at[i], zs.at[t, i], zr.at[t, i], rep, row(i))

    def r1(t, i):
        m = MATS[t]
        load(t, i).wait()
        first(t, i).wait_recv()
        at = pl.ds(mo(row(i) * m.block, 16), m.block)
        add_rows(buf1[t].at[at, :], own[t].at[at, :], buf1[t].at[at, :], m.block)
        for j in range(2):
            acopy(t, i, j, 2 * j + (1 - x)).start()
            bcopy(t, i, j, 2 * (1 - y) + j).start()

    def r2(t, i):
        m = MATS[t]
        for j in range(2):
            acopy(t, i, j, 2 * j + x).wait_recv()
            kk = 2 * j + x
            add_rows(cell(buf2[t], m, row(i), kk, 0), cell(buf1[t], m, row(i), kk, 0), cell(buf2[t], m, row(i), kk, 0), m.sub[0][1])
        a2copy(t, i, 2 * (1 - y) + x).start()
        for j in range(2):
            bcopy(t, i, j, 2 * y + j).wait_recv()
            kk = 2 * y + j
            add_rows(cell(buf2[t], m, row(i), kk, 1), cell(buf1[t], m, row(i), kk, 1), cell(buf2[t], m, row(i), kk, 1), m.sub[1][1])
        b2copy(t, i, 2 * y + (1 - x)).start()

    def r3(t, i):
        m = MATS[t]
        a2copy(t, i, k).wait_recv()
        b2copy(t, i, k).wait_recv()
        whole = (cell(buf3[t], m, row(i), k), cell(buf2[t], m, row(i), k))
        add_rows(whole[0], whole[1], whole[0], m.quarter)
        if i < groups - 1:
            zcopy(t, i).start()

    def fpart(t, kk, hh, sub=None):
        return part(outs[t], MATS[t], 0, kk, hh, sub)

    def fslab(t, hh):
        return slab(outs[t], MATS[t], 0, hh)

    def keep(t):
        return pltpu.make_async_copy(fin[t].at[highs], fpart(t, k, h), os.at[t])

    def xsend(t):
        return remote(fin[t].at[highs], fpart(t, k, h), xs.at[t], xr.at[t], xn, g)

    def ysend(t):
        return remote(fin[t].at[highs], fpart(t, k, h), ys.at[t], yr.at[t], yn, g)

    def xgot(t):
        return remote(fpart(t, kx, h), fpart(t, kx, h), xs.at[t], xr.at[t], xn, g)

    def ygot(t):
        return remote(fpart(t, ky, h), fpart(t, ky, h), ys.at[t], yr.at[t], yn, g)

    def fwd(t, sub, kk):
        reg = fpart(t, kk, h, sub)
        return remote(reg, reg, (fas, fbs)[sub].at[t], (far, fbr)[sub].at[t], (yn, xn)[sub], g)

    def cross(t, hh):
        return remote(fslab(t, hh), fslab(t, hh), cs.at[t], cr.at[t], core, g)

    def r4(t):
        m = MATS[t]
        for i in range(groups - 1):
            zcopy(t, i).wait_recv()
        mine = cell(buf3[t], m, g, k)

        def body(n, c):
            at = pl.ds(mo(n * 16, 16), 16)
            total = mine[at, :].astype(F32)
            for i in range(groups - 1):
                total = total + zbuf[t][i, at, :].astype(F32)
            fin[t][0, at, :] = total.astype(BF)
            return c
        lax.fori_loop(0, m.quarter // 16, body, 0)
        for b in range(highs):
            cp = remote(fin[t].at[b], fin[t].at[highs + 1 + b], fxs.at[t, b], fxr.at[t, b], flip(rep, 8 << b), g)
            cp.start()
            cp.wait()
            add_rows(fin[t].at[b + 1], fin[t].at[b], fin[t].at[highs + 1 + b], m.quarter)
        keep(t).start()
        xsend(t).start()
        ysend(t).start()

    def r5(t):
        xgot(t).wait_recv()
        fwd(t, 0, kx).start()
        ygot(t).wait_recv()
        fwd(t, 1, ky).start()

    def r6(t):
        fwd(t, 0, kd).wait_recv()
        fwd(t, 1, kd).wait_recv()
        keep(t).wait()
        cross(t, h).start()

    def r7(t):
        cross(t, 1 - h).wait_recv()

    partners = [(core, g), (xn, g), (yn, g)] + [(flip(rep, 8 << b), g) for b in range(highs)]
    bit = 1
    while bit < groups:
        partners.append((rep, flip(g, bit)))
        bit *= 2

    def smcopy(j):
        return remote(smacc.at[j], smin.at[j], sms.at[j], smr.at[j], *partners[j])

    def small(j):
        if j:
            smcopy(j - 1).wait_recv()
            smacc[j] = smacc[j - 1] + smin[j - 1]
        else:
            smacc[0] = sm_ref[...]
        if j < len(partners):
            smcopy(j).start()
        else:
            osm[...] = smacc[j, g]

    chunks = [(t, i) for t in ORDER for i in range(groups)]
    small(0)
    for t, i in chunks:
        first(t, i).start()
        load(t, i).start()
    done4 = {}
    total = len(chunks)
    smalls = 1
    for n in range(total + 16):
        if n < total:
            r1(*chunks[n])
        if 0 <= n - 2 < total:
            r2(*chunks[n - 2])
        if n % 2 and smalls <= len(partners):
            small(smalls)
            smalls += 1
        if 0 <= n - 4 < total:
            r3(*chunks[n - 4])
        for q, t in enumerate(ORDER):
            last = groups * q + groups - 1 + 4
            if n == last + 2:
                r4(t)
            if n == last + 4:
                r5(t)
            if n == last + 6:
                r6(t)
    for t in ORDER:
        r7(t)
    for t, i in chunks:
        first(t, i).wait_send()
        for j in range(2):
            acopy(t, i, j, 2 * j + x).wait_send()
            bcopy(t, i, j, 2 * y + j).wait_send()
        a2copy(t, i, k).wait_send()
        b2copy(t, i, k).wait_send()
        if i < groups - 1:
            zcopy(t, i).wait_send()
    for t in ORDER:
        xsend(t).wait_send()
        ysend(t).wait_send()
        fwd(t, 0, kx).wait_send()
        fwd(t, 1, ky).wait_send()
        cross(t, h).wait_send()
    for j in range(len(partners)):
        smcopy(j).wait_send()


def reduce_grads(grads, smalls, groups, reps):
    dma = pltpu.SemaphoreType.DMA
    highs = (reps // 8).bit_length() - 1
    steps = 3 + highs + groups.bit_length() - 1
    wide = [pltpu.VMEM((m.block * groups, m.half), BF) for m in MATS]
    scratch = wide * 4
    scratch += [pltpu.VMEM((groups, m.quarter, m.half), BF) for m in MATS]
    scratch += [pltpu.VMEM((2 * highs + 1, m.quarter, m.half), BF) for m in MATS]
    scratch += [pltpu.VMEM((steps + 1, groups, SROWS, LANE), F32), pltpu.VMEM((steps, groups, SROWS, LANE), F32)]
    scratch += [dma((4, groups))] * 3 + [dma((4, groups, 2))] * 4 + [dma((4, groups))] * 6
    scratch += [dma((4, max(highs, 1)))] * 2 + [dma((4,))] * 11 + [dma((steps,))] * 2
    return pl.pallas_call(
        functools.partial(reduce_kernel, groups, highs),
        out_shape=[jax.ShapeDtypeStruct((m.block, m.cols), BF) for m in MATS] + [jax.ShapeDtypeStruct((SROWS, LANE), F32)],
        in_specs=[pl.BlockSpec(memory_space=pl.ANY)] * 4 + [pl.BlockSpec(memory_space=pltpu.VMEM)],
        out_specs=[pl.BlockSpec(memory_space=pl.ANY)] * 4 + [pl.BlockSpec(memory_space=pltpu.VMEM)],
        scratch_shapes=scratch,
        compiler_params=pltpu.CompilerParams(collective_id=1, has_side_effects=True, vmem_limit_bytes=44 << 20),
        name="reduce",
    )(*grads, smalls)


BETA_ONE = 0.9
BETA_TWO = 0.98
ADAM_EPS = 1e-06
LEARN_RATE = 0.006
DECAY = 0.01
ADAM_STEP = 4
ROWS = 1736
STEPS = -(-FROWS // ROWS)


def flatten(m, block, flat, late):
    def body(i, carry):
        base = m.row0 + i * (48 * m.tiles)
        for c in range(m.tiles):
            tile = block[pl.ds(mo(i * 48, 16), 48), c * LANE:(c + 1) * LANE].astype(F32)
            if m.shifted:
                tile = pltpu.roll(tile, 64, 1)
                late[pl.ds(base + c + 1, 48, stride=m.tiles), :] = tile
            flat[pl.ds(base + c, 48, stride=m.tiles), :] = tile
        return carry
    lax.fori_loop(0, m.block // 48, body, 0)


def adam_kernel(scale, gq, go, gu, gd, sm, p_ref, m_ref, v_ref, o_g, o_p, o_m, o_v, flat, late):
    step = pl.program_id(0)

    @pl.when(step == 0)
    def _():
        flatten(QKV, gq, flat, late)
        flatten(OUT, go, flat, late)
        flatten(UP, gu, flat, late)
        flatten(DOWN, gd, flat, late)
        flat[0:3, :] = sm[0:3, :]
        flat[3459:3462, :] = sm[3:6, :]
        flat[4614:4618, :] = sm[6:10, :]
        flat[4618:4619, 0:64] = sm[10:11, 0:64]
        flat[9226:9227, 64:128] = sm[11:12, 64:128]
        flat[9227:9232, :] = sm[12:17, :]
        flat[9232:9233, 0:64] = sm[17:18, 0:64]
        flat[13840:13841, 64:128] = sm[18:19, 64:128]
        flat[13841:13842, :] = sm[19:20, :]
        late[9227:9232, :] = sm[12:17, :]
        late[9232:9233, 0:64] = sm[17:18, 0:64]
        late[13841:13842, :] = sm[19:20, :]

    at = pl.ds(mo(step * ROWS, 8), ROWS)
    number = step * ROWS + lax.broadcasted_iota(jnp.int32, (ROWS, LANE), 0)
    low = lax.broadcasted_iota(jnp.int32, (ROWS, LANE), 1) < 64
    grad = jnp.where(jnp.logical_and(number > UP.row0, low), late[at, :], flat[at, :]).reshape(1, ROWS * LANE) * scale
    first = BETA_ONE * m_ref[...] + (1.0 - BETA_ONE) * grad
    second = BETA_TWO * v_ref[...] + (1.0 - BETA_TWO) * grad * grad
    o_g[...] = grad
    o_m[...] = first
    o_v[...] = second
    first_hat = first * (1.0 / (1.0 - BETA_ONE**ADAM_STEP))
    second_hat = second * (1.0 / (1.0 - BETA_TWO**ADAM_STEP))
    current = p_ref[...].astype(F32)
    o_p[...] = current - LEARN_RATE * (first_hat / (jnp.sqrt(second_hat) + ADAM_EPS) + DECAY * current)


def adam(blocks, smalls, params, first, second, reps):
    spec = pl.BlockSpec((1, ROWS * LANE), lambda i: (0, i))
    vmem = pl.BlockSpec(memory_space=pltpu.VMEM)
    return pl.pallas_call(
        functools.partial(adam_kernel, 1.0 / reps),
        grid=(STEPS,),
        out_shape=[jax.ShapeDtypeStruct((1, FLAT), F32)] * 4,
        in_specs=[vmem] * 5 + [spec] * 3,
        out_specs=[spec] * 4,
        scratch_shapes=[pltpu.VMEM((STEPS * ROWS, LANE), F32)] * 2,
        compiler_params=pltpu.CompilerParams(vmem_limit_bytes=50 << 20),
        name="adam",
    )(*blocks, smalls, params, first, second)


EPS_NORM = 1e-05


def norm_forward(values):
    center = values - jnp.mean(values, axis=-1, keepdims=True)
    inverse = lax.rsqrt(jnp.mean(center * center, axis=-1, keepdims=True) + EPS_NORM)
    return (center * inverse, inverse)


def norm_backward(upstream, normalized, inverse, gain):
    scaled = upstream * gain
    return inverse * (
        scaled
        - jnp.mean(scaled, axis=-1, keepdims=True)
        - normalized * jnp.mean(scaled * normalized, axis=-1, keepdims=True)
    )


def gelu(values):
    return 0.5 * values * (1.0 + lax.erf(values * 0.7071067811865476))


def gelu_slope(values):
    return (
        0.5 * (1.0 + lax.erf(values * 0.7071067811865476))
        + values * jnp.exp(-0.5 * values * values) * 0.3989422804014327
    )


def to_pairs(matrix):
    heads = matrix.shape[1] // HDIM
    return matrix.reshape(matrix.shape[0], heads // 2, 2, HDIM).transpose(1, 0, 2, 3)


def from_pairs(stacked):
    return stacked.transpose(1, 0, 2, 3).reshape(stacked.shape[1], -1)


def attend(query, keys, values):
    scale = HDIM ** (-0.5)

    def attend_one_pair(items):
        query_pair, key_pair, value_pair = items
        scores = (
            jnp.einsum("qhd,khd->hqk", query_pair, key_pair, preferred_element_type=jnp.float32)
            * scale
        )
        highest = jnp.max(scores, axis=-1, keepdims=True)
        log_total = highest + jnp.log(jnp.sum(jnp.exp(scores - highest), axis=-1, keepdims=True))
        shares = jnp.exp(scores - log_total).astype(jnp.bfloat16)
        mixed = jnp.einsum("hqk,khd->qhd", shares, value_pair, preferred_element_type=jnp.float32)
        return (mixed, log_total[..., 0])

    mixed, log_total = lax.map(attend_one_pair, (to_pairs(query), to_pairs(keys), to_pairs(values)))
    return (from_pairs(mixed).astype(jnp.bfloat16), log_total)


def row_centre(upstream, attended):
    product = to_pairs(upstream).astype(jnp.float32) * to_pairs(attended).astype(jnp.float32)
    return jnp.sum(product, axis=-1).transpose(0, 2, 1)


def back_blocks(query, keys, values, upstream, log_total, centre):
    scale = HDIM ** (-0.5)

    def back_one_pair(items):
        query_pair, key_pair, value_pair, upstream_pair, log_pair, centre_pair = items
        scores = (
            jnp.einsum("qhd,khd->hqk", query_pair, key_pair, preferred_element_type=jnp.float32)
            * scale
        )
        shares = jnp.exp(scores - log_pair[..., None])
        share_grad = jnp.einsum(
            "qhd,khd->hqk", upstream_pair, value_pair, preferred_element_type=jnp.float32
        )
        score_grad = (shares * (share_grad - centre_pair[..., None]) * scale).astype(jnp.bfloat16)
        result = []
        result.append(
            jnp.einsum("hqk,khd->qhd", score_grad, key_pair, preferred_element_type=jnp.float32)
        )
        result.append(
            jnp.einsum("hqk,qhd->khd", score_grad, query_pair, preferred_element_type=jnp.float32)
        )
        result.append(
            jnp.einsum(
                "hqk,qhd->khd",
                shares.astype(jnp.bfloat16),
                upstream_pair,
                preferred_element_type=jnp.float32,
            )
        )
        return tuple(result)

    stacked = (
        to_pairs(query),
        to_pairs(keys),
        to_pairs(values),
        to_pairs(upstream),
        log_total,
        centre,
    )
    outputs = lax.map(back_one_pair, stacked)
    return tuple((from_pairs(item) for item in outputs))


def vectors(smalls, groups):
    rows = smalls.reshape(groups, SROWS * LANE)

    def pick(first, count):
        return rows[:, first:first + count].reshape(1, groups * count)
    qv = pick(384, 384)
    return (pick(0, 192), pick(192, 192), qv, pick(768, 192), pick(960, 192), pick(1152, 192), pick(1472, 768), pick(2368, 192))


def small_image(gain_one, shift_one, qv, out_bias, gain_two, shift_two, up_bias, down_bias, groups):
    def rows(item):
        return item.reshape(groups, -1)
    gap = jnp.zeros((groups, 64), F32)
    pieces = [rows(gain_one), rows(shift_one), rows(qv), rows(out_bias), rows(gain_two), rows(shift_two), gap,
              gap, rows(up_bias), gap, gap, rows(down_bias), jnp.zeros((groups, 512), F32)]
    return jnp.concatenate(pieces, axis=1).reshape(groups, SROWS, LANE)


def on_device(frames, cotangent, params, first_moment, second_moment):
    groups, reps = lax.axis_size("grp"), lax.axis_size("rep")
    qkv_weight, out_weight, up_weight, down_weight, clip, smalls = gather(params, frames, groups)
    gain_one, shift_one, qv_bias, out_bias, gain_two, shift_two, up_bias, down_bias = vectors(smalls, groups)
    width = frames.shape[1]
    tokens = frames.shape[0]
    wide = clip.astype(F32)
    normal_all, inverse_all = norm_forward(wide)
    normed_all = (normal_all * gain_one + shift_one).astype(BF)
    start = lax.axis_index("grp") * tokens
    inputs = frames.astype(F32)
    normal_one, inverse_one = norm_forward(inputs)
    normed_one = (normal_one * gain_one + shift_one).astype(BF)
    query = (jnp.dot(normed_one, qkv_weight[:, :width], preferred_element_type=F32) + qv_bias[:, :width]).astype(BF)
    kv_bias = jnp.concatenate([jnp.zeros((1, width), F32), qv_bias[:, width:]], axis=1)
    key_value = (jnp.dot(normed_all, qkv_weight[:, width:], preferred_element_type=F32) + kv_bias).astype(BF)
    keys = key_value[:, :width]
    values = key_value[:, width:]
    attended, log_total = attend(query, keys, values)
    middle = jnp.dot(attended, out_weight, preferred_element_type=F32) + out_bias + inputs
    normal_two, inverse_two = norm_forward(middle)
    normed_two = (normal_two * gain_two + shift_two).astype(BF)
    hidden_pre = jnp.dot(normed_two, up_weight, preferred_element_type=F32) + up_bias
    activated = gelu(hidden_pre).astype(BF)
    out_frames = (jnp.dot(activated, down_weight, preferred_element_type=F32) + down_bias + middle).astype(BF)
    upstream = cotangent.astype(F32)
    pre_grad = jnp.dot(cotangent, down_weight.T, preferred_element_type=F32) * gelu_slope(hidden_pre)
    pre_grad_half = pre_grad.astype(BF)
    normed_two_grad = jnp.dot(pre_grad_half, up_weight.T, preferred_element_type=F32)
    middle_grad = upstream + norm_backward(normed_two_grad, normal_two, inverse_two, gain_two)
    middle_half = middle_grad.astype(BF)
    attended_grad = jnp.dot(middle_half, out_weight.T, preferred_element_type=F32).astype(BF)
    centre = row_centre(attended_grad, attended)
    query_grad, key_grad, value_grad = back_blocks(query, keys, values, attended_grad, log_total, centre)
    owned = lax.psum_scatter(jnp.concatenate([key_grad, value_grad], axis=1), "grp", scatter_dimension=0, tiled=True)
    projected_grad = jnp.concatenate([query_grad, owned], axis=1).astype(BF)
    normed_one_grad = jnp.dot(projected_grad, qkv_weight.T, preferred_element_type=F32)
    frames_grad = (middle_grad + norm_backward(normed_one_grad, normal_one, inverse_one, gain_one)).astype(BF)
    grads = [jnp.dot(a.T, b, preferred_element_type=F32).astype(BF) for a, b in (
        (normed_one, projected_grad), (attended, middle_half), (normed_two, pre_grad_half), (activated, cotangent))]
    image = small_image(
        jnp.sum(normed_one_grad * normal_one, axis=0), jnp.sum(normed_one_grad, axis=0),
        jnp.concatenate([jnp.sum(query_grad, axis=0), jnp.sum(owned[:, width:], axis=0)]),
        jnp.sum(middle_grad, axis=0), jnp.sum(normed_two_grad * normal_two, axis=0), jnp.sum(normed_two_grad, axis=0),
        jnp.sum(pre_grad, axis=0), jnp.sum(upstream, axis=0), groups)
    *blocks, small = reduce_grads(grads, image, groups, reps)
    param_grad, new_params, new_first, new_second = adam(blocks, small, params, first_moment, second_moment, reps)
    return (out_frames, frames_grad, param_grad, new_params, new_first, new_second)


def solution(mesh):
    in_specs = (
        P(("rep", "grp"), None),
        P(("rep", "grp"), None),
        P("grp", None),
        P("grp", None),
        P("grp", None),
    )
    out_specs = (
        P(("rep", "grp"), None),
        P(("rep", "grp"), None),
        P("grp", None),
        P("grp", None),
        P("grp", None),
        P("grp", None),
    )
    return jax.shard_map(
        on_device, mesh=mesh, in_specs=in_specs, out_specs=out_specs, check_vma=False
    )
```

```python
import functools
import jax
import jax.numpy as jnp
from jax import lax
from jax.sharding import PartitionSpec as P
from jax.experimental import pallas as pl
from jax.experimental.pallas import tpu as pltpu

MESH = pl.DeviceIdType.MESH
BF = jnp.bfloat16
F32 = jnp.float32
D = 768
FF = 3072
HDIM = 64
LANE = 128
FLAT = 1771776
FROWS = FLAT // LANE


class Mat:
    def __init__(self, offset, block, cols, suba, subb):
        self.offset, self.block, self.cols = offset, block, cols
        self.tiles = cols // LANE
        self.row0 = offset // LANE
        self.shifted = offset % LANE != 0
        self.quarter = block // 4
        self.half = cols // 2
        self.sub = (suba, subb)


QKV = Mat(384, 192, 2304, (0, 48, 0, 640), (0, 48, 640, 512))
OUT = Mat(443136, 192, 768, (0, 48, 0, 128), (0, 48, 128, 256))
UP = Mat(591168, 192, 3072, (0, 48, 0, 768), (0, 48, 768, 768))
DOWN = Mat(1181760, 768, 768, (0, 96, 0, 384), (96, 96, 0, 384))
MATS = (QKV, OUT, UP, DOWN)
SMALL = ((0, 3), (3459, 3), (4614, 5), (9226, 7), (13840, 2))
SROWS = 24


def flip(index, bit):
    return index + bit - 2 * bit * ((index // bit) % 2)


def mo(value, by):
    return pl.multiple_of(value, by)


def part(ref, m, r, k, h, sub=None):
    r0, rn, c0, cn = m.sub[sub] if sub is not None else (0, m.quarter, 0, m.half)
    row = mo(r * m.block + k * m.quarter + r0, 16)
    col = mo(h * m.half + c0, LANE)
    return ref.at[pl.ds(row, rn), pl.ds(col, cn)]


def slab(ref, m, r, h):
    return ref.at[pl.ds(mo(r * m.block, 16), m.block), pl.ds(mo(h * m.half, LANE), m.half)]


def remote(src, dst, send, recv, rep, grp):
    return pltpu.make_async_remote_copy(
        src_ref=src, dst_ref=dst, send_sem=send, recv_sem=recv,
        device_id={"rep": rep, "grp": grp}, device_id_type=MESH)


def greet(rep, g, groups, everyone=False):
    barrier = pltpu.get_barrier_semaphore()
    peers = [(flip(rep, b), g) for b in (1, 2, 4)]
    peers += [(rep, lax.rem(g + i, groups)) for i in range(1, groups)]
    return barrier, peers


def do_barrier(barrier, peers):
    for r, gg in peers:
        pl.semaphore_signal(barrier, inc=1, device_id={"rep": r, "grp": gg}, device_id_type=MESH)
    pl.semaphore_wait(barrier, len(peers))


def relayout(m, k, pbuf, fbuf, out):
    nrows = m.quarter * m.tiles
    extra = 8 if m.shifted else 0
    start = mo((m.row0 + k * nrows) * LANE, LANE)
    piece = pbuf[:, pl.ds(start, (nrows + extra) * LANE)]
    fbuf[0:nrows + extra, :] = piece.astype(F32).reshape(nrows + extra, LANE)
    low = lax.broadcasted_iota(jnp.int32, (m.quarter, LANE), 1) < 64
    for c in range(m.tiles):
        a = fbuf[pl.ds(c, m.quarter, stride=m.tiles), :]
        if m.shifted:
            b = fbuf[pl.ds(c + 1, m.quarter, stride=m.tiles), :]
            a = pltpu.roll(jnp.where(low, b, a), 64, 1)
        out[pl.ds(mo(k * m.quarter, 16), m.quarter), c * LANE:(c + 1) * LANE] = a.astype(BF)


def gather_kernel(groups, p_ref, fr_ref, wq, wo, wu, wd, fa, sm, pbuf, fbuf, sq, so, su, sd, smb,
                  lsem, osem, zs, zr, xs, xr, ys, yr, fas, far, fbs, fbr, cs, cr, ms, mr):
    rep, g = lax.axis_index("rep"), lax.axis_index("grp")
    s = lax.rem(rep, 8)
    h = lax.rem(s, 2)
    k = s // 2
    kx, ky, kd = flip(k, 1), flip(k, 2), 3 - k
    full = (wq, wo, wu, wd)
    blocks = (sq, so, su, sd)
    tokens = fr_ref.shape[0]
    barrier, peers = greet(rep, g, groups)
    bounds = [0]
    for m in MATS[1:]:
        bounds.append(m.offset // LANE * LANE)
    bounds.append(FLAT)
    loads = []
    for i in range(4):
        view = (slice(None), pl.ds(bounds[i], bounds[i + 1] - bounds[i]))
        cp = pltpu.make_async_copy(p_ref.at[view], pbuf.at[view], lsem.at[i])
        cp.start()
        loads.append(cp)
    do_barrier(barrier, peers)

    def zcopy(t, d, step, src, dst):
        target = lax.rem(g + (1 if d == 0 else groups - 1), groups)
        return remote(src, dst, zs.at[t, d, step], zr.at[t, d, step], rep, target)

    def has_next(d):
        return g < groups - 1 if d == 0 else g > 0

    def own_send(t):
        for d in range(2):
            @pl.when(has_next(d))
            def _():
                if t == 4:
                    zcopy(t, d, 0, fr_ref, fa.at[pl.ds(mo(g * tokens, 16), tokens), :]).start()
                else:
                    m = MATS[t]
                    src = blocks[t].at[pl.ds(mo(k * m.quarter, 16), m.quarter), pl.ds(mo(h * m.half, LANE), m.half)]
                    zcopy(t, d, 0, src, part(full[t], m, g, k, h)).start()

    def rest(t):
        def body(i, c):
            relayout(MATS[t], lax.rem(k + i, 4), pbuf, fbuf, blocks[t])
            return c
        lax.fori_loop(1, 4, body, 0)
        pltpu.make_async_copy(blocks[t], full[t].at[pl.ds(mo(g * MATS[t].block, 16), MATS[t].block), :], osem.at[t]).start()

    def row_of(d, step):
        return g - 1 - step if d == 0 else g + 1 + step

    def valid(d, step):
        return g - 1 - step >= 0 if d == 0 else g + 1 + step <= groups - 1

    slots = [(d, step) for step in range(groups - 1) for d in range(2)]

    def zregion(t, r):
        if t == 4:
            return fa.at[pl.ds(mo(r * tokens, 16), tokens), :]
        return part(full[t], MATS[t], r, k, h)

    def stage0(t, d, step):
        @pl.when(valid(d, step))
        def _():
            r = row_of(d, step)
            reg = zregion(t, r)
            zcopy(t, d, step, reg, reg).wait_recv()
            if step < groups - 2:
                @pl.when(has_next(d))
                def _():
                    zcopy(t, d, step + 1, reg, reg).start()
            if t < 4:
                i = d * (groups - 1) + step
                remote(reg, reg, xs.at[t, i], xr.at[t, i], flip(rep, 2), g).start()
                remote(reg, reg, ys.at[t, i], yr.at[t, i], flip(rep, 4), g).start()

    def stage1(t, d, step):
        @pl.when(valid(d, step))
        def _():
            r, i, m = row_of(d, step), d * (groups - 1) + step, MATS[t]
            reg = part(full[t], m, r, kx, h)
            remote(reg, reg, xs.at[t, i], xr.at[t, i], flip(rep, 2), g).wait_recv()
            a = part(full[t], m, r, kx, h, 0)
            remote(a, a, fas.at[t, i], far.at[t, i], flip(rep, 4), g).start()
            reg = part(full[t], m, r, ky, h)
            remote(reg, reg, ys.at[t, i], yr.at[t, i], flip(rep, 4), g).wait_recv()
            b = part(full[t], m, r, ky, h, 1)
            remote(b, b, fbs.at[t, i], fbr.at[t, i], flip(rep, 2), g).start()

    def stage2(t, d, step):
        @pl.when(valid(d, step))
        def _():
            r, i, m = row_of(d, step), d * (groups - 1) + step, MATS[t]
            a, b = part(full[t], m, r, kd, h, 0), part(full[t], m, r, kd, h, 1)
            remote(a, a, fas.at[t, i], far.at[t, i], flip(rep, 4), g).wait_recv()
            remote(b, b, fbs.at[t, i], fbr.at[t, i], flip(rep, 2), g).wait_recv()
            c = slab(full[t], m, r, h)
            remote(c, c, cs.at[t, i], cr.at[t, i], flip(rep, 1), g).start()

    def stage3(t, d, step):
        @pl.when(valid(d, step))
        def _():
            r, i, m = row_of(d, step), d * (groups - 1) + step, MATS[t]
            c = slab(full[t], m, r, 1 - h)
            remote(c, c, cs.at[t, i], cr.at[t, i], flip(rep, 1), g).wait_recv()

    loads[0].wait()
    relayout(QKV, k, pbuf, fbuf, sq)
    own_send(0)
    own_send(4)
    loads[1].wait()
    relayout(OUT, k, pbuf, fbuf, so)
    own_send(1)
    loads[2].wait()
    loads[3].wait()
    relayout(UP, k, pbuf, fbuf, su)
    own_send(2)
    relayout(DOWN, k, pbuf, fbuf, sd)
    own_send(3)
    row = 0
    for first, count in SMALL:
        smb[row:row + count, :] = pbuf[:, first * LANE:(first + count) * LANE].astype(F32).reshape(count, LANE)
        row += count
    smb[row:SROWS, :] = jnp.zeros((SROWS - row, LANE), F32)
    for i in range(1, groups):
        remote(smb, sm.at[g], ms.at[i - 1], mr.at[i - 1], rep, lax.rem(g + i, groups)).start()
    pltpu.make_async_copy(smb, sm.at[g], osem.at[4]).start()
    pltpu.make_async_copy(fr_ref, fa.at[pl.ds(mo(g * tokens, 16), tokens), :], osem.at[5]).start()

    items = [(t, d, step) for step in range(groups - 1) for t in (0, 4, 1, 2, 3) for d in range(2)]
    mats = [it for it in items if it[0] < 4]
    fillers = {1: 0, 3: 1, 5: 2, 7: 3}
    lag = 2
    n1 = n2 = n3 = 0
    count = 0
    for n, it in enumerate(items):
        stage0(*it)
        if it[0] < 4:
            count += 1
        if n in fillers:
            rest(fillers[n])
        while n1 < count - lag:
            stage1(*mats[n1])
            n1 += 1
        while n2 < n1 - lag:
            stage2(*mats[n2])
            n2 += 1
    while n1 < len(mats):
        stage1(*mats[n1])
        n1 += 1
        if n2 < n1 - lag:
            stage2(*mats[n2])
            n2 += 1
    while n2 < len(mats):
        stage2(*mats[n2])
        n2 += 1
    for it in mats:
        stage3(*it)
    for t in (0, 4, 1, 2, 3):
        reg = zregion(t, g)
        for d in range(2):
            @pl.when(has_next(d))
            def _():
                zcopy(t, d, 0, reg, reg).wait_send()
        for (d, step) in slots:
            i = d * (groups - 1) + step

            @pl.when(valid(d, step))
            def _():
                r = row_of(d, step)
                if step < groups - 2:
                    @pl.when(has_next(d))
                    def _():
                        zcopy(t, d, step + 1, reg, reg).wait_send()
                if t < 4:
                    m = MATS[t]
                    remote(reg, reg, xs.at[t, i], xr.at[t, i], flip(rep, 2), g).wait_send()
                    remote(reg, reg, ys.at[t, i], yr.at[t, i], flip(rep, 4), g).wait_send()
                    a, b = part(full[t], m, r, kx, h, 0), part(full[t], m, r, ky, h, 1)
                    remote(a, a, fas.at[t, i], far.at[t, i], flip(rep, 4), g).wait_send()
                    remote(b, b, fbs.at[t, i], fbr.at[t, i], flip(rep, 2), g).wait_send()
                    c = slab(full[t], m, r, h)
                    remote(c, c, cs.at[t, i], cr.at[t, i], flip(rep, 1), g).wait_send()
        if t < 4:
            pltpu.make_async_copy(blocks[t], full[t].at[pl.ds(mo(g * MATS[t].block, 16), MATS[t].block), :], osem.at[t]).wait()
    for i in range(1, groups):
        cp = remote(smb, sm.at[lax.rem(g + groups - i, groups)], ms.at[i - 1], mr.at[i - 1], rep, lax.rem(g + i, groups))
        cp.wait_send()
        cp.wait_recv()
    pltpu.make_async_copy(smb, sm.at[g], osem.at[4]).wait()
    pltpu.make_async_copy(fr_ref, fa.at[pl.ds(mo(g * tokens, 16), tokens), :], osem.at[5]).wait()


def gather(params, frames, groups):
    dma = pltpu.SemaphoreType.DMA
    n = 2 * (groups - 1)
    tokens = frames.shape[0]
    shapes = [jax.ShapeDtypeStruct((m.block * groups, m.cols), BF) for m in MATS]
    shapes += [jax.ShapeDtypeStruct((tokens * groups, D), BF), jax.ShapeDtypeStruct((groups, SROWS, LANE), F32)]
    return pl.pallas_call(
        functools.partial(gather_kernel, groups),
        out_shape=shapes,
        in_specs=[pl.BlockSpec(memory_space=pl.ANY), pl.BlockSpec(memory_space=pltpu.VMEM)],
        out_specs=[pl.BlockSpec(memory_space=pl.ANY)] * 6,
        scratch_shapes=[
            pltpu.VMEM((1, FLAT + 8 * LANE), BF),
            pltpu.VMEM((48 * 24 + 16, LANE), F32),
        ] + [pltpu.VMEM((m.block, m.cols), BF) for m in MATS] + [
            pltpu.VMEM((SROWS, LANE), F32),
            dma((4,)), dma((6,)), dma((5, 2, groups)), dma((5, 2, groups)),
            dma((4, n)), dma((4, n)), dma((4, n)), dma((4, n)), dma((4, n)), dma((4, n)), dma((4, n)), dma((4, n)),
            dma((4, n)), dma((4, n)), dma((groups,)), dma((groups,)),
        ],
        compiler_params=pltpu.CompilerParams(collective_id=0, has_side_effects=True, vmem_limit_bytes=40 << 20),
        name="gather",
    )(params, frames)


def add_rows(dst, a, b, rows, step=16):
    def body(i, c):
        at = pl.ds(mo(i * step, 16), step)
        dst[at, :] = (a[at, :].astype(F32) + b[at, :].astype(F32)).astype(dst.dtype)
        return c
    lax.fori_loop(0, rows // step, body, 0)


def cell(ref, m, r, kk, sub=None):
    r0, rn, c0, cn = m.sub[sub] if sub is not None else (0, m.quarter, 0, m.half)
    return ref.at[pl.ds(mo(r * m.block + kk * m.quarter + r0, 16), rn), pl.ds(c0, cn)]


ORDER = (2, 3, 0, 1)


def reduce_kernel(groups, highs, gq, go, gu, gd, sm_ref, oq, oo, ou, od, osm, *scratch):
    own, scratch = scratch[:4], scratch[4:]
    buf1, scratch = scratch[:4], scratch[4:]
    buf2, scratch = scratch[:4], scratch[4:]
    buf3, scratch = scratch[:4], scratch[4:]
    zbuf, scratch = scratch[:4], scratch[4:]
    fin, scratch = scratch[:4], scratch[4:]
    (smacc, smin, lsem, c1s, c1r, a1s, a1r, b1s, b1r, a2s, a2r, b2s, b2r, zs, zr, fxs, fxr, os, xs, xr, ys, yr,
     fas, far, fbs, fbr, cs, cr, sms, smr) = scratch
    rep, g = lax.axis_index("rep"), lax.axis_index("grp")
    s = lax.rem(rep, 8)
    h = lax.rem(s, 2)
    k = s // 2
    x, y = lax.rem(k, 2), k // 2
    kx, ky, kd = flip(k, 1), flip(k, 2), 3 - k
    core, xn, yn = flip(rep, 1), flip(rep, 2), flip(rep, 4)
    grads = (gq, go, gu, gd)
    outs = (oq, oo, ou, od)
    barrier, peers = greet(rep, g, groups)
    peers += [(flip(rep, 8 << b), g) for b in range(highs)]
    do_barrier(barrier, peers)

    def row(i):
        return lax.rem(g + 1 + i, groups)

    def load(t, i):
        m = MATS[t]
        at = pl.ds(mo(row(i) * m.block, 16), m.block)
        return pltpu.make_async_copy(grads[t].at[at, pl.ds(mo(h * m.half, LANE), m.half)], own[t].at[at, :], lsem.at[t, i])

    def first(t, i):
        m = MATS[t]
        at = pl.ds(mo(row(i) * m.block, 16), m.block)
        return remote(grads[t].at[at, pl.ds(mo((1 - h) * m.half, LANE), m.half)], buf1[t].at[at, :],
                      c1s.at[t, i], c1r.at[t, i], core, g)

    def acopy(t, i, j, kk):
        return remote(cell(buf1[t], MATS[t], row(i), kk, 0), cell(buf2[t], MATS[t], row(i), kk, 0),
                      a1s.at[t, i, j], a1r.at[t, i, j], xn, g)

    def bcopy(t, i, j, kk):
        return remote(cell(buf1[t], MATS[t], row(i), kk, 1), cell(buf2[t], MATS[t], row(i), kk, 1),
                      b1s.at[t, i, j], b1r.at[t, i, j], yn, g)

    def a2copy(t, i, kk):
        return remote(cell(buf2[t], MATS[t], row(i), kk, 0), cell(buf3[t], MATS[t], row(i), kk, 0),
                      a2s.at[t, i], a2r.at[t, i], yn, g)

    def b2copy(t, i, kk):
        return remote(cell(buf2[t], MATS[t], row(i), kk, 1), cell(buf3[t], MATS[t], row(i), kk, 1),
                      b2s.at[t, i], b2r.at[t, i], xn, g)

    def zcopy(t, i):
        return remote(cell(buf3[t], MATS[t], row(i), k), zbuf[t].at[i], zs.at[t, i], zr.at[t, i], rep, row(i))

    def r1(t, i):
        m = MATS[t]
        load(t, i).wait()
        first(t, i).wait_recv()
        at = pl.ds(mo(row(i) * m.block, 16), m.block)
        add_rows(buf1[t].at[at, :], own[t].at[at, :], buf1[t].at[at, :], m.block)
        for j in range(2):
            acopy(t, i, j, 2 * j + (1 - x)).start()
            bcopy(t, i, j, 2 * (1 - y) + j).start()

    def r2(t, i):
        m = MATS[t]
        for j in range(2):
            acopy(t, i, j, 2 * j + x).wait_recv()
            kk = 2 * j + x
            add_rows(cell(buf2[t], m, row(i), kk, 0), cell(buf1[t], m, row(i), kk, 0), cell(buf2[t], m, row(i), kk, 0), m.sub[0][1])
        a2copy(t, i, 2 * (1 - y) + x).start()
        for j in range(2):
            bcopy(t, i, j, 2 * y + j).wait_recv()
            kk = 2 * y + j
            add_rows(cell(buf2[t], m, row(i), kk, 1), cell(buf1[t], m, row(i), kk, 1), cell(buf2[t], m, row(i), kk, 1), m.sub[1][1])
        b2copy(t, i, 2 * y + (1 - x)).start()

    def r3(t, i):
        m = MATS[t]
        a2copy(t, i, k).wait_recv()
        b2copy(t, i, k).wait_recv()
        whole = (cell(buf3[t], m, row(i), k), cell(buf2[t], m, row(i), k))
        add_rows(whole[0], whole[1], whole[0], m.quarter)
        if i < groups - 1:
            zcopy(t, i).start()

    def fpart(t, kk, hh, sub=None):
        return part(outs[t], MATS[t], 0, kk, hh, sub)

    def fslab(t, hh):
        return slab(outs[t], MATS[t], 0, hh)

    def keep(t):
        return pltpu.make_async_copy(fin[t].at[highs], fpart(t, k, h), os.at[t])

    def xsend(t):
        return remote(fin[t].at[highs], fpart(t, k, h), xs.at[t], xr.at[t], xn, g)

    def ysend(t):
        return remote(fin[t].at[highs], fpart(t, k, h), ys.at[t], yr.at[t], yn, g)

    def xgot(t):
        return remote(fpart(t, kx, h), fpart(t, kx, h), xs.at[t], xr.at[t], xn, g)

    def ygot(t):
        return remote(fpart(t, ky, h), fpart(t, ky, h), ys.at[t], yr.at[t], yn, g)

    def fwd(t, sub, kk):
        reg = fpart(t, kk, h, sub)
        return remote(reg, reg, (fas, fbs)[sub].at[t], (far, fbr)[sub].at[t], (yn, xn)[sub], g)

    def cross(t, hh):
        return remote(fslab(t, hh), fslab(t, hh), cs.at[t], cr.at[t], core, g)

    def r4(t):
        m = MATS[t]
        for i in range(groups - 1):
            zcopy(t, i).wait_recv()
        mine = cell(buf3[t], m, g, k)

        def body(n, c):
            at = pl.ds(mo(n * 16, 16), 16)
            total = mine[at, :].astype(F32)
            for i in range(groups - 1):
                total = total + zbuf[t][i, at, :].astype(F32)
            fin[t][0, at, :] = total.astype(BF)
            return c
        lax.fori_loop(0, m.quarter // 16, body, 0)
        for b in range(highs):
            cp = remote(fin[t].at[b], fin[t].at[highs + 1 + b], fxs.at[t, b], fxr.at[t, b], flip(rep, 8 << b), g)
            cp.start()
            cp.wait()
            add_rows(fin[t].at[b + 1], fin[t].at[b], fin[t].at[highs + 1 + b], m.quarter)
        keep(t).start()
        xsend(t).start()
        ysend(t).start()

    def r5(t):
        xgot(t).wait_recv()
        fwd(t, 0, kx).start()
        ygot(t).wait_recv()
        fwd(t, 1, ky).start()

    def r6(t):
        fwd(t, 0, kd).wait_recv()
        fwd(t, 1, kd).wait_recv()
        keep(t).wait()
        cross(t, h).start()

    def r7(t):
        cross(t, 1 - h).wait_recv()

    partners = [(core, g), (xn, g), (yn, g)] + [(flip(rep, 8 << b), g) for b in range(highs)]
    bit = 1
    while bit < groups:
        partners.append((rep, flip(g, bit)))
        bit *= 2

    def smcopy(j):
        return remote(smacc.at[j], smin.at[j], sms.at[j], smr.at[j], *partners[j])

    def small(j):
        if j:
            smcopy(j - 1).wait_recv()
            smacc[j] = smacc[j - 1] + smin[j - 1]
        else:
            smacc[0] = sm_ref[...]
        if j < len(partners):
            smcopy(j).start()
        else:
            osm[...] = smacc[j, g]

    chunks = [(t, i) for t in ORDER for i in range(groups)]
    small(0)
    for t, i in chunks:
        first(t, i).start()
        load(t, i).start()
    done4 = {}
    total = len(chunks)
    smalls = 1
    for n in range(total + 16):
        if n < total:
            r1(*chunks[n])
        if 0 <= n - 2 < total:
            r2(*chunks[n - 2])
        if n % 2 and smalls <= len(partners):
            small(smalls)
            smalls += 1
        if 0 <= n - 4 < total:
            r3(*chunks[n - 4])
        for q, t in enumerate(ORDER):
            last = groups * q + groups - 1 + 4
            if n == last + 2:
                r4(t)
            if n == last + 4:
                r5(t)
            if n == last + 6:
                r6(t)
    for t in ORDER:
        r7(t)
    for t, i in chunks:
        first(t, i).wait_send()
        for j in range(2):
            acopy(t, i, j, 2 * j + x).wait_send()
            bcopy(t, i, j, 2 * y + j).wait_send()
        a2copy(t, i, k).wait_send()
        b2copy(t, i, k).wait_send()
        if i < groups - 1:
            zcopy(t, i).wait_send()
    for t in ORDER:
        xsend(t).wait_send()
        ysend(t).wait_send()
        fwd(t, 0, kx).wait_send()
        fwd(t, 1, ky).wait_send()
        cross(t, h).wait_send()
    for j in range(len(partners)):
        smcopy(j).wait_send()


def reduce_grads(grads, smalls, groups, reps):
    dma = pltpu.SemaphoreType.DMA
    highs = (reps // 8).bit_length() - 1
    steps = 3 + highs + groups.bit_length() - 1
    wide = [pltpu.VMEM((m.block * groups, m.half), BF) for m in MATS]
    scratch = wide * 4
    scratch += [pltpu.VMEM((groups, m.quarter, m.half), BF) for m in MATS]
    scratch += [pltpu.VMEM((2 * highs + 1, m.quarter, m.half), BF) for m in MATS]
    scratch += [pltpu.VMEM((steps + 1, groups, SROWS, LANE), F32), pltpu.VMEM((steps, groups, SROWS, LANE), F32)]
    scratch += [dma((4, groups))] * 3 + [dma((4, groups, 2))] * 4 + [dma((4, groups))] * 6
    scratch += [dma((4, max(highs, 1)))] * 2 + [dma((4,))] * 11 + [dma((steps,))] * 2
    return pl.pallas_call(
        functools.partial(reduce_kernel, groups, highs),
        out_shape=[jax.ShapeDtypeStruct((m.block, m.cols), BF) for m in MATS] + [jax.ShapeDtypeStruct((SROWS, LANE), F32)],
        in_specs=[pl.BlockSpec(memory_space=pl.ANY)] * 4 + [pl.BlockSpec(memory_space=pltpu.VMEM)],
        out_specs=[pl.BlockSpec(memory_space=pl.ANY)] * 4 + [pl.BlockSpec(memory_space=pltpu.VMEM)],
        scratch_shapes=scratch,
        compiler_params=pltpu.CompilerParams(collective_id=1, has_side_effects=True, vmem_limit_bytes=44 << 20),
        name="reduce",
    )(*grads, smalls)


BETA_ONE = 0.9
BETA_TWO = 0.98
ADAM_EPS = 1e-06
LEARN_RATE = 0.006
DECAY = 0.01
ADAM_STEP = 4
ROWS = 1736
STEPS = -(-FROWS // ROWS)


def flatten(m, block, flat, late):
    def body(i, carry):
        base = m.row0 + i * (48 * m.tiles)
        for c in range(m.tiles):
            tile = block[pl.ds(mo(i * 48, 16), 48), c * LANE:(c + 1) * LANE].astype(F32)
            if m.shifted:
                tile = pltpu.roll(tile, 64, 1)
                late[pl.ds(base + c + 1, 48, stride=m.tiles), :] = tile
            flat[pl.ds(base + c, 48, stride=m.tiles), :] = tile
        return carry
    lax.fori_loop(0, m.block // 48, body, 0)


def adam_kernel(scale, gq, go, gu, gd, sm, p_ref, m_ref, v_ref, o_g, o_p, o_m, o_v, flat, late):
    step = pl.program_id(0)

    @pl.when(step == 0)
    def _():
        flatten(QKV, gq, flat, late)
        flatten(OUT, go, flat, late)
        flatten(UP, gu, flat, late)
        flatten(DOWN, gd, flat, late)
        flat[0:3, :] = sm[0:3, :]
        flat[3459:3462, :] = sm[3:6, :]
        flat[4614:4618, :] = sm[6:10, :]
        flat[4618:4619, 0:64] = sm[10:11, 0:64]
        flat[9226:9227, 64:128] = sm[11:12, 64:128]
        flat[9227:9232, :] = sm[12:17, :]
        flat[9232:9233, 0:64] = sm[17:18, 0:64]
        flat[13840:13841, 64:128] = sm[18:19, 64:128]
        flat[13841:13842, :] = sm[19:20, :]
        late[9227:9232, :] = sm[12:17, :]
        late[9232:9233, 0:64] = sm[17:18, 0:64]
        late[13841:13842, :] = sm[19:20, :]

    at = pl.ds(mo(step * ROWS, 8), ROWS)
    number = step * ROWS + lax.broadcasted_iota(jnp.int32, (ROWS, LANE), 0)
    low = lax.broadcasted_iota(jnp.int32, (ROWS, LANE), 1) < 64
    grad = jnp.where(jnp.logical_and(number > UP.row0, low), late[at, :], flat[at, :]).reshape(1, ROWS * LANE) * scale
    first = BETA_ONE * m_ref[...] + (1.0 - BETA_ONE) * grad
    second = BETA_TWO * v_ref[...] + (1.0 - BETA_TWO) * grad * grad
    o_g[...] = grad
    o_m[...] = first
    o_v[...] = second
    first_hat = first * (1.0 / (1.0 - BETA_ONE**ADAM_STEP))
    second_hat = second * (1.0 / (1.0 - BETA_TWO**ADAM_STEP))
    current = p_ref[...].astype(F32)
    o_p[...] = current - LEARN_RATE * (first_hat / (jnp.sqrt(second_hat) + ADAM_EPS) + DECAY * current)


def adam(blocks, smalls, params, first, second, reps):
    spec = pl.BlockSpec((1, ROWS * LANE), lambda i: (0, i))
    vmem = pl.BlockSpec(memory_space=pltpu.VMEM)
    return pl.pallas_call(
        functools.partial(adam_kernel, 1.0 / reps),
        grid=(STEPS,),
        out_shape=[jax.ShapeDtypeStruct((1, FLAT), F32)] * 4,
        in_specs=[vmem] * 5 + [spec] * 3,
        out_specs=[spec] * 4,
        scratch_shapes=[pltpu.VMEM((STEPS * ROWS, LANE), F32)] * 2,
        compiler_params=pltpu.CompilerParams(vmem_limit_bytes=50 << 20),
        name="adam",
    )(*blocks, smalls, params, first, second)


EPS_NORM = 1e-05
ROOT_HALF = 0.7071067811865476
ROOT_TWO_PI = 0.3989422804014327
HEADS = D // HDIM
GAIN_ONE, SHIFT_ONE, QV_BIAS, OUT_BIAS, GAIN_TWO, SHIFT_TWO, UP_BIAS, DOWN_BIAS = (
    (0, 3), (3, 3), (6, 6), (12, 3), (15, 3), (18, 3), (23, 12), (37, 3))


def low_lanes():
    return lax.broadcasted_iota(jnp.int32, (1, LANE), 1) < 64


def assemble(sm, place, out):
    first, count = place
    halves = [(gi, first + i) for gi in range(sm.shape[0]) for i in range(count)]
    for t in range(len(halves) // 2):
        (g0, h0), (g1, h1) = halves[2 * t], halves[2 * t + 1]
        a = sm[g0, h0 // 2:h0 // 2 + 1, :]
        b = sm[g1, h1 // 2:h1 // 2 + 1, :]
        a = pltpu.roll(a, 64, 1) if h0 % 2 else a
        b = b if h1 % 2 else pltpu.roll(b, 64, 1)
        out[0:1, t * LANE:(t + 1) * LANE] = jnp.where(low_lanes(), a, b)


def fill_image(image, rows, vectors):
    where = {}
    for place, ref in vectors:
        for i in range(place[1]):
            where[place[0] + i] = (place[1], i, ref)
    for gi in range(image.shape[0]):
        for r in rows:
            parts = []
            for side in range(2):
                spot = where.get(2 * r + side)
                if spot is None:
                    parts.append(jnp.zeros((1, LANE), F32))
                    continue
                count, i, ref = spot
                q = gi * count + i
                v = ref[0:1, q // 2 * LANE:(q // 2 + 1) * LANE]
                parts.append(v if q % 2 == side else pltpu.roll(v, 64, 1))
            image[gi, r:r + 1, :] = jnp.where(low_lanes(), parts[0], parts[1])


def mean(v):
    return jnp.sum(v, axis=-1, keepdims=True) * (1.0 / D)


def normalize(v):
    centered = v - mean(v)
    inverse = lax.rsqrt(mean(centered * centered) + EPS_NORM)
    return centered * inverse, inverse


def norm_back(upstream, normal, inverse, gain):
    s = upstream * gain
    return inverse * (s - mean(s) - normal * mean(s * normal))


def nn(a, b):
    return lax.dot_general(a, b, (((1,), (0,)), ((), ())), preferred_element_type=F32)


def nt(a, b):
    return lax.dot_general(a, b, (((1,), (1,)), ((), ())), preferred_element_type=F32)


def loop(count, body):
    def step(i, c):
        body(i)
        return c
    lax.fori_loop(0, count, step, 0)


def head_mask(rows):
    return lax.broadcasted_iota(jnp.int32, (rows, LANE), 1) < HDIM


def project_block(j, fa, gain, shift, bias, wq, q_all, k_all, v_all, normed, tokens):
    at = pl.ds(mo(j * tokens, 16), tokens)
    normal, _ = normalize(fa[at, :].astype(F32))
    normed[...] = (normal * gain[...] + shift[...]).astype(BF)
    for third, out in enumerate((q_all, k_all, v_all)):
        def body(n):
            col = pl.ds(mo(n * 256, 256), 256)
            wide = nn(normed[...], wq[:, pl.ds(mo(third * D + n * 256, 256), 256)])
            if third != 1:
                wide = wide + bias[0:1, pl.ds(mo((third // 2) * D + n * 256, 256), 256)]
            out[at, col] = wide.astype(BF)
        loop(D // 256, body)


def attend_pair(p, g, q_all, k_all, v_all, attended, stats, tokens):
    col = pl.ds(mo(p * LANE, LANE), LANE)
    query = q_all[pl.ds(mo(g * tokens, 16), tokens), col] * jnp.asarray(HDIM**-0.5, BF)
    keys, values = k_all[:, col], v_all[:, col]
    mask = head_mask(tokens)
    zero = jnp.zeros_like(query)
    lanes = lax.broadcasted_iota(jnp.int32, (tokens, LANE), 1)
    results = []
    for side in range(2):
        scores = nt(jnp.where(mask, query, zero) if side == 0 else jnp.where(mask, zero, query), keys)
        highest = jnp.max(scores, axis=-1, keepdims=True)
        shares = jnp.exp(scores - highest)
        total = jnp.sum(shares, axis=-1, keepdims=True)
        results.append(nn(shares.astype(BF), values) * (1.0 / total))
        stats[...] = jnp.where(lanes == 2 * p + side, highest + jnp.log(total), stats[...])
    attended[:, col] = jnp.where(mask, results[0], results[1]).astype(BF)


def fwd_kernel(fa, wq, sm, q_all, k_all, v_all, attended, stats, normed, gain, shift, bias):
    g = lax.axis_index("grp")
    tokens = attended.shape[0]
    assemble(sm, GAIN_ONE, gain)
    assemble(sm, SHIFT_ONE, shift)
    assemble(sm, QV_BIAS, bias)
    loop(fa.shape[0] // tokens, lambda j: project_block(j, fa, gain, shift, bias, wq, q_all, k_all, v_all, normed, tokens))
    stats[...] = jnp.zeros_like(stats)
    loop(HEADS // 2, lambda p: attend_pair(p, g, q_all, k_all, v_all, attended, stats, tokens))


def forward(clip, wq, smalls, tokens):
    vmem = pl.BlockSpec(memory_space=pltpu.VMEM)
    wide = jax.ShapeDtypeStruct(clip.shape, BF)
    return pl.pallas_call(
        fwd_kernel,
        out_shape=[wide] * 3 + [jax.ShapeDtypeStruct((tokens, D), BF), jax.ShapeDtypeStruct((tokens, LANE), F32)],
        in_specs=[vmem] * 3, out_specs=[vmem] * 5,
        scratch_shapes=[pltpu.VMEM((tokens, D), BF), pltpu.VMEM((1, D), F32), pltpu.VMEM((1, D), F32), pltpu.VMEM((1, 2 * D), F32)],
        compiler_params=pltpu.CompilerParams(vmem_limit_bytes=40 << 20),
        name="forward",
    )(clip, wq, smalls)


def mid_kernel(attended, fr, ct, wo_h, wu_h, wd_h, sm, lse, out_frames, agrad, mgrad, stats, rows, go, gu, gd, image,
               wo, wu, wd, middle, normal, normed, act, pre, half, turned, wide, gain, shift, obias, ubias, dbias,
               v_gain, v_shift, v_out, v_up, v_down, sem):
    tokens = attended.shape[0]
    loads = [pltpu.make_async_copy(a, b, sem.at[i]) for i, (a, b) in enumerate(((wo_h, wo), (wu_h, wu), (wd_h, wd)))]
    for cp in loads:
        cp.start()
    assemble(sm, GAIN_TWO, gain)
    assemble(sm, SHIFT_TWO, shift)
    assemble(sm, OUT_BIAS, obias)
    assemble(sm, UP_BIAS, ubias)
    assemble(sm, DOWN_BIAS, dbias)
    loads[0].wait()

    def out_block(n):
        col = pl.ds(mo(n * 256, 256), 256)
        middle[:, col] = nn(attended[...], wo[:, col]) + obias[0:1, col] + fr[:, col].astype(F32)
    loop(D // 256, out_block)
    value, inverse = normalize(middle[...])
    normal[...] = value
    normed[...] = (value * gain[...] + shift[...]).astype(BF)
    loads[1].wait()
    loads[2].wait()

    def hidden_block(n):
        col = pl.ds(mo(n * 256, 256), 256)
        hidden = nn(normed[...], wu[:, col]) + ubias[0:1, col]
        bell = 0.5 * (1.0 + lax.erf(hidden * ROOT_HALF))
        act[:, col] = (hidden * bell).astype(BF)
        slope = bell + hidden * jnp.exp(-0.5 * hidden * hidden) * ROOT_TWO_PI
        grad = nt(ct[...], wd[pl.ds(mo(n * 256, 256), 256), :]) * slope
        v_up[0:1, col] = jnp.sum(grad, axis=0, keepdims=True)
        pre[:, col] = grad.astype(BF)
    loop(FF // 256, hidden_block)

    def down_block(n):
        col = pl.ds(mo(n * 256, 256), 256)
        out_frames[:, col] = (nn(act[...], wd[:, col]) + dbias[0:1, col] + middle[:, col]).astype(BF)
    loop(D // 256, down_block)

    def back_block(n):
        col = pl.ds(mo(n * 256, 256), 256)
        wide[:, col] = nt(pre[...], wu[pl.ds(mo(n * 256, 256), 256), :])
    loop(D // 256, back_block)
    upstream = wide[...]
    v_gain[...] = jnp.sum(upstream * normal[...], axis=0, keepdims=True)
    v_shift[...] = jnp.sum(upstream, axis=0, keepdims=True)
    total = ct[...].astype(F32) + norm_back(upstream, normal[...], inverse, gain[...])
    mgrad[...] = total
    half[...] = total.astype(BF)
    v_out[...] = jnp.sum(total, axis=0, keepdims=True)
    v_down[...] = jnp.sum(ct[...].astype(F32), axis=0, keepdims=True)

    def attended_block(n):
        col = pl.ds(mo(n * 256, 256), 256)
        agrad[:, col] = nt(half[...], wo[pl.ds(mo(n * 256, 256), 256), :]).astype(BF)
    loop(D // 256, attended_block)
    lanes = lax.broadcasted_iota(jnp.int32, (tokens, LANE), 1)
    mask = head_mask(tokens)
    both = lse[...]
    for p in range(HEADS // 2):
        product = agrad[:, p * LANE:(p + 1) * LANE].astype(F32) * attended[:, p * LANE:(p + 1) * LANE].astype(F32)
        for side in range(2):
            mine = jnp.where(mask if side == 0 else jnp.logical_not(mask), product, 0.0)
            both = jnp.where(lanes == HEADS + 2 * p + side, jnp.sum(mine, axis=-1, keepdims=True), both)
    stats[...] = both
    rows[...] = both.T[0:2 * HEADS, :]

    def weight(left, right, out):
        count = left.shape[1]
        turned[0:count, :] = left[...].T

        def block(i):
            def inner(n):
                r, c = pl.ds(mo(i * 256, 256), 256), pl.ds(mo(n * 256, 256), 256)
                out[r, c] = nn(turned[r, :], right[:, c]).astype(BF)
            loop(right.shape[1] // 256, inner)
        loop(count // 256, block)
    weight(act, ct, gd)
    weight(normed, pre, gu)
    weight(attended, half, go)
    fill_image(image, range(6, SROWS), ((OUT_BIAS, v_out), (GAIN_TWO, v_gain), (SHIFT_TWO, v_shift), (UP_BIAS, v_up), (DOWN_BIAS, v_down)))


def middle_step(attended, frames, cotangent, weights, smalls, lse):
    vmem, hbm = pl.BlockSpec(memory_space=pltpu.VMEM), pl.BlockSpec(memory_space=pl.ANY)
    tokens = frames.shape[0]
    groups = smalls.shape[0]
    sds = jax.ShapeDtypeStruct
    vec = [pltpu.VMEM((1, n), F32) for n in (D, D, D, FF, D)]
    return pl.pallas_call(
        mid_kernel,
        out_shape=[sds((tokens, D), BF), sds((tokens, D), BF), sds((tokens, D), F32), sds((tokens, LANE), F32),
                   sds((2 * HEADS, tokens), F32), sds((D, D), BF), sds((D, FF), BF), sds((FF, D), BF),
                   sds((groups, SROWS, LANE), F32)],
        in_specs=[vmem] * 3 + [hbm] * 3 + [vmem] * 2, out_specs=[vmem] * 9,
        scratch_shapes=[pltpu.VMEM((D, D), BF), pltpu.VMEM((D, FF), BF), pltpu.VMEM((FF, D), BF),
                        pltpu.VMEM((tokens, D), F32), pltpu.VMEM((tokens, D), F32), pltpu.VMEM((tokens, D), BF),
                        pltpu.VMEM((tokens, FF), BF), pltpu.VMEM((tokens, FF), BF), pltpu.VMEM((tokens, D), BF),
                        pltpu.VMEM((FF, tokens), BF), pltpu.VMEM((tokens, D), F32)] + vec + vec[:3] + [vec[3], vec[4]]
                       + [pltpu.SemaphoreType.DMA((3,))],
        compiler_params=pltpu.CompilerParams(vmem_limit_bytes=56 << 20),
        name="middle",
    )(attended, frames, cotangent, *weights, smalls, lse)


def share_kernel(groups, a_ref, r_ref, a_all, r_all, osem, zs, zr, rs, rr):
    rep, g = lax.axis_index("rep"), lax.axis_index("grp")
    tokens = a_ref.shape[0]
    do_barrier(pltpu.get_barrier_semaphore(), [(rep, lax.rem(g + i, groups)) for i in range(1, groups)])

    def place(r):
        return a_all.at[pl.ds(mo(r * tokens, 16), tokens), :]

    def zcopy(d, step, src, dst):
        target = lax.rem(g + (1 if d == 0 else groups - 1), groups)
        return remote(src, dst, zs.at[d, step], zr.at[d, step], rep, target)

    def has_next(d):
        return g < groups - 1 if d == 0 else g > 0

    keep = pltpu.make_async_copy(a_ref, place(g), osem.at[0])
    keep.start()
    for i in range(1, groups):
        remote(r_ref, r_all.at[g], rs.at[i - 1], rr.at[i - 1], rep, lax.rem(g + i, groups)).start()
    for d in range(2):
        @pl.when(has_next(d))
        def _():
            zcopy(d, 0, a_ref, place(g)).start()
    r_all[g] = r_ref[...]
    for step in range(groups - 1):
        for d in range(2):
            r = g - 1 - step if d == 0 else g + 1 + step

            @pl.when(r >= 0 if d == 0 else r <= groups - 1)
            def _():
                zcopy(d, step, place(r), place(r)).wait_recv()
                if step < groups - 2:
                    @pl.when(has_next(d))
                    def _():
                        zcopy(d, step + 1, place(r), place(r)).start()
    for step in range(groups - 1):
        for d in range(2):
            r = g - step if d == 0 else g + step

            @pl.when(jnp.logical_and(r >= 0 if d == 0 else r <= groups - 1, has_next(d)))
            def _():
                zcopy(d, step, place(g), place(g)).wait_send()
    for i in range(1, groups):
        cp = remote(r_ref, r_all.at[lax.rem(g + groups - i, groups)], rs.at[i - 1], rr.at[i - 1], rep, lax.rem(g + i, groups))
        cp.wait_send()
        cp.wait_recv()
    keep.wait()


def share(agrad, rows, groups):
    dma = pltpu.SemaphoreType.DMA
    vmem, hbm = pl.BlockSpec(memory_space=pltpu.VMEM), pl.BlockSpec(memory_space=pl.ANY)
    return pl.pallas_call(
        functools.partial(share_kernel, groups),
        out_shape=[jax.ShapeDtypeStruct((groups * agrad.shape[0], D), BF), jax.ShapeDtypeStruct((groups,) + rows.shape, F32)],
        in_specs=[vmem] * 2, out_specs=[hbm, vmem],
        scratch_shapes=[dma((1,)), dma((2, groups)), dma((2, groups)), dma((groups,)), dma((groups,))],
        compiler_params=pltpu.CompilerParams(collective_id=2, has_side_effects=True),
        name="share",
    )(agrad, rows)


def query_back(p, g, q_all, k_all, v_all, a_all, stats, grad, tokens):
    col = pl.ds(mo(p * LANE, LANE), LANE)
    own = pl.ds(mo(g * tokens, 16), tokens)
    scale = jnp.asarray(HDIM**-0.5, BF)
    query, upstream = q_all[own, col] * scale, a_all[own, col]
    keys, values = k_all[:, col], v_all[:, col]
    mask = head_mask(tokens)
    zero = jnp.zeros_like(query)
    lanes = lax.broadcasted_iota(jnp.int32, (tokens, LANE), 1)
    results = []
    for side in range(2):
        def pick(v):
            return jnp.where(mask, v, zero) if side == 0 else jnp.where(mask, zero, v)
        total = jnp.sum(jnp.where(lanes == 2 * p + side, stats[...], 0.0), axis=-1, keepdims=True)
        centre = jnp.sum(jnp.where(lanes == HEADS + 2 * p + side, stats[...], 0.0), axis=-1, keepdims=True)
        shares = jnp.exp(nt(pick(query), keys) - total)
        back = (shares * (nt(pick(upstream), values) - centre)).astype(BF) * scale
        results.append(nn(back, keys))
    grad[:, col] = jnp.where(mask, results[0], results[1])


def key_back(p, g, q_all, k_all, v_all, a_all, rows, kgrad, vgrad, tokens):
    col = pl.ds(mo(p * LANE, LANE), LANE)
    own = pl.ds(mo(g * tokens, 16), tokens)
    scale = jnp.asarray(HDIM**-0.5, BF)
    keys, values = k_all[own, col] * scale, v_all[own, col]
    queries, upstream = q_all[:, col], a_all[:, col]
    mask = head_mask(tokens)
    zero = jnp.zeros_like(keys)
    ks, vs = [], []
    for side in range(2):
        def pick(v):
            return jnp.where(mask, v, zero) if side == 0 else jnp.where(mask, zero, v)
        total = rows[pl.ds(2 * p + side, 1), :]
        centre = rows[pl.ds(HEADS + 2 * p + side, 1), :]
        shares = jnp.exp(nt(pick(keys), queries) - total)
        vs.append(nn(shares.astype(BF), upstream))
        back = (shares * (nt(pick(values), upstream) - centre)).astype(BF) * scale
        ks.append(nn(back, queries))
    kgrad[:, col] = jnp.where(mask, ks[0], ks[1])
    vgrad[:, col] = jnp.where(mask, vs[0], vs[1])


def input_back(wq, fr, mgrad, gain, shift, qg, kg, vg, pgrad, normed, turned, wide, frames_grad, gq, v_gain, v_shift, v_qv):
    for i, ref in enumerate((qg, kg, vg)):
        pgrad[:, i * D:(i + 1) * D] = ref[...].astype(BF)
    v_qv[0:1, 0:D] = jnp.sum(qg[...], axis=0, keepdims=True)
    v_qv[0:1, D:2 * D] = jnp.sum(vg[...], axis=0, keepdims=True)

    def block(n):
        col = pl.ds(mo(n * 256, 256), 256)
        wide[:, col] = nt(pgrad[...], wq[pl.ds(mo(n * 256, 256), 256), :])
    loop(D // 256, block)
    normal, inverse = normalize(fr[...].astype(F32))
    normed[...] = (normal * gain[...] + shift[...]).astype(BF)
    upstream = wide[...]
    v_gain[...] = jnp.sum(upstream * normal, axis=0, keepdims=True)
    v_shift[...] = jnp.sum(upstream, axis=0, keepdims=True)
    frames_grad[...] = (mgrad[...] + norm_back(upstream, normal, inverse, gain[...])).astype(BF)
    turned[...] = normed[...].T

    def outer(i):
        def inner(n):
            r, c = pl.ds(mo(i * 256, 256), 256), pl.ds(mo(n * 256, 256), 256)
            gq[r, c] = nn(turned[r, :], pgrad[:, c]).astype(BF)
        loop(3 * D // 256, inner)
    loop(D // 256, outer)


def back_kernel(q_all, k_all, v_all, a_all, rows3, stats, wq, fr, mgrad, sm, image_in, frames_grad, gq, image,
                rows, gain, shift, qg, kg, vg, pgrad, normed, turned, wide, v_gain, v_shift, v_qv):
    g = lax.axis_index("grp")
    tokens = fr.shape[0]
    assemble(sm, GAIN_ONE, gain)
    assemble(sm, SHIFT_ONE, shift)
    for i in range(rows3.shape[0]):
        rows[:, i * tokens:(i + 1) * tokens] = rows3[i]
    loop(HEADS // 2, lambda p: query_back(p, g, q_all, k_all, v_all, a_all, stats, qg, tokens))
    loop(HEADS // 2, lambda p: key_back(p, g, q_all, k_all, v_all, a_all, rows, kg, vg, tokens))
    input_back(wq, fr, mgrad, gain, shift, qg, kg, vg, pgrad, normed, turned, wide, frames_grad, gq, v_gain, v_shift, v_qv)
    image[...] = image_in[...]
    fill_image(image, range(6), ((GAIN_ONE, v_gain), (SHIFT_ONE, v_shift), (QV_BIAS, v_qv)))


def backward(q_all, k_all, v_all, a_all, rows, stats, wq, frames, mgrad, smalls, image):
    vmem = pl.BlockSpec(memory_space=pltpu.VMEM)
    tokens = frames.shape[0]
    clip = q_all.shape[0]
    sds = jax.ShapeDtypeStruct
    return pl.pallas_call(
        back_kernel,
        out_shape=[sds((tokens, D), BF), sds((D, 3 * D), BF), sds(image.shape, F32)],
        in_specs=[vmem] * 11, out_specs=[vmem] * 3,
        scratch_shapes=[pltpu.VMEM((2 * HEADS, clip), F32), pltpu.VMEM((1, D), F32), pltpu.VMEM((1, D), F32)]
        + [pltpu.VMEM((tokens, D), F32)] * 3 + [pltpu.VMEM((tokens, 3 * D), BF), pltpu.VMEM((tokens, D), BF),
           pltpu.VMEM((D, tokens), BF), pltpu.VMEM((tokens, D), F32), pltpu.VMEM((1, D), F32), pltpu.VMEM((1, D), F32),
           pltpu.VMEM((1, 2 * D), F32)],
        compiler_params=pltpu.CompilerParams(vmem_limit_bytes=50 << 20),
        name="backward",
    )(q_all, k_all, v_all, a_all, rows, stats, wq, frames, mgrad, smalls, image)


def on_device(frames, cotangent, params, first_moment, second_moment):
    groups, reps = lax.axis_size("grp"), lax.axis_size("rep")
    wq, wo, wu, wd, clip, smalls = gather(params, frames, groups)
    q_all, k_all, v_all, attended, lse = forward(clip, wq, smalls, frames.shape[0])
    out_frames, agrad, mgrad, stats, rows, go, gu, gd, image = middle_step(
        attended, frames, cotangent, (wo, wu, wd), smalls, lse)
    a_all, rows_all = share(agrad, rows, groups)
    frames_grad, gq, image = backward(q_all, k_all, v_all, a_all, rows_all, stats, wq, frames, mgrad, smalls, image)
    *blocks, small = reduce_grads((gq, go, gu, gd), image, groups, reps)
    param_grad, new_params, new_first, new_second = adam(blocks, small, params, first_moment, second_moment, reps)
    return (out_frames, frames_grad, param_grad, new_params, new_first, new_second)


def solution(mesh):
    in_specs = (
        P(("rep", "grp"), None),
        P(("rep", "grp"), None),
        P("grp", None),
        P("grp", None),
        P("grp", None),
    )
    out_specs = (
        P(("rep", "grp"), None),
        P(("rep", "grp"), None),
        P("grp", None),
        P("grp", None),
        P("grp", None),
        P("grp", None),
    )
    return jax.shard_map(
        on_device, mesh=mesh, in_specs=in_specs, out_specs=out_specs, check_vma=False
    )
```

```python
import functools
import jax
import jax.numpy as jnp
from jax import lax
from jax.sharding import PartitionSpec as P
from jax.experimental import pallas as pl
from jax.experimental.pallas import tpu as pltpu

MESH = pl.DeviceIdType.MESH
BF = jnp.bfloat16
F32 = jnp.float32
D = 768
FF = 3072
HDIM = 64
LANE = 128
FLAT = 1771776
FROWS = FLAT // LANE


class Mat:
    def __init__(self, offset, block, cols, suba, subb):
        self.offset, self.block, self.cols = offset, block, cols
        self.tiles = cols // LANE
        self.row0 = offset // LANE
        self.shifted = offset % LANE != 0
        self.quarter = block // 4
        self.half = cols // 2
        self.sub = (suba, subb)


QKV = Mat(384, 192, 2304, (0, 48, 0, 640), (0, 48, 640, 512))
OUT = Mat(443136, 192, 768, (0, 48, 0, 128), (0, 48, 128, 256))
UP = Mat(591168, 192, 3072, (0, 48, 0, 768), (0, 48, 768, 768))
DOWN = Mat(1181760, 768, 768, (0, 96, 0, 384), (96, 96, 0, 384))
MATS = (QKV, OUT, UP, DOWN)
SMALL = ((0, 3), (3459, 3), (4614, 5), (9226, 7), (13840, 2))
SROWS = 24


def flip(index, bit):
    return index + bit - 2 * bit * ((index // bit) % 2)


def mo(value, by):
    return pl.multiple_of(value, by)


def part(ref, m, r, k, h, sub=None):
    r0, rn, c0, cn = m.sub[sub] if sub is not None else (0, m.quarter, 0, m.half)
    row = mo(r * m.block + k * m.quarter + r0, 16)
    col = mo(h * m.half + c0, LANE)
    return ref.at[pl.ds(row, rn), pl.ds(col, cn)]


def slab(ref, m, r, h):
    return ref.at[pl.ds(mo(r * m.block, 16), m.block), pl.ds(mo(h * m.half, LANE), m.half)]


def remote(src, dst, send, recv, rep, grp):
    return pltpu.make_async_remote_copy(
        src_ref=src, dst_ref=dst, send_sem=send, recv_sem=recv,
        device_id={"rep": rep, "grp": grp}, device_id_type=MESH)


def greet(rep, g, groups, everyone=False):
    barrier = pltpu.get_barrier_semaphore()
    peers = [(flip(rep, b), g) for b in (1, 2, 4)]
    peers += [(rep, lax.rem(g + i, groups)) for i in range(1, groups)]
    return barrier, peers


def do_barrier(barrier, peers):
    for r, gg in peers:
        pl.semaphore_signal(barrier, inc=1, device_id={"rep": r, "grp": gg}, device_id_type=MESH)
    pl.semaphore_wait(barrier, len(peers))


def relayout(m, k, pbuf, fbuf, out):
    nrows = m.quarter * m.tiles
    extra = 8 if m.shifted else 0
    start = mo((m.row0 + k * nrows) * LANE, LANE)
    piece = pbuf[:, pl.ds(start, (nrows + extra) * LANE)]
    fbuf[0:nrows + extra, :] = piece.astype(F32).reshape(nrows + extra, LANE)
    low = lax.broadcasted_iota(jnp.int32, (m.quarter, LANE), 1) < 64
    for c in range(m.tiles):
        a = fbuf[pl.ds(c, m.quarter, stride=m.tiles), :]
        if m.shifted:
            b = fbuf[pl.ds(c + 1, m.quarter, stride=m.tiles), :]
            a = pltpu.roll(jnp.where(low, b, a), 64, 1)
        out[pl.ds(mo(k * m.quarter, 16), m.quarter), c * LANE:(c + 1) * LANE] = a.astype(BF)


def gather_kernel(groups, p_ref, fr_ref, wq, wo, wu, wd, fa, sm, pbuf, fbuf, sq, so, su, sd, smb,
                  lsem, osem, zs, zr, xs, xr, ys, yr, fas, far, fbs, fbr, cs, cr, ms, mr):
    rep, g = lax.axis_index("rep"), lax.axis_index("grp")
    s = lax.rem(rep, 8)
    h = lax.rem(s, 2)
    k = s // 2
    kx, ky, kd = flip(k, 1), flip(k, 2), 3 - k
    full = (wq, wo, wu, wd)
    blocks = (sq, so, su, sd)
    tokens = fr_ref.shape[0]
    barrier, peers = greet(rep, g, groups)
    bounds = [0]
    for m in MATS[1:]:
        bounds.append(m.offset // LANE * LANE)
    bounds.append(FLAT)
    loads = []
    for i in range(4):
        view = (slice(None), pl.ds(bounds[i], bounds[i + 1] - bounds[i]))
        cp = pltpu.make_async_copy(p_ref.at[view], pbuf.at[view], lsem.at[i])
        cp.start()
        loads.append(cp)
    do_barrier(barrier, peers)

    def zcopy(t, d, step, src, dst):
        target = lax.rem(g + (1 if d == 0 else groups - 1), groups)
        return remote(src, dst, zs.at[t, d, step], zr.at[t, d, step], rep, target)

    def has_next(d):
        return g < groups - 1 if d == 0 else g > 0

    def own_send(t):
        for d in range(2):
            @pl.when(has_next(d))
            def _():
                if t == 4:
                    zcopy(t, d, 0, fr_ref, fa.at[pl.ds(mo(g * tokens, 16), tokens), :]).start()
                else:
                    m = MATS[t]
                    src = blocks[t].at[pl.ds(mo(k * m.quarter, 16), m.quarter), pl.ds(mo(h * m.half, LANE), m.half)]
                    zcopy(t, d, 0, src, part(full[t], m, g, k, h)).start()

    def rest(t):
        def body(i, c):
            relayout(MATS[t], lax.rem(k + i, 4), pbuf, fbuf, blocks[t])
            return c
        lax.fori_loop(1, 4, body, 0)
        pltpu.make_async_copy(blocks[t], full[t].at[pl.ds(mo(g * MATS[t].block, 16), MATS[t].block), :], osem.at[t]).start()

    def row_of(d, step):
        return g - 1 - step if d == 0 else g + 1 + step

    def valid(d, step):
        return g - 1 - step >= 0 if d == 0 else g + 1 + step <= groups - 1

    slots = [(d, step) for step in range(groups - 1) for d in range(2)]

    def zregion(t, r):
        if t == 4:
            return fa.at[pl.ds(mo(r * tokens, 16), tokens), :]
        return part(full[t], MATS[t], r, k, h)

    def stage0(t, d, step):
        @pl.when(valid(d, step))
        def _():
            r = row_of(d, step)
            reg = zregion(t, r)
            zcopy(t, d, step, reg, reg).wait_recv()
            if step < groups - 2:
                @pl.when(has_next(d))
                def _():
                    zcopy(t, d, step + 1, reg, reg).start()
            if t < 4:
                i = d * (groups - 1) + step
                remote(reg, reg, xs.at[t, i], xr.at[t, i], flip(rep, 2), g).start()
                remote(reg, reg, ys.at[t, i], yr.at[t, i], flip(rep, 4), g).start()

    def stage1(t, d, step):
        @pl.when(valid(d, step))
        def _():
            r, i, m = row_of(d, step), d * (groups - 1) + step, MATS[t]
            reg = part(full[t], m, r, kx, h)
            remote(reg, reg, xs.at[t, i], xr.at[t, i], flip(rep, 2), g).wait_recv()
            a = part(full[t], m, r, kx, h, 0)
            remote(a, a, fas.at[t, i], far.at[t, i], flip(rep, 4), g).start()
            reg = part(full[t], m, r, ky, h)
            remote(reg, reg, ys.at[t, i], yr.at[t, i], flip(rep, 4), g).wait_recv()
            b = part(full[t], m, r, ky, h, 1)
            remote(b, b, fbs.at[t, i], fbr.at[t, i], flip(rep, 2), g).start()

    def stage2(t, d, step):
        @pl.when(valid(d, step))
        def _():
            r, i, m = row_of(d, step), d * (groups - 1) + step, MATS[t]
            a, b = part(full[t], m, r, kd, h, 0), part(full[t], m, r, kd, h, 1)
            remote(a, a, fas.at[t, i], far.at[t, i], flip(rep, 4), g).wait_recv()
            remote(b, b, fbs.at[t, i], fbr.at[t, i], flip(rep, 2), g).wait_recv()
            c = slab(full[t], m, r, h)
            remote(c, c, cs.at[t, i], cr.at[t, i], flip(rep, 1), g).start()

    def stage3(t, d, step):
        @pl.when(valid(d, step))
        def _():
            r, i, m = row_of(d, step), d * (groups - 1) + step, MATS[t]
            c = slab(full[t], m, r, 1 - h)
            remote(c, c, cs.at[t, i], cr.at[t, i], flip(rep, 1), g).wait_recv()

    loads[0].wait()
    relayout(QKV, k, pbuf, fbuf, sq)
    own_send(0)
    own_send(4)
    loads[1].wait()
    relayout(OUT, k, pbuf, fbuf, so)
    own_send(1)
    loads[2].wait()
    loads[3].wait()
    relayout(UP, k, pbuf, fbuf, su)
    own_send(2)
    relayout(DOWN, k, pbuf, fbuf, sd)
    own_send(3)
    row = 0
    for first, count in SMALL:
        smb[row:row + count, :] = pbuf[:, first * LANE:(first + count) * LANE].astype(F32).reshape(count, LANE)
        row += count
    smb[row:SROWS, :] = jnp.zeros((SROWS - row, LANE), F32)
    for i in range(1, groups):
        remote(smb, sm.at[g], ms.at[i - 1], mr.at[i - 1], rep, lax.rem(g + i, groups)).start()
    pltpu.make_async_copy(smb, sm.at[g], osem.at[4]).start()
    pltpu.make_async_copy(fr_ref, fa.at[pl.ds(mo(g * tokens, 16), tokens), :], osem.at[5]).start()

    items = [(t, d, step) for step in range(groups - 1) for t in (0, 4, 1, 2, 3) for d in range(2)]
    mats = [it for it in items if it[0] < 4]
    fillers = {1: 0, 3: 1, 5: 2, 7: 3}
    lag = 2
    n1 = n2 = n3 = 0
    count = 0
    for n, it in enumerate(items):
        stage0(*it)
        if it[0] < 4:
            count += 1
        if n in fillers:
            rest(fillers[n])
        while n1 < count - lag:
            stage1(*mats[n1])
            n1 += 1
        while n2 < n1 - lag:
            stage2(*mats[n2])
            n2 += 1
    while n1 < len(mats):
        stage1(*mats[n1])
        n1 += 1
        if n2 < n1 - lag:
            stage2(*mats[n2])
            n2 += 1
    while n2 < len(mats):
        stage2(*mats[n2])
        n2 += 1
    for it in mats:
        stage3(*it)
    for t in (0, 4, 1, 2, 3):
        reg = zregion(t, g)
        for d in range(2):
            @pl.when(has_next(d))
            def _():
                zcopy(t, d, 0, reg, reg).wait_send()
        for (d, step) in slots:
            i = d * (groups - 1) + step

            @pl.when(valid(d, step))
            def _():
                r = row_of(d, step)
                if step < groups - 2:
                    @pl.when(has_next(d))
                    def _():
                        zcopy(t, d, step + 1, reg, reg).wait_send()
                if t < 4:
                    m = MATS[t]
                    remote(reg, reg, xs.at[t, i], xr.at[t, i], flip(rep, 2), g).wait_send()
                    remote(reg, reg, ys.at[t, i], yr.at[t, i], flip(rep, 4), g).wait_send()
                    a, b = part(full[t], m, r, kx, h, 0), part(full[t], m, r, ky, h, 1)
                    remote(a, a, fas.at[t, i], far.at[t, i], flip(rep, 4), g).wait_send()
                    remote(b, b, fbs.at[t, i], fbr.at[t, i], flip(rep, 2), g).wait_send()
                    c = slab(full[t], m, r, h)
                    remote(c, c, cs.at[t, i], cr.at[t, i], flip(rep, 1), g).wait_send()
        if t < 4:
            pltpu.make_async_copy(blocks[t], full[t].at[pl.ds(mo(g * MATS[t].block, 16), MATS[t].block), :], osem.at[t]).wait()
    for i in range(1, groups):
        cp = remote(smb, sm.at[lax.rem(g + groups - i, groups)], ms.at[i - 1], mr.at[i - 1], rep, lax.rem(g + i, groups))
        cp.wait_send()
        cp.wait_recv()
    pltpu.make_async_copy(smb, sm.at[g], osem.at[4]).wait()
    pltpu.make_async_copy(fr_ref, fa.at[pl.ds(mo(g * tokens, 16), tokens), :], osem.at[5]).wait()


def gather(params, frames, groups):
    dma = pltpu.SemaphoreType.DMA
    n = 2 * (groups - 1)
    tokens = frames.shape[0]
    shapes = [jax.ShapeDtypeStruct((m.block * groups, m.cols), BF) for m in MATS]
    shapes += [jax.ShapeDtypeStruct((tokens * groups, D), BF), jax.ShapeDtypeStruct((groups, SROWS, LANE), F32)]
    return pl.pallas_call(
        functools.partial(gather_kernel, groups),
        out_shape=shapes,
        in_specs=[pl.BlockSpec(memory_space=pl.ANY), pl.BlockSpec(memory_space=pltpu.VMEM)],
        out_specs=[pl.BlockSpec(memory_space=pl.ANY)] * 6,
        scratch_shapes=[
            pltpu.VMEM((1, FLAT + 8 * LANE), BF),
            pltpu.VMEM((48 * 24 + 16, LANE), F32),
        ] + [pltpu.VMEM((m.block, m.cols), BF) for m in MATS] + [
            pltpu.VMEM((SROWS, LANE), F32),
            dma((4,)), dma((6,)), dma((5, 2, groups)), dma((5, 2, groups)),
            dma((4, n)), dma((4, n)), dma((4, n)), dma((4, n)), dma((4, n)), dma((4, n)), dma((4, n)), dma((4, n)),
            dma((4, n)), dma((4, n)), dma((groups,)), dma((groups,)),
        ],
        compiler_params=pltpu.CompilerParams(collective_id=0, has_side_effects=True, vmem_limit_bytes=40 << 20),
        name="gather",
    )(params, frames)


def add_rows(dst, a, b, rows, step=16):
    def body(i, c):
        at = pl.ds(mo(i * step, 16), step)
        dst[at, :] = (a[at, :].astype(F32) + b[at, :].astype(F32)).astype(dst.dtype)
        return c
    lax.fori_loop(0, rows // step, body, 0)


def cell(ref, m, r, kk, sub=None):
    r0, rn, c0, cn = m.sub[sub] if sub is not None else (0, m.quarter, 0, m.half)
    return ref.at[pl.ds(mo(r * m.block + kk * m.quarter + r0, 16), rn), pl.ds(c0, cn)]


EPS_NORM = 1e-05
ROOT_HALF = 0.7071067811865476
ROOT_TWO_PI = 0.3989422804014327
HEADS = D // HDIM
GAIN_ONE, SHIFT_ONE, QV_BIAS, OUT_BIAS, GAIN_TWO, SHIFT_TWO, UP_BIAS, DOWN_BIAS = (
    (0, 3), (3, 3), (6, 6), (12, 3), (15, 3), (18, 3), (23, 12), (37, 3))


def low_lanes():
    return lax.broadcasted_iota(jnp.int32, (1, LANE), 1) < 64


def assemble(sm, place, out):
    first, count = place
    halves = [(gi, first + i) for gi in range(sm.shape[0]) for i in range(count)]
    for t in range(len(halves) // 2):
        (g0, h0), (g1, h1) = halves[2 * t], halves[2 * t + 1]
        a = sm[g0, h0 // 2:h0 // 2 + 1, :]
        b = sm[g1, h1 // 2:h1 // 2 + 1, :]
        a = pltpu.roll(a, 64, 1) if h0 % 2 else a
        b = b if h1 % 2 else pltpu.roll(b, 64, 1)
        out[0:1, t * LANE:(t + 1) * LANE] = jnp.where(low_lanes(), a, b)


def fill_image(image, rows, vectors):
    where = {}
    for place, ref in vectors:
        for i in range(place[1]):
            where[place[0] + i] = (place[1], i, ref)
    for gi in range(image.shape[0]):
        for r in rows:
            parts = []
            for side in range(2):
                spot = where.get(2 * r + side)
                if spot is None:
                    parts.append(jnp.zeros((1, LANE), F32))
                    continue
                count, i, ref = spot
                q = gi * count + i
                v = ref[0:1, q // 2 * LANE:(q // 2 + 1) * LANE]
                parts.append(v if q % 2 == side else pltpu.roll(v, 64, 1))
            image[gi, r:r + 1, :] = jnp.where(low_lanes(), parts[0], parts[1])


def mean(v):
    return jnp.sum(v, axis=-1, keepdims=True) * (1.0 / D)


def normalize(v):
    centered = v - mean(v)
    inverse = lax.rsqrt(mean(centered * centered) + EPS_NORM)
    return centered * inverse, inverse


def norm_back(upstream, normal, inverse, gain):
    s = upstream * gain
    return inverse * (s - mean(s) - normal * mean(s * normal))


def nn(a, b):
    return lax.dot_general(a, b, (((1,), (0,)), ((), ())), preferred_element_type=F32)


def nt(a, b):
    return lax.dot_general(a, b, (((1,), (1,)), ((), ())), preferred_element_type=F32)


def loop(count, body):
    def step(i, c):
        body(i)
        return c
    lax.fori_loop(0, count, step, 0)


def head_mask(rows):
    return lax.broadcasted_iota(jnp.int32, (rows, LANE), 1) < HDIM


def project_block(j, fa, gain, shift, bias, wq, q_all, k_all, v_all, normed, tokens):
    at = pl.ds(mo(j * tokens, 16), tokens)
    normal, _ = normalize(fa[at, :].astype(F32))
    normed[...] = (normal * gain[...] + shift[...]).astype(BF)
    for third, out in enumerate((q_all, k_all, v_all)):
        def body(n):
            col = pl.ds(mo(n * 256, 256), 256)
            wide = nn(normed[...], wq[:, pl.ds(mo(third * D + n * 256, 256), 256)])
            if third != 1:
                wide = wide + bias[0:1, pl.ds(mo((third // 2) * D + n * 256, 256), 256)]
            out[at, col] = wide.astype(BF)
        loop(D // 256, body)


def attend_pair(p, g, q_all, k_all, v_all, attended, stats, tokens):
    col = pl.ds(mo(p * LANE, LANE), LANE)
    query = q_all[pl.ds(mo(g * tokens, 16), tokens), col] * jnp.asarray(HDIM**-0.5, BF)
    keys, values = k_all[:, col], v_all[:, col]
    mask = head_mask(tokens)
    zero = jnp.zeros_like(query)
    lanes = lax.broadcasted_iota(jnp.int32, (tokens, LANE), 1)
    results = []
    for side in range(2):
        scores = nt(jnp.where(mask, query, zero) if side == 0 else jnp.where(mask, zero, query), keys)
        highest = jnp.max(scores, axis=-1, keepdims=True)
        shares = jnp.exp(scores - highest)
        total = jnp.sum(shares, axis=-1, keepdims=True)
        results.append(nn(shares.astype(BF), values) * (1.0 / total))
        stats[...] = jnp.where(lanes == 2 * p + side, highest + jnp.log(total), stats[...])
    attended[:, col] = jnp.where(mask, results[0], results[1]).astype(BF)


def fwd_kernel(fa, wq, sm, q_all, k_all, v_all, attended, stats, normed, gain, shift, bias):
    g = lax.axis_index("grp")
    tokens = attended.shape[0]
    assemble(sm, GAIN_ONE, gain)
    assemble(sm, SHIFT_ONE, shift)
    assemble(sm, QV_BIAS, bias)
    loop(fa.shape[0] // tokens, lambda j: project_block(j, fa, gain, shift, bias, wq, q_all, k_all, v_all, normed, tokens))
    stats[...] = jnp.zeros_like(stats)
    loop(HEADS // 2, lambda p: attend_pair(p, g, q_all, k_all, v_all, attended, stats, tokens))


def forward(clip, wq, smalls, tokens):
    vmem = pl.BlockSpec(memory_space=pltpu.VMEM)
    wide = jax.ShapeDtypeStruct(clip.shape, BF)
    return pl.pallas_call(
        fwd_kernel,
        out_shape=[wide] * 3 + [jax.ShapeDtypeStruct((tokens, D), BF), jax.ShapeDtypeStruct((tokens, LANE), F32)],
        in_specs=[vmem] * 3, out_specs=[vmem] * 5,
        scratch_shapes=[pltpu.VMEM((tokens, D), BF), pltpu.VMEM((1, D), F32), pltpu.VMEM((1, D), F32), pltpu.VMEM((1, 2 * D), F32)],
        compiler_params=pltpu.CompilerParams(vmem_limit_bytes=40 << 20),
        name="forward",
    )(clip, wq, smalls)


def mid_kernel(attended, fr, ct, wo_h, wu_h, wd_h, sm, lse, out_frames, agrad, mgrad, stats, rows, go, gu, gd, image,
               wo, wu, wd, middle, normal, normed, act, pre, half, turned, wide, gain, shift, obias, ubias, dbias,
               v_gain, v_shift, v_out, v_up, v_down, sem):
    tokens = attended.shape[0]
    loads = [pltpu.make_async_copy(a, b, sem.at[i]) for i, (a, b) in enumerate(((wo_h, wo), (wu_h, wu), (wd_h, wd)))]
    for cp in loads:
        cp.start()
    assemble(sm, GAIN_TWO, gain)
    assemble(sm, SHIFT_TWO, shift)
    assemble(sm, OUT_BIAS, obias)
    assemble(sm, UP_BIAS, ubias)
    assemble(sm, DOWN_BIAS, dbias)
    loads[0].wait()

    def out_block(n):
        col = pl.ds(mo(n * 256, 256), 256)
        middle[:, col] = nn(attended[...], wo[:, col]) + obias[0:1, col] + fr[:, col].astype(F32)
    loop(D // 256, out_block)
    value, inverse = normalize(middle[...])
    normal[...] = value
    normed[...] = (value * gain[...] + shift[...]).astype(BF)
    loads[1].wait()
    loads[2].wait()

    def hidden_block(n):
        col = pl.ds(mo(n * 256, 256), 256)
        hidden = nn(normed[...], wu[:, col]) + ubias[0:1, col]
        bell = 0.5 * (1.0 + lax.erf(hidden * ROOT_HALF))
        act[:, col] = (hidden * bell).astype(BF)
        slope = bell + hidden * jnp.exp(-0.5 * hidden * hidden) * ROOT_TWO_PI
        grad = nt(ct[...], wd[pl.ds(mo(n * 256, 256), 256), :]) * slope
        v_up[0:1, col] = jnp.sum(grad, axis=0, keepdims=True)
        pre[:, col] = grad.astype(BF)
    loop(FF // 256, hidden_block)

    def down_block(n):
        col = pl.ds(mo(n * 256, 256), 256)
        out_frames[:, col] = (nn(act[...], wd[:, col]) + dbias[0:1, col] + middle[:, col]).astype(BF)
    loop(D // 256, down_block)

    def back_block(n):
        col = pl.ds(mo(n * 256, 256), 256)
        wide[:, col] = nt(pre[...], wu[pl.ds(mo(n * 256, 256), 256), :])
    loop(D // 256, back_block)
    upstream = wide[...]
    v_gain[...] = jnp.sum(upstream * normal[...], axis=0, keepdims=True)
    v_shift[...] = jnp.sum(upstream, axis=0, keepdims=True)
    total = ct[...].astype(F32) + norm_back(upstream, normal[...], inverse, gain[...])
    mgrad[...] = total
    half[...] = total.astype(BF)
    v_out[...] = jnp.sum(total, axis=0, keepdims=True)
    v_down[...] = jnp.sum(ct[...].astype(F32), axis=0, keepdims=True)

    def attended_block(n):
        col = pl.ds(mo(n * 256, 256), 256)
        agrad[:, col] = nt(half[...], wo[pl.ds(mo(n * 256, 256), 256), :]).astype(BF)
    loop(D // 256, attended_block)
    lanes = lax.broadcasted_iota(jnp.int32, (tokens, LANE), 1)
    mask = head_mask(tokens)
    both = lse[...]
    for p in range(HEADS // 2):
        product = agrad[:, p * LANE:(p + 1) * LANE].astype(F32) * attended[:, p * LANE:(p + 1) * LANE].astype(F32)
        for side in range(2):
            mine = jnp.where(mask if side == 0 else jnp.logical_not(mask), product, 0.0)
            both = jnp.where(lanes == HEADS + 2 * p + side, jnp.sum(mine, axis=-1, keepdims=True), both)
    stats[...] = both
    rows[...] = both.T[0:2 * HEADS, :]

    def weight(left, right, out):
        count = left.shape[1]
        turned[0:count, :] = left[...].T

        def block(i):
            def inner(n):
                r, c = pl.ds(mo(i * 256, 256), 256), pl.ds(mo(n * 256, 256), 256)
                out[r, c] = nn(turned[r, :], right[:, c]).astype(BF)
            loop(right.shape[1] // 256, inner)
        loop(count // 256, block)
    weight(act, ct, gd)
    weight(normed, pre, gu)
    weight(attended, half, go)
    fill_image(image, range(6, SROWS), ((OUT_BIAS, v_out), (GAIN_TWO, v_gain), (SHIFT_TWO, v_shift), (UP_BIAS, v_up), (DOWN_BIAS, v_down)))


def middle_step(attended, frames, cotangent, weights, smalls, lse):
    vmem, hbm = pl.BlockSpec(memory_space=pltpu.VMEM), pl.BlockSpec(memory_space=pl.ANY)
    tokens = frames.shape[0]
    groups = smalls.shape[0]
    sds = jax.ShapeDtypeStruct
    vec = [pltpu.VMEM((1, n), F32) for n in (D, D, D, FF, D)]
    return pl.pallas_call(
        mid_kernel,
        out_shape=[sds((tokens, D), BF), sds((tokens, D), BF), sds((tokens, D), F32), sds((tokens, LANE), F32),
                   sds((2 * HEADS, tokens), F32), sds((D, D), BF), sds((D, FF), BF), sds((FF, D), BF),
                   sds((groups, SROWS, LANE), F32)],
        in_specs=[vmem] * 3 + [hbm] * 3 + [vmem] * 2, out_specs=[vmem] * 9,
        scratch_shapes=[pltpu.VMEM((D, D), BF), pltpu.VMEM((D, FF), BF), pltpu.VMEM((FF, D), BF),
                        pltpu.VMEM((tokens, D), F32), pltpu.VMEM((tokens, D), F32), pltpu.VMEM((tokens, D), BF),
                        pltpu.VMEM((tokens, FF), BF), pltpu.VMEM((tokens, FF), BF), pltpu.VMEM((tokens, D), BF),
                        pltpu.VMEM((FF, tokens), BF), pltpu.VMEM((tokens, D), F32)] + vec + vec[:3] + [vec[3], vec[4]]
                       + [pltpu.SemaphoreType.DMA((3,))],
        compiler_params=pltpu.CompilerParams(vmem_limit_bytes=56 << 20),
        name="middle",
    )(attended, frames, cotangent, *weights, smalls, lse)


def query_back(p, g, q_all, k_all, v_all, a_all, stats, grad, tokens):
    col = pl.ds(mo(p * LANE, LANE), LANE)
    own = pl.ds(mo(g * tokens, 16), tokens)
    scale = jnp.asarray(HDIM**-0.5, BF)
    query, upstream = q_all[own, col] * scale, a_all[own, col]
    keys, values = k_all[:, col], v_all[:, col]
    mask = head_mask(tokens)
    zero = jnp.zeros_like(query)
    lanes = lax.broadcasted_iota(jnp.int32, (tokens, LANE), 1)
    results = []
    for side in range(2):
        def pick(v):
            return jnp.where(mask, v, zero) if side == 0 else jnp.where(mask, zero, v)
        total = jnp.sum(jnp.where(lanes == 2 * p + side, stats[...], 0.0), axis=-1, keepdims=True)
        centre = jnp.sum(jnp.where(lanes == HEADS + 2 * p + side, stats[...], 0.0), axis=-1, keepdims=True)
        shares = jnp.exp(nt(pick(query), keys) - total)
        back = (shares * (nt(pick(upstream), values) - centre)).astype(BF) * scale
        results.append(nn(back, keys))
    grad[:, col] = jnp.where(mask, results[0], results[1])


def key_back(p, g, q_all, k_all, v_all, a_all, rows, kgrad, vgrad, tokens):
    col = pl.ds(mo(p * LANE, LANE), LANE)
    own = pl.ds(mo(g * tokens, 16), tokens)
    scale = jnp.asarray(HDIM**-0.5, BF)
    keys, values = k_all[own, col] * scale, v_all[own, col]
    queries, upstream = q_all[:, col], a_all[:, col]
    mask = head_mask(tokens)
    zero = jnp.zeros_like(keys)
    ks, vs = [], []
    for side in range(2):
        def pick(v):
            return jnp.where(mask, v, zero) if side == 0 else jnp.where(mask, zero, v)
        total = rows[pl.ds(2 * p + side, 1), :]
        centre = rows[pl.ds(HEADS + 2 * p + side, 1), :]
        shares = jnp.exp(nt(pick(keys), queries) - total)
        vs.append(nn(shares.astype(BF), upstream))
        back = (shares * (nt(pick(values), upstream) - centre)).astype(BF) * scale
        ks.append(nn(back, queries))
    kgrad[:, col] = jnp.where(mask, ks[0], ks[1])
    vgrad[:, col] = jnp.where(mask, vs[0], vs[1])


def input_back(wq, fr, mgrad, gain, shift, qg, kg, vg, pgrad, normed, turned, wide, frames_grad, gq, v_gain, v_shift, v_qv):
    for i, ref in enumerate((qg, kg, vg)):
        pgrad[:, i * D:(i + 1) * D] = ref[...].astype(BF)
    v_qv[0:1, 0:D] = jnp.sum(qg[...], axis=0, keepdims=True)
    v_qv[0:1, D:2 * D] = jnp.sum(vg[...], axis=0, keepdims=True)

    def block(n):
        col = pl.ds(mo(n * 256, 256), 256)
        wide[:, col] = nt(pgrad[...], wq[pl.ds(mo(n * 256, 256), 256), :])
    loop(D // 256, block)
    normal, inverse = normalize(fr[...].astype(F32))
    normed[...] = (normal * gain[...] + shift[...]).astype(BF)
    upstream = wide[...]
    v_gain[...] = jnp.sum(upstream * normal, axis=0, keepdims=True)
    v_shift[...] = jnp.sum(upstream, axis=0, keepdims=True)
    frames_grad[...] = (mgrad[...] + norm_back(upstream, normal, inverse, gain[...])).astype(BF)
    turned[...] = normed[...].T

    def outer(i):
        def inner(n):
            r, c = pl.ds(mo(i * 256, 256), 256), pl.ds(mo(n * 256, 256), 256)
            gq[r, c] = nn(turned[r, :], pgrad[:, c]).astype(BF)
        loop(3 * D // 256, inner)
    loop(D // 256, outer)


ORDER = (3, 2, 1, 0)


def finish_kernel(groups, highs, go, gu, gd, q_all, k_all, v_all, agrad, rows_own, stats, wq, fr, mgrad, sm, image_in,
                  oq, oo, ou, od, osm, frames_grad, *scratch):
    (a_all, rows3, rows, gq, gain, shift, qg, kg, vg, pgrad, normed, turned, wide, v_gain, v_shift, v_qv, sm_ref,
     ksem, szs, szr, rs, rr), scratch = scratch[:22], scratch[22:]
    own, scratch = scratch[:4], scratch[4:]
    buf1, scratch = scratch[:4], scratch[4:]
    buf2, scratch = scratch[:4], scratch[4:]
    buf3, scratch = scratch[:4], scratch[4:]
    zbuf, scratch = scratch[:4], scratch[4:]
    fin, scratch = scratch[:4], scratch[4:]
    (smacc, smin, lsem, c1s, c1r, a1s, a1r, b1s, b1r, a2s, a2r, b2s, b2r, zs, zr, fxs, fxr, os, xs, xr, ys, yr,
     fas, far, fbs, fbr, cs, cr, sms, smr) = scratch
    rep, g = lax.axis_index("rep"), lax.axis_index("grp")
    s = lax.rem(rep, 8)
    h = lax.rem(s, 2)
    k = s // 2
    x, y = lax.rem(k, 2), k // 2
    kx, ky, kd = flip(k, 1), flip(k, 2), 3 - k
    core, xn, yn = flip(rep, 1), flip(rep, 2), flip(rep, 4)
    grads = (gq, go, gu, gd)
    outs = (oq, oo, ou, od)
    tokens = fr.shape[0]
    barrier, peers = greet(rep, g, groups)
    peers += [(flip(rep, 8 << b), g) for b in range(highs)]
    do_barrier(barrier, peers)

    def place(r):
        return a_all.at[pl.ds(mo(r * tokens, 16), tokens), :]

    def acopy_z(d, step, src, dst):
        target = lax.rem(g + (1 if d == 0 else groups - 1), groups)
        return remote(src, dst, szs.at[d, step], szr.at[d, step], rep, target)

    def has_next(d):
        return g < groups - 1 if d == 0 else g > 0

    def share_start():
        for d in range(2):
            @pl.when(has_next(d))
            def _():
                acopy_z(d, 0, agrad, place(g)).start()
        pltpu.make_async_copy(agrad, place(g), ksem.at[0]).start()
        for i in range(1, groups):
            remote(rows_own, rows3.at[g], rs.at[i - 1], rr.at[i - 1], rep, lax.rem(g + i, groups)).start()
        rows3[g] = rows_own[...]
        pltpu.make_async_copy(agrad, place(g), ksem.at[0]).wait()

    def share_step(step):
        for d in range(2):
            r = g - 1 - step if d == 0 else g + 1 + step

            @pl.when(r >= 0 if d == 0 else r <= groups - 1)
            def _():
                acopy_z(d, step, place(r), place(r)).wait_recv()
                if step < groups - 2:
                    @pl.when(has_next(d))
                    def _():
                        acopy_z(d, step + 1, place(r), place(r)).start()

    def share_rows():
        for i in range(1, groups):
            remote(rows_own, rows3.at[lax.rem(g + groups - i, groups)], rs.at[i - 1], rr.at[i - 1], rep,
                   lax.rem(g + i, groups)).wait_recv()
        for i in range(groups):
            rows[:, i * tokens:(i + 1) * tokens] = rows3[i]

    def share_sent():
        for step in range(groups - 1):
            for d in range(2):
                r = g - step if d == 0 else g + step

                @pl.when(jnp.logical_and(r >= 0 if d == 0 else r <= groups - 1, has_next(d)))
                def _():
                    acopy_z(d, step, place(g), place(g)).wait_send()
        for i in range(1, groups):
            remote(rows_own, rows3.at[g], rs.at[i - 1], rr.at[i - 1], rep, lax.rem(g + i, groups)).wait_send()

    def row(i):
        return lax.rem(g + 1 + i, groups)

    def load(t, i):
        m = MATS[t]
        at = pl.ds(mo(row(i) * m.block, 16), m.block)
        return pltpu.make_async_copy(grads[t].at[at, pl.ds(mo(h * m.half, LANE), m.half)], own[t].at[at, :], lsem.at[t, i])

    def first(t, i):
        m = MATS[t]
        at = pl.ds(mo(row(i) * m.block, 16), m.block)
        return remote(grads[t].at[at, pl.ds(mo((1 - h) * m.half, LANE), m.half)], buf1[t].at[at, :],
                      c1s.at[t, i], c1r.at[t, i], core, g)

    def acopy(t, i, j, kk):
        return remote(cell(buf1[t], MATS[t], row(i), kk, 0), cell(buf2[t], MATS[t], row(i), kk, 0),
                      a1s.at[t, i, j], a1r.at[t, i, j], xn, g)

    def bcopy(t, i, j, kk):
        return remote(cell(buf1[t], MATS[t], row(i), kk, 1), cell(buf2[t], MATS[t], row(i), kk, 1),
                      b1s.at[t, i, j], b1r.at[t, i, j], yn, g)

    def a2copy(t, i, kk):
        return remote(cell(buf2[t], MATS[t], row(i), kk, 0), cell(buf3[t], MATS[t], row(i), kk, 0),
                      a2s.at[t, i], a2r.at[t, i], yn, g)

    def b2copy(t, i, kk):
        return remote(cell(buf2[t], MATS[t], row(i), kk, 1), cell(buf3[t], MATS[t], row(i), kk, 1),
                      b2s.at[t, i], b2r.at[t, i], xn, g)

    def zcopy(t, i):
        return remote(cell(buf3[t], MATS[t], row(i), k), zbuf[t].at[i], zs.at[t, i], zr.at[t, i], rep, row(i))

    def r1(t, i):
        m = MATS[t]
        first(t, i).wait_recv()
        at = pl.ds(mo(row(i) * m.block, 16), m.block)
        if t:
            load(t, i).wait()
            mine = own[t].at[at, :]
        else:
            mine = gq.at[at, pl.ds(mo(h * m.half, LANE), m.half)]
        add_rows(buf1[t].at[at, :], mine, buf1[t].at[at, :], m.block)
        for j in range(2):
            acopy(t, i, j, 2 * j + (1 - x)).start()
            bcopy(t, i, j, 2 * (1 - y) + j).start()

    def r2(t, i):
        m = MATS[t]
        for j in range(2):
            acopy(t, i, j, 2 * j + x).wait_recv()
            kk = 2 * j + x
            add_rows(cell(buf2[t], m, row(i), kk, 0), cell(buf1[t], m, row(i), kk, 0), cell(buf2[t], m, row(i), kk, 0), m.sub[0][1])
        a2copy(t, i, 2 * (1 - y) + x).start()
        for j in range(2):
            bcopy(t, i, j, 2 * y + j).wait_recv()
            kk = 2 * y + j
            add_rows(cell(buf2[t], m, row(i), kk, 1), cell(buf1[t], m, row(i), kk, 1), cell(buf2[t], m, row(i), kk, 1), m.sub[1][1])
        b2copy(t, i, 2 * y + (1 - x)).start()

    def r3(t, i):
        m = MATS[t]
        a2copy(t, i, k).wait_recv()
        b2copy(t, i, k).wait_recv()
        whole = (cell(buf3[t], m, row(i), k), cell(buf2[t], m, row(i), k))
        add_rows(whole[0], whole[1], whole[0], m.quarter)
        if i < groups - 1:
            zcopy(t, i).start()

    def fpart(t, kk, hh, sub=None):
        return part(outs[t], MATS[t], 0, kk, hh, sub)

    def fslab(t, hh):
        return slab(outs[t], MATS[t], 0, hh)

    def keep(t):
        return pltpu.make_async_copy(fin[t].at[highs], fpart(t, k, h), os.at[t])

    def xsend(t):
        return remote(fin[t].at[highs], fpart(t, k, h), xs.at[t], xr.at[t], xn, g)

    def ysend(t):
        return remote(fin[t].at[highs], fpart(t, k, h), ys.at[t], yr.at[t], yn, g)

    def xgot(t):
        return remote(fpart(t, kx, h), fpart(t, kx, h), xs.at[t], xr.at[t], xn, g)

    def ygot(t):
        return remote(fpart(t, ky, h), fpart(t, ky, h), ys.at[t], yr.at[t], yn, g)

    def fwd(t, sub, kk):
        reg = fpart(t, kk, h, sub)
        return remote(reg, reg, (fas, fbs)[sub].at[t], (far, fbr)[sub].at[t], (yn, xn)[sub], g)

    def cross(t, hh):
        return remote(fslab(t, hh), fslab(t, hh), cs.at[t], cr.at[t], core, g)

    def r4(t):
        m = MATS[t]
        for i in range(groups - 1):
            zcopy(t, i).wait_recv()
        mine = cell(buf3[t], m, g, k)

        def body(n, c):
            at = pl.ds(mo(n * 16, 16), 16)
            total = mine[at, :].astype(F32)
            for i in range(groups - 1):
                total = total + zbuf[t][i, at, :].astype(F32)
            fin[t][0, at, :] = total.astype(BF)
            return c
        lax.fori_loop(0, m.quarter // 16, body, 0)
        for b in range(highs):
            cp = remote(fin[t].at[b], fin[t].at[highs + 1 + b], fxs.at[t, b], fxr.at[t, b], flip(rep, 8 << b), g)
            cp.start()
            cp.wait()
            add_rows(fin[t].at[b + 1], fin[t].at[b], fin[t].at[highs + 1 + b], m.quarter)
        keep(t).start()
        xsend(t).start()
        ysend(t).start()

    def r5(t):
        xgot(t).wait_recv()
        fwd(t, 0, kx).start()
        ygot(t).wait_recv()
        fwd(t, 1, ky).start()

    def r6(t):
        fwd(t, 0, kd).wait_recv()
        fwd(t, 1, kd).wait_recv()
        keep(t).wait()
        cross(t, h).start()

    def r7(t):
        cross(t, 1 - h).wait_recv()

    partners = [(core, g), (xn, g), (yn, g)] + [(flip(rep, 8 << b), g) for b in range(highs)]
    bit = 1
    while bit < groups:
        partners.append((rep, flip(g, bit)))
        bit *= 2

    def smcopy(j):
        return remote(smacc.at[j], smin.at[j], sms.at[j], smr.at[j], *partners[j])

    def small(j):
        if j:
            smcopy(j - 1).wait_recv()
            smacc[j] = smacc[j - 1] + smin[j - 1]
        else:
            smacc[0] = sm_ref[...]
        if j < len(partners):
            smcopy(j).start()
        else:
            osm[...] = smacc[j, g]

    chunks = [(t, i) for t in ORDER for i in range(groups)]
    share_start()
    for t, i in chunks:
        if t:
            first(t, i).start()
            load(t, i).start()
    assemble(sm, GAIN_ONE, gain)
    assemble(sm, SHIFT_ONE, shift)

    def queries(p):
        loop(2, lambda i: query_back(p + i, g, q_all, k_all, v_all, a_all, stats, qg, tokens))

    def keys(p):
        loop(2, lambda i: key_back(p + i, g, q_all, k_all, v_all, a_all, rows, kg, vg, tokens))

    def inputs():
        input_back(wq, fr, mgrad, gain, shift, qg, kg, vg, pgrad, normed, turned, wide, frames_grad, gq, v_gain, v_shift, v_qv)
        sm_ref[...] = image_in[...]
        fill_image(sm_ref, range(6), ((GAIN_ONE, v_gain), (SHIFT_ONE, v_shift), (QV_BIAS, v_qv)))
        for i in range(groups):
            first(0, i).start()
        small(0)

    work = {0: [lambda: queries(0)], 1: [lambda: queries(2), lambda: share_step(0)],
            2: [lambda: queries(4)], 3: [lambda: share_step(1)], 5: [lambda: share_step(2), share_rows, lambda: keys(0)],
            6: [lambda: keys(2)], 7: [lambda: keys(4)], 8: [inputs]}
    total = len(chunks)
    smalls = 1
    for n in range(total + 16):
        if n < total:
            r1(*chunks[n])
        if 0 <= n - 2 < total:
            r2(*chunks[n - 2])
        if n > 9 and smalls <= len(partners):
            small(smalls)
            smalls += 1
        if 0 <= n - 4 < total:
            r3(*chunks[n - 4])
        for q, t in enumerate(ORDER):
            last = groups * q + groups - 1 + 4
            if n == last + 2:
                r4(t)
            if n == last + 4:
                r5(t)
            if n == last + 6:
                r6(t)
        for piece in work.get(n, ()):
            piece()
    share_sent()
    for t in ORDER:
        r7(t)
    for t, i in chunks:
        first(t, i).wait_send()
        for j in range(2):
            acopy(t, i, j, 2 * j + x).wait_send()
            bcopy(t, i, j, 2 * y + j).wait_send()
        a2copy(t, i, k).wait_send()
        b2copy(t, i, k).wait_send()
        if i < groups - 1:
            zcopy(t, i).wait_send()
    for t in ORDER:
        xsend(t).wait_send()
        ysend(t).wait_send()
        fwd(t, 0, kx).wait_send()
        fwd(t, 1, ky).wait_send()
        cross(t, h).wait_send()
    for j in range(len(partners)):
        smcopy(j).wait_send()


def finish(grads, q_all, k_all, v_all, agrad, rows, stats, wq, frames, mgrad, smalls, image, reps):
    dma = pltpu.SemaphoreType.DMA
    groups = smalls.shape[0]
    tokens = frames.shape[0]
    clip = q_all.shape[0]
    highs = (reps // 8).bit_length() - 1
    steps = 3 + highs + groups.bit_length() - 1
    vmem, hbm = pl.BlockSpec(memory_space=pltpu.VMEM), pl.BlockSpec(memory_space=pl.ANY)
    wide = [pltpu.VMEM((m.block * groups, m.half), BF) for m in MATS]
    scratch = [pltpu.VMEM((clip, D), BF), pltpu.VMEM((groups, 2 * HEADS, tokens), F32), pltpu.VMEM((2 * HEADS, clip), F32),
               pltpu.VMEM((D, 3 * D), BF), pltpu.VMEM((1, D), F32), pltpu.VMEM((1, D), F32)]
    scratch += [pltpu.VMEM((tokens, D), F32)] * 3
    scratch += [pltpu.VMEM((tokens, 3 * D), BF), pltpu.VMEM((tokens, D), BF), pltpu.VMEM((D, tokens), BF),
                pltpu.VMEM((tokens, D), F32), pltpu.VMEM((1, D), F32), pltpu.VMEM((1, D), F32), pltpu.VMEM((1, 2 * D), F32),
                pltpu.VMEM(image.shape, F32), dma((1,)), dma((2, groups)), dma((2, groups)), dma((groups,)), dma((groups,))]
    scratch += [pltpu.VMEM((16, LANE), BF)] + wide[1:]
    scratch += wide * 3
    scratch += [pltpu.VMEM((groups, m.quarter, m.half), BF) for m in MATS]
    scratch += [pltpu.VMEM((2 * highs + 1, m.quarter, m.half), BF) for m in MATS]
    scratch += [pltpu.VMEM((steps + 1, groups, SROWS, LANE), F32), pltpu.VMEM((steps, groups, SROWS, LANE), F32)]
    scratch += [dma((4, groups))] * 3 + [dma((4, groups, 2))] * 4 + [dma((4, groups))] * 6
    scratch += [dma((4, max(highs, 1)))] * 2 + [dma((4,))] * 11 + [dma((steps,))] * 2
    return pl.pallas_call(
        functools.partial(finish_kernel, groups, highs),
        out_shape=[jax.ShapeDtypeStruct((m.block, m.cols), BF) for m in MATS]
        + [jax.ShapeDtypeStruct((SROWS, LANE), F32), jax.ShapeDtypeStruct((tokens, D), BF)],
        in_specs=[hbm] * 3 + [vmem] * 11,
        out_specs=[hbm] * 4 + [vmem] * 2,
        scratch_shapes=scratch,
        compiler_params=pltpu.CompilerParams(collective_id=1, has_side_effects=True, vmem_limit_bytes=62 << 20),
        name="finish",
    )(*grads, q_all, k_all, v_all, agrad, rows, stats, wq, frames, mgrad, smalls, image)


BETA_ONE = 0.9
BETA_TWO = 0.98
ADAM_EPS = 1e-06
LEARN_RATE = 0.006
DECAY = 0.01
ADAM_STEP = 4
ROWS = 1736
STEPS = -(-FROWS // ROWS)


def flatten(m, block, flat, late):
    def body(i, carry):
        base = m.row0 + i * (48 * m.tiles)
        for c in range(m.tiles):
            tile = block[pl.ds(mo(i * 48, 16), 48), c * LANE:(c + 1) * LANE].astype(F32)
            if m.shifted:
                tile = pltpu.roll(tile, 64, 1)
                late[pl.ds(base + c + 1, 48, stride=m.tiles), :] = tile
            flat[pl.ds(base + c, 48, stride=m.tiles), :] = tile
        return carry
    lax.fori_loop(0, m.block // 48, body, 0)


def adam_kernel(scale, gq, go, gu, gd, sm, p_ref, m_ref, v_ref, o_g, o_p, o_m, o_v, flat, late):
    step = pl.program_id(0)

    @pl.when(step == 0)
    def _():
        flatten(QKV, gq, flat, late)
        flatten(OUT, go, flat, late)
        flatten(UP, gu, flat, late)
        flatten(DOWN, gd, flat, late)
        flat[0:3, :] = sm[0:3, :]
        flat[3459:3462, :] = sm[3:6, :]
        flat[4614:4618, :] = sm[6:10, :]
        flat[4618:4619, 0:64] = sm[10:11, 0:64]
        flat[9226:9227, 64:128] = sm[11:12, 64:128]
        flat[9227:9232, :] = sm[12:17, :]
        flat[9232:9233, 0:64] = sm[17:18, 0:64]
        flat[13840:13841, 64:128] = sm[18:19, 64:128]
        flat[13841:13842, :] = sm[19:20, :]
        late[9227:9232, :] = sm[12:17, :]
        late[9232:9233, 0:64] = sm[17:18, 0:64]
        late[13841:13842, :] = sm[19:20, :]

    at = pl.ds(mo(step * ROWS, 8), ROWS)
    number = step * ROWS + lax.broadcasted_iota(jnp.int32, (ROWS, LANE), 0)
    low = lax.broadcasted_iota(jnp.int32, (ROWS, LANE), 1) < 64
    grad = jnp.where(jnp.logical_and(number > UP.row0, low), late[at, :], flat[at, :]).reshape(1, ROWS * LANE) * scale
    first = BETA_ONE * m_ref[...] + (1.0 - BETA_ONE) * grad
    second = BETA_TWO * v_ref[...] + (1.0 - BETA_TWO) * grad * grad
    o_g[...] = grad
    o_m[...] = first
    o_v[...] = second
    first_hat = first * (1.0 / (1.0 - BETA_ONE**ADAM_STEP))
    second_hat = second * (1.0 / (1.0 - BETA_TWO**ADAM_STEP))
    current = p_ref[...].astype(F32)
    o_p[...] = current - LEARN_RATE * (first_hat / (jnp.sqrt(second_hat) + ADAM_EPS) + DECAY * current)


def adam(blocks, smalls, params, first, second, reps):
    spec = pl.BlockSpec((1, ROWS * LANE), lambda i: (0, i))
    vmem = pl.BlockSpec(memory_space=pltpu.VMEM)
    return pl.pallas_call(
        functools.partial(adam_kernel, 1.0 / reps),
        grid=(STEPS,),
        out_shape=[jax.ShapeDtypeStruct((1, FLAT), F32)] * 4,
        in_specs=[vmem] * 5 + [spec] * 3,
        out_specs=[spec] * 4,
        scratch_shapes=[pltpu.VMEM((STEPS * ROWS, LANE), F32)] * 2,
        compiler_params=pltpu.CompilerParams(vmem_limit_bytes=50 << 20),
        name="adam",
    )(*blocks, smalls, params, first, second)


def on_device(frames, cotangent, params, first_moment, second_moment):
    groups, reps = lax.axis_size("grp"), lax.axis_size("rep")
    wq, wo, wu, wd, clip, smalls = gather(params, frames, groups)
    q_all, k_all, v_all, attended, lse = forward(clip, wq, smalls, frames.shape[0])
    out_frames, agrad, mgrad, stats, rows, go, gu, gd, image = middle_step(
        attended, frames, cotangent, (wo, wu, wd), smalls, lse)
    *blocks, small, frames_grad = finish(
        (go, gu, gd), q_all, k_all, v_all, agrad, rows, stats, wq, frames, mgrad, smalls, image, reps)
    param_grad, new_params, new_first, new_second = adam(blocks, small, params, first_moment, second_moment, reps)
    return (out_frames, frames_grad, param_grad, new_params, new_first, new_second)


def solution(mesh):
    in_specs = (
        P(("rep", "grp"), None),
        P(("rep", "grp"), None),
        P("grp", None),
        P("grp", None),
        P("grp", None),
    )
    out_specs = (
        P(("rep", "grp"), None),
        P(("rep", "grp"), None),
        P("grp", None),
        P("grp", None),
        P("grp", None),
        P("grp", None),
    )
    return jax.shard_map(
        on_device, mesh=mesh, in_specs=in_specs, out_specs=out_specs, check_vma=False
    )
```

```python
import functools
import types

import jax
import jax.numpy as jnp
from jax import lax
from jax.sharding import PartitionSpec as P
from jax.experimental import pallas as pl
from jax.experimental.pallas import tpu as pltpu

MESH = pl.DeviceIdType.MESH
BF = jnp.bfloat16
F32 = jnp.float32
D = 768
FF = 3072
HDIM = 64
LANE = 128
FLAT = 1771776
FROWS = FLAT // LANE


class Mat:
    def __init__(self, offset, block, cols, suba, subb):
        self.offset, self.block, self.cols = offset, block, cols
        self.tiles = cols // LANE
        self.row0 = offset // LANE
        self.shifted = offset % LANE != 0
        self.quarter = block // 4
        self.half = cols // 2
        self.sub = (suba, subb)


QKV = Mat(384, 192, 2304, (0, 48, 0, 640), (0, 48, 640, 512))
OUT = Mat(443136, 192, 768, (0, 48, 0, 128), (0, 48, 128, 256))
UP = Mat(591168, 192, 3072, (0, 48, 0, 768), (0, 48, 768, 768))
DOWN = Mat(1181760, 768, 768, (0, 96, 0, 384), (96, 96, 0, 384))
MATS = (QKV, OUT, UP, DOWN)
SMALL = ((0, 3), (3459, 3), (4614, 5), (9226, 7), (13840, 2))
SROWS = 24


def flip(index, bit):
    return index + bit - 2 * bit * ((index // bit) % 2)


def mo(value, by):
    return pl.multiple_of(value, by)


def part(ref, m, r, k, h, sub=None):
    r0, rn, c0, cn = m.sub[sub] if sub is not None else (0, m.quarter, 0, m.half)
    row = mo(r * m.block + k * m.quarter + r0, 16)
    col = mo(h * m.half + c0, LANE)
    return ref.at[pl.ds(row, rn), pl.ds(col, cn)]


def slab(ref, m, r, h):
    return ref.at[pl.ds(mo(r * m.block, 16), m.block), pl.ds(mo(h * m.half, LANE), m.half)]


def remote(src, dst, send, recv, rep, grp):
    return pltpu.make_async_remote_copy(
        src_ref=src, dst_ref=dst, send_sem=send, recv_sem=recv,
        device_id={"rep": rep, "grp": grp}, device_id_type=MESH)


def greet(rep, g, groups):
    barrier = pltpu.get_barrier_semaphore()
    peers = [(flip(rep, b), g) for b in (1, 2, 4)]
    peers += [(rep, lax.rem(g + i, groups)) for i in range(1, groups)]
    return barrier, peers


def do_barrier(barrier, peers):
    for r, gg in peers:
        pl.semaphore_signal(barrier, inc=1, device_id={"rep": r, "grp": gg}, device_id_type=MESH)
    pl.semaphore_wait(barrier, len(peers))


def add_rows(dst, a, b, rows, step=16):
    def body(i, c):
        at = pl.ds(mo(i * step, 16), step)
        dst[at, :] = (a[at, :].astype(F32) + b[at, :].astype(F32)).astype(dst.dtype)
        return c
    lax.fori_loop(0, rows // step, body, 0)


EPS_NORM = 1e-05
ROOT_HALF = 0.7071067811865476
ROOT_TWO_PI = 0.3989422804014327
HEADS = D // HDIM
GAIN_ONE, SHIFT_ONE, QV_BIAS, OUT_BIAS, GAIN_TWO, SHIFT_TWO, UP_BIAS, DOWN_BIAS = (
    (0, 3), (3, 3), (6, 6), (12, 3), (15, 3), (18, 3), (23, 12), (37, 3))


def low_lanes():
    return lax.broadcasted_iota(jnp.int32, (1, LANE), 1) < 64


def assemble(sm, place, out):
    first, count = place
    halves = [(gi, first + i) for gi in range(sm.shape[0]) for i in range(count)]
    for t in range(len(halves) // 2):
        (g0, h0), (g1, h1) = halves[2 * t], halves[2 * t + 1]
        a = sm[g0, h0 // 2:h0 // 2 + 1, :]
        b = sm[g1, h1 // 2:h1 // 2 + 1, :]
        a = pltpu.roll(a, 64, 1) if h0 % 2 else a
        b = b if h1 % 2 else pltpu.roll(b, 64, 1)
        out[0:1, t * LANE:(t + 1) * LANE] = jnp.where(low_lanes(), a, b)


def fill_image(image, rows, vectors):
    where = {}
    for place, ref in vectors:
        for i in range(place[1]):
            where[place[0] + i] = (place[1], i, ref)
    for gi in range(image.shape[0]):
        for r in rows:
            parts = []
            for side in range(2):
                spot = where.get(2 * r + side)
                if spot is None:
                    parts.append(jnp.zeros((1, LANE), F32))
                    continue
                count, i, ref = spot
                q = gi * count + i
                v = ref[0:1, q // 2 * LANE:(q // 2 + 1) * LANE]
                parts.append(v if q % 2 == side else pltpu.roll(v, 64, 1))
            image[gi, r:r + 1, :] = jnp.where(low_lanes(), parts[0], parts[1])


def mean(v):
    return jnp.sum(v, axis=-1, keepdims=True) * (1.0 / D)


def normalize(v):
    centered = v - mean(v)
    inverse = lax.rsqrt(mean(centered * centered) + EPS_NORM)
    return centered * inverse, inverse


def norm_back(upstream, normal, inverse, gain):
    s = upstream * gain
    return inverse * (s - mean(s) - normal * mean(s * normal))


def nn(a, b):
    return lax.dot_general(a, b, (((1,), (0,)), ((), ())), preferred_element_type=F32)


def nt(a, b):
    return lax.dot_general(a, b, (((1,), (1,)), ((), ())), preferred_element_type=F32)


def loop(count, body):
    def step(i, c):
        body(i)
        return c
    lax.fori_loop(0, count, step, 0)


def head_mask(rows):
    return lax.broadcasted_iota(jnp.int32, (rows, LANE), 1) < HDIM


def project_block(j, fa, gain, shift, bias, wq, q_all, k_all, v_all, normed, tokens):
    at = pl.ds(mo(j * tokens, 16), tokens)
    normal, _ = normalize(fa[at, :].astype(F32))
    normed[...] = (normal * gain[...] + shift[...]).astype(BF)
    for third, out in enumerate((q_all, k_all, v_all)):
        def body(n):
            col = pl.ds(mo(n * 256, 256), 256)
            wide = nn(normed[...], wq[:, pl.ds(mo(third * D + n * 256, 256), 256)])
            if third != 1:
                wide = wide + bias[0:1, pl.ds(mo((third // 2) * D + n * 256, 256), 256)]
            out[at, col] = wide.astype(BF)
        loop(D // 256, body)


def attend_pair(p, g, q_all, k_all, v_all, attended, stats, tokens):
    col = pl.ds(mo(p * LANE, LANE), LANE)
    query = q_all[pl.ds(mo(g * tokens, 16), tokens), col] * jnp.asarray(HDIM**-0.5, BF)
    keys, values = k_all[:, col], v_all[:, col]
    mask = head_mask(tokens)
    zero = jnp.zeros_like(query)
    lanes = lax.broadcasted_iota(jnp.int32, (tokens, LANE), 1)
    results = []
    for side in range(2):
        scores = nt(jnp.where(mask, query, zero) if side == 0 else jnp.where(mask, zero, query), keys)
        highest = jnp.max(scores, axis=-1, keepdims=True)
        shares = jnp.exp(scores - highest)
        total = jnp.sum(shares, axis=-1, keepdims=True)
        results.append(nn(shares.astype(BF), values) * (1.0 / total))
        stats[...] = jnp.where(lanes == 2 * p + side, highest + jnp.log(total), stats[...])
    attended[:, col] = jnp.where(mask, results[0], results[1]).astype(BF)


def query_back(p, g, q_all, k_all, v_all, a_all, stats, pgrad, v_qv, tokens):
    col = pl.ds(mo(p * LANE, LANE), LANE)
    own = pl.ds(mo(g * tokens, 16), tokens)
    scale = jnp.asarray(HDIM**-0.5, BF)
    query, upstream = q_all[own, col] * scale, a_all[own, col]
    keys, values = k_all[:, col], v_all[:, col]
    mask = head_mask(tokens)
    zero = jnp.zeros_like(query)
    lanes = lax.broadcasted_iota(jnp.int32, (tokens, LANE), 1)
    results = []
    for side in range(2):
        def pick(v):
            return jnp.where(mask, v, zero) if side == 0 else jnp.where(mask, zero, v)
        total = jnp.sum(jnp.where(lanes == 2 * p + side, stats[...], 0.0), axis=-1, keepdims=True)
        centre = jnp.sum(jnp.where(lanes == HEADS + 2 * p + side, stats[...], 0.0), axis=-1, keepdims=True)
        shares = jnp.exp(nt(pick(query), keys) - total)
        back = (shares * (nt(pick(upstream), values) - centre)).astype(BF) * scale
        results.append(nn(back, keys))
    grad = jnp.where(mask, results[0], results[1])
    pgrad[:, col] = grad.astype(BF)
    v_qv[0:1, col] = jnp.sum(grad, axis=0, keepdims=True)


def key_back(p, g, q_all, k_all, v_all, a_all, rows, pgrad, v_qv, tokens):
    col = pl.ds(mo(p * LANE, LANE), LANE)
    own = pl.ds(mo(g * tokens, 16), tokens)
    scale = jnp.asarray(HDIM**-0.5, BF)
    keys, values = k_all[own, col] * scale, v_all[own, col]
    queries, upstream = q_all[:, col], a_all[:, col]
    mask = head_mask(tokens)
    zero = jnp.zeros_like(keys)
    ks, vs = [], []
    for side in range(2):
        def pick(v):
            return jnp.where(mask, v, zero) if side == 0 else jnp.where(mask, zero, v)
        total = rows[pl.ds(2 * p + side, 1), :]
        centre = rows[pl.ds(HEADS + 2 * p + side, 1), :]
        shares = jnp.exp(nt(pick(keys), queries) - total)
        vs.append(nn(shares.astype(BF), upstream))
        back = (shares * (nt(pick(values), upstream) - centre)).astype(BF) * scale
        ks.append(nn(back, queries))
    pgrad[:, pl.ds(mo(D + p * LANE, LANE), LANE)] = jnp.where(mask, ks[0], ks[1]).astype(BF)
    grad = jnp.where(mask, vs[0], vs[1])
    pgrad[:, pl.ds(mo(2 * D + p * LANE, LANE), LANE)] = grad.astype(BF)
    v_qv[0:1, pl.ds(mo(D + p * LANE, LANE), LANE)] = jnp.sum(grad, axis=0, keepdims=True)


def cell(ref, m, row, sub=None):
    r0, rn, c0, cn = m.sub[sub] if sub is not None else (0, m.quarter, 0, m.half)
    return ref.at[pl.ds(mo(row + r0, 16), rn), pl.ds(c0, cn)]


ORDER = (3, 2, 1, 0)


def layer_kernel(groups, highs, names, fr, ct, p_ref, oq, oo, ou, od, osm, out_frames, frames_grad, *scratch):
    s = types.SimpleNamespace(**dict(zip(names, scratch)))
    rep, g = lax.axis_index("rep"), lax.axis_index("grp")
    tokens = fr.shape[0]
    share_of = lax.rem(rep, 8)
    h = lax.rem(share_of, 2)
    k = share_of // 2
    x, y = lax.rem(k, 2), k // 2
    kx, ky, kd = flip(k, 1), flip(k, 2), 3 - k
    core, xn, yn = flip(rep, 1), flip(rep, 2), flip(rep, 4)
    full = (s.wq, s.wo, s.wu, s.wd)
    outs = (oq, oo, ou, od)
    grads = (s.wu, s.go, s.gu, s.gd)
    last = groups - 1

    def has_next(d):
        return g < last if d == 0 else g > 0

    def toward(d):
        return lax.rem(g + (1 if d == 0 else last), groups)

    def row_of(d, step):
        return g - 1 - step if d == 0 else g + 1 + step

    def valid(d, step):
        return row_of(d, step) >= 0 if d == 0 else row_of(d, step) <= last

    slots = [(d, step) for step in range(last) for d in range(2)]

    order = [(0, 0), (0, 1), (0, 2), (0, 3), (1, 0), (2, 0), (3, 0)] + [(t, i) for t in (1, 2, 3) for i in (1, 2, 3)]

    def piece_load(n):
        t, i = order[n]
        m = MATS[t]
        count = (m.quarter * m.tiles + (2 if m.shifted else 0)) * LANE
        start = mo((m.row0 + lax.rem(k + i, 4) * (m.quarter * m.tiles)) * LANE, LANE)
        return pltpu.make_async_copy(p_ref.at[:, pl.ds(start, count)], s.pbuf.at[n % 3, :, pl.ds(0, count)], s.lsem.at[n % 3])

    def relayout(n):
        t, i = order[n]
        m = MATS[t]
        piece_load(n).wait()
        count = m.quarter * m.tiles + (8 if m.shifted else 0)
        s.fbuf[0:count, :] = s.pbuf[n % 3, :, 0:count * LANE].astype(F32).reshape(count, LANE)
        if n + 3 < len(order):
            piece_load(n + 3).start()
        at = pl.ds(mo(g * m.block + lax.rem(k + i, 4) * m.quarter, 16), m.quarter)
        low = lax.broadcasted_iota(jnp.int32, (m.quarter, LANE), 1) < 64
        for c in range(m.tiles):
            a = s.fbuf[pl.ds(c, m.quarter, stride=m.tiles), :]
            if m.shifted:
                b = s.fbuf[pl.ds(c + 1, m.quarter, stride=m.tiles), :]
                a = pltpu.roll(jnp.where(low, b, a), 64, 1)
            full[t][at, c * LANE:(c + 1) * LANE] = a.astype(BF)

    def small_loads():
        at, result = 0, []
        for n, (first, count) in enumerate(SMALL):
            result.append(pltpu.make_async_copy(
                p_ref.at[:, pl.ds(first * LANE, count * LANE)], s.spbuf.at[:, pl.ds(at * LANE, count * LANE)], s.ssem.at[n]))
            at += count
        return result

    def zregion(t, r):
        if t == 4:
            return s.fa.at[pl.ds(mo(r * tokens, 16), tokens), :]
        return part(full[t], MATS[t], r, k, h)

    def zcopy(t, d, step, r):
        reg = zregion(t, r)
        return remote(reg, reg, s.zs.at[t, d, step], s.zr.at[t, d, step], rep, toward(d))

    def own_send(t):
        for d in range(2):
            @pl.when(has_next(d))
            def _():
                zcopy(t, d, 0, g).start()

    def xcopy(t, i, r, kk):
        reg = part(full[t], MATS[t], r, kk, h)
        return remote(reg, reg, s.xs.at[t, i], s.xr.at[t, i], xn, g)

    def ycopy(t, i, r, kk):
        reg = part(full[t], MATS[t], r, kk, h)
        return remote(reg, reg, s.ys.at[t, i], s.yr.at[t, i], yn, g)

    def acopy(t, i, r, kk):
        reg = part(full[t], MATS[t], r, kk, h, 0)
        return remote(reg, reg, s.fas.at[t, i], s.far.at[t, i], yn, g)

    def bcopy(t, i, r, kk):
        reg = part(full[t], MATS[t], r, kk, h, 1)
        return remote(reg, reg, s.fbs.at[t, i], s.fbr.at[t, i], xn, g)

    def ccopy(t, i, r, hh):
        reg = slab(full[t], MATS[t], r, hh)
        return remote(reg, reg, s.cs.at[t, i], s.cr.at[t, i], core, g)

    def stage(number, t, d, step):
        i = d * last + step

        @pl.when(valid(d, step))
        def _():
            r = row_of(d, step)
            if number == 0:
                zcopy(t, d, step, r).wait_recv()
                if step < last - 1:
                    @pl.when(has_next(d))
                    def _():
                        zcopy(t, d, step + 1, r).start()
                if t < 4:
                    xcopy(t, i, r, k).start()
                    ycopy(t, i, r, k).start()
            if number == 1:
                xcopy(t, i, r, kx).wait_recv()
                acopy(t, i, r, kx).start()
                ycopy(t, i, r, ky).wait_recv()
                bcopy(t, i, r, ky).start()
            if number == 2:
                acopy(t, i, r, kd).wait_recv()
                bcopy(t, i, r, kd).wait_recv()
                ccopy(t, i, r, h).start()
            if number == 3:
                ccopy(t, i, r, 1 - h).wait_recv()

    def both(number, t, step):
        for d in range(2):
            stage(number, t, d, step)

    def gather_sent():
        for t in range(5):
            for d in range(2):
                @pl.when(has_next(d))
                def _():
                    zcopy(t, d, 0, g).wait_send()
            for (d, step) in slots:
                i = d * last + step

                @pl.when(valid(d, step))
                def _():
                    r = row_of(d, step)
                    if step < last - 1:
                        @pl.when(has_next(d))
                        def _():
                            zcopy(t, d, step + 1, r).wait_send()
                    if t < 4:
                        xcopy(t, i, r, k).wait_send()
                        ycopy(t, i, r, k).wait_send()
                        acopy(t, i, r, kx).wait_send()
                        bcopy(t, i, r, ky).wait_send()
                        ccopy(t, i, r, h).wait_send()

    def vcopy(i, owner):
        return remote(s.smb, s.sm.at[owner], s.ms.at[i - 1], s.mr.at[i - 1], rep, lax.rem(g + i, groups))

    def place(r):
        return s.a_all.at[pl.ds(mo(r * tokens, 16), tokens), :]

    def scopy(d, step, r):
        return remote(place(r), place(r), s.szs.at[d, step], s.szr.at[d, step], rep, toward(d))

    def rcopy(i, owner):
        return remote(s.rows3.at[groups], s.rows3.at[owner], s.rs.at[i - 1], s.rr.at[i - 1], rep, lax.rem(g + i, groups))

    def share_start():
        for d in range(2):
            @pl.when(has_next(d))
            def _():
                scopy(d, 0, g).start()
        for i in range(1, groups):
            rcopy(i, g).start()

    def share_step(step):
        for d in range(2):
            @pl.when(valid(d, step))
            def _():
                r = row_of(d, step)
                scopy(d, step, r).wait_recv()
                if step < last - 1:
                    @pl.when(has_next(d))
                    def _():
                        scopy(d, step + 1, r).start()

    def share_rows():
        for i in range(1, groups):
            rcopy(i, lax.rem(g + groups - i, groups)).wait_recv()
        for i in range(groups):
            s.rows[:, i * tokens:(i + 1) * tokens] = s.rows3[i]
        s.rows[:, pl.ds(mo(g * tokens, LANE), tokens)] = s.rows3[groups]

    def share_sent():
        for d in range(2):
            @pl.when(has_next(d))
            def _():
                scopy(d, 0, g).wait_send()
            for step in range(last - 1):
                @pl.when(jnp.logical_and(valid(d, step), has_next(d)))
                def _():
                    scopy(d, step + 1, g).wait_send()
        for i in range(1, groups):
            rcopy(i, g).wait_send()

    def row(i):
        return lax.rem(g + 1 + i, groups)

    def first(t, i):
        m = MATS[t]
        at = pl.ds(mo(row(i) * m.block, 16), m.block)
        return remote(grads[t].at[at, pl.ds(mo((1 - h) * m.half, LANE), m.half)], s.buf1[t].at[at, :],
                      s.c1s.at[t, i], s.c1r.at[t, i], core, g)

    def cell1(t, i, kk, sub=None):
        return cell(s.buf1[t], MATS[t], row(i) * MATS[t].block + kk * MATS[t].quarter, sub)

    def cell2(t, i, j, sub):
        return cell(s.buf2[t], MATS[t], (row(i) * 2 + j) * MATS[t].quarter, sub)

    def cell3(t, i, sub=None):
        return cell(s.buf3[t], MATS[t], row(i) * MATS[t].quarter, sub)

    def a1(t, i, j, kk):
        return remote(cell1(t, i, kk, 0), cell2(t, i, j, 0), s.a1s.at[t, i, j], s.a1r.at[t, i, j], xn, g)

    def b1(t, i, j, kk):
        return remote(cell1(t, i, kk, 1), cell2(t, i, j, 1), s.b1s.at[t, i, j], s.b1r.at[t, i, j], yn, g)

    def a2(t, i, j):
        return remote(cell2(t, i, j, 0), cell3(t, i, 0), s.a2s.at[t, i], s.a2r.at[t, i], yn, g)

    def b2(t, i, j):
        return remote(cell2(t, i, j, 1), cell3(t, i, 1), s.b2s.at[t, i], s.b2r.at[t, i], xn, g)

    def z2(t, i):
        return remote(cell3(t, i), s.zbuf[t].at[i], s.z2s.at[t, i], s.z2r.at[t, i], rep, row(i))

    def r1(t, i):
        m = MATS[t]
        first(t, i).wait_recv()
        at = pl.ds(mo(row(i) * m.block, 16), m.block)
        mine = grads[t].at[at, pl.ds(mo(h * m.half, LANE), m.half)]
        add_rows(s.buf1[t].at[at, :], mine, s.buf1[t].at[at, :], m.block)
        for j in range(2):
            a1(t, i, j, 2 * j + (1 - x)).start()
            b1(t, i, j, 2 * (1 - y) + j).start()

    def r2(t, i):
        m = MATS[t]
        for j in range(2):
            a1(t, i, j, 2 * j + x).wait_recv()
            add_rows(cell2(t, i, j, 0), cell1(t, i, 2 * j + x, 0), cell2(t, i, j, 0), m.sub[0][1])
        a2(t, i, 1 - y).start()
        for j in range(2):
            b1(t, i, j, 2 * y + j).wait_recv()
            add_rows(cell2(t, i, j, 1), cell1(t, i, 2 * y + j, 1), cell2(t, i, j, 1), m.sub[1][1])
        b2(t, i, 1 - x).start()

    def r3(t, i):
        m = MATS[t]
        a2(t, i, y).wait_recv()
        b2(t, i, x).wait_recv()
        add_rows(cell3(t, i, 0), cell2(t, i, y, 0), cell3(t, i, 0), m.sub[0][1])
        add_rows(cell3(t, i, 1), cell2(t, i, x, 1), cell3(t, i, 1), m.sub[1][1])
        if i < last:
            z2(t, i).start()

    def fpart(t, kk, hh, sub=None):
        return part(outs[t], MATS[t], 0, kk, hh, sub)

    def keep(t):
        return pltpu.make_async_copy(s.fin[t].at[0], fpart(t, k, h), s.os.at[t])

    def xsend(t):
        return remote(s.fin[t].at[0], fpart(t, k, h), s.oxs.at[t], s.oxr.at[t], xn, g)

    def ysend(t):
        return remote(s.fin[t].at[0], fpart(t, k, h), s.oys.at[t], s.oyr.at[t], yn, g)

    def xgot(t):
        return remote(fpart(t, kx, h), fpart(t, kx, h), s.oxs.at[t], s.oxr.at[t], xn, g)

    def ygot(t):
        return remote(fpart(t, ky, h), fpart(t, ky, h), s.oys.at[t], s.oyr.at[t], yn, g)

    def fwd(t, sub, kk):
        reg = fpart(t, kk, h, sub)
        return remote(reg, reg, (s.oas, s.obs)[sub].at[t], (s.oar, s.obr)[sub].at[t], (yn, xn)[sub], g)

    def cross(t, hh):
        reg = slab(outs[t], MATS[t], 0, hh)
        return remote(reg, reg, s.ocs.at[t], s.ocr.at[t], core, g)

    def r4(t):
        m = MATS[t]
        for i in range(last):
            z2(t, i).wait_recv()
        mine = cell3(t, last)

        def body(n):
            at = pl.ds(mo(n * 16, 16), 16)
            total = mine[at, :].astype(F32)
            for i in range(last):
                total = total + s.zbuf[t][i, at, :].astype(F32)
            s.fin[t][0, at, :] = total.astype(BF)
        loop(m.quarter // 16, body)
        for b in range(highs):
            cp = remote(s.fin[t].at[0], s.fin[t].at[1 + b], s.fxs.at[t, b], s.fxr.at[t, b], flip(rep, 8 << b), g)
            cp.start()
            cp.wait()
            add_rows(s.fin[t].at[0], s.fin[t].at[0], s.fin[t].at[1 + b], m.quarter)
        keep(t).start()
        xsend(t).start()
        ysend(t).start()

    def r5(t):
        xgot(t).wait_recv()
        fwd(t, 0, kx).start()
        ygot(t).wait_recv()
        fwd(t, 1, ky).start()

    def r6(t):
        fwd(t, 0, kd).wait_recv()
        fwd(t, 1, kd).wait_recv()
        keep(t).wait()
        cross(t, h).start()

    partners = [(core, g), (xn, g), (yn, g)] + [(flip(rep, 8 << b), g) for b in range(highs)]
    bit = 1
    while bit < groups:
        partners.append((rep, flip(g, bit)))
        bit *= 2

    def smcopy(j):
        return remote(s.smacc.at[j], s.smin.at[j], s.sms.at[j], s.smr.at[j], *partners[j])

    def small(j):
        if j:
            smcopy(j - 1).wait_recv()
            s.smacc[j] = s.smacc[j - 1] + s.smin[j - 1]
        if j < len(partners):
            smcopy(j).start()
        else:
            osm[...] = s.smacc[j, g]

    def project(j):
        project_block(j, s.fa, s.gain1, s.shift1, s.qvbias, s.wq, s.q_all, s.k_all, s.v_all, s.normed, tokens)

    def attention(p):
        loop(2, lambda i: attend_pair(p + i, g, s.q_all, s.k_all, s.v_all, s.attended, s.stats, tokens))

    def block(n):
        return pl.ds(mo(n * 256, 256), 256)

    def to_middle():
        def body(n):
            c = block(n)
            s.middle[:, c] = nn(s.attended[...], s.wo[:, c]) + s.obias[0:1, c] + fr[:, c].astype(F32)
        loop(D // 256, body)
        value, inverse = normalize(s.middle[...])
        s.normal[...] = value
        s.inverse[...] = jnp.broadcast_to(inverse, (tokens, LANE))
        s.normed[...] = (value * s.gain2[...] + s.shift2[...]).astype(BF)

    def hidden():
        def body(n):
            c = block(n)
            u = nn(s.normed[...], s.wu[:, c]) + s.ubias[0:1, c]
            bell = 0.5 * (1.0 + lax.erf(u * ROOT_HALF))
            s.act[:, c] = (u * bell).astype(BF)
            slope = bell + u * jnp.exp(-0.5 * u * u) * ROOT_TWO_PI
            grad = nt(ct[...], s.wd[block(n), :]) * slope
            s.v_up[0:1, c] = jnp.sum(grad, axis=0, keepdims=True)
            s.pre[:, c] = grad.astype(BF)
        loop(FF // 256, body)

    def to_output():
        def body(n):
            c = block(n)
            out_frames[:, c] = (nn(s.act[...], s.wd[:, c]) + s.dbias[0:1, c] + s.middle[:, c]).astype(BF)
        loop(D // 256, body)

    def back_up():
        def body(n):
            s.wide[:, block(n)] = nt(s.pre[...], s.wu[block(n), :])
        loop(D // 256, body)

    def back_norm():
        upstream, normal = s.wide[...], s.normal[...]
        s.v_gain2[...] = jnp.sum(upstream * normal, axis=0, keepdims=True)
        s.v_shift2[...] = jnp.sum(upstream, axis=0, keepdims=True)
        total = ct[...].astype(F32) + norm_back(upstream, normal, s.inverse[:, 0:1], s.gain2[...])
        s.mgrad[...] = total
        s.half[...] = total.astype(BF)
        s.v_out[...] = jnp.sum(total, axis=0, keepdims=True)
        s.v_down[...] = jnp.sum(ct[...].astype(F32), axis=0, keepdims=True)

        def body(n):
            s.a_all[own, block(n)] = nt(s.half[...], s.wo[block(n), :]).astype(BF)
        own = pl.ds(mo(g * tokens, 16), tokens)
        loop(D // 256, body)
        lanes = lax.broadcasted_iota(jnp.int32, (tokens, LANE), 1)
        mask = head_mask(tokens)
        stats = s.stats[...]
        for p in range(HEADS // 2):
            c = slice(p * LANE, (p + 1) * LANE)
            product = s.a_all[own, c].astype(F32) * s.attended[:, c].astype(F32)
            for side in range(2):
                mine = jnp.where(mask if side == 0 else jnp.logical_not(mask), product, 0.0)
                stats = jnp.where(lanes == HEADS + 2 * p + side, jnp.sum(mine, axis=-1, keepdims=True), stats)
        s.stats[...] = stats
        s.rows3[groups] = stats.T[0:2 * HEADS, :]

    def weight(t, i, left, right):
        m = MATS[t]
        s.turned[0:m.block, :] = left[:, pl.ds(mo(row(i) * m.block, LANE if m.block % LANE == 0 else 64), m.block)].T

        def body(n):
            c = block(n)
            grads[t][pl.ds(mo(row(i) * m.block, 16), m.block), c] = nn(s.turned[0:m.block, :], right[:, c]).astype(BF)
        loop(m.cols // 256, body)
        first(t, i).start()

    def turn(left, out):
        out[...] = left[...].T

    def weight_from(t, i, left, right):
        m = MATS[t]
        at = pl.ds(mo(row(i) * m.block, 16), m.block)

        def body(n):
            c = block(n)
            grads[t][at, c] = nn(left[at, :], right[:, c]).astype(BF)
        loop(m.cols // 256, body)
        first(t, i).start()

    def queries(p):
        loop(2, lambda i: query_back(p + i, g, s.q_all, s.k_all, s.v_all, s.a_all, s.stats, s.pgrad, s.v_qv, tokens))

    def keys(p):
        loop(2, lambda i: key_back(p + i, g, s.q_all, s.k_all, s.v_all, s.a_all, s.rows, s.pgrad, s.v_qv, tokens))

    def to_inputs():
        normal, _ = normalize(fr[...].astype(F32))
        s.normed[...] = (normal * s.gain1[...] + s.shift1[...]).astype(BF)
        turn(s.normed, s.turned)

    def input_grad():
        def body(n):
            s.wide[:, block(n)] = nt(s.pgrad[...], s.wq[block(n), :])
        loop(D // 256, body)
        normal, inverse = normalize(fr[...].astype(F32))
        upstream = s.wide[...]
        s.v_gain1[...] = jnp.sum(upstream * normal, axis=0, keepdims=True)
        s.v_shift1[...] = jnp.sum(upstream, axis=0, keepdims=True)
        frames_grad[...] = (s.mgrad[...] + norm_back(upstream, normal, inverse, s.gain1[...])).astype(BF)
        fill_image(s.smacc.at[0], range(SROWS), (
            (GAIN_ONE, s.v_gain1), (SHIFT_ONE, s.v_shift1), (QV_BIAS, s.v_qv), (OUT_BIAS, s.v_out), (GAIN_TWO, s.v_gain2),
            (SHIFT_TWO, s.v_shift2), (UP_BIAS, s.v_up), (DOWN_BIAS, s.v_down)))
        small(0)

    barrier, peers = greet(rep, g, groups)
    peers += [(flip(rep, 8 << b), g) for b in range(highs)]
    for n in range(3):
        piece_load(n).start()
    for cp in small_loads():
        cp.start()
    own_frames = pltpu.make_async_copy(fr, zregion(4, g), s.ssem.at[len(SMALL)])
    own_frames.start()
    do_barrier(barrier, peers)
    relayout(0)
    own_send(0)
    for cp in small_loads():
        cp.wait()
    s.smb[...] = jnp.zeros_like(s.smb)
    count = sum(c for _, c in SMALL)
    s.smb[0:count, :] = s.spbuf[...].astype(F32).reshape(count, LANE)
    for i in range(1, groups):
        vcopy(i, g).start()
    own_frames.wait()
    both(0, 0, 0)
    both(0, 0, 1)
    own_send(4)
    for n in (1, 2, 3):
        relayout(n)
    both(0, 0, 2)
    for n in (4, 5, 6):
        relayout(n)
        own_send(n - 3)
    for step in range(last):
        both(1, 0, step)
    for n in (7, 8, 9):
        relayout(n)
    for step in range(last):
        both(2, 0, step)
    for i in range(1, groups):
        vcopy(i, lax.rem(g + groups - i, groups)).wait_recv()
    s.sm[g] = s.smb[...]
    for spot, ref in ((GAIN_ONE, s.gain1), (SHIFT_ONE, s.shift1), (QV_BIAS, s.qvbias), (GAIN_TWO, s.gain2), (SHIFT_TWO, s.shift2),
                      (OUT_BIAS, s.obias), (UP_BIAS, s.ubias), (DOWN_BIAS, s.dbias)):
        assemble(s.sm, spot, ref)
    s.stats[...] = jnp.zeros_like(s.stats)
    for n in (10, 11, 12):
        relayout(n)
    for step in range(last):
        both(3, 0, step)
    both(0, 4, 0)
    project(g)
    for n in (13, 14, 15):
        relayout(n)
    rest = [(t, step) for step in range(last) for t in (1, 2, 3)]
    for step in range(last):
        if step:
            both(0, 4, step)
        for t in (1, 2, 3):
            both(0, t, step)
        for d in range(2):
            @pl.when(valid(d, step))
            def _():
                project(row_of(d, step))
        for t in (1, 2, 3):
            both(1, t, step)
        if step:
            for t in (1, 2, 3):
                both(2, t, step - 1)
    attention(0)
    attention(2)
    for t in (1, 2, 3):
        both(2, t, last - 1)
    attention(4)
    for t, step in rest:
        both(3, t, step)
    to_middle()
    hidden()
    for i in range(groups):
        weight(3, i, s.act, ct)
    turn(s.normed, s.turned2)
    work = {
        0: [back_up], 1: [back_norm, share_start],
        2: [lambda: weight_from(2, 0, s.turned2, s.pre), lambda: weight_from(2, 1, s.turned2, s.pre)],
        3: [lambda: weight_from(2, 2, s.turned2, s.pre), lambda: weight_from(2, 3, s.turned2, s.pre), gather_sent],
        4: [lambda: share_step(0), lambda: turn(s.attended, s.turned2)]
        + [functools.partial(weight_from, 1, i, s.turned2, s.half) for i in range(groups)],
        5: [to_output, lambda: queries(0)],
        6: [lambda: share_step(1), lambda: queries(2)],
        7: [lambda: queries(4), to_inputs],
        8: [lambda: share_step(2), share_rows, lambda: keys(0)],
        9: [lambda: keys(2)],
        10: [lambda: keys(4)],
        11: [functools.partial(weight_from, 0, i, s.turned, s.pgrad) for i in range(groups)] + [input_grad],
    }
    chunks = [(t, i) for t in ORDER for i in range(groups)]
    total = len(chunks)
    smalls = 1
    for n in range(total + 16):
        if n < total:
            r1(*chunks[n])
        if 0 <= n - 2 < total:
            r2(*chunks[n - 2])
        if n > 12 and smalls <= len(partners):
            small(smalls)
            smalls += 1
        if 0 <= n - 4 < total:
            r3(*chunks[n - 4])
        for q, t in enumerate(ORDER):
            done = groups * q + groups - 1 + 4
            if n == done + 2:
                r4(t)
            if n == done + 4:
                r5(t)
            if n == done + 6:
                r6(t)
        for piece in work.get(n, ()):
            piece()
    for t in ORDER:
        cross(t, 1 - h).wait_recv()
    share_sent()
    for i in range(1, groups):
        vcopy(i, g).wait_send()
    for t, i in chunks:
        first(t, i).wait_send()
        for j in range(2):
            a1(t, i, j, 2 * j + x).wait_send()
            b1(t, i, j, 2 * y + j).wait_send()
        a2(t, i, y).wait_send()
        b2(t, i, x).wait_send()
        if i < last:
            z2(t, i).wait_send()
    for t in ORDER:
        xsend(t).wait_send()
        ysend(t).wait_send()
        fwd(t, 0, kx).wait_send()
        fwd(t, 1, ky).wait_send()
        cross(t, h).wait_send()
    for j in range(len(partners)):
        smcopy(j).wait_send()


def layer(frames, cotangent, params, groups, reps):
    dma = pltpu.SemaphoreType.DMA
    tokens = frames.shape[0]
    clip = tokens * groups
    highs = (reps // 8).bit_length() - 1
    steps = 3 + highs + groups.bit_length() - 1
    n = 2 * (groups - 1)

    def bf(*shape):
        return pltpu.VMEM(shape, BF)

    def wide(*shape):
        return pltpu.VMEM(shape, F32)

    scratch = {name: bf(m.block * groups, m.cols) for name, m in zip(("wq", "wo", "wu", "wd"), MATS)}
    scratch.update(go=bf(D, D), gu=bf(D, FF), gd=bf(FF, D))
    scratch.update(buf1=[bf(m.block * groups, m.half) for m in MATS], buf2=[bf(m.quarter * groups * 2, m.half) for m in MATS],
                   buf3=[bf(m.quarter * groups, m.half) for m in MATS], zbuf=[bf(groups - 1, m.quarter, m.half) for m in MATS],
                   fin=[bf(highs + 1, m.quarter, m.half) for m in MATS])
    scratch.update(fa=bf(clip, D), q_all=bf(clip, D), k_all=bf(clip, D), v_all=bf(clip, D), a_all=bf(clip, D))
    scratch.update(attended=bf(tokens, D), normed=bf(tokens, D), half=bf(tokens, D),
                   act=bf(tokens, FF), pre=bf(tokens, FF), pgrad=bf(tokens, 3 * D), turned=bf(D, tokens), turned2=bf(D, tokens))
    scratch.update(middle=wide(tokens, D), normal=wide(tokens, D), mgrad=wide(tokens, D), wide=wide(tokens, D),
                   inverse=wide(tokens, LANE), stats=wide(tokens, LANE))
    scratch.update(rows3=wide(groups + 1, 2 * HEADS, tokens), rows=wide(2 * HEADS, clip))
    scratch.update({name: wide(1, D) for name in ("gain1", "shift1", "gain2", "shift2", "obias", "dbias", "v_gain1", "v_shift1",
                                                  "v_gain2", "v_shift2", "v_out", "v_down")})
    scratch.update(qvbias=wide(1, 2 * D), v_qv=wide(1, 2 * D), ubias=wide(1, FF), v_up=wide(1, FF))
    piece = max(m.quarter * m.tiles + 8 for m in MATS)
    scratch.update(pbuf=bf(3, 1, piece * LANE), fbuf=wide(piece, LANE), spbuf=bf(1, sum(c for _, c in SMALL) * LANE),
                   smb=wide(SROWS, LANE), sm=wide(groups, SROWS, LANE),
                   smacc=wide(steps + 1, groups, SROWS, LANE), smin=wide(steps, groups, SROWS, LANE))
    scratch.update(lsem=dma((3,)), ssem=dma((len(SMALL) + 1,)), zs=dma((5, 2, groups)), zr=dma((5, 2, groups)))
    scratch.update({name: dma((4, n)) for name in ("xs", "xr", "ys", "yr", "fas", "far", "fbs", "fbr", "cs", "cr")})
    scratch.update({name: dma((groups,)) for name in ("ms", "mr", "rs", "rr")})
    scratch.update(szs=dma((2, groups)), szr=dma((2, groups)))
    scratch.update({name: dma((4, groups)) for name in ("c1s", "c1r", "a2s", "a2r", "b2s", "b2r", "z2s", "z2r")})
    scratch.update({name: dma((4, groups, 2)) for name in ("a1s", "a1r", "b1s", "b1r")})
    scratch.update({name: dma((4, max(highs, 1))) for name in ("fxs", "fxr")})
    scratch.update({name: dma((4,)) for name in ("os", "oxs", "oxr", "oys", "oyr", "oas", "oar", "obs", "obr", "ocs", "ocr")})
    scratch.update(sms=dma((steps,)), smr=dma((steps,)))
    vmem, hbm = pl.BlockSpec(memory_space=pltpu.VMEM), pl.BlockSpec(memory_space=pl.ANY)
    sds = jax.ShapeDtypeStruct
    names = tuple(scratch)
    flat, tree = jax.tree.flatten(list(scratch.values()))

    def body(*refs):
        fixed = 10
        layer_kernel(groups, highs, names, *refs[:fixed], *jax.tree.unflatten(tree, refs[fixed:]))

    return pl.pallas_call(
        body,
        out_shape=[sds((m.block, m.cols), BF) for m in MATS] + [sds((SROWS, LANE), F32), sds((tokens, D), BF), sds((tokens, D), BF)],
        in_specs=[vmem, vmem, hbm],
        out_specs=[hbm] * 4 + [vmem] * 3,
        scratch_shapes=flat,
        compiler_params=pltpu.CompilerParams(collective_id=0, has_side_effects=True, vmem_limit_bytes=67043328),
        name="layer",
    )(frames, cotangent, params)


BETA_ONE = 0.9
BETA_TWO = 0.98
ADAM_EPS = 1e-06
LEARN_RATE = 0.006
DECAY = 0.01
ADAM_STEP = 4
ROWS = 1736
STEPS = -(-FROWS // ROWS)


def flatten(m, block, flat, late):
    def body(i, carry):
        base = m.row0 + i * (48 * m.tiles)
        for c in range(m.tiles):
            tile = block[pl.ds(mo(i * 48, 16), 48), c * LANE:(c + 1) * LANE].astype(F32)
            if m.shifted:
                tile = pltpu.roll(tile, 64, 1)
                late[pl.ds(base + c + 1, 48, stride=m.tiles), :] = tile
            flat[pl.ds(base + c, 48, stride=m.tiles), :] = tile
        return carry
    lax.fori_loop(0, m.block // 48, body, 0)


def adam_kernel(scale, gq, go, gu, gd, sm, p_ref, m_ref, v_ref, o_g, o_p, o_m, o_v, flat, late):
    step = pl.program_id(0)

    @pl.when(step == 0)
    def _():
        flatten(QKV, gq, flat, late)
        flatten(OUT, go, flat, late)
        flatten(UP, gu, flat, late)
        flatten(DOWN, gd, flat, late)
        flat[0:3, :] = sm[0:3, :]
        flat[3459:3462, :] = sm[3:6, :]
        flat[4614:4618, :] = sm[6:10, :]
        flat[4618:4619, 0:64] = sm[10:11, 0:64]
        flat[9226:9227, 64:128] = sm[11:12, 64:128]
        flat[9227:9232, :] = sm[12:17, :]
        flat[9232:9233, 0:64] = sm[17:18, 0:64]
        flat[13840:13841, 64:128] = sm[18:19, 64:128]
        flat[13841:13842, :] = sm[19:20, :]
        late[9227:9232, :] = sm[12:17, :]
        late[9232:9233, 0:64] = sm[17:18, 0:64]
        late[13841:13842, :] = sm[19:20, :]

    at = pl.ds(mo(step * ROWS, 8), ROWS)
    number = step * ROWS + lax.broadcasted_iota(jnp.int32, (ROWS, LANE), 0)
    low = lax.broadcasted_iota(jnp.int32, (ROWS, LANE), 1) < 64
    grad = jnp.where(jnp.logical_and(number > UP.row0, low), late[at, :], flat[at, :]).reshape(1, ROWS * LANE) * scale
    first = BETA_ONE * m_ref[...] + (1.0 - BETA_ONE) * grad
    second = BETA_TWO * v_ref[...] + (1.0 - BETA_TWO) * grad * grad
    o_g[...] = grad
    o_m[...] = first
    o_v[...] = second
    first_hat = first * (1.0 / (1.0 - BETA_ONE**ADAM_STEP))
    second_hat = second * (1.0 / (1.0 - BETA_TWO**ADAM_STEP))
    current = p_ref[...].astype(F32)
    o_p[...] = current - LEARN_RATE * (first_hat / (jnp.sqrt(second_hat) + ADAM_EPS) + DECAY * current)


def adam(blocks, smalls, params, first, second, reps):
    spec = pl.BlockSpec((1, ROWS * LANE), lambda i: (0, i))
    vmem = pl.BlockSpec(memory_space=pltpu.VMEM)
    return pl.pallas_call(
        functools.partial(adam_kernel, 1.0 / reps),
        grid=(STEPS,),
        out_shape=[jax.ShapeDtypeStruct((1, FLAT), F32)] * 4,
        in_specs=[vmem] * 5 + [spec] * 3,
        out_specs=[spec] * 4,
        scratch_shapes=[pltpu.VMEM((STEPS * ROWS, LANE), F32)] * 2,
        compiler_params=pltpu.CompilerParams(vmem_limit_bytes=50 << 20),
        name="adam",
    )(*blocks, smalls, params, first, second)


def on_device(frames, cotangent, params, first_moment, second_moment):
    groups, reps = lax.axis_size("grp"), lax.axis_size("rep")
    *blocks, small, out_frames, frames_grad = layer(frames, cotangent, params, groups, reps)
    param_grad, new_params, new_first, new_second = adam(blocks, small, params, first_moment, second_moment, reps)
    return (out_frames, frames_grad, param_grad, new_params, new_first, new_second)


def solution(mesh):
    in_specs = (
        P(("rep", "grp"), None),
        P(("rep", "grp"), None),
        P("grp", None),
        P("grp", None),
        P("grp", None),
    )
    out_specs = (
        P(("rep", "grp"), None),
        P(("rep", "grp"), None),
        P("grp", None),
        P("grp", None),
        P("grp", None),
        P("grp", None),
    )
    return jax.shard_map(
        on_device, mesh=mesh, in_specs=in_specs, out_specs=out_specs, check_vma=False
    )
```

```python
import functools
import types

import jax
import jax.numpy as jnp
from jax import lax
from jax.sharding import PartitionSpec as P
from jax.experimental import pallas as pl
from jax.experimental.pallas import tpu as pltpu

MESH = pl.DeviceIdType.MESH
BF = jnp.bfloat16
F32 = jnp.float32
D = 768
FF = 3072
HDIM = 64
LANE = 128
FLAT = 1771776
FROWS = FLAT // LANE


class Mat:
    def __init__(self, offset, block, cols, suba, subb):
        self.offset, self.block, self.cols = offset, block, cols
        self.tiles = cols // LANE
        self.row0 = offset // LANE
        self.shifted = offset % LANE != 0
        self.quarter = block // 4
        self.half = cols // 2
        self.sub = (suba, subb)


QKV = Mat(384, 192, 2304, (0, 48, 0, 640), (0, 48, 640, 512))
OUT = Mat(443136, 192, 768, (0, 48, 0, 128), (0, 48, 128, 256))
UP = Mat(591168, 192, 3072, (0, 48, 0, 768), (0, 48, 768, 768))
DOWN = Mat(1181760, 768, 768, (0, 96, 0, 384), (96, 96, 0, 384))
MATS = (QKV, OUT, UP, DOWN)
SMALL = ((0, 3), (3459, 3), (4614, 5), (9226, 7), (13840, 2))
SROWS = 24


def flip(index, bit):
    return index + bit - 2 * bit * ((index // bit) % 2)


def mo(value, by):
    return pl.multiple_of(value, by)


def part(ref, m, r, k, h, sub=None):
    r0, rn, c0, cn = m.sub[sub] if sub is not None else (0, m.quarter, 0, m.half)
    row = mo(r * m.block + k * m.quarter + r0, 16)
    col = mo(h * m.half + c0, LANE)
    return ref.at[pl.ds(row, rn), pl.ds(col, cn)]


def slab(ref, m, r, h):
    return ref.at[pl.ds(mo(r * m.block, 16), m.block), pl.ds(mo(h * m.half, LANE), m.half)]


def remote(src, dst, send, recv, rep, grp):
    return pltpu.make_async_remote_copy(
        src_ref=src, dst_ref=dst, send_sem=send, recv_sem=recv,
        device_id={"rep": rep, "grp": grp}, device_id_type=MESH)


def greet(rep, g, groups):
    barrier = pltpu.get_barrier_semaphore()
    peers = [(flip(rep, b), g) for b in (1, 2, 4)]
    peers += [(rep, lax.rem(g + i, groups)) for i in range(1, groups)]
    return barrier, peers


def do_barrier(barrier, peers):
    for r, gg in peers:
        pl.semaphore_signal(barrier, inc=1, device_id={"rep": r, "grp": gg}, device_id_type=MESH)
    pl.semaphore_wait(barrier, len(peers))


def add_rows(dst, a, b, rows, step=16):
    def body(i, c):
        at = pl.ds(mo(i * step, 16), step)
        dst[at, :] = (a[at, :].astype(F32) + b[at, :].astype(F32)).astype(dst.dtype)
        return c
    lax.fori_loop(0, rows // step, body, 0)


EPS_NORM = 1e-05
ROOT_HALF = 0.7071067811865476
ROOT_TWO_PI = 0.3989422804014327
HEADS = D // HDIM
GAIN_ONE, SHIFT_ONE, QV_BIAS, OUT_BIAS, GAIN_TWO, SHIFT_TWO, UP_BIAS, DOWN_BIAS = (
    (0, 3), (3, 3), (6, 6), (12, 3), (15, 3), (18, 3), (23, 12), (37, 3))


def low_lanes():
    return lax.broadcasted_iota(jnp.int32, (1, LANE), 1) < 64


def assemble(sm, place, out):
    first, count = place
    halves = [(gi, first + i) for gi in range(sm.shape[0]) for i in range(count)]
    for t in range(len(halves) // 2):
        (g0, h0), (g1, h1) = halves[2 * t], halves[2 * t + 1]
        a = sm[g0, h0 // 2:h0 // 2 + 1, :]
        b = sm[g1, h1 // 2:h1 // 2 + 1, :]
        a = pltpu.roll(a, 64, 1) if h0 % 2 else a
        b = b if h1 % 2 else pltpu.roll(b, 64, 1)
        out[0:1, t * LANE:(t + 1) * LANE] = jnp.where(low_lanes(), a, b)


def fill_image(image, rows, vectors):
    where = {}
    for place, ref in vectors:
        for i in range(place[1]):
            where[place[0] + i] = (place[1], i, ref)
    for gi in range(image.shape[0]):
        for r in rows:
            parts = []
            for side in range(2):
                spot = where.get(2 * r + side)
                if spot is None:
                    parts.append(jnp.zeros((1, LANE), F32))
                    continue
                count, i, ref = spot
                q = gi * count + i
                v = ref[0:1, q // 2 * LANE:(q // 2 + 1) * LANE]
                parts.append(v if q % 2 == side else pltpu.roll(v, 64, 1))
            image[gi, r:r + 1, :] = jnp.where(low_lanes(), parts[0], parts[1])


def mean(v):
    return jnp.sum(v, axis=-1, keepdims=True) * (1.0 / D)


def normalize(v):
    centered = v - mean(v)
    inverse = lax.rsqrt(mean(centered * centered) + EPS_NORM)
    return centered * inverse, inverse


def norm_back(upstream, normal, inverse, gain):
    s = upstream * gain
    return inverse * (s - mean(s) - normal * mean(s * normal))


def nn(a, b):
    return lax.dot_general(a, b, (((1,), (0,)), ((), ())), preferred_element_type=F32)


def nt(a, b):
    return lax.dot_general(a, b, (((1,), (1,)), ((), ())), preferred_element_type=F32)


def loop(count, body):
    def step(i, c):
        body(i)
        return c
    lax.fori_loop(0, count, step, 0)


def head_mask(rows):
    return lax.broadcasted_iota(jnp.int32, (rows, LANE), 1) < HDIM


def project_block(j, fa, gain, shift, bias, wq, q_all, k_all, v_all, normed, tokens):
    at = pl.ds(mo(j * tokens, 16), tokens)
    normal, _ = normalize(fa[at, :].astype(F32))
    normed[...] = (normal * gain[...] + shift[...]).astype(BF)
    for third, out in enumerate((q_all, k_all, v_all)):
        def body(n):
            col = pl.ds(mo(n * 256, 256), 256)
            wide = nn(normed[...], wq[:, pl.ds(mo(third * D + n * 256, 256), 256)])
            if third != 1:
                wide = wide + bias[0:1, pl.ds(mo((third // 2) * D + n * 256, 256), 256)]
            out[at, col] = wide.astype(BF)
        loop(D // 256, body)


def attend_pair(p, g, q_all, k_all, v_all, attended, stats, tokens):
    col = pl.ds(mo(p * LANE, LANE), LANE)
    query = q_all[pl.ds(mo(g * tokens, 16), tokens), col] * jnp.asarray(HDIM**-0.5, BF)
    keys, values = k_all[:, col], v_all[:, col]
    mask = head_mask(tokens)
    zero = jnp.zeros_like(query)
    lanes = lax.broadcasted_iota(jnp.int32, (tokens, LANE), 1)
    results = []
    for side in range(2):
        scores = nt(jnp.where(mask, query, zero) if side == 0 else jnp.where(mask, zero, query), keys)
        highest = jnp.max(scores, axis=-1, keepdims=True)
        shares = jnp.exp(scores - highest)
        total = jnp.sum(shares, axis=-1, keepdims=True)
        results.append(nn(shares.astype(BF), values) * (1.0 / total))
        stats[...] = jnp.where(lanes == 2 * p + side, highest + jnp.log(total), stats[...])
    attended[:, col] = jnp.where(mask, results[0], results[1]).astype(BF)


def query_back(p, g, q_all, k_all, v_all, a_all, stats, pgrad, v_qv, tokens):
    col = pl.ds(mo(p * LANE, LANE), LANE)
    own = pl.ds(mo(g * tokens, 16), tokens)
    scale = jnp.asarray(HDIM**-0.5, BF)
    query, upstream = q_all[own, col] * scale, a_all[own, col]
    keys, values = k_all[:, col], v_all[:, col]
    mask = head_mask(tokens)
    zero = jnp.zeros_like(query)
    lanes = lax.broadcasted_iota(jnp.int32, (tokens, LANE), 1)
    results = []
    for side in range(2):
        def pick(v):
            return jnp.where(mask, v, zero) if side == 0 else jnp.where(mask, zero, v)
        total = jnp.sum(jnp.where(lanes == 2 * p + side, stats[...], 0.0), axis=-1, keepdims=True)
        centre = jnp.sum(jnp.where(lanes == HEADS + 2 * p + side, stats[...], 0.0), axis=-1, keepdims=True)
        shares = jnp.exp(nt(pick(query), keys) - total)
        back = (shares * (nt(pick(upstream), values) - centre)).astype(BF) * scale
        results.append(nn(back, keys))
    grad = jnp.where(mask, results[0], results[1])
    pgrad[:, col] = grad.astype(BF)
    v_qv[0:1, col] = jnp.sum(grad, axis=0, keepdims=True)


def key_back(p, g, q_all, k_all, v_all, a_all, rows, pgrad, v_qv, tokens):
    col = pl.ds(mo(p * LANE, LANE), LANE)
    own = pl.ds(mo(g * tokens, 16), tokens)
    scale = jnp.asarray(HDIM**-0.5, BF)
    keys, values = k_all[own, col] * scale, v_all[own, col]
    queries, upstream = q_all[:, col], a_all[:, col]
    mask = head_mask(tokens)
    zero = jnp.zeros_like(keys)
    ks, vs = [], []
    for side in range(2):
        def pick(v):
            return jnp.where(mask, v, zero) if side == 0 else jnp.where(mask, zero, v)
        total = rows[pl.ds(2 * p + side, 1), :]
        centre = rows[pl.ds(HEADS + 2 * p + side, 1), :]
        shares = jnp.exp(nt(pick(keys), queries) - total)
        vs.append(nn(shares.astype(BF), upstream))
        back = (shares * (nt(pick(values), upstream) - centre)).astype(BF) * scale
        ks.append(nn(back, queries))
    pgrad[:, pl.ds(mo(D + p * LANE, LANE), LANE)] = jnp.where(mask, ks[0], ks[1]).astype(BF)
    grad = jnp.where(mask, vs[0], vs[1])
    pgrad[:, pl.ds(mo(2 * D + p * LANE, LANE), LANE)] = grad.astype(BF)
    v_qv[0:1, pl.ds(mo(D + p * LANE, LANE), LANE)] = jnp.sum(grad, axis=0, keepdims=True)


def cell(ref, m, row, sub=None):
    r0, rn, c0, cn = m.sub[sub] if sub is not None else (0, m.quarter, 0, m.half)
    return ref.at[pl.ds(mo(row + r0, 16), rn), pl.ds(c0, cn)]


ORDER = (3, 2, 1, 0)


def layer_kernel(groups, highs, names, fr, ct, p_ref, oq, oo, ou, od, osm, out_frames, frames_grad, *scratch):
    s = types.SimpleNamespace(**dict(zip(names, scratch)))
    rep, g = lax.axis_index("rep"), lax.axis_index("grp")
    tokens = fr.shape[0]
    share_of = lax.rem(rep, 8)
    h = lax.rem(share_of, 2)
    k = share_of // 2
    x, y = lax.rem(k, 2), k // 2
    kx, ky, kd = flip(k, 1), flip(k, 2), 3 - k
    core, xn, yn = flip(rep, 1), flip(rep, 2), flip(rep, 4)
    full = (s.wq, s.wo, s.wu, s.wd)
    outs = (oq, oo, ou, od)
    grads = (s.wu, s.go, s.gu, s.gd)
    last = groups - 1

    def has_next(d):
        return g < last if d == 0 else g > 0

    def toward(d):
        return lax.rem(g + (1 if d == 0 else last), groups)

    def row_of(d, step):
        return g - 1 - step if d == 0 else g + 1 + step

    def valid(d, step):
        return row_of(d, step) >= 0 if d == 0 else row_of(d, step) <= last

    slots = [(d, step) for step in range(last) for d in range(2)]

    order = [(0, 0), (1, 0), (2, 0), (3, 0)] + [(t, i) for t in range(4) for i in (1, 2, 3)]

    def piece_load(n):
        t, i = order[n]
        m = MATS[t]
        count = (m.quarter * m.tiles + (2 if m.shifted else 0)) * LANE
        start = mo((m.row0 + lax.rem(k + i, 4) * (m.quarter * m.tiles)) * LANE, LANE)
        return pltpu.make_async_copy(p_ref.at[:, pl.ds(start, count)], s.pbuf.at[n % 3, :, pl.ds(0, count)], s.lsem.at[n % 3])

    def relayout(n):
        t, i = order[n]
        m = MATS[t]
        piece_load(n).wait()
        count = m.quarter * m.tiles + (8 if m.shifted else 0)
        s.fbuf[0:count, :] = s.pbuf[n % 3, :, 0:count * LANE].astype(F32).reshape(count, LANE)
        if n + 3 < len(order):
            piece_load(n + 3).start()
        at = pl.ds(mo(g * m.block + lax.rem(k + i, 4) * m.quarter, 16), m.quarter)
        low = lax.broadcasted_iota(jnp.int32, (m.quarter, LANE), 1) < 64
        for c in range(m.tiles):
            a = s.fbuf[pl.ds(c, m.quarter, stride=m.tiles), :]
            if m.shifted:
                b = s.fbuf[pl.ds(c + 1, m.quarter, stride=m.tiles), :]
                a = pltpu.roll(jnp.where(low, b, a), 64, 1)
            full[t][at, c * LANE:(c + 1) * LANE] = a.astype(BF)

    def small_loads():
        at, result = 0, []
        for n, (first, count) in enumerate(SMALL):
            result.append(pltpu.make_async_copy(
                p_ref.at[:, pl.ds(first * LANE, count * LANE)], s.spbuf.at[:, pl.ds(at * LANE, count * LANE)], s.ssem.at[n]))
            at += count
        return result

    def zregion(t, r):
        if t == 4:
            return s.fa.at[pl.ds(mo(r * tokens, 16), tokens), :]
        return part(full[t], MATS[t], r, k, h)

    def zcopy(t, d, step, r):
        reg = zregion(t, r)
        return remote(reg, reg, s.zs.at[t, d, step], s.zr.at[t, d, step], rep, toward(d))

    def own_send(t):
        for d in range(2):
            @pl.when(has_next(d))
            def _():
                zcopy(t, d, 0, g).start()

    def xcopy(t, i, r, kk):
        reg = part(full[t], MATS[t], r, kk, h)
        return remote(reg, reg, s.xs.at[t, i], s.xr.at[t, i], xn, g)

    def ycopy(t, i, r, kk):
        reg = part(full[t], MATS[t], r, kk, h)
        return remote(reg, reg, s.ys.at[t, i], s.yr.at[t, i], yn, g)

    def acopy(t, i, r, kk):
        reg = part(full[t], MATS[t], r, kk, h, 0)
        return remote(reg, reg, s.fas.at[t, i], s.far.at[t, i], yn, g)

    def bcopy(t, i, r, kk):
        reg = part(full[t], MATS[t], r, kk, h, 1)
        return remote(reg, reg, s.fbs.at[t, i], s.fbr.at[t, i], xn, g)

    def ccopy(t, i, r, hh):
        reg = slab(full[t], MATS[t], r, hh)
        return remote(reg, reg, s.cs.at[t, i], s.cr.at[t, i], core, g)

    def stage(number, t, d, step):
        i = d * last + step

        @pl.when(valid(d, step))
        def _():
            r = row_of(d, step)
            if number == 0:
                zcopy(t, d, step, r).wait_recv()
                if step < last - 1:
                    @pl.when(has_next(d))
                    def _():
                        zcopy(t, d, step + 1, r).start()
                if t < 4:
                    xcopy(t, i, r, k).start()
                    ycopy(t, i, r, k).start()
            if number == 1:
                xcopy(t, i, r, kx).wait_recv()
                acopy(t, i, r, kx).start()
                ycopy(t, i, r, ky).wait_recv()
                bcopy(t, i, r, ky).start()
            if number == 2:
                acopy(t, i, r, kd).wait_recv()
                bcopy(t, i, r, kd).wait_recv()
                ccopy(t, i, r, h).start()
            if number == 3:
                ccopy(t, i, r, 1 - h).wait_recv()

    def both(number, t, step):
        for d in range(2):
            stage(number, t, d, step)

    def gather_sent():
        for t in range(5):
            for d in range(2):
                @pl.when(has_next(d))
                def _():
                    zcopy(t, d, 0, g).wait_send()
            for (d, step) in slots:
                i = d * last + step

                @pl.when(valid(d, step))
                def _():
                    r = row_of(d, step)
                    if step < last - 1:
                        @pl.when(has_next(d))
                        def _():
                            zcopy(t, d, step + 1, r).wait_send()
                    if t < 4:
                        xcopy(t, i, r, k).wait_send()
                        ycopy(t, i, r, k).wait_send()
                        acopy(t, i, r, kx).wait_send()
                        bcopy(t, i, r, ky).wait_send()
                        ccopy(t, i, r, h).wait_send()

    def vcopy(i, owner):
        return remote(s.smb, s.sm.at[owner], s.ms.at[i - 1], s.mr.at[i - 1], rep, lax.rem(g + i, groups))

    def place(r):
        return s.a_all.at[pl.ds(mo(r * tokens, 16), tokens), :]

    def scopy(d, step, r):
        return remote(place(r), place(r), s.szs.at[d, step], s.szr.at[d, step], rep, toward(d))

    def rcopy(i, owner):
        return remote(s.rows3.at[groups], s.rows3.at[owner], s.rs.at[i - 1], s.rr.at[i - 1], rep, lax.rem(g + i, groups))

    def share_start():
        for d in range(2):
            @pl.when(has_next(d))
            def _():
                scopy(d, 0, g).start()
        for i in range(1, groups):
            rcopy(i, g).start()

    def share_step(step):
        for d in range(2):
            @pl.when(valid(d, step))
            def _():
                r = row_of(d, step)
                scopy(d, step, r).wait_recv()
                if step < last - 1:
                    @pl.when(has_next(d))
                    def _():
                        scopy(d, step + 1, r).start()

    def share_rows():
        for i in range(1, groups):
            rcopy(i, lax.rem(g + groups - i, groups)).wait_recv()
        for i in range(groups):
            s.rows[:, i * tokens:(i + 1) * tokens] = s.rows3[i]
        s.rows[:, pl.ds(mo(g * tokens, LANE), tokens)] = s.rows3[groups]

    def share_sent():
        for d in range(2):
            @pl.when(has_next(d))
            def _():
                scopy(d, 0, g).wait_send()
            for step in range(last - 1):
                @pl.when(jnp.logical_and(valid(d, step), has_next(d)))
                def _():
                    scopy(d, step + 1, g).wait_send()
        for i in range(1, groups):
            rcopy(i, g).wait_send()

    def row(i):
        return lax.rem(g + 1 + i, groups)

    def first(t, i):
        m = MATS[t]
        at = pl.ds(mo(row(i) * m.block, 16), m.block)
        return remote(grads[t].at[at, pl.ds(mo((1 - h) * m.half, LANE), m.half)], s.buf1[t].at[at, :],
                      s.c1s.at[t, i], s.c1r.at[t, i], core, g)

    def cell1(t, i, kk, sub=None):
        return cell(s.buf1[t], MATS[t], row(i) * MATS[t].block + kk * MATS[t].quarter, sub)

    def cell2(t, i, j, sub):
        return cell(s.buf2[t], MATS[t], (row(i) * 2 + j) * MATS[t].quarter, sub)

    def cell3(t, i, sub=None):
        return cell(s.buf3[t], MATS[t], row(i) * MATS[t].quarter, sub)

    def a1(t, i, j, kk):
        return remote(cell1(t, i, kk, 0), cell2(t, i, j, 0), s.a1s.at[t, i, j], s.a1r.at[t, i, j], xn, g)

    def b1(t, i, j, kk):
        return remote(cell1(t, i, kk, 1), cell2(t, i, j, 1), s.b1s.at[t, i, j], s.b1r.at[t, i, j], yn, g)

    def a2(t, i, j):
        return remote(cell2(t, i, j, 0), cell3(t, i, 0), s.a2s.at[t, i], s.a2r.at[t, i], yn, g)

    def b2(t, i, j):
        return remote(cell2(t, i, j, 1), cell3(t, i, 1), s.b2s.at[t, i], s.b2r.at[t, i], xn, g)

    def z2(t, i):
        slot = (1 - lax.rem(g, 2)) if i == 0 else lax.rem(g, 2)
        return remote(cell3(t, i), s.zbuf[t].at[slot], s.z2s.at[t, slot], s.z2r.at[t, slot], rep, flip(g, 1))

    def z2_got(t, slot):
        return remote(s.zbuf[t].at[slot], s.zbuf[t].at[slot], s.z2s.at[t, slot], s.z2r.at[t, slot], rep, flip(g, 1))

    def z3(t):
        return remote(cell3(t, 1), s.zbuf[t].at[2], s.z2s.at[t, 2], s.z2r.at[t, 2], rep, flip(g, 2))

    def r1(t, i):
        m = MATS[t]
        first(t, i).wait_recv()
        at = pl.ds(mo(row(i) * m.block, 16), m.block)
        mine = grads[t].at[at, pl.ds(mo(h * m.half, LANE), m.half)]
        add_rows(s.buf1[t].at[at, :], mine, s.buf1[t].at[at, :], m.block)
        for j in range(2):
            a1(t, i, j, 2 * j + (1 - x)).start()
            b1(t, i, j, 2 * (1 - y) + j).start()

    def r2(t, i):
        m = MATS[t]
        for j in range(2):
            a1(t, i, j, 2 * j + x).wait_recv()
            add_rows(cell2(t, i, j, 0), cell1(t, i, 2 * j + x, 0), cell2(t, i, j, 0), m.sub[0][1])
        a2(t, i, 1 - y).start()
        for j in range(2):
            b1(t, i, j, 2 * y + j).wait_recv()
            add_rows(cell2(t, i, j, 1), cell1(t, i, 2 * y + j, 1), cell2(t, i, j, 1), m.sub[1][1])
        b2(t, i, 1 - x).start()

    def r3(t, i):
        m = MATS[t]
        a2(t, i, y).wait_recv()
        b2(t, i, x).wait_recv()
        add_rows(cell3(t, i, 0), cell2(t, i, y, 0), cell3(t, i, 0), m.sub[0][1])
        add_rows(cell3(t, i, 1), cell2(t, i, x, 1), cell3(t, i, 1), m.sub[1][1])
        if i % 2 == 0:
            z2(t, i).start()

    def r3b(t):
        z2_got(t, 0).wait_recv()
        add_rows(cell3(t, 1), cell3(t, 1), s.zbuf[t].at[0], MATS[t].quarter)
        z3(t).start()

    def fpart(t, kk, hh, sub=None):
        return part(outs[t], MATS[t], 0, kk, hh, sub)

    def keep(t):
        return pltpu.make_async_copy(s.fin[t].at[0], fpart(t, k, h), s.os.at[t])

    def xsend(t):
        return remote(s.fin[t].at[0], fpart(t, k, h), s.oxs.at[t], s.oxr.at[t], xn, g)

    def ysend(t):
        return remote(s.fin[t].at[0], fpart(t, k, h), s.oys.at[t], s.oyr.at[t], yn, g)

    def xgot(t):
        return remote(fpart(t, kx, h), fpart(t, kx, h), s.oxs.at[t], s.oxr.at[t], xn, g)

    def ygot(t):
        return remote(fpart(t, ky, h), fpart(t, ky, h), s.oys.at[t], s.oyr.at[t], yn, g)

    def fwd(t, sub, kk):
        reg = fpart(t, kk, h, sub)
        return remote(reg, reg, (s.oas, s.obs)[sub].at[t], (s.oar, s.obr)[sub].at[t], (yn, xn)[sub], g)

    def cross(t, hh):
        reg = slab(outs[t], MATS[t], 0, hh)
        return remote(reg, reg, s.ocs.at[t], s.ocr.at[t], core, g)

    def r4(t):
        m = MATS[t]
        z2_got(t, 1).wait_recv()
        z3(t).wait_recv()
        mine = cell3(t, last)

        def body(n):
            at = pl.ds(mo(n * 16, 16), 16)
            total = mine[at, :].astype(F32) + s.zbuf[t][1, at, :].astype(F32) + s.zbuf[t][2, at, :].astype(F32)
            s.fin[t][0, at, :] = total.astype(BF)
        loop(m.quarter // 16, body)
        for b in range(highs):
            cp = remote(s.fin[t].at[0], s.fin[t].at[1 + b], s.fxs.at[t, b], s.fxr.at[t, b], flip(rep, 8 << b), g)
            cp.start()
            cp.wait()
            add_rows(s.fin[t].at[0], s.fin[t].at[0], s.fin[t].at[1 + b], m.quarter)
        keep(t).start()
        xsend(t).start()
        ysend(t).start()

    def r5(t):
        xgot(t).wait_recv()
        fwd(t, 0, kx).start()
        ygot(t).wait_recv()
        fwd(t, 1, ky).start()

    def r6(t):
        fwd(t, 0, kd).wait_recv()
        fwd(t, 1, kd).wait_recv()
        keep(t).wait()
        cross(t, h).start()

    partners = [(core, g), (xn, g), (yn, g)] + [(flip(rep, 8 << b), g) for b in range(highs)]
    bit = 1
    while bit < groups:
        partners.append((rep, flip(g, bit)))
        bit *= 2

    def smcopy(j):
        return remote(s.smacc.at[j], s.smin.at[j], s.sms.at[j], s.smr.at[j], *partners[j])

    def small(j):
        if j:
            smcopy(j - 1).wait_recv()
            s.smacc[j] = s.smacc[j - 1] + s.smin[j - 1]
        if j < len(partners):
            smcopy(j).start()
        else:
            osm[...] = s.smacc[j, g]

    def crossed():
        for t in ORDER:
            cross(t, 1 - h).wait_recv()

    def chunks_sent():
        for t in ORDER:
            for i in range(groups):
                first(t, i).wait_send()
                for j in range(2):
                    a1(t, i, j, 2 * j + x).wait_send()
                    b1(t, i, j, 2 * y + j).wait_send()
                a2(t, i, y).wait_send()
                b2(t, i, x).wait_send()
                if i % 2 == 0:
                    z2(t, i).wait_send()
            z3(t).wait_send()

    def outs_sent():
        for i in range(1, groups):
            vcopy(i, g).wait_send()
        for t in ORDER:
            xsend(t).wait_send()
            ysend(t).wait_send()
            fwd(t, 0, kx).wait_send()
            fwd(t, 1, ky).wait_send()
            cross(t, h).wait_send()
        for j in range(len(partners)):
            smcopy(j).wait_send()

    def project(j):
        project_block(j, s.fa, s.gain1, s.shift1, s.qvbias, s.wq, s.q_all, s.k_all, s.v_all, s.normed, tokens)

    def attention(p):
        loop(2, lambda i: attend_pair(p + i, g, s.q_all, s.k_all, s.v_all, s.attended, s.stats, tokens))

    def block(n):
        return pl.ds(mo(n * 256, 256), 256)

    def to_middle():
        def body(n):
            c = block(n)
            s.middle[:, c] = nn(s.attended[...], s.wo[:, c]) + s.obias[0:1, c] + fr[:, c].astype(F32)
        loop(D // 256, body)
        value, inverse = normalize(s.middle[...])
        s.normal[...] = value
        s.inverse[...] = jnp.broadcast_to(inverse, (tokens, LANE))
        s.normed[...] = (value * s.gain2[...] + s.shift2[...]).astype(BF)

    def hidden(i):
        def body(j):
            n = row(i) * (FF // 256 // groups) + j
            c = block(n)
            u = nn(s.normed[...], s.wu[:, c]) + s.ubias[0:1, c]
            bell = 0.5 * (1.0 + lax.erf(u * ROOT_HALF))
            s.act[:, c] = (u * bell).astype(BF)
            slope = bell + u * jnp.exp(-0.5 * u * u) * ROOT_TWO_PI
            grad = nt(ct[...], s.wd[block(n), :]) * slope
            s.v_up[0:1, c] = jnp.sum(grad, axis=0, keepdims=True)
            s.pre[:, c] = grad.astype(BF)
        loop(FF // 256 // groups, body)

    def to_output():
        def body(n):
            c = block(n)
            out_frames[:, c] = (nn(s.act[...], s.wd[:, c]) + s.dbias[0:1, c] + s.middle[:, c]).astype(BF)
        loop(D // 256, body)

    def back_up():
        def body(n):
            s.wide[:, block(n)] = nt(s.pre[...], s.wu[block(n), :])
        loop(D // 256, body)

    def back_norm():
        upstream, normal = s.wide[...], s.normal[...]
        s.v_gain2[...] = jnp.sum(upstream * normal, axis=0, keepdims=True)
        s.v_shift2[...] = jnp.sum(upstream, axis=0, keepdims=True)
        total = ct[...].astype(F32) + norm_back(upstream, normal, s.inverse[:, 0:1], s.gain2[...])
        s.mgrad[...] = total
        s.half[...] = total.astype(BF)
        s.v_out[...] = jnp.sum(total, axis=0, keepdims=True)
        s.v_down[...] = jnp.sum(ct[...].astype(F32), axis=0, keepdims=True)

        def body(n):
            s.a_all[own, block(n)] = nt(s.half[...], s.wo[block(n), :]).astype(BF)
        own = pl.ds(mo(g * tokens, 16), tokens)
        loop(D // 256, body)
        lanes = lax.broadcasted_iota(jnp.int32, (tokens, LANE), 1)
        mask = head_mask(tokens)
        stats = s.stats[...]
        for p in range(HEADS // 2):
            c = slice(p * LANE, (p + 1) * LANE)
            product = s.a_all[own, c].astype(F32) * s.attended[:, c].astype(F32)
            for side in range(2):
                mine = jnp.where(mask if side == 0 else jnp.logical_not(mask), product, 0.0)
                stats = jnp.where(lanes == HEADS + 2 * p + side, jnp.sum(mine, axis=-1, keepdims=True), stats)
        s.stats[...] = stats
        s.rows3[groups] = stats.T[0:2 * HEADS, :]

    def weight(t, i, left, right):
        m = MATS[t]
        s.turned[0:m.block, :] = left[:, pl.ds(mo(row(i) * m.block, LANE if m.block % LANE == 0 else 64), m.block)].T

        def body(n):
            c = block(n)
            grads[t][pl.ds(mo(row(i) * m.block, 16), m.block), c] = nn(s.turned[0:m.block, :], right[:, c]).astype(BF)
        loop(m.cols // 256, body)
        first(t, i).start()

    def turn(left, out):
        out[...] = left[...].T

    def weight_all(t, left, right):
        def body(n):
            c = block(n)
            grads[t][:, c] = nn(left[...], right[:, c]).astype(BF)
        loop(MATS[t].cols // 256, body)
        for i in (0, 2, 1, 3):
            first(t, i).start()

    def queries(p):
        loop(2, lambda i: query_back(p + i, g, s.q_all, s.k_all, s.v_all, s.a_all, s.stats, s.pgrad, s.v_qv, tokens))

    def keys(p):
        loop(2, lambda i: key_back(p + i, g, s.q_all, s.k_all, s.v_all, s.a_all, s.rows, s.pgrad, s.v_qv, tokens))

    def to_inputs():
        normal, _ = normalize(fr[...].astype(F32))
        s.normed[...] = (normal * s.gain1[...] + s.shift1[...]).astype(BF)
        turn(s.normed, s.turned)

    def input_grad():
        def body(n):
            s.wide[:, block(n)] = nt(s.pgrad[...], s.wq[block(n), :])
        loop(D // 256, body)
        normal, inverse = normalize(fr[...].astype(F32))
        upstream = s.wide[...]
        s.v_gain1[...] = jnp.sum(upstream * normal, axis=0, keepdims=True)
        s.v_shift1[...] = jnp.sum(upstream, axis=0, keepdims=True)
        frames_grad[...] = (s.mgrad[...] + norm_back(upstream, normal, inverse, s.gain1[...])).astype(BF)
        fill_image(s.smacc.at[0], range(SROWS), (
            (GAIN_ONE, s.v_gain1), (SHIFT_ONE, s.v_shift1), (QV_BIAS, s.v_qv), (OUT_BIAS, s.v_out), (GAIN_TWO, s.v_gain2),
            (SHIFT_TWO, s.v_shift2), (UP_BIAS, s.v_up), (DOWN_BIAS, s.v_down)))
        small(0)

    barrier, peers = greet(rep, g, groups)
    peers += [(flip(rep, 8 << b), g) for b in range(highs)]
    for n in range(3):
        piece_load(n).start()
    for cp in small_loads():
        cp.start()
    own_frames = pltpu.make_async_copy(fr, zregion(4, g), s.ssem.at[len(SMALL)])
    own_frames.start()
    do_barrier(barrier, peers)
    relayout(0)
    own_send(0)
    relayout(1)
    own_send(1)
    relayout(2)
    own_send(2)
    for cp in small_loads():
        cp.wait()
    s.smb[...] = jnp.zeros_like(s.smb)
    count = sum(c for _, c in SMALL)
    s.smb[0:count, :] = s.spbuf[...].astype(F32).reshape(count, LANE)
    for i in range(1, groups):
        vcopy(i, g).start()
    both(0, 0, 0)
    both(0, 0, 1)
    own_frames.wait()
    own_send(4)
    relayout(3)
    own_send(3)
    for n in (4, 5, 6):
        relayout(n)
    both(0, 0, 2)
    both(1, 0, 0)
    both(1, 0, 1)
    both(0, 1, 0)
    both(0, 2, 0)
    both(1, 0, 2)
    both(2, 0, 0)
    both(2, 0, 1)
    for n in (7, 8, 9):
        relayout(n)
    both(2, 0, 2)
    for i in range(1, groups):
        vcopy(i, lax.rem(g + groups - i, groups)).wait_recv()
    s.sm[g] = s.smb[...]
    for spot, ref in ((GAIN_ONE, s.gain1), (SHIFT_ONE, s.shift1), (QV_BIAS, s.qvbias), (GAIN_TWO, s.gain2), (SHIFT_TWO, s.shift2),
                      (OUT_BIAS, s.obias), (UP_BIAS, s.ubias), (DOWN_BIAS, s.dbias)):
        assemble(s.sm, spot, ref)
    s.stats[...] = jnp.zeros_like(s.stats)
    both(0, 4, 0)
    for n in (10, 11, 12):
        relayout(n)
    both(1, 1, 0)
    both(1, 2, 0)
    for step in range(last):
        both(3, 0, step)
    project(g)
    both(0, 3, 0)

    def project_rows(step):
        for d in range(2):
            @pl.when(valid(d, step))
            def _():
                project(row_of(d, step))
    project_rows(0)
    both(0, 4, 1)
    for n in (13, 14, 15):
        relayout(n)
    both(2, 1, 0)
    both(2, 2, 0)
    both(1, 3, 0)
    both(0, 1, 1)
    both(0, 2, 1)
    project_rows(1)
    both(0, 3, 1)
    both(2, 3, 0)
    both(1, 1, 1)
    both(1, 2, 1)
    both(0, 4, 2)
    project_rows(2)
    both(0, 1, 2)
    both(1, 3, 1)
    both(2, 1, 1)
    both(2, 2, 1)
    both(0, 2, 2)
    attention(0)
    both(0, 3, 2)
    both(1, 1, 2)
    both(2, 3, 1)
    attention(2)
    both(1, 2, 2)
    attention(4)
    both(1, 3, 2)
    both(2, 1, 2)
    both(2, 2, 2)
    both(2, 3, 2)
    rest = [(t, step) for step in range(last) for t in (1, 2, 3)]
    for t, step in rest:
        if t == 1:
            both(3, t, step)
    to_middle()
    for t, step in rest:
        if t > 1:
            both(3, t, step)
    hidden(0)
    weight(3, 0, s.act, ct)
    hidden(1)
    hidden(2)
    r1(3, 0)
    hidden(3)
    back_up()
    back_norm()
    share_start()
    weight(3, 2, s.act, ct)
    r2(3, 0)
    weight(3, 1, s.act, ct)
    r1(3, 2)
    weight(3, 3, s.act, ct)
    r1(3, 1)
    turn(s.normed, s.turned2)
    r1(3, 3)
    r2(3, 2)
    weight_all(2, s.turned2, s.pre)
    r2(3, 1)
    r1(2, 0)
    to_output()
    share_step(0)
    r1(2, 2)
    r2(3, 3)
    turn(s.attended, s.turned2)
    weight_all(1, s.turned2, s.half)
    gather_sent()
    r2(2, 0)
    r1(2, 1)
    queries(0)
    share_step(1)
    r2(2, 2)
    r1(2, 3)
    queries(2)
    queries(4)
    r2(2, 1)
    r1(1, 0)
    r1(1, 2)
    share_step(2)
    share_rows()
    r3(3, 0)
    r3(3, 2)
    keys(0)
    r2(2, 3)
    r1(1, 1)
    r1(1, 3)
    r3(3, 1)
    r3(3, 3)
    r2(1, 0)
    r2(1, 2)
    to_inputs()
    keys(2)
    r2(1, 1)
    r2(1, 3)
    keys(4)
    r3b(3)
    r3(2, 0)
    r3(2, 2)
    weight_all(0, s.turned, s.pgrad)
    r3(2, 1)
    r3(2, 3)
    input_grad()
    r1(0, 0)
    r1(0, 2)
    r4(3)
    r2(0, 0)
    r2(0, 2)
    r1(0, 1)
    r1(0, 3)
    r3(1, 0)
    r3(1, 2)
    r3b(2)
    r3(0, 0)
    r3(0, 2)
    r5(3)
    r2(0, 1)
    small(1)
    r3(1, 1)
    r3(1, 3)
    r2(0, 3)
    r4(2)
    r6(3)
    r3b(1)
    r3(0, 1)
    r3(0, 3)
    r3b(0)
    r5(2)
    r4(1)
    small(2)
    r6(2)
    r4(0)
    r5(1)
    small(3)
    r5(0)
    small(4)
    r6(1)
    r6(0)
    for j in range(5, len(partners) + 1):
        small(j)
    crossed()
    share_sent()
    chunks_sent()
    outs_sent()


def layer(frames, cotangent, params, groups, reps):
    dma = pltpu.SemaphoreType.DMA
    tokens = frames.shape[0]
    clip = tokens * groups
    highs = (reps // 8).bit_length() - 1
    steps = 3 + highs + groups.bit_length() - 1
    n = 2 * (groups - 1)

    def bf(*shape):
        return pltpu.VMEM(shape, BF)

    def wide(*shape):
        return pltpu.VMEM(shape, F32)

    scratch = {name: bf(m.block * groups, m.cols) for name, m in zip(("wq", "wo", "wu", "wd"), MATS)}
    scratch.update(go=bf(D, D), gu=bf(D, FF), gd=bf(FF, D))
    scratch.update(buf1=[bf(m.block * groups, m.half) for m in MATS], buf2=[bf(m.quarter * groups * 2, m.half) for m in MATS],
                   buf3=[bf(m.quarter * groups, m.half) for m in MATS], zbuf=[bf(groups - 1, m.quarter, m.half) for m in MATS],
                   fin=[bf(highs + 1, m.quarter, m.half) for m in MATS])
    scratch.update(fa=bf(clip, D), q_all=bf(clip, D), k_all=bf(clip, D), v_all=bf(clip, D), a_all=bf(clip, D))
    scratch.update(attended=bf(tokens, D), normed=bf(tokens, D), half=bf(tokens, D),
                   act=bf(tokens, FF), pre=bf(tokens, FF), pgrad=bf(tokens, 3 * D), turned=bf(D, tokens), turned2=bf(D, tokens))
    scratch.update(middle=wide(tokens, D), normal=wide(tokens, D), mgrad=wide(tokens, D), wide=wide(tokens, D),
                   inverse=wide(tokens, LANE), stats=wide(tokens, LANE))
    scratch.update(rows3=wide(groups + 1, 2 * HEADS, tokens), rows=wide(2 * HEADS, clip))
    scratch.update({name: wide(1, D) for name in ("gain1", "shift1", "gain2", "shift2", "obias", "dbias", "v_gain1", "v_shift1",
                                                  "v_gain2", "v_shift2", "v_out", "v_down")})
    scratch.update(qvbias=wide(1, 2 * D), v_qv=wide(1, 2 * D), ubias=wide(1, FF), v_up=wide(1, FF))
    piece = max(m.quarter * m.tiles + 8 for m in MATS)
    scratch.update(pbuf=bf(3, 1, piece * LANE), fbuf=wide(piece, LANE), spbuf=bf(1, sum(c for _, c in SMALL) * LANE),
                   smb=wide(SROWS, LANE), sm=wide(groups, SROWS, LANE),
                   smacc=wide(steps + 1, groups, SROWS, LANE), smin=wide(steps, groups, SROWS, LANE))
    scratch.update(lsem=dma((3,)), ssem=dma((len(SMALL) + 1,)), zs=dma((5, 2, groups)), zr=dma((5, 2, groups)))
    scratch.update({name: dma((4, n)) for name in ("xs", "xr", "ys", "yr", "fas", "far", "fbs", "fbr", "cs", "cr")})
    scratch.update({name: dma((groups,)) for name in ("ms", "mr", "rs", "rr")})
    scratch.update(szs=dma((2, groups)), szr=dma((2, groups)))
    scratch.update({name: dma((4, groups)) for name in ("c1s", "c1r", "a2s", "a2r", "b2s", "b2r", "z2s", "z2r")})
    scratch.update({name: dma((4, groups, 2)) for name in ("a1s", "a1r", "b1s", "b1r")})
    scratch.update({name: dma((4, max(highs, 1))) for name in ("fxs", "fxr")})
    scratch.update({name: dma((4,)) for name in ("os", "oxs", "oxr", "oys", "oyr", "oas", "oar", "obs", "obr", "ocs", "ocr")})
    scratch.update(sms=dma((steps,)), smr=dma((steps,)))
    vmem, hbm = pl.BlockSpec(memory_space=pltpu.VMEM), pl.BlockSpec(memory_space=pl.ANY)
    sds = jax.ShapeDtypeStruct
    names = tuple(scratch)
    flat, tree = jax.tree.flatten(list(scratch.values()))

    def body(*refs):
        fixed = 10
        layer_kernel(groups, highs, names, *refs[:fixed], *jax.tree.unflatten(tree, refs[fixed:]))

    return pl.pallas_call(
        body,
        out_shape=[sds((m.block, m.cols), BF) for m in MATS] + [sds((SROWS, LANE), F32), sds((tokens, D), BF), sds((tokens, D), BF)],
        in_specs=[vmem, vmem, hbm],
        out_specs=[hbm] * 4 + [vmem] * 3,
        scratch_shapes=flat,
        compiler_params=pltpu.CompilerParams(collective_id=0, has_side_effects=True, vmem_limit_bytes=67043328),
        name="layer",
    )(frames, cotangent, params)


BETA_ONE = 0.9
BETA_TWO = 0.98
ADAM_EPS = 1e-06
LEARN_RATE = 0.006
DECAY = 0.01
ADAM_STEP = 4
ROWS = 1792
CHUNKS = -(-FROWS // ROWS)
SUB = 224


def flatten(m, block, flat, late):
    def body(i):
        base = m.row0 + i * (48 * m.tiles)
        for c in range(m.tiles):
            tile = block[pl.ds(mo(i * 48, 16), 48), c * LANE:(c + 1) * LANE].astype(F32)
            if m.shifted:
                tile = pltpu.roll(tile, 64, 1)
                late[pl.ds(base + c + 1, 48, stride=m.tiles), :] = tile
            flat[pl.ds(base + c, 48, stride=m.tiles), :] = tile
    loop(m.block // 48, body)


def adam_kernel(scale, gq, go, gu, gd, sm, p_hbm, m_hbm, v_hbm, fo, fg, o_g, o_p, o_m, o_v, o_fo, o_fg,
                bq, bo, bu, bd, flat, late, pb, mb, vb, gb, nb, frames, bsem, isem, osem, fsem):
    blocks = (bq, bo, bu, bd)

    def view(ref, c):
        return ref.at[:, pl.ds(c * ROWS * LANE, min(ROWS, FROWS - c * ROWS) * LANE)]

    loads = [pltpu.make_async_copy(a, b, bsem.at[i]) for i, (a, b) in enumerate(zip((gq, go, gu, gd), blocks))]
    pairs = ((p_hbm, pb), (m_hbm, mb), (v_hbm, vb))
    ins = [[pltpu.make_async_copy(view(a, c), view(b, c), isem.at[c, i]) for i, (a, b) in enumerate(pairs)] for c in range(CHUNKS)]
    results = ((gb, o_g), (nb, o_p), (mb, o_m), (vb, o_v))
    puts = [[pltpu.make_async_copy(view(a, c), view(b, c), osem.at[c, i]) for i, (a, b) in enumerate(results)] for c in range(CHUNKS)]
    takes = [pltpu.make_async_copy(a, frames.at[i], fsem.at[i]) for i, a in enumerate((fo, fg))]
    gives = [pltpu.make_async_copy(frames.at[i], a, fsem.at[2 + i]) for i, a in enumerate((o_fo, o_fg))]
    def fetch(c):
        if c < CHUNKS:
            for cp in ins[c]:
                cp.start()

    loads[0].start()
    fetch(0)
    loads[1].start()
    fetch(1)
    loads[2].start()

    def update(c):
        for cp in ins[c]:
            cp.wait()

        def body(j):
            start = c * ROWS + j * SUB
            at = pl.ds(mo(start, 8), SUB)
            lanes = (slice(None), pl.ds(mo(start * LANE, LANE), SUB * LANE))
            number = start + lax.broadcasted_iota(jnp.int32, (SUB, LANE), 0)
            low = lax.broadcasted_iota(jnp.int32, (SUB, LANE), 1) < 64
            grad = jnp.where(jnp.logical_and(number > UP.row0, low), late[at, :], flat[at, :]).reshape(1, SUB * LANE) * scale
            first = BETA_ONE * mb[lanes] + (1.0 - BETA_ONE) * grad
            second = BETA_TWO * vb[lanes] + (1.0 - BETA_TWO) * grad * grad
            gb[lanes] = grad
            mb[lanes] = first
            vb[lanes] = second
            first_hat = first * (1.0 / (1.0 - BETA_ONE**ADAM_STEP))
            second_hat = second * (1.0 / (1.0 - BETA_TWO**ADAM_STEP))
            current = pb[lanes].astype(F32)
            nb[lanes] = current - LEARN_RATE * (first_hat / (jnp.sqrt(second_hat) + ADAM_EPS) + DECAY * current)
        loop(-(-min(ROWS, FROWS - c * ROWS) // SUB), body)
        fetch(c + 2)
        for cp in puts[c]:
            cp.start()

    loads[0].wait()
    flatten(QKV, bq, flat, late)
    flat[0:3, :] = sm[0:3, :]
    update(0)
    loads[1].wait()
    flatten(OUT, bo, flat, late)
    flat[3459:3462, :] = sm[3:6, :]
    update(1)
    loads[2].wait()
    flatten(UP, bu, flat, late)
    flat[4614:4618, :] = sm[6:10, :]
    flat[4618:4619, 0:64] = sm[10:11, 0:64]
    flat[9226:9227, 64:128] = sm[11:12, 64:128]
    update(2)
    loads[3].start()
    for cp in takes:
        cp.start()
    update(3)
    update(4)
    loads[3].wait()
    flatten(DOWN, bd, flat, late)
    for ref in (flat, late):
        ref[9227:9232, :] = sm[12:17, :]
        ref[9232:9233, 0:64] = sm[17:18, 0:64]
        ref[13841:13842, :] = sm[19:20, :]
    flat[13840:13841, 64:128] = sm[18:19, 64:128]
    update(5)
    for cp in takes:
        cp.wait()
    for cp in gives:
        cp.start()
    for c in range(6, CHUNKS):
        update(c)
    for cp in gives:
        cp.wait()
    for chunk in puts:
        for cp in chunk:
            cp.wait()


def adam(blocks, smalls, params, first, second, reps, *outputs):
    vmem, hbm = pl.BlockSpec(memory_space=pltpu.VMEM), pl.BlockSpec(memory_space=pl.ANY)
    dma = pltpu.SemaphoreType.DMA
    row = pltpu.VMEM((1, CHUNKS * ROWS * LANE), F32)
    return pl.pallas_call(
        functools.partial(adam_kernel, 1.0 / reps),
        out_shape=[jax.ShapeDtypeStruct((1, FLAT), F32)] * 4 + [jax.ShapeDtypeStruct(o.shape, o.dtype) for o in outputs],
        in_specs=[hbm] * 4 + [vmem] + [hbm] * 5,
        out_specs=[hbm] * 6,
        scratch_shapes=[pltpu.VMEM(b.shape, BF) for b in blocks] + [pltpu.VMEM((CHUNKS * ROWS, LANE), F32)] * 2
        + [pltpu.VMEM((1, CHUNKS * ROWS * LANE), BF)] + [row] * 4 + [pltpu.VMEM((2,) + outputs[0].shape, BF)]
        + [dma((4,)), dma((CHUNKS, 3)), dma((CHUNKS, 4)), dma((4,))],
        compiler_params=pltpu.CompilerParams(vmem_limit_bytes=67043328),
        name="adam",
    )(*blocks, smalls, params, first, second, *outputs)


def on_device(frames, cotangent, params, first_moment, second_moment):
    groups, reps = lax.axis_size("grp"), lax.axis_size("rep")
    *blocks, small, out_frames, frames_grad = layer(frames, cotangent, params, groups, reps)
    param_grad, new_params, new_first, new_second, out_frames, frames_grad = adam(
        blocks, small, params, first_moment, second_moment, reps, out_frames, frames_grad)
    return (out_frames, frames_grad, param_grad, new_params, new_first, new_second)


def solution(mesh):
    in_specs = (
        P(("rep", "grp"), None),
        P(("rep", "grp"), None),
        P("grp", None),
        P("grp", None),
        P("grp", None),
    )
    out_specs = (
        P(("rep", "grp"), None),
        P(("rep", "grp"), None),
        P("grp", None),
        P("grp", None),
        P("grp", None),
        P("grp", None),
    )
    return jax.shard_map(
        on_device, mesh=mesh, in_specs=in_specs, out_specs=out_specs, check_vma=False
    )
```

```python
import functools
import types

import jax
import jax.numpy as jnp
from jax import lax
from jax.sharding import PartitionSpec as P
from jax.experimental import pallas as pl
from jax.experimental.pallas import tpu as pltpu

MESH = pl.DeviceIdType.MESH
BF = jnp.bfloat16
F32 = jnp.float32
D = 768
FF = 3072
HDIM = 64
LANE = 128
FLAT = 1771776
FROWS = FLAT // LANE


class Mat:
    def __init__(self, offset, block, cols, suba, subb):
        self.offset, self.block, self.cols = offset, block, cols
        self.tiles = cols // LANE
        self.row0 = offset // LANE
        self.shifted = offset % LANE != 0
        self.quarter = block // 4
        self.half = cols // 2
        self.sub = (suba, subb)


QKV = Mat(384, 192, 2304, (0, 48, 0, 640), (0, 48, 640, 512))
OUT = Mat(443136, 192, 768, (0, 48, 0, 128), (0, 48, 128, 256))
UP = Mat(591168, 192, 3072, (0, 48, 0, 768), (0, 48, 768, 768))
DOWN = Mat(1181760, 768, 768, (0, 96, 0, 384), (96, 96, 0, 384))
MATS = (QKV, OUT, UP, DOWN)
SMALL = ((0, 3), (3459, 3), (4614, 5), (9226, 7), (13840, 2))
SROWS = 24


def flip(index, bit):
    return index + bit - 2 * bit * ((index // bit) % 2)


def mo(value, by):
    return pl.multiple_of(value, by)


def part(ref, m, r, k, h, sub=None):
    r0, rn, c0, cn = m.sub[sub] if sub is not None else (0, m.quarter, 0, m.half)
    row = mo(r * m.block + k * m.quarter + r0, 16)
    col = mo(h * m.half + c0, LANE)
    return ref.at[pl.ds(row, rn), pl.ds(col, cn)]


def slab(ref, m, r, h):
    return ref.at[pl.ds(mo(r * m.block, 16), m.block), pl.ds(mo(h * m.half, LANE), m.half)]


def remote(src, dst, send, recv, rep, grp):
    return pltpu.make_async_remote_copy(
        src_ref=src, dst_ref=dst, send_sem=send, recv_sem=recv,
        device_id={"rep": rep, "grp": grp}, device_id_type=MESH)


def greet(rep, g, groups):
    barrier = pltpu.get_barrier_semaphore()
    peers = [(flip(rep, b), g) for b in (1, 2, 4)]
    peers += [(rep, lax.rem(g + i, groups)) for i in range(1, groups)]
    return barrier, peers


def do_barrier(barrier, peers):
    for r, gg in peers:
        pl.semaphore_signal(barrier, inc=1, device_id={"rep": r, "grp": gg}, device_id_type=MESH)
    pl.semaphore_wait(barrier, len(peers))


def add_rows(dst, a, b, rows, step=16):
    def body(i, c):
        at = pl.ds(mo(i * step, 16), step)
        dst[at, :] = (a[at, :].astype(F32) + b[at, :].astype(F32)).astype(dst.dtype)
        return c
    lax.fori_loop(0, rows // step, body, 0)


EPS_NORM = 1e-05
ROOT_HALF = 0.7071067811865476
ROOT_TWO_PI = 0.3989422804014327
HEADS = D // HDIM
GAIN_ONE, SHIFT_ONE, QV_BIAS, OUT_BIAS, GAIN_TWO, SHIFT_TWO, UP_BIAS, DOWN_BIAS = (
    (0, 3), (3, 3), (6, 6), (12, 3), (15, 3), (18, 3), (23, 12), (37, 3))


def low_lanes():
    return lax.broadcasted_iota(jnp.int32, (1, LANE), 1) < 64


def assemble(sm, place, out):
    first, count = place
    halves = [(gi, first + i) for gi in range(sm.shape[0]) for i in range(count)]
    for t in range(len(halves) // 2):
        (g0, h0), (g1, h1) = halves[2 * t], halves[2 * t + 1]
        a = sm[g0, h0 // 2:h0 // 2 + 1, :]
        b = sm[g1, h1 // 2:h1 // 2 + 1, :]
        a = pltpu.roll(a, 64, 1) if h0 % 2 else a
        b = b if h1 % 2 else pltpu.roll(b, 64, 1)
        out[0:1, t * LANE:(t + 1) * LANE] = jnp.where(low_lanes(), a, b)


def fill_image(image, rows, vectors):
    where = {}
    for place, ref in vectors:
        for i in range(place[1]):
            where[place[0] + i] = (place[1], i, ref)
    for gi in range(image.shape[0]):
        for r in rows:
            parts = []
            for side in range(2):
                spot = where.get(2 * r + side)
                if spot is None:
                    parts.append(jnp.zeros((1, LANE), F32))
                    continue
                count, i, ref = spot
                q = gi * count + i
                v = ref[0:1, q // 2 * LANE:(q // 2 + 1) * LANE]
                parts.append(v if q % 2 == side else pltpu.roll(v, 64, 1))
            image[gi, r:r + 1, :] = jnp.where(low_lanes(), parts[0], parts[1])


def mean(v):
    return jnp.sum(v, axis=-1, keepdims=True) * (1.0 / D)


def normalize(v):
    centered = v - mean(v)
    inverse = lax.rsqrt(mean(centered * centered) + EPS_NORM)
    return centered * inverse, inverse


def norm_back(upstream, normal, inverse, gain):
    s = upstream * gain
    return inverse * (s - mean(s) - normal * mean(s * normal))


def nn(a, b):
    return lax.dot_general(a, b, (((1,), (0,)), ((), ())), preferred_element_type=F32)


def nt(a, b):
    return lax.dot_general(a, b, (((1,), (1,)), ((), ())), preferred_element_type=F32)


def loop(count, body):
    def step(i, c):
        body(i)
        return c
    lax.fori_loop(0, count, step, 0)


def head_mask(rows):
    return lax.broadcasted_iota(jnp.int32, (rows, LANE), 1) < HDIM


def third(p, n):
    return pl.ds(mo(n * D + p * LANE, LANE), LANE)


def project_block(j, fa, gain, shift, bias, wq, qkv, normed, tokens):
    at = pl.ds(mo(j * tokens, 16), tokens)
    normal, _ = normalize(fa[at, :].astype(F32))
    normed[...] = (normal * gain[...] + shift[...]).astype(BF)

    def body(n):
        col = pl.ds(mo(n * 256, 256), 256)
        qkv[at, col] = (nn(normed[...], wq[:, col]) + bias[0:1, col]).astype(BF)
    loop(3 * D // 256, body)


def attend_pair(p, g, qkv, attended, stats, tokens):
    col = third(p, 0)
    query = qkv[pl.ds(mo(g * tokens, 16), tokens), col] * jnp.asarray(HDIM**-0.5, BF)
    keys, values = qkv[:, third(p, 1)], qkv[:, third(p, 2)]
    mask = head_mask(tokens)
    zero = jnp.zeros_like(query)
    lanes = lax.broadcasted_iota(jnp.int32, (tokens, LANE), 1)
    results = []
    for side in range(2):
        scores = nt(jnp.where(mask, query, zero) if side == 0 else jnp.where(mask, zero, query), keys)
        highest = jnp.max(scores, axis=-1, keepdims=True)
        shares = jnp.exp(scores - highest)
        total = jnp.sum(shares, axis=-1, keepdims=True)
        results.append(nn(shares.astype(BF), values) * (1.0 / total))
        stats[...] = jnp.where(lanes == 2 * p + side, highest + jnp.log(total), stats[...])
    attended[:, col] = jnp.where(mask, results[0], results[1]).astype(BF)


def query_back(p, g, qkv, a_all, stats, pgrad, v_qv, tokens):
    col = pl.ds(mo(p * LANE, LANE), LANE)
    own = pl.ds(mo(g * tokens, 16), tokens)
    scale = jnp.asarray(HDIM**-0.5, BF)
    query, upstream = qkv[own, col] * scale, a_all[own, col]
    keys, values = qkv[:, third(p, 1)], qkv[:, third(p, 2)]
    mask = head_mask(tokens)
    zero = jnp.zeros_like(query)
    lanes = lax.broadcasted_iota(jnp.int32, (tokens, LANE), 1)
    results = []
    for side in range(2):
        def pick(v):
            return jnp.where(mask, v, zero) if side == 0 else jnp.where(mask, zero, v)
        total = jnp.sum(jnp.where(lanes == 2 * p + side, stats[...], 0.0), axis=-1, keepdims=True)
        centre = jnp.sum(jnp.where(lanes == HEADS + 2 * p + side, stats[...], 0.0), axis=-1, keepdims=True)
        shares = jnp.exp(nt(pick(query), keys) - total)
        back = (shares * (nt(pick(upstream), values) - centre)).astype(BF) * scale
        results.append(nn(back, keys))
    grad = jnp.where(mask, results[0], results[1])
    pgrad[:, col] = grad.astype(BF)
    v_qv[0:1, col] = jnp.sum(grad, axis=0, keepdims=True)


def key_back(p, g, qkv, a_all, rows, pgrad, v_qv, tokens):
    col = pl.ds(mo(p * LANE, LANE), LANE)
    own = pl.ds(mo(g * tokens, 16), tokens)
    scale = jnp.asarray(HDIM**-0.5, BF)
    keys, values = qkv[own, third(p, 1)] * scale, qkv[own, third(p, 2)]
    queries, upstream = qkv[:, col], a_all[:, col]
    mask = head_mask(tokens)
    zero = jnp.zeros_like(keys)
    ks, vs = [], []
    for side in range(2):
        def pick(v):
            return jnp.where(mask, v, zero) if side == 0 else jnp.where(mask, zero, v)
        total = rows[pl.ds(2 * p + side, 1), :]
        centre = rows[pl.ds(HEADS + 2 * p + side, 1), :]
        shares = jnp.exp(nt(pick(keys), queries) - total)
        vs.append(nn(shares.astype(BF), upstream))
        back = (shares * (nt(pick(values), upstream) - centre)).astype(BF) * scale
        ks.append(nn(back, queries))
    pgrad[:, pl.ds(mo(D + p * LANE, LANE), LANE)] = jnp.where(mask, ks[0], ks[1]).astype(BF)
    grad = jnp.where(mask, vs[0], vs[1])
    pgrad[:, pl.ds(mo(2 * D + p * LANE, LANE), LANE)] = grad.astype(BF)
    v_qv[0:1, pl.ds(mo(D + p * LANE, LANE), LANE)] = jnp.sum(grad, axis=0, keepdims=True)


def cell(ref, m, row, sub=None):
    r0, rn, c0, cn = m.sub[sub] if sub is not None else (0, m.quarter, 0, m.half)
    return ref.at[pl.ds(mo(row + r0, 16), rn), pl.ds(c0, cn)]


ORDER = (3, 2, 1, 0)


def layer_kernel(groups, highs, names, fr, ct, p_ref, oq, oo, ou, od, osm, out_frames, frames_grad, *scratch):
    s = types.SimpleNamespace(**dict(zip(names, scratch)))
    rep, g = lax.axis_index("rep"), lax.axis_index("grp")
    tokens = fr.shape[0]
    share_of = lax.rem(rep, 8)
    h = lax.rem(share_of, 2)
    k = share_of // 2
    x, y = lax.rem(k, 2), k // 2
    kx, ky, kd = flip(k, 1), flip(k, 2), 3 - k
    core, xn, yn = flip(rep, 1), flip(rep, 2), flip(rep, 4)
    full = (s.wq, s.wo, s.wu, s.wd)
    outs = (oq, oo, ou, od)
    grads = (s.wu, s.go, s.gu, s.gd)
    last = groups - 1

    def has_next(d):
        return g < last if d == 0 else g > 0

    def toward(d):
        return lax.rem(g + (1 if d == 0 else last), groups)

    def row_of(d, step):
        return g - 1 - step if d == 0 else g + 1 + step

    def valid(d, step):
        return row_of(d, step) >= 0 if d == 0 else row_of(d, step) <= last

    slots = [(d, step) for step in range(last) for d in range(2)]

    def slot_of(d, step):
        return step if d else last - 1 - step

    def sent(region, sem):
        remote(region, region, sem, s.smr.at[0], core, g).wait_send()

    def arrived(region, sem):
        pltpu.make_async_copy(region, region, sem).wait()

    def piece_load(t, i, slot):
        m = MATS[t]
        count = (m.quarter * m.tiles + (2 if m.shifted else 0)) * LANE
        start = mo((m.row0 + lax.rem(k + i, 4) * (m.quarter * m.tiles)) * LANE, LANE)
        return pltpu.make_async_copy(p_ref.at[:, pl.ds(start, count)], s.pbuf.at[slot, :, pl.ds(0, count)], s.lsem.at[slot])

    def relayout(t, i, slot):
        m = MATS[t]
        piece_load(t, i, slot).wait()
        count = m.quarter * m.tiles + (8 if m.shifted else 0)
        s.fbuf[0:count, :] = s.pbuf[slot, :, 0:count * LANE].astype(F32).reshape(count, LANE)
        at = pl.ds(mo(g * m.block + lax.rem(k + i, 4) * m.quarter, 16), m.quarter)
        low = lax.broadcasted_iota(jnp.int32, (m.quarter, LANE), 1) < 64
        for c in range(m.tiles):
            a = s.fbuf[pl.ds(c, m.quarter, stride=m.tiles), :]
            if m.shifted:
                b = s.fbuf[pl.ds(c + 1, m.quarter, stride=m.tiles), :]
                a = pltpu.roll(jnp.where(low, b, a), 64, 1)
            full[t][at, c * LANE:(c + 1) * LANE] = a.astype(BF)

    def rest_load(t):
        for i in range(3):
            piece_load(t, i + 1, i).start()

    def rest(t):
        loop(3, lambda i: relayout(t, i + 1, i))

    def small_loads():
        at, result = 0, []
        for first, count in SMALL:
            result.append(pltpu.make_async_copy(
                p_ref.at[:, pl.ds(first * LANE, count * LANE)], s.spbuf.at[:, pl.ds(at * LANE, count * LANE)], s.ssem.at[0]))
            at += count
        return result

    def zregion(t, r):
        if t == 4:
            return s.fa.at[pl.ds(mo(r * tokens, 16), tokens), :]
        return part(full[t], MATS[t], r, k, h)

    def zcopy(t, d, step, r):
        reg = zregion(t, r)
        send = s.zs.at[t] if t < 4 else s.zfs.at[d, step]
        return remote(reg, reg, send, s.zr.at[t, slot_of(d, step)], rep, toward(d))

    def own_send(t):
        for d in range(2):
            @pl.when(has_next(d))
            def _():
                zcopy(t, d, 0, g).start()

    def xcopy(t, i, r, kk):
        reg = part(full[t], MATS[t], r, kk, h)
        return remote(reg, reg, s.gs.at[t, i], s.xr.at[t, i], xn, g)

    def ycopy(t, i, r, kk):
        reg = part(full[t], MATS[t], r, kk, h)
        return remote(reg, reg, s.gs.at[t, i], s.yr.at[t, i], yn, g)

    def acopy(t, i, r, kk):
        reg = part(full[t], MATS[t], r, kk, h, 0)
        return remote(reg, reg, s.gs.at[t, i], s.fr.at[t, i], yn, g)

    def bcopy(t, i, r, kk):
        reg = part(full[t], MATS[t], r, kk, h, 1)
        return remote(reg, reg, s.gs.at[t, i], s.fr.at[t, i], xn, g)

    def ccopy(t, i, r, hh):
        reg = slab(full[t], MATS[t], r, hh)
        return remote(reg, reg, s.gs.at[t, i], s.cr.at[t, i], core, g)

    def stage(number, t, d, step):
        i = slot_of(d, step)

        @pl.when(valid(d, step))
        def _():
            r = row_of(d, step)
            if number == 0:
                zcopy(t, d, step, r).wait_recv()
                if step < last - 1:
                    @pl.when(has_next(d))
                    def _():
                        zcopy(t, d, step + 1, r).start()
                if t < 4:
                    xcopy(t, i, r, k).start()
                    ycopy(t, i, r, k).start()
            if number == 1:
                xcopy(t, i, r, kx).wait_recv()
                acopy(t, i, r, kx).start()
                ycopy(t, i, r, ky).wait_recv()
                bcopy(t, i, r, ky).start()
            if number == 2:
                arrived(part(full[t], MATS[t], r, kd, h), s.fr.at[t, i])
                ccopy(t, i, r, h).start()
            if number == 3:
                ccopy(t, i, r, 1 - h).wait_recv()

    def both(number, t, step):
        for d in range(2):
            stage(number, t, d, step)

    def gather_sent():
        inner = jnp.logical_and(g > 0, g < last)
        for t in range(4):
            m = MATS[t]

            @pl.when(inner)
            def _():
                sent(full[t].at[pl.ds(0, (2 + last) * m.quarter), pl.ds(0, m.half)], s.zs.at[t])

            @pl.when(jnp.logical_not(inner))
            def _():
                sent(full[t].at[pl.ds(0, m.quarter), pl.ds(0, m.half)], s.zs.at[t])
            for i in range(last):
                sent(full[t].at[pl.ds(0, 7 * m.quarter), pl.ds(0, m.half)], s.gs.at[t, i])
        for d in range(2):
            @pl.when(has_next(d))
            def _():
                zcopy(4, d, 0, g).wait_send()
            for step in range(last - 1):
                @pl.when(jnp.logical_and(valid(d, step), has_next(d)))
                def _():
                    zcopy(4, d, step + 1, g).wait_send()

    def vcopy(i, owner):
        return remote(s.smb, s.sm.at[owner], s.ms.at[0], s.mr.at[0], rep, lax.rem(g + i, groups))

    def place(r):
        return s.a_all.at[pl.ds(mo(r * tokens, 16), tokens), :]

    def scopy(d, step, r):
        return remote(place(r), place(r), s.szs.at[d, step], s.szr.at[slot_of(d, step)], rep, toward(d))

    def rcopy(i, owner):
        return remote(s.rows3.at[groups], s.rows3.at[owner], s.rs.at[0], s.rr.at[0], rep, lax.rem(g + i, groups))

    def share_start():
        for d in range(2):
            @pl.when(has_next(d))
            def _():
                scopy(d, 0, g).start()
        for i in range(1, groups):
            rcopy(i, g).start()

    def share_step(step):
        for d in range(2):
            @pl.when(valid(d, step))
            def _():
                r = row_of(d, step)
                scopy(d, step, r).wait_recv()
                if step < last - 1:
                    @pl.when(has_next(d))
                    def _():
                        scopy(d, step + 1, r).start()

    def share_rows():
        arrived(s.rows3.at[pl.ds(0, last)], s.rr.at[0])
        for i in range(groups):
            s.rows[:, i * tokens:(i + 1) * tokens] = s.rows3[i]
        s.rows[:, pl.ds(mo(g * tokens, LANE), tokens)] = s.rows3[groups]

    def share_sent():
        for d in range(2):
            @pl.when(has_next(d))
            def _():
                scopy(d, 0, g).wait_send()
            for step in range(last - 1):
                @pl.when(jnp.logical_and(valid(d, step), has_next(d)))
                def _():
                    scopy(d, step + 1, g).wait_send()
        sent(s.rows3.at[pl.ds(0, last)], s.rs.at[0])

    def row(i):
        return lax.rem(g + 1 + i, groups)

    def first(t, i):
        m = MATS[t]
        at = pl.ds(mo(row(i) * m.block, 16), m.block)
        return remote(grads[t].at[at, pl.ds(mo((1 - h) * m.half, LANE), m.half)], s.buf1[t].at[at, :],
                      s.gone.at[t, i], s.c1r.at[t, i], core, g)

    def cell1(t, i, kk, sub=None):
        return cell(s.buf1[t], MATS[t], row(i) * MATS[t].block + kk * MATS[t].quarter, sub)

    def cell2(t, i, j, sub):
        return cell(s.buf2[t], MATS[t], (row(i) * 2 + j) * MATS[t].quarter, sub)

    def cell3(t, i, sub=None):
        return cell(s.buf3[t], MATS[t], row(i) * MATS[t].quarter, sub)

    def a1(t, i, j, kk):
        return remote(cell1(t, i, kk, 0), cell2(t, i, j, 0), s.gone.at[t, i], s.ab1r.at[t, i], xn, g)

    def b1(t, i, j, kk):
        return remote(cell1(t, i, kk, 1), cell2(t, i, j, 1), s.gone.at[t, i], s.ab1r.at[t, i], yn, g)

    def a2(t, i, j):
        return remote(cell2(t, i, j, 0), cell3(t, i, 0), s.gone.at[t, i], s.ab2r.at[t, i], yn, g)

    def b2(t, i, j):
        return remote(cell2(t, i, j, 1), cell3(t, i, 1), s.gone.at[t, i], s.ab2r.at[t, i], xn, g)

    def z2(t, i):
        slot = (1 - lax.rem(g, 2)) if i == 0 else lax.rem(g, 2)
        return remote(cell3(t, i), s.zbuf[t].at[slot], s.gone.at[t, i], s.z2r.at[t, slot], rep, flip(g, 1))

    def z2_got(t, slot):
        arrived(s.zbuf[t].at[slot], s.z2r.at[t, slot])

    def z3(t):
        return remote(cell3(t, 1), s.zbuf[t].at[2], s.gone.at[t, 1], s.z2r.at[t, 2], rep, flip(g, 2))

    def r1(t, i):
        m = MATS[t]
        first(t, i).wait_recv()
        at = pl.ds(mo(row(i) * m.block, 16), m.block)
        mine = grads[t].at[at, pl.ds(mo(h * m.half, LANE), m.half)]
        add_rows(s.buf1[t].at[at, :], mine, s.buf1[t].at[at, :], m.block)
        for j in range(2):
            a1(t, i, j, 2 * j + (1 - x)).start()
            b1(t, i, j, 2 * (1 - y) + j).start()

    def r2(t, i):
        m = MATS[t]
        arrived(s.buf2[t].at[pl.ds(mo(row(i) * 2 * m.quarter, 16), 2 * m.quarter), :], s.ab1r.at[t, i])
        for j in range(2):
            add_rows(cell2(t, i, j, 0), cell1(t, i, 2 * j + x, 0), cell2(t, i, j, 0), m.sub[0][1])
        a2(t, i, 1 - y).start()
        for j in range(2):
            add_rows(cell2(t, i, j, 1), cell1(t, i, 2 * y + j, 1), cell2(t, i, j, 1), m.sub[1][1])
        b2(t, i, 1 - x).start()

    def r3(t, i):
        m = MATS[t]
        arrived(cell3(t, i), s.ab2r.at[t, i])
        add_rows(cell3(t, i, 0), cell2(t, i, y, 0), cell3(t, i, 0), m.sub[0][1])
        add_rows(cell3(t, i, 1), cell2(t, i, x, 1), cell3(t, i, 1), m.sub[1][1])
        if i % 2 == 0:
            z2(t, i).start()

    def r3b(t):
        z2_got(t, 0)
        add_rows(cell3(t, 1), cell3(t, 1), s.zbuf[t].at[0], MATS[t].quarter)
        z3(t).start()

    def fpart(t, kk, hh, sub=None):
        return part(outs[t], MATS[t], 0, kk, hh, sub)

    def keep(t):
        return pltpu.make_async_copy(s.fin[t].at[0], fpart(t, k, h), s.os.at[t])

    def xsend(t):
        return remote(s.fin[t].at[0], fpart(t, k, h), s.osent.at[t], s.oxr.at[t], xn, g)

    def ysend(t):
        return remote(s.fin[t].at[0], fpart(t, k, h), s.osent.at[t], s.oyr.at[t], yn, g)

    def xgot(t):
        return remote(fpart(t, kx, h), fpart(t, kx, h), s.osent.at[t], s.oxr.at[t], xn, g)

    def ygot(t):
        return remote(fpart(t, ky, h), fpart(t, ky, h), s.osent.at[t], s.oyr.at[t], yn, g)

    def fwd(t, sub, kk):
        reg = fpart(t, kk, h, sub)
        return remote(reg, reg, s.osent.at[t], s.oar.at[t], (yn, xn)[sub], g)

    def cross(t, hh):
        reg = slab(outs[t], MATS[t], 0, hh)
        return remote(reg, reg, s.osent.at[t], s.ocr.at[t], core, g)

    def r4(t):
        m = MATS[t]
        z2_got(t, 1)
        z3(t).wait_recv()
        mine = cell3(t, last)

        def body(n):
            at = pl.ds(mo(n * 16, 16), 16)
            total = mine[at, :].astype(F32) + s.zbuf[t][1, at, :].astype(F32) + s.zbuf[t][2, at, :].astype(F32)
            s.fin[t][0, at, :] = total.astype(BF)
        loop(m.quarter // 16, body)
        for b in range(highs):
            cp = remote(s.fin[t].at[0], s.fin[t].at[1 + b], s.fxs.at[t, b], s.fxr.at[t, b], flip(rep, 8 << b), g)
            cp.start()
            cp.wait()
            add_rows(s.fin[t].at[0], s.fin[t].at[0], s.fin[t].at[1 + b], m.quarter)
        keep(t).start()
        xsend(t).start()
        ysend(t).start()

    def r5(t):
        xgot(t).wait_recv()
        fwd(t, 0, kx).start()
        ygot(t).wait_recv()
        fwd(t, 1, ky).start()

    def r6(t):
        arrived(fpart(t, kd, h), s.oar.at[t])
        keep(t).wait()
        cross(t, h).start()

    partners = [(core, g), (xn, g), (yn, g)] + [(flip(rep, 8 << b), g) for b in range(highs)]
    bit = 1
    while bit < groups:
        partners.append((rep, flip(g, bit)))
        bit *= 2

    def smcopy(j):
        return remote(s.smacc.at[j], s.smin.at[j], s.sms.at[j], s.smr.at[j], *partners[j])

    def small(j):
        if j:
            smcopy(j - 1).wait_recv()
            s.smacc[j] = s.smacc[j - 1] + s.smin[j - 1]
        if j < len(partners):
            smcopy(j).start()
        else:
            osm[...] = s.smacc[j, g]

    def crossed():
        for t in ORDER:
            cross(t, 1 - h).wait_recv()

    def chunks_sent():
        for t in ORDER:
            m = MATS[t]
            for i in range(groups):
                sent(grads[t].at[pl.ds(0, (8 if i < last else 7) * m.quarter), pl.ds(0, m.half)], s.gone.at[t, i])

    def outs_sent():
        sent(s.sm.at[pl.ds(0, last)], s.ms.at[0])
        for t in ORDER:
            m = MATS[t]
            sent(grads[t].at[pl.ds(0, 7 * m.quarter), pl.ds(0, m.half)], s.osent.at[t])
        for j in range(len(partners)):
            smcopy(j).wait_send()

    def project(j):
        project_block(j, s.fa, s.gain1, s.shift1, s.bias3, s.wq, s.qkv, s.normed, tokens)

    def attention(p):
        loop(2, lambda i: attend_pair(p + i, g, s.qkv, s.attended, s.stats, tokens))

    def block(n):
        return pl.ds(mo(n * 256, 256), 256)

    def to_middle():
        def body(n):
            c = block(n)
            s.middle[:, c] = nn(s.attended[...], s.wo[:, c]) + s.obias[0:1, c] + fr[:, c].astype(F32)
        loop(D // 256, body)
        value, inverse = normalize(s.middle[...])
        s.normal[...] = value
        s.inverse[...] = jnp.broadcast_to(inverse, (tokens, LANE))
        s.normed[...] = (value * s.gain2[...] + s.shift2[...]).astype(BF)

    def hidden(i):
        def body(j):
            n = row(i) * (FF // 256 // groups) + j
            c = block(n)
            u = nn(s.normed[...], s.wu[:, c]) + s.ubias[0:1, c]
            bell = 0.5 * (1.0 + lax.erf(u * ROOT_HALF))
            s.act[:, c] = (u * bell).astype(BF)
            slope = bell + u * jnp.exp(-0.5 * u * u) * ROOT_TWO_PI
            grad = nt(ct[...], s.wd[block(n), :]) * slope
            s.v_up[0:1, c] = jnp.sum(grad, axis=0, keepdims=True)
            s.pre[:, c] = grad.astype(BF)
        loop(FF // 256 // groups, body)

    def to_output():
        def body(n):
            c = block(n)
            out_frames[:, c] = (nn(s.act[...], s.wd[:, c]) + s.dbias[0:1, c] + s.middle[:, c]).astype(BF)
        loop(D // 256, body)

    def back_up():
        def body(n):
            s.wide[:, block(n)] = nt(s.pre[...], s.wu[block(n), :])
        loop(D // 256, body)

    def back_norm():
        upstream, normal = s.wide[...], s.normal[...]
        s.v_gain2[...] = jnp.sum(upstream * normal, axis=0, keepdims=True)
        s.v_shift2[...] = jnp.sum(upstream, axis=0, keepdims=True)
        total = ct[...].astype(F32) + norm_back(upstream, normal, s.inverse[:, 0:1], s.gain2[...])
        s.mgrad[...] = total
        s.half[...] = total.astype(BF)
        s.v_out[...] = jnp.sum(total, axis=0, keepdims=True)
        s.v_down[...] = jnp.sum(ct[...].astype(F32), axis=0, keepdims=True)

        def body(n):
            s.a_all[own, block(n)] = nt(s.half[...], s.wo[block(n), :]).astype(BF)
        own = pl.ds(mo(g * tokens, 16), tokens)
        loop(D // 256, body)
        lanes = lax.broadcasted_iota(jnp.int32, (tokens, LANE), 1)
        mask = head_mask(tokens)
        stats = s.stats[...]
        for p in range(HEADS // 2):
            c = slice(p * LANE, (p + 1) * LANE)
            product = s.a_all[own, c].astype(F32) * s.attended[:, c].astype(F32)
            for side in range(2):
                mine = jnp.where(mask if side == 0 else jnp.logical_not(mask), product, 0.0)
                stats = jnp.where(lanes == HEADS + 2 * p + side, jnp.sum(mine, axis=-1, keepdims=True), stats)
        s.stats[...] = stats
        s.rows3[groups] = stats.T[0:2 * HEADS, :]

    def weight(t, i, left, right):
        m = MATS[t]
        s.turned[0:m.block, :] = left[:, pl.ds(mo(row(i) * m.block, LANE if m.block % LANE == 0 else 64), m.block)].T

        def body(n):
            c = block(n)
            grads[t][pl.ds(mo(row(i) * m.block, 16), m.block), c] = nn(s.turned[0:m.block, :], right[:, c]).astype(BF)
        loop(m.cols // 256, body)
        first(t, i).start()

    def turn(left, out):
        out[...] = left[...].T

    def weight_all(t, left, right):
        def body(n):
            c = block(n)
            grads[t][:, c] = nn(left[...], right[:, c]).astype(BF)
        loop(MATS[t].cols // 256, body)
        for i in (0, 2, 1, 3):
            first(t, i).start()

    def queries(p):
        loop(2, lambda i: query_back(p + i, g, s.qkv, s.a_all, s.stats, s.pgrad, s.v_qv, tokens))

    def keys(p):
        loop(2, lambda i: key_back(p + i, g, s.qkv, s.a_all, s.rows, s.pgrad, s.v_qv, tokens))

    def to_inputs():
        normal, _ = normalize(fr[...].astype(F32))
        s.normed[...] = (normal * s.gain1[...] + s.shift1[...]).astype(BF)
        turn(s.normed, s.turned)

    def input_grad():
        def body(n):
            s.wide[:, block(n)] = nt(s.pgrad[...], s.wq[block(n), :])
        loop(D // 256, body)
        normal, inverse = normalize(fr[...].astype(F32))
        upstream = s.wide[...]
        s.v_gain1[...] = jnp.sum(upstream * normal, axis=0, keepdims=True)
        s.v_shift1[...] = jnp.sum(upstream, axis=0, keepdims=True)
        frames_grad[...] = (s.mgrad[...] + norm_back(upstream, normal, inverse, s.gain1[...])).astype(BF)
        fill_image(s.smacc.at[0], range(SROWS), (
            (GAIN_ONE, s.v_gain1), (SHIFT_ONE, s.v_shift1), (QV_BIAS, s.v_qv), (OUT_BIAS, s.v_out), (GAIN_TWO, s.v_gain2),
            (SHIFT_TWO, s.v_shift2), (UP_BIAS, s.v_up), (DOWN_BIAS, s.v_down)))
        small(0)

    barrier, peers = greet(rep, g, groups)
    peers += [(flip(rep, 8 << b), g) for b in range(highs)]
    for t in range(3):
        piece_load(t, 0, t).start()
    for cp in small_loads():
        cp.start()
    own_frames = pltpu.make_async_copy(fr, zregion(4, g), s.ssem.at[1])
    own_frames.start()
    do_barrier(barrier, peers)
    relayout(0, 0, 0)
    own_send(0)
    piece_load(3, 0, 0).start()
    relayout(1, 0, 1)
    own_send(1)
    relayout(2, 0, 2)
    own_send(2)
    pltpu.make_async_copy(s.spbuf, s.spbuf, s.ssem.at[0]).wait()
    s.smb[...] = jnp.zeros_like(s.smb)
    count = sum(c for _, c in SMALL)
    s.smb[0:count, :] = s.spbuf[...].astype(F32).reshape(count, LANE)
    for i in range(1, groups):
        vcopy(i, g).start()
    both(0, 0, 0)
    both(0, 0, 1)
    own_frames.wait()
    own_send(4)
    relayout(3, 0, 0)
    own_send(3)
    rest_load(0)
    rest(0)
    rest_load(1)
    both(0, 0, 2)
    both(1, 0, 0)
    both(1, 0, 1)
    both(0, 1, 0)
    both(0, 2, 0)
    both(1, 0, 2)
    both(2, 0, 0)
    both(2, 0, 1)
    rest(1)
    rest_load(2)
    both(2, 0, 2)
    arrived(s.sm.at[pl.ds(0, last)], s.mr.at[0])
    s.sm[g] = s.smb[...]
    for spot, ref in ((GAIN_ONE, s.gain1), (SHIFT_ONE, s.shift1), (QV_BIAS, s.qvbias), (GAIN_TWO, s.gain2), (SHIFT_TWO, s.shift2),
                      (OUT_BIAS, s.obias), (UP_BIAS, s.ubias), (DOWN_BIAS, s.dbias)):
        assemble(s.sm, spot, ref)
    s.bias3[...] = jnp.zeros_like(s.bias3)
    s.bias3[0:1, 0:D] = s.qvbias[0:1, 0:D]
    s.bias3[0:1, 2 * D:3 * D] = s.qvbias[0:1, D:2 * D]
    s.stats[...] = jnp.zeros_like(s.stats)
    both(0, 4, 0)
    rest(2)
    rest_load(3)
    both(1, 1, 0)
    both(1, 2, 0)
    for step in range(last):
        both(3, 0, step)
    project(g)
    both(0, 3, 0)

    def project_rows(step):
        def body(d):
            r = g + (2 * d - 1) * (1 + step)

            @pl.when(jnp.logical_and(r >= 0, r <= last))
            def _():
                project(r)
        loop(2, body)
    project_rows(0)
    both(0, 4, 1)
    rest(3)
    both(2, 1, 0)
    both(2, 2, 0)
    both(1, 3, 0)
    both(0, 1, 1)
    both(0, 2, 1)
    project_rows(1)
    both(0, 3, 1)
    both(2, 3, 0)
    both(1, 1, 1)
    both(1, 2, 1)
    both(0, 4, 2)
    project_rows(2)
    both(0, 1, 2)
    both(1, 3, 1)
    both(2, 1, 1)
    both(2, 2, 1)
    both(0, 2, 2)
    attention(0)
    both(0, 3, 2)
    both(1, 1, 2)
    both(2, 3, 1)
    attention(2)
    both(1, 2, 2)
    attention(4)
    both(1, 3, 2)
    both(2, 1, 2)
    both(2, 2, 2)
    both(2, 3, 2)
    rest = [(t, step) for step in range(last) for t in (1, 2, 3)]
    for t, step in rest:
        if t == 1:
            both(3, t, step)
    to_middle()
    for t, step in rest:
        if t > 1:
            both(3, t, step)
    hidden(0)
    weight(3, 0, s.act, ct)
    hidden(1)
    hidden(2)
    r1(3, 0)
    hidden(3)
    back_up()
    back_norm()
    share_start()
    weight(3, 2, s.act, ct)
    r2(3, 0)
    weight(3, 1, s.act, ct)
    r1(3, 2)
    weight(3, 3, s.act, ct)
    r1(3, 1)
    turn(s.normed, s.turned2)
    r1(3, 3)
    r2(3, 2)
    weight_all(2, s.turned2, s.pre)
    r2(3, 1)
    r1(2, 0)
    to_output()
    share_step(0)
    r1(2, 2)
    r2(3, 3)
    turn(s.attended, s.turned2)
    weight_all(1, s.turned2, s.half)
    gather_sent()
    r2(2, 0)
    r1(2, 1)
    queries(0)
    share_step(1)
    r2(2, 2)
    r1(2, 3)
    queries(2)
    queries(4)
    r2(2, 1)
    r1(1, 0)
    r1(1, 2)
    share_step(2)
    share_rows()
    r3(3, 0)
    r3(3, 2)
    keys(0)
    r2(2, 3)
    r1(1, 1)
    r1(1, 3)
    r3(3, 1)
    r3(3, 3)
    r2(1, 0)
    r2(1, 2)
    to_inputs()
    keys(2)
    r2(1, 1)
    r2(1, 3)
    keys(4)
    r3b(3)
    r3(2, 0)
    r3(2, 2)
    weight_all(0, s.turned, s.pgrad)
    r3(2, 1)
    r3(2, 3)
    input_grad()
    r1(0, 0)
    r1(0, 2)
    r4(3)
    r2(0, 0)
    r2(0, 2)
    r1(0, 1)
    r1(0, 3)
    r3(1, 0)
    r3(1, 2)
    r3b(2)
    r3(0, 0)
    r3(0, 2)
    r5(3)
    r2(0, 1)
    small(1)
    r3(1, 1)
    r3(1, 3)
    r2(0, 3)
    r4(2)
    r6(3)
    r3b(1)
    r3(0, 1)
    r3(0, 3)
    r3b(0)
    r5(2)
    r4(1)
    small(2)
    r6(2)
    r4(0)
    r5(1)
    small(3)
    r5(0)
    small(4)
    r6(1)
    r6(0)
    for j in range(5, len(partners) + 1):
        small(j)
    crossed()
    share_sent()
    chunks_sent()
    outs_sent()


def layer(frames, cotangent, params, groups, reps):
    dma = pltpu.SemaphoreType.DMA
    tokens = frames.shape[0]
    clip = tokens * groups
    highs = (reps // 8).bit_length() - 1
    steps = 3 + highs + groups.bit_length() - 1
    n = 2 * (groups - 1)

    def bf(*shape):
        return pltpu.VMEM(shape, BF)

    def wide(*shape):
        return pltpu.VMEM(shape, F32)

    scratch = {name: bf(m.block * groups, m.cols) for name, m in zip(("wq", "wo", "wu", "wd"), MATS)}
    scratch.update(go=bf(D, D), gu=bf(D, FF), gd=bf(FF, D))
    scratch.update(buf1=[bf(m.block * groups, m.half) for m in MATS], buf2=[bf(m.quarter * groups * 2, m.half) for m in MATS],
                   buf3=[bf(m.quarter * groups, m.half) for m in MATS], zbuf=[bf(groups - 1, m.quarter, m.half) for m in MATS],
                   fin=[bf(highs + 1, m.quarter, m.half) for m in MATS])
    scratch.update(fa=bf(clip, D), qkv=bf(clip, 3 * D), a_all=bf(clip, D))
    scratch.update(attended=bf(tokens, D), normed=bf(tokens, D), half=bf(tokens, D),
                   act=bf(tokens, FF), pre=bf(tokens, FF), pgrad=bf(tokens, 3 * D), turned=bf(D, tokens), turned2=bf(D, tokens))
    scratch.update(middle=wide(tokens, D), normal=wide(tokens, D), mgrad=wide(tokens, D), wide=wide(tokens, D),
                   inverse=wide(tokens, LANE), stats=wide(tokens, LANE))
    scratch.update(rows3=wide(groups + 1, 2 * HEADS, tokens), rows=wide(2 * HEADS, clip))
    scratch.update({name: wide(1, D) for name in ("gain1", "shift1", "gain2", "shift2", "obias", "dbias", "v_gain1", "v_shift1",
                                                  "v_gain2", "v_shift2", "v_out", "v_down")})
    scratch.update(qvbias=wide(1, 2 * D), bias3=wide(1, 3 * D), v_qv=wide(1, 2 * D), ubias=wide(1, FF), v_up=wide(1, FF))
    piece = max(m.quarter * m.tiles + 8 for m in MATS)
    scratch.update(pbuf=bf(3, 1, piece * LANE), fbuf=wide(piece, LANE), spbuf=bf(1, sum(c for _, c in SMALL) * LANE),
                   smb=wide(SROWS, LANE), sm=wide(groups, SROWS, LANE),
                   smacc=wide(steps + 1, groups, SROWS, LANE), smin=wide(steps, groups, SROWS, LANE))
    scratch.update(lsem=dma((3,)), ssem=dma((2,)), zs=dma((4,)), zfs=dma((2, groups - 1)), zr=dma((5, groups - 1)))
    scratch.update({name: dma((4, groups - 1)) for name in ("gs", "xr", "yr", "fr", "cr", "z2r")})
    scratch.update({name: dma((1,)) for name in ("ms", "mr", "rs", "rr")})
    scratch.update(szs=dma((2, groups - 1)), szr=dma((groups - 1,)))
    scratch.update({name: dma((4, groups)) for name in ("gone", "c1r", "ab1r", "ab2r")})
    if highs:
        scratch.update({name: dma((4, highs)) for name in ("fxs", "fxr")})
    scratch.update({name: dma((4,)) for name in ("os", "osent", "oxr", "oyr", "oar", "ocr")})
    scratch.update(sms=dma((steps,)), smr=dma((steps,)))
    vmem, hbm = pl.BlockSpec(memory_space=pltpu.VMEM), pl.BlockSpec(memory_space=pl.ANY)
    sds = jax.ShapeDtypeStruct
    names = tuple(scratch)
    flat, tree = jax.tree.flatten(list(scratch.values()))

    def body(*refs):
        fixed = 10
        layer_kernel(groups, highs, names, *refs[:fixed], *jax.tree.unflatten(tree, refs[fixed:]))

    return pl.pallas_call(
        body,
        out_shape=[sds((m.block, m.cols), BF) for m in MATS] + [sds((SROWS, LANE), F32), sds((tokens, D), BF), sds((tokens, D), BF)],
        in_specs=[vmem, vmem, hbm],
        out_specs=[hbm] * 4 + [vmem] * 3,
        scratch_shapes=flat,
        compiler_params=pltpu.CompilerParams(collective_id=0, has_side_effects=True, vmem_limit_bytes=67043328),
        name="layer",
    )(frames, cotangent, params)


BETA_ONE = 0.9
BETA_TWO = 0.98
ADAM_EPS = 1e-06
LEARN_RATE = 0.006
DECAY = 0.01
ADAM_STEP = 4
ROWS = 1792
CHUNKS = -(-FROWS // ROWS)
SUB = 224


def flatten(m, block, flat, late):
    def body(i):
        base = m.row0 + i * (48 * m.tiles)
        for c in range(m.tiles):
            tile = block[pl.ds(mo(i * 48, 16), 48), c * LANE:(c + 1) * LANE].astype(F32)
            if m.shifted:
                tile = pltpu.roll(tile, 64, 1)
                late[pl.ds(base + c + 1, 48, stride=m.tiles), :] = tile
            flat[pl.ds(base + c, 48, stride=m.tiles), :] = tile
    loop(m.block // 48, body)


def adam_kernel(scale, gq, go, gu, gd, sm, p_hbm, m_hbm, v_hbm, fo, fg, o_g, o_p, o_m, o_v, o_fo, o_fg,
                bq, bo, bu, bd, flat, late, pb, mb, vb, gb, nb, frames, bsem, isem, osem, fsem):
    blocks = (bq, bo, bu, bd)

    def view(ref, c):
        return ref.at[:, pl.ds(c * ROWS * LANE, min(ROWS, FROWS - c * ROWS) * LANE)]

    loads = [pltpu.make_async_copy(a, b, bsem.at[i]) for i, (a, b) in enumerate(zip((gq, go, gu, gd), blocks))]
    pairs = ((p_hbm, pb), (m_hbm, mb), (v_hbm, vb))
    ins = [[pltpu.make_async_copy(view(a, c), view(b, c), isem.at[c, i]) for i, (a, b) in enumerate(pairs)] for c in range(CHUNKS)]
    results = ((gb, o_g), (nb, o_p), (mb, o_m), (vb, o_v))
    puts = [[pltpu.make_async_copy(view(a, c), view(b, c), osem.at[c, i]) for i, (a, b) in enumerate(results)] for c in range(CHUNKS)]
    takes = [pltpu.make_async_copy(a, frames.at[i], fsem.at[i]) for i, a in enumerate((fo, fg))]
    gives = [pltpu.make_async_copy(frames.at[i], a, fsem.at[2 + i]) for i, a in enumerate((o_fo, o_fg))]
    def fetch(c):
        if c < CHUNKS:
            for cp in ins[c]:
                cp.start()

    loads[0].start()
    fetch(0)
    loads[1].start()
    fetch(1)
    loads[2].start()

    def update(c):
        for cp in ins[c]:
            cp.wait()

        def body(j):
            start = c * ROWS + j * SUB
            at = pl.ds(mo(start, 8), SUB)
            lanes = (slice(None), pl.ds(mo(start * LANE, LANE), SUB * LANE))
            number = start + lax.broadcasted_iota(jnp.int32, (SUB, LANE), 0)
            low = lax.broadcasted_iota(jnp.int32, (SUB, LANE), 1) < 64
            grad = jnp.where(jnp.logical_and(number > UP.row0, low), late[at, :], flat[at, :]).reshape(1, SUB * LANE) * scale
            first = BETA_ONE * mb[lanes] + (1.0 - BETA_ONE) * grad
            second = BETA_TWO * vb[lanes] + (1.0 - BETA_TWO) * grad * grad
            gb[lanes] = grad
            mb[lanes] = first
            vb[lanes] = second
            first_hat = first * (1.0 / (1.0 - BETA_ONE**ADAM_STEP))
            second_hat = second * (1.0 / (1.0 - BETA_TWO**ADAM_STEP))
            current = pb[lanes].astype(F32)
            nb[lanes] = current - LEARN_RATE * (first_hat / (jnp.sqrt(second_hat) + ADAM_EPS) + DECAY * current)
        loop(-(-min(ROWS, FROWS - c * ROWS) // SUB), body)
        fetch(c + 2)
        for cp in puts[c]:
            cp.start()

    loads[0].wait()
    flatten(QKV, bq, flat, late)
    flat[0:3, :] = sm[0:3, :]
    update(0)
    loads[1].wait()
    flatten(OUT, bo, flat, late)
    flat[3459:3462, :] = sm[3:6, :]
    update(1)
    loads[2].wait()
    flatten(UP, bu, flat, late)
    flat[4614:4618, :] = sm[6:10, :]
    flat[4618:4619, 0:64] = sm[10:11, 0:64]
    flat[9226:9227, 64:128] = sm[11:12, 64:128]
    update(2)
    loads[3].start()
    for cp in takes:
        cp.start()
    update(3)
    update(4)
    loads[3].wait()
    flatten(DOWN, bd, flat, late)
    for ref in (flat, late):
        ref[9227:9232, :] = sm[12:17, :]
        ref[9232:9233, 0:64] = sm[17:18, 0:64]
        ref[13841:13842, :] = sm[19:20, :]
    flat[13840:13841, 64:128] = sm[18:19, 64:128]
    update(5)
    for cp in takes:
        cp.wait()
    for cp in gives:
        cp.start()
    for c in range(6, CHUNKS):
        update(c)
    for cp in gives:
        cp.wait()
    for chunk in puts:
        for cp in chunk:
            cp.wait()


def adam(blocks, smalls, params, first, second, reps, *outputs):
    vmem, hbm = pl.BlockSpec(memory_space=pltpu.VMEM), pl.BlockSpec(memory_space=pl.ANY)
    dma = pltpu.SemaphoreType.DMA
    row = pltpu.VMEM((1, CHUNKS * ROWS * LANE), F32)
    return pl.pallas_call(
        functools.partial(adam_kernel, 1.0 / reps),
        out_shape=[jax.ShapeDtypeStruct((1, FLAT), F32)] * 4 + [jax.ShapeDtypeStruct(o.shape, o.dtype) for o in outputs],
        in_specs=[hbm] * 4 + [vmem] + [hbm] * 5,
        out_specs=[hbm] * 6,
        scratch_shapes=[pltpu.VMEM(b.shape, BF) for b in blocks] + [pltpu.VMEM((CHUNKS * ROWS, LANE), F32)] * 2
        + [pltpu.VMEM((1, CHUNKS * ROWS * LANE), BF)] + [row] * 4 + [pltpu.VMEM((2,) + outputs[0].shape, BF)]
        + [dma((4,)), dma((CHUNKS, 3)), dma((CHUNKS, 4)), dma((4,))],
        compiler_params=pltpu.CompilerParams(vmem_limit_bytes=67043328),
        name="adam",
    )(*blocks, smalls, params, first, second, *outputs)


def on_device(frames, cotangent, params, first_moment, second_moment):
    groups, reps = lax.axis_size("grp"), lax.axis_size("rep")
    *blocks, small, out_frames, frames_grad = layer(frames, cotangent, params, groups, reps)
    param_grad, new_params, new_first, new_second, out_frames, frames_grad = adam(
        blocks, small, params, first_moment, second_moment, reps, out_frames, frames_grad)
    return (out_frames, frames_grad, param_grad, new_params, new_first, new_second)


def solution(mesh):
    in_specs = (
        P(("rep", "grp"), None),
        P(("rep", "grp"), None),
        P("grp", None),
        P("grp", None),
        P("grp", None),
    )
    out_specs = (
        P(("rep", "grp"), None),
        P(("rep", "grp"), None),
        P("grp", None),
        P("grp", None),
        P("grp", None),
        P("grp", None),
    )
    return jax.shard_map(
        on_device, mesh=mesh, in_specs=in_specs, out_specs=out_specs, check_vma=False
    )
```

```python
import functools
import types

import jax
import jax.numpy as jnp
from jax import lax
from jax.sharding import PartitionSpec as P
from jax.experimental import pallas as pl
from jax.experimental.pallas import tpu as pltpu

MESH = pl.DeviceIdType.MESH
BF = jnp.bfloat16
F32 = jnp.float32
D = 768
FF = 3072
HDIM = 64
LANE = 128
FLAT = 1771776
FROWS = FLAT // LANE


class Mat:
    def __init__(self, offset, block, cols, suba, subb):
        self.offset, self.block, self.cols = offset, block, cols
        self.tiles = cols // LANE
        self.row0 = offset // LANE
        self.shifted = offset % LANE != 0
        self.quarter = block // 4
        self.half = cols // 2
        self.sub = (suba, subb)


QKV = Mat(384, 192, 2304, (0, 48, 0, 640), (0, 48, 640, 512))
OUT = Mat(443136, 192, 768, (0, 48, 0, 128), (0, 48, 128, 256))
UP = Mat(591168, 192, 3072, (0, 48, 0, 768), (0, 48, 768, 768))
DOWN = Mat(1181760, 768, 768, (0, 96, 0, 384), (96, 96, 0, 384))
MATS = (QKV, OUT, UP, DOWN)
SMALL = ((0, 3), (3459, 3), (4614, 5), (9226, 7), (13840, 2))
SROWS = 24


def flip(index, bit):
    return index + bit - 2 * bit * ((index // bit) % 2)


def mo(value, by):
    return pl.multiple_of(value, by)


def part(ref, m, r, k, h, sub=None):
    r0, rn, c0, cn = m.sub[sub] if sub is not None else (0, m.quarter, 0, m.half)
    row = mo(r * m.block + k * m.quarter + r0, 16)
    col = mo(h * m.half + c0, LANE)
    return ref.at[pl.ds(row, rn), pl.ds(col, cn)]


def slab(ref, m, r, h):
    return ref.at[pl.ds(mo(r * m.block, 16), m.block), pl.ds(mo(h * m.half, LANE), m.half)]


def remote(src, dst, send, recv, rep, grp):
    return pltpu.make_async_remote_copy(
        src_ref=src, dst_ref=dst, send_sem=send, recv_sem=recv,
        device_id={"rep": rep, "grp": grp}, device_id_type=MESH)


def greet(rep, g, groups):
    barrier = pltpu.get_barrier_semaphore()
    peers = [(flip(rep, b), g) for b in (1, 2, 4)]
    peers += [(rep, lax.rem(g + i, groups)) for i in range(1, groups)]
    return barrier, peers


def do_barrier(barrier, peers):
    for r, gg in peers:
        pl.semaphore_signal(barrier, inc=1, device_id={"rep": r, "grp": gg}, device_id_type=MESH)
    pl.semaphore_wait(barrier, len(peers))


def add_rows(dst, a, b, rows, step=16):
    def body(i, c):
        at = pl.ds(mo(i * step, 16), step)
        dst[at, :] = (a[at, :].astype(F32) + b[at, :].astype(F32)).astype(dst.dtype)
        return c
    lax.fori_loop(0, rows // step, body, 0)


EPS_NORM = 1e-05
ROOT_HALF = 0.7071067811865476
ROOT_TWO_PI = 0.3989422804014327
HEADS = D // HDIM
GAIN_ONE, SHIFT_ONE, QV_BIAS, OUT_BIAS, GAIN_TWO, SHIFT_TWO, UP_BIAS, DOWN_BIAS = (
    (0, 3), (3, 3), (6, 6), (12, 3), (15, 3), (18, 3), (23, 12), (37, 3))


def low_lanes():
    return lax.broadcasted_iota(jnp.int32, (1, LANE), 1) < 64


def assemble(sm, place, out):
    first, count = place
    halves = [(gi, first + i) for gi in range(sm.shape[0]) for i in range(count)]
    for t in range(len(halves) // 2):
        (g0, h0), (g1, h1) = halves[2 * t], halves[2 * t + 1]
        a = sm[g0, h0 // 2:h0 // 2 + 1, :]
        b = sm[g1, h1 // 2:h1 // 2 + 1, :]
        a = pltpu.roll(a, 64, 1) if h0 % 2 else a
        b = b if h1 % 2 else pltpu.roll(b, 64, 1)
        out[0:1, t * LANE:(t + 1) * LANE] = jnp.where(low_lanes(), a, b)


def fill_image(image, rows, vectors):
    where = {}
    for place, ref in vectors:
        for i in range(place[1]):
            where[place[0] + i] = (place[1], i, ref)
    for gi in range(image.shape[0]):
        for r in rows:
            parts = []
            for side in range(2):
                spot = where.get(2 * r + side)
                if spot is None:
                    parts.append(jnp.zeros((1, LANE), F32))
                    continue
                count, i, ref = spot
                q = gi * count + i
                v = ref[0:1, q // 2 * LANE:(q // 2 + 1) * LANE]
                parts.append(v if q % 2 == side else pltpu.roll(v, 64, 1))
            image[gi, r:r + 1, :] = jnp.where(low_lanes(), parts[0], parts[1])


def mean(v):
    return jnp.sum(v, axis=-1, keepdims=True) * (1.0 / D)


def normalize(v):
    centered = v - mean(v)
    inverse = lax.rsqrt(mean(centered * centered) + EPS_NORM)
    return centered * inverse, inverse


def norm_back(upstream, normal, inverse, gain):
    s = upstream * gain
    return inverse * (s - mean(s) - normal * mean(s * normal))


def nn(a, b):
    return lax.dot_general(a, b, (((1,), (0,)), ((), ())), preferred_element_type=F32)


def nt(a, b):
    return lax.dot_general(a, b, (((1,), (1,)), ((), ())), preferred_element_type=F32)


def loop(count, body):
    def step(i, c):
        body(i)
        return c
    lax.fori_loop(0, count, step, 0)


def head_mask(rows):
    return lax.broadcasted_iota(jnp.int32, (rows, LANE), 1) < HDIM


def third(p, n):
    return pl.ds(mo(n * D + p * LANE, LANE), LANE)


def project_block(j, fa, gain, shift, bias, wq, qkv, normed, tokens):
    at = pl.ds(mo(j * tokens, 16), tokens)
    normal, _ = normalize(fa[at, :].astype(F32))
    normed[...] = (normal * gain[...] + shift[...]).astype(BF)

    def body(n):
        col = pl.ds(mo(n * 256, 256), 256)
        qkv[at, col] = (nn(normed[...], wq[:, col]) + bias[0:1, col]).astype(BF)
    loop(3 * D // 256, body)


def attend_pair(p, g, qkv, attended, stats, tokens):
    col = third(p, 0)
    query = qkv[pl.ds(mo(g * tokens, 16), tokens), col] * jnp.asarray(HDIM**-0.5, BF)
    keys, values = qkv[:, third(p, 1)], qkv[:, third(p, 2)]
    mask = head_mask(tokens)
    zero = jnp.zeros_like(query)
    lanes = lax.broadcasted_iota(jnp.int32, (tokens, LANE), 1)
    results = []
    for side in range(2):
        scores = nt(jnp.where(mask, query, zero) if side == 0 else jnp.where(mask, zero, query), keys)
        highest = jnp.max(scores, axis=-1, keepdims=True)
        shares = jnp.exp(scores - highest)
        total = jnp.sum(shares, axis=-1, keepdims=True)
        results.append(nn(shares.astype(BF), values) * (1.0 / total))
        stats[...] = jnp.where(lanes == 2 * p + side, highest + jnp.log(total), stats[...])
    attended[:, col] = jnp.where(mask, results[0], results[1]).astype(BF)


def query_back(w, p, j, qkv, upstream_all, cols, pgh, csum, tokens):
    own = pl.ds(mo(j * tokens, 16), tokens)
    scale = jnp.asarray(HDIM**-0.5, BF)
    query, upstream = qkv[own, third(p, 0)] * scale, upstream_all[w, own, :]
    keys, values = qkv[:, third(p, 1)], qkv[:, third(p, 2)]
    mask = head_mask(tokens)
    zero = jnp.zeros_like(query)
    lanes = lax.broadcasted_iota(jnp.int32, (tokens, LANE), 1)
    stats = cols[own, :]
    results = []
    for side in range(2):
        def pick(v):
            return jnp.where(mask, v, zero) if side == 0 else jnp.where(mask, zero, v)
        total = jnp.sum(jnp.where(lanes == 2 * p + side, stats, 0.0), axis=-1, keepdims=True)
        centre = jnp.sum(jnp.where(lanes == HEADS + 2 * p + side, stats, 0.0), axis=-1, keepdims=True)
        shares = jnp.exp(nt(pick(query), keys) - total)
        back = (shares * (nt(pick(upstream), values) - centre)).astype(BF) * scale
        results.append(nn(back, keys))
    store_grad(3 * w, own, jnp.where(mask, results[0], results[1]), pgh, csum)


def store_grad(n, own, grad, pgh, csum):
    col = pl.ds(mo(n * LANE, LANE), LANE)
    pgh[own, col] = grad.astype(BF)
    csum[0:1, col] = csum[0:1, col] + jnp.sum(grad, axis=0, keepdims=True)


def key_back(w, p, j, qkv, upstream_all, rows, pgh, csum, tokens):
    own = pl.ds(mo(j * tokens, 16), tokens)
    scale = jnp.asarray(HDIM**-0.5, BF)
    keys, values = qkv[own, third(p, 1)] * scale, qkv[own, third(p, 2)]
    queries, upstream = qkv[:, third(p, 0)], upstream_all[w]
    mask = head_mask(tokens)
    zero = jnp.zeros_like(keys)
    ks, vs = [], []
    for side in range(2):
        def pick(v):
            return jnp.where(mask, v, zero) if side == 0 else jnp.where(mask, zero, v)
        total = rows[pl.ds(2 * p + side, 1), :]
        centre = rows[pl.ds(HEADS + 2 * p + side, 1), :]
        shares = jnp.exp(nt(pick(keys), queries) - total)
        vs.append(nn(shares.astype(BF), upstream))
        back = (shares * (nt(pick(values), upstream) - centre)).astype(BF) * scale
        ks.append(nn(back, queries))
    store_grad(3 * w + 1, own, jnp.where(mask, ks[0], ks[1]), pgh, csum)
    store_grad(3 * w + 2, own, jnp.where(mask, vs[0], vs[1]), pgh, csum)


def cell(ref, m, row, sub=None):
    r0, rn, c0, cn = m.sub[sub] if sub is not None else (0, m.quarter, 0, m.half)
    return ref.at[pl.ds(mo(row + r0, 16), rn), pl.ds(c0, cn)]


ORDER = (3, 2, 1, 0)
SUMS = (OUT, OUT, UP, DOWN)
WHOLES = (UP, OUT, UP, DOWN)
PAIR = 3 * LANE


def layer_kernel(groups, highs, names, fr, ct, p_ref, oq, oo, ou, od, osm, out_frames, frames_grad, *scratch):
    s = types.SimpleNamespace(**dict(zip(names, scratch)))
    rep, g = lax.axis_index("rep"), lax.axis_index("grp")
    tokens = fr.shape[0]
    share_of = lax.rem(rep, 8)
    h = lax.rem(share_of, 2)
    k = share_of // 2
    x, y = lax.rem(k, 2), k // 2
    kx, ky, kd = flip(k, 1), flip(k, 2), 3 - k
    core, xn, yn = flip(rep, 1), flip(rep, 2), flip(rep, 4)
    full = (s.wq, s.wo, s.wu, s.wd)
    outs = (oq, oo, ou, od)
    grads = (s.wu, s.go, s.gu, s.gd)
    last = groups - 1

    def has_next(d):
        return g < last if d == 0 else g > 0

    def toward(d):
        return lax.rem(g + (1 if d == 0 else last), groups)

    def row_of(d, step):
        return g - 1 - step if d == 0 else g + 1 + step

    def valid(d, step):
        return row_of(d, step) >= 0 if d == 0 else row_of(d, step) <= last

    slots = [(d, step) for step in range(last) for d in range(2)]

    def slot_of(d, step):
        return step if d else last - 1 - step

    def sent(region, sem):
        remote(region, region, sem, s.smr.at[0], core, g).wait_send()

    def arrived(region, sem):
        pltpu.make_async_copy(region, region, sem).wait()

    def piece_load(t, i, slot):
        m = MATS[t]
        count = (m.quarter * m.tiles + (2 if m.shifted else 0)) * LANE
        start = mo((m.row0 + lax.rem(k + i, 4) * (m.quarter * m.tiles)) * LANE, LANE)
        return pltpu.make_async_copy(p_ref.at[:, pl.ds(start, count)], s.pbuf.at[slot, :, pl.ds(0, count)], s.lsem.at[slot])

    def relayout(t, i, slot):
        m = MATS[t]
        piece_load(t, i, slot).wait()
        count = m.quarter * m.tiles + (8 if m.shifted else 0)
        s.fbuf[0:count, :] = s.pbuf[slot, :, 0:count * LANE].astype(F32).reshape(count, LANE)
        at = pl.ds(mo(g * m.block + lax.rem(k + i, 4) * m.quarter, 16), m.quarter)
        low = lax.broadcasted_iota(jnp.int32, (m.quarter, LANE), 1) < 64
        for c in range(m.tiles):
            a = s.fbuf[pl.ds(c, m.quarter, stride=m.tiles), :]
            if m.shifted:
                b = s.fbuf[pl.ds(c + 1, m.quarter, stride=m.tiles), :]
                a = pltpu.roll(jnp.where(low, b, a), 64, 1)
            full[t][at, c * LANE:(c + 1) * LANE] = a.astype(BF)

    def rest_load(t):
        for i in range(3):
            piece_load(t, i + 1, i).start()

    def rest(t):
        loop(3, lambda i: relayout(t, i + 1, i))

    def small_loads():
        at, result = 0, []
        for first, count in SMALL:
            result.append(pltpu.make_async_copy(
                p_ref.at[:, pl.ds(first * LANE, count * LANE)], s.spbuf.at[:, pl.ds(at * LANE, count * LANE)], s.ssem.at[0]))
            at += count
        return result

    def zregion(t, r):
        if t == 4:
            return s.fa.at[pl.ds(mo(r * tokens, 16), tokens), :]
        return part(full[t], MATS[t], r, k, h)

    def zcopy(t, d, step, r):
        reg = zregion(t, r)
        send = s.zs.at[t] if t < 4 else s.zfs.at[d, step]
        return remote(reg, reg, send, s.zr.at[t, slot_of(d, step)], rep, toward(d))

    def own_send(t):
        for d in range(2):
            @pl.when(has_next(d))
            def _():
                zcopy(t, d, 0, g).start()

    def xcopy(t, i, r, kk):
        reg = part(full[t], MATS[t], r, kk, h)
        return remote(reg, reg, s.gs.at[t, i], s.xr.at[t, i], xn, g)

    def ycopy(t, i, r, kk):
        reg = part(full[t], MATS[t], r, kk, h)
        return remote(reg, reg, s.gs.at[t, i], s.yr.at[t, i], yn, g)

    def acopy(t, i, r, kk):
        reg = part(full[t], MATS[t], r, kk, h, 0)
        return remote(reg, reg, s.gs.at[t, i], s.fr.at[t, i], yn, g)

    def bcopy(t, i, r, kk):
        reg = part(full[t], MATS[t], r, kk, h, 1)
        return remote(reg, reg, s.gs.at[t, i], s.fr.at[t, i], xn, g)

    def ccopy(t, i, r, hh):
        reg = slab(full[t], MATS[t], r, hh)
        return remote(reg, reg, s.gs.at[t, i], s.cr.at[t, i], core, g)

    def stage(number, t, d, step):
        i = slot_of(d, step)

        @pl.when(valid(d, step))
        def _():
            r = row_of(d, step)
            if number == 0:
                zcopy(t, d, step, r).wait_recv()
                if step < last - 1:
                    @pl.when(has_next(d))
                    def _():
                        zcopy(t, d, step + 1, r).start()
                if t < 4:
                    xcopy(t, i, r, k).start()
                    ycopy(t, i, r, k).start()
            if number == 1:
                xcopy(t, i, r, kx).wait_recv()
                acopy(t, i, r, kx).start()
                ycopy(t, i, r, ky).wait_recv()
                bcopy(t, i, r, ky).start()
            if number == 2:
                arrived(part(full[t], MATS[t], r, kd, h), s.fr.at[t, i])
                ccopy(t, i, r, h).start()
            if number == 3:
                ccopy(t, i, r, 1 - h).wait_recv()

    def both(number, t, step):
        for d in range(2):
            stage(number, t, d, step)

    def gather_sent():
        inner = jnp.logical_and(g > 0, g < last)
        for t in range(4):
            m = MATS[t]

            @pl.when(inner)
            def _():
                sent(full[t].at[pl.ds(0, (2 + last) * m.quarter), pl.ds(0, m.half)], s.zs.at[t])

            @pl.when(jnp.logical_not(inner))
            def _():
                sent(full[t].at[pl.ds(0, m.quarter), pl.ds(0, m.half)], s.zs.at[t])
            for i in range(last):
                sent(full[t].at[pl.ds(0, 7 * m.quarter), pl.ds(0, m.half)], s.gs.at[t, i])
        for d in range(2):
            @pl.when(has_next(d))
            def _():
                zcopy(4, d, 0, g).wait_send()
            for step in range(last - 1):
                @pl.when(jnp.logical_and(valid(d, step), has_next(d)))
                def _():
                    zcopy(4, d, step + 1, g).wait_send()

    def vcopy(i, owner):
        return remote(s.smb, s.sm.at[owner], s.ms.at[0], s.mr.at[0], rep, lax.rem(g + i, groups))

    def pair(owner, w):
        return (3 * owner + 1) // 2 + w

    def second(owner):
        return lax.rem(owner, 2) == 0

    def rows_at(r):
        return pl.ds(mo(r * tokens, 16), tokens)

    def scopy(i, w):
        dest = lax.rem(g + i, groups)
        return remote(s.agrad.at[:, third(pair(dest, w), 0)], s.a_h.at[w, rows_at(g), :], s.shs.at[w, i - 1], s.shr.at[w],
                      rep, dest)

    def rcopy(i, owner):
        return remote(s.rows3.at[groups], s.rows3.at[owner], s.rs.at[0], s.rr.at[0], rep, lax.rem(g + i, groups))

    def share_start():
        for i in range(1, groups):
            scopy(i, 0).start()

            @pl.when(second(lax.rem(g + i, groups)))
            def _():
                scopy(i, 1).start()
            rcopy(i, g).start()
        s.a_h[0, rows_at(g), :] = s.agrad[:, third(pair(g, 0), 0)]

        @pl.when(second(g))
        def _():
            s.a_h[1, rows_at(g), :] = s.agrad[:, third(pair(g, 1), 0)]
        s.csum[...] = jnp.zeros_like(s.csum)

    def share_got():
        arrived(s.a_h.at[0, pl.ds(0, last * tokens), :], s.shr.at[0])

        @pl.when(second(g))
        def _():
            arrived(s.a_h.at[1, pl.ds(0, last * tokens), :], s.shr.at[1])
        arrived(s.rows3.at[pl.ds(0, last)], s.rr.at[0])
        for i in range(groups):
            s.rows[0:2 * HEADS, i * tokens:(i + 1) * tokens] = s.rows3[i]
        s.rows[0:2 * HEADS, pl.ds(mo(g * tokens, LANE), tokens)] = s.rows3[groups]
        s.cols[...] = jnp.concatenate([s.rows[...], jnp.zeros((LANE - 2 * HEADS, groups * tokens), F32)], axis=0).T

    def share_sent():
        for i in range(1, groups):
            scopy(i, 0).wait_send()

            @pl.when(second(lax.rem(g + i, groups)))
            def _():
                scopy(i, 1).wait_send()
        sent(s.rows3.at[pl.ds(0, last)], s.rs.at[0])

    def bcopy_back(i, w, n):
        dest = lax.rem(g + i, groups)
        return remote(s.pgh.at[rows_at(dest), pl.ds((3 * w + n) * LANE, LANE)], s.pgrad.at[:, third(pair(g, w), n)],
                      s.bks.at[w], s.bkr.at[0], rep, dest)

    def each_pair(body):
        body(0)

        @pl.when(second(g))
        def _():
            body(1)

    def return_queries():
        def body(w):
            for i in range(1, groups):
                bcopy_back(i, w, 0).start()
            s.pgrad[:, third(pair(g, w), 0)] = s.pgh[rows_at(g), 3 * w * LANE:(3 * w + 1) * LANE]
        each_pair(body)

    def return_keys(i):
        def body(w):
            for n in (1, 2):
                if i:
                    bcopy_back(i, w, n).start()
                else:
                    s.pgrad[:, third(pair(g, w), n)] = s.pgh[rows_at(g), (3 * w + n) * LANE:(3 * w + n + 1) * LANE]
        each_pair(body)

    def return_got():
        @pl.when(second(g))
        def _():
            arrived(s.pgrad.at[:, pl.ds(0, 3 * D - 2 * PAIR)], s.bkr.at[0])

        @pl.when(jnp.logical_not(second(g)))
        def _():
            arrived(s.pgrad.at[:, pl.ds(0, 3 * D - PAIR)], s.bkr.at[0])

    def return_sent():
        sent(s.pgh.at[pl.ds(0, last * tokens), pl.ds(0, PAIR)], s.bks.at[0])

        @pl.when(second(g))
        def _():
            sent(s.pgh.at[pl.ds(0, last * tokens), pl.ds(0, PAIR)], s.bks.at[1])

    def row(i):
        return lax.rem(g + 1 + i, groups)

    def first(t, i):
        m = SUMS[t]
        at = pl.ds(mo(row(i) * m.block, 16), m.block)
        return remote(grads[t].at[at, pl.ds(mo((1 - h) * m.half, LANE), m.half)], s.buf1[t].at[at, :],
                      s.gone.at[t, i], s.c1r.at[t, i], core, g)

    def cell1(t, i, kk, sub=None):
        return cell(s.buf1[t], SUMS[t], row(i) * SUMS[t].block + kk * SUMS[t].quarter, sub)

    def cell2(t, i, j, sub):
        return cell(s.buf2[t], SUMS[t], (row(i) * 2 + j) * SUMS[t].quarter, sub)

    def cell3(t, i, sub=None):
        return cell(s.buf3[t], SUMS[t], row(i) * SUMS[t].quarter, sub)

    def a1(t, i, j, kk):
        return remote(cell1(t, i, kk, 0), cell2(t, i, j, 0), s.gone.at[t, i], s.ab1r.at[t, i], xn, g)

    def b1(t, i, j, kk):
        return remote(cell1(t, i, kk, 1), cell2(t, i, j, 1), s.gone.at[t, i], s.ab1r.at[t, i], yn, g)

    def a2(t, i, j):
        return remote(cell2(t, i, j, 0), cell3(t, i, 0), s.gone.at[t, i], s.ab2r.at[t, i], yn, g)

    def b2(t, i, j):
        return remote(cell2(t, i, j, 1), cell3(t, i, 1), s.gone.at[t, i], s.ab2r.at[t, i], xn, g)

    def z2(t, i):
        slot = (1 - lax.rem(g, 2)) if i == 0 else lax.rem(g, 2)
        return remote(cell3(t, i), s.zbuf[t].at[slot], s.gone.at[t, i], s.z2r.at[t, slot], rep, flip(g, 1))

    def z2_got(t, slot):
        arrived(s.zbuf[t].at[slot], s.z2r.at[t, slot])

    def z3(t):
        return remote(cell3(t, 1), s.zbuf[t].at[2], s.gone.at[t, 1], s.z2r.at[t, 2], rep, flip(g, 2))

    def z4(i):
        return remote(cell3(0, i), s.fin[0].at[0, :, pl.ds(mo(g * PAIR, LANE), PAIR)], s.gone.at[0, i], s.zqr.at[0], rep, row(i))

    def r1(t, i):
        m = SUMS[t]
        first(t, i).wait_recv()
        at = pl.ds(mo(row(i) * m.block, 16), m.block)
        mine = grads[t].at[at, pl.ds(mo(h * m.half, LANE), m.half)]
        add_rows(s.buf1[t].at[at, :], mine, s.buf1[t].at[at, :], m.block)
        for j in range(2):
            a1(t, i, j, 2 * j + (1 - x)).start()
            b1(t, i, j, 2 * (1 - y) + j).start()

    def r2(t, i):
        m = SUMS[t]
        arrived(s.buf2[t].at[pl.ds(mo(row(i) * 2 * m.quarter, 16), 2 * m.quarter), :], s.ab1r.at[t, i])
        for j in range(2):
            add_rows(cell2(t, i, j, 0), cell1(t, i, 2 * j + x, 0), cell2(t, i, j, 0), m.sub[0][1])
        a2(t, i, 1 - y).start()
        for j in range(2):
            add_rows(cell2(t, i, j, 1), cell1(t, i, 2 * y + j, 1), cell2(t, i, j, 1), m.sub[1][1])
        b2(t, i, 1 - x).start()

    def r3(t, i):
        m = SUMS[t]
        arrived(cell3(t, i), s.ab2r.at[t, i])
        add_rows(cell3(t, i, 0), cell2(t, i, y, 0), cell3(t, i, 0), m.sub[0][1])
        add_rows(cell3(t, i, 1), cell2(t, i, x, 1), cell3(t, i, 1), m.sub[1][1])
        if t == 0:
            if i < last:
                z4(i).start()
            else:
                s.fin[0][0, :, pl.ds(mo(g * PAIR, LANE), PAIR)] = cell3(0, last)[...]
        elif i % 2 == 0:
            z2(t, i).start()

    def r3b(t):
        z2_got(t, 0)
        add_rows(cell3(t, 1), cell3(t, 1), s.zbuf[t].at[0], SUMS[t].quarter)
        z3(t).start()

    def fpart(t, kk, hh, sub=None):
        return part(outs[t], WHOLES[t], 0, kk, hh, sub)

    def keep(t):
        return pltpu.make_async_copy(s.fin[t].at[0], fpart(t, k, h), s.os.at[t])

    def xsend(t):
        return remote(s.fin[t].at[0], fpart(t, k, h), s.osent.at[t], s.oxr.at[t], xn, g)

    def ysend(t):
        return remote(s.fin[t].at[0], fpart(t, k, h), s.osent.at[t], s.oyr.at[t], yn, g)

    def xgot(t):
        return remote(fpart(t, kx, h), fpart(t, kx, h), s.osent.at[t], s.oxr.at[t], xn, g)

    def ygot(t):
        return remote(fpart(t, ky, h), fpart(t, ky, h), s.osent.at[t], s.oyr.at[t], yn, g)

    def fwd(t, sub, kk):
        reg = fpart(t, kk, h, sub)
        return remote(reg, reg, s.osent.at[t], s.oar.at[t], (yn, xn)[sub], g)

    def cross(t, hh):
        reg = slab(outs[t], WHOLES[t], 0, hh)
        return remote(reg, reg, s.osent.at[t], s.ocr.at[t], core, g)

    def r4(t):
        m = WHOLES[t]
        if t == 0:
            arrived(s.fin[0].at[0, :, pl.ds(0, last * PAIR)], s.zqr.at[0])
        else:
            z2_got(t, 1)
            z3(t).wait_recv()
        mine = cell3(t, last)

        def body(n):
            at = pl.ds(mo(n * 16, 16), 16)
            total = mine[at, :].astype(F32) + s.zbuf[t][1, at, :].astype(F32) + s.zbuf[t][2, at, :].astype(F32)
            s.fin[t][0, at, :] = total.astype(BF)
        if t:
            loop(m.quarter // 16, body)
        for b in range(highs):
            cp = remote(s.fin[t].at[0], s.fin[t].at[1 + b], s.fxs.at[t, b], s.fxr.at[t, b], flip(rep, 8 << b), g)
            cp.start()
            cp.wait()
            add_rows(s.fin[t].at[0], s.fin[t].at[0], s.fin[t].at[1 + b], m.quarter)
        keep(t).start()
        xsend(t).start()
        ysend(t).start()

    def r5(t):
        xgot(t).wait_recv()
        fwd(t, 0, kx).start()
        ygot(t).wait_recv()
        fwd(t, 1, ky).start()

    def r6(t):
        arrived(fpart(t, kd, h), s.oar.at[t])
        keep(t).wait()
        cross(t, h).start()

    partners = []
    bit = 1
    while bit < groups:
        partners.append((rep, flip(g, bit)))
        bit *= 2
    partners += [(core, g), (xn, g), (yn, g)] + [(flip(rep, 8 << b), g) for b in range(highs)]

    def smcopy(j):
        return remote(s.smacc.at[j], s.smin.at[j], s.sms.at[j], s.smr.at[j], *partners[j])

    def small(j):
        if j:
            smcopy(j - 1).wait_recv()
            s.smacc[j] = s.smacc[j - 1] + s.smin[j - 1]
        if j < len(partners):
            smcopy(j).start()
        else:
            osm[...] = s.smacc[j, g]

    def crossed():
        for t in ORDER:
            cross(t, 1 - h).wait_recv()

    def chunks_sent():
        for t in ORDER:
            m = SUMS[t]
            for i in range(groups):
                sent(grads[t].at[pl.ds(0, (8 if i < last else 7) * m.quarter), pl.ds(0, m.half)], s.gone.at[t, i])

    def outs_sent():
        sent(s.sm.at[pl.ds(0, last)], s.ms.at[0])
        for t in ORDER:
            m = WHOLES[t]
            sent(grads[t].at[pl.ds(0, 7 * m.quarter), pl.ds(0, m.half)], s.osent.at[t])
        for j in range(len(partners)):
            smcopy(j).wait_send()

    def project(j):
        project_block(j, s.fa, s.gain1, s.shift1, s.bias3, s.wq, s.qkv, s.normed, tokens)

    def attention(p):
        loop(2, lambda i: attend_pair(p + i, g, s.qkv, s.attended, s.stats, tokens))

    def block(n):
        return pl.ds(mo(n * 256, 256), 256)

    def to_middle():
        def body(n):
            c = block(n)
            s.middle[:, c] = nn(s.attended[...], s.wo[:, c]) + s.obias[0:1, c] + fr[:, c].astype(F32)
        loop(D // 256, body)
        value, _ = normalize(s.middle[...])
        s.normed[...] = (value * s.gain2[...] + s.shift2[...]).astype(BF)

    def hidden(i):
        def body(j):
            n = row(i) * (FF // 256 // groups) + j
            c = block(n)
            u = nn(s.normed[...], s.wu[:, c]) + s.ubias[0:1, c]
            bell = 0.5 * (1.0 + lax.erf(u * ROOT_HALF))
            s.act[:, c] = (u * bell).astype(BF)
            slope = bell + u * jnp.exp(-0.5 * u * u) * ROOT_TWO_PI
            grad = nt(ct[...], s.wd[block(n), :]) * slope
            s.v_up[0:1, c] = jnp.sum(grad, axis=0, keepdims=True)
            s.pre[:, c] = grad.astype(BF)
        loop(FF // 256 // groups, body)

    def to_output():
        def body(n):
            c = block(n)
            out_frames[:, c] = (nn(s.act[...], s.wd[:, c]) + s.dbias[0:1, c] + s.middle[:, c]).astype(BF)
        loop(D // 256, body)

    def back_up():
        def body(n):
            s.wide[:, block(n)] = nt(s.pre[...], s.wu[block(n), :])
        loop(D // 256, body)

    def back_norm():
        upstream = s.wide[...]
        normal, inverse = normalize(s.middle[...])
        s.v_gain2[...] = jnp.sum(upstream * normal, axis=0, keepdims=True)
        s.v_shift2[...] = jnp.sum(upstream, axis=0, keepdims=True)
        total = ct[...].astype(F32) + norm_back(upstream, normal, inverse, s.gain2[...])
        s.mgrad[...] = total
        s.half[...] = total.astype(BF)
        s.v_out[...] = jnp.sum(total, axis=0, keepdims=True)
        s.v_down[...] = jnp.sum(ct[...].astype(F32), axis=0, keepdims=True)

        def body(n):
            s.agrad[:, block(n)] = nt(s.half[...], s.wo[block(n), :]).astype(BF)
        loop(D // 256, body)
        lanes = lax.broadcasted_iota(jnp.int32, (tokens, LANE), 1)
        mask = head_mask(tokens)
        stats = s.stats[...]
        for p in range(HEADS // 2):
            c = slice(p * LANE, (p + 1) * LANE)
            product = s.agrad[:, c].astype(F32) * s.attended[:, c].astype(F32)
            for side in range(2):
                mine = jnp.where(mask if side == 0 else jnp.logical_not(mask), product, 0.0)
                stats = jnp.where(lanes == HEADS + 2 * p + side, jnp.sum(mine, axis=-1, keepdims=True), stats)
        s.stats[...] = stats
        s.rows3[groups] = stats.T[0:2 * HEADS, :]

    def weight(t, i, left, right):
        m = MATS[t]
        s.turned[0:m.block, :] = left[:, pl.ds(mo(row(i) * m.block, LANE if m.block % LANE == 0 else 64), m.block)].T

        def body(n):
            c = block(n)
            grads[t][pl.ds(mo(row(i) * m.block, 16), m.block), c] = nn(s.turned[0:m.block, :], right[:, c]).astype(BF)
        loop(m.cols // 256, body)
        first(t, i).start()

    def turn(left, out):
        out[...] = left[...].T

    def weight_all(t, left, right):
        def body(n):
            c = block(n)
            grads[t][:, c] = nn(left[...], right[:, c]).astype(BF)
        loop(MATS[t].cols // 256, body)
        for i in (0, 2, 1, 3):
            first(t, i).start()

    pairs_here = 2 - lax.rem(g, 2)

    def queries(j):
        loop(pairs_here, lambda w: query_back(w, pair(g, w), j, s.qkv, s.a_h, s.cols, s.pgh, s.csum, tokens))

    def keys(i):
        j = lax.rem(g + i, groups)
        loop(pairs_here, lambda w: key_back(w, pair(g, w), j, s.qkv, s.a_h, s.rows, s.pgh, s.csum, tokens))

    def turn_all():
        def body(j):
            normal, _ = normalize(s.fa[rows_at(j), :].astype(F32))
            s.turned_all[:, pl.ds(mo(j * tokens, LANE), tokens)] = normal.astype(BF).T
        loop(groups, body)

    def weight_pairs():
        s.acc[...] = jnp.zeros_like(s.acc)

        def body(w):
            product = nn(s.turned_all[...], s.pgh[:, pl.ds(mo(w * PAIR, LANE), PAIR)])
            sums = s.csum[0:1, pl.ds(mo(w * PAIR, LANE), PAIR)]
            s.wu[:, pl.ds(mo(w * PAIR, LANE), PAIR)] = (product * s.columns[:, 0:1] + s.columns[:, 1:2] * sums).astype(BF)
            for n in range(3):
                weights = s.wq[:, third(pair(g, w), n)].astype(F32)
                c = slice(n * LANE, (n + 1) * LANE)
                s.acc[0] = s.acc[0] + weights * product[:, c]
                s.acc[1] = s.acc[1] + weights * sums[:, c]
        loop(pairs_here, body)

        @pl.when(jnp.logical_not(second(g)))
        def _():
            s.wu[:, PAIR:2 * PAIR] = jnp.zeros((D, PAIR), BF)
        for i in (0, 2, 1, 3):
            first(0, i).start()

    def send_small():
        s.v_gain1[...] = jnp.sum(s.acc[0].T, axis=0, keepdims=True)
        s.v_shift1[...] = jnp.sum(s.acc[1].T, axis=0, keepdims=True)
        s.v_qv[...] = jnp.zeros_like(s.v_qv)

        def body(w):
            p = pair(g, w)
            s.v_qv[0:1, third(p, 0)] = s.csum[0:1, pl.ds(mo(w * PAIR, LANE), LANE)]
            s.v_qv[0:1, third(p, 1)] = s.csum[0:1, pl.ds(mo(w * PAIR + 2 * LANE, LANE), LANE)]
        loop(pairs_here, body)
        fill_image(s.smacc.at[0], range(SROWS), (
            (GAIN_ONE, s.v_gain1), (SHIFT_ONE, s.v_shift1), (QV_BIAS, s.v_qv), (OUT_BIAS, s.v_out), (GAIN_TWO, s.v_gain2),
            (SHIFT_TWO, s.v_shift2), (UP_BIAS, s.v_up), (DOWN_BIAS, s.v_down)))
        small(0)

    def input_grad():
        def body(n):
            s.wide[:, block(n)] = nt(s.pgrad[...], s.wq[block(n), :])
        loop(D // 256, body)
        normal, inverse = normalize(fr[...].astype(F32))
        frames_grad[...] = (s.mgrad[...] + norm_back(s.wide[...], normal, inverse, s.gain1[...])).astype(BF)

    barrier, peers = greet(rep, g, groups)
    peers += [(flip(rep, 8 << b), g) for b in range(highs)]
    for t in range(3):
        piece_load(t, 0, t).start()
    for cp in small_loads():
        cp.start()
    own_frames = pltpu.make_async_copy(fr, zregion(4, g), s.ssem.at[1])
    own_frames.start()
    do_barrier(barrier, peers)
    relayout(0, 0, 0)
    own_send(0)
    piece_load(3, 0, 0).start()
    relayout(1, 0, 1)
    own_send(1)
    relayout(2, 0, 2)
    own_send(2)
    pltpu.make_async_copy(s.spbuf, s.spbuf, s.ssem.at[0]).wait()
    s.smb[...] = jnp.zeros_like(s.smb)
    count = sum(c for _, c in SMALL)
    s.smb[0:count, :] = s.spbuf[...].astype(F32).reshape(count, LANE)
    for i in range(1, groups):
        vcopy(i, g).start()
    both(0, 0, 0)
    both(0, 0, 1)
    own_frames.wait()
    own_send(4)
    relayout(3, 0, 0)
    own_send(3)
    rest_load(0)
    rest(0)
    rest_load(1)
    both(0, 0, 2)
    both(1, 0, 0)
    both(1, 0, 1)
    both(0, 1, 0)
    both(0, 2, 0)
    both(1, 0, 2)
    both(2, 0, 0)
    both(2, 0, 1)
    rest(1)
    rest_load(2)
    both(2, 0, 2)
    arrived(s.sm.at[pl.ds(0, last)], s.mr.at[0])
    s.sm[g] = s.smb[...]
    for spot, ref in ((GAIN_ONE, s.gain1), (SHIFT_ONE, s.shift1), (QV_BIAS, s.qvbias), (GAIN_TWO, s.gain2), (SHIFT_TWO, s.shift2),
                      (OUT_BIAS, s.obias), (UP_BIAS, s.ubias), (DOWN_BIAS, s.dbias)):
        assemble(s.sm, spot, ref)
    lower = lax.broadcasted_iota(jnp.int32, (LANE, D), 0) == 0
    s.columns[...] = jnp.where(lower, s.gain1[...], s.shift1[...]).T
    s.bias3[...] = jnp.zeros_like(s.bias3)
    s.bias3[0:1, 0:D] = s.qvbias[0:1, 0:D]
    s.bias3[0:1, 2 * D:3 * D] = s.qvbias[0:1, D:2 * D]
    s.stats[...] = jnp.zeros_like(s.stats)
    both(0, 4, 0)
    rest(2)
    rest_load(3)
    both(1, 1, 0)
    both(1, 2, 0)
    for step in range(last):
        both(3, 0, step)
    project(g)
    both(0, 3, 0)

    def project_rows(step):
        def body(d):
            r = g + (2 * d - 1) * (1 + step)

            @pl.when(jnp.logical_and(r >= 0, r <= last))
            def _():
                project(r)
        loop(2, body)
    project_rows(0)
    both(0, 4, 1)
    rest(3)
    both(2, 1, 0)
    both(2, 2, 0)
    both(1, 3, 0)
    both(0, 1, 1)
    both(0, 2, 1)
    project_rows(1)
    both(0, 3, 1)
    both(2, 3, 0)
    both(1, 1, 1)
    both(1, 2, 1)
    both(0, 4, 2)
    project_rows(2)
    both(0, 1, 2)
    both(1, 3, 1)
    both(2, 1, 1)
    both(2, 2, 1)
    both(0, 2, 2)
    attention(0)
    both(0, 3, 2)
    both(1, 1, 2)
    both(2, 3, 1)
    attention(2)
    both(1, 2, 2)
    attention(4)
    both(1, 3, 2)
    both(2, 1, 2)
    both(2, 2, 2)
    both(2, 3, 2)
    rest = [(t, step) for step in range(last) for t in (1, 2, 3)]
    for t, step in rest:
        if t == 1:
            both(3, t, step)
    to_middle()
    turn_all()
    for t, step in rest:
        if t > 1:
            both(3, t, step)
    hidden(0)
    weight(3, 0, s.act, ct)
    hidden(1)
    hidden(2)
    r1(3, 0)
    hidden(3)
    back_up()
    back_norm()
    share_start()
    weight(3, 2, s.act, ct)
    r2(3, 0)
    weight(3, 1, s.act, ct)
    r1(3, 2)
    weight(3, 3, s.act, ct)
    r1(3, 1)
    turn(s.normed, s.turned)
    r1(3, 3)
    r2(3, 2)
    weight_all(2, s.turned, s.pre)
    r2(3, 1)
    r1(2, 0)
    share_got()
    r1(2, 2)
    turn(s.attended, s.turned)
    weight_all(1, s.turned, s.half)
    r2(3, 3)
    queries(0)
    r3(3, 0)
    r3(3, 2)
    queries(1)
    r2(2, 0)
    r1(2, 1)
    queries(2)
    gather_sent()
    r3(3, 1)
    r3(3, 3)
    queries(3)
    r2(2, 2)
    r1(2, 3)
    keys(1)
    r3b(3)
    r2(2, 1)
    for i in (0, 2, 1, 3):
        r1(1, i)
    keys(2)
    r3(2, 0)
    r3(2, 2)
    r2(2, 3)
    keys(3)
    r2(1, 0)
    r2(1, 2)
    keys(0)
    r3(2, 1)
    r3(2, 3)
    r4(3)
    r3b(2)
    return_queries()
    weight_pairs()
    r2(1, 1)
    r2(1, 3)
    send_small()
    r5(3)
    for i in (0, 2, 1, 3):
        r1(0, i)
    r3(1, 0)
    r3(1, 2)
    for i in (0, 2, 1, 3):
        r2(0, i)
    r6(3)
    r3(1, 1)
    r3(1, 3)
    r4(2)
    for i in (0, 2, 1, 3):
        r3(0, i)
    small(1)
    r3b(1)
    for i in (1, 2, 3, 0):
        return_keys(i)
    to_output()
    r5(2)
    small(2)
    r4(0)
    r6(2)
    small(3)
    r4(1)
    small(4)
    r5(0)
    r5(1)
    for j in range(5, len(partners) + 1):
        small(j)
    r6(0)
    r6(1)
    return_got()
    input_grad()
    return_sent()
    crossed()
    share_sent()
    chunks_sent()
    outs_sent()


def layer(frames, cotangent, params, groups, reps):
    dma = pltpu.SemaphoreType.DMA
    tokens = frames.shape[0]
    clip = tokens * groups
    highs = (reps // 8).bit_length() - 1
    steps = 3 + highs + groups.bit_length() - 1
    n = 2 * (groups - 1)

    def bf(*shape):
        return pltpu.VMEM(shape, BF)

    def wide(*shape):
        return pltpu.VMEM(shape, F32)

    scratch = {name: bf(m.block * groups, m.cols) for name, m in zip(("wq", "wo", "wu", "wd"), MATS)}
    scratch.update(go=bf(D, D), gu=bf(D, FF), gd=bf(FF, D))
    scratch.update(buf1=[bf(m.block * groups, m.half) for m in SUMS], buf2=[bf(m.quarter * groups * 2, m.half) for m in SUMS],
                   buf3=[bf(m.quarter * groups, m.half) for m in SUMS], zbuf=[bf(groups - 1 if t else 1, m.quarter, m.half) for t, m in enumerate(SUMS)],
                   fin=[bf(highs + 1, m.quarter, m.half) for m in WHOLES])
    scratch.update(fa=bf(clip, D), qkv=bf(clip, 3 * D), a_h=bf(2, clip, LANE), agrad=bf(tokens, D), pgh=bf(clip, 2 * PAIR), turned_all=bf(D, clip))
    scratch.update(attended=bf(tokens, D), normed=bf(tokens, D), half=bf(tokens, D),
                   act=bf(tokens, FF), pre=bf(tokens, FF), pgrad=bf(tokens, 3 * D), turned=bf(D, tokens))
    scratch.update(middle=wide(tokens, D), mgrad=wide(tokens, D), wide=wide(tokens, D),
                   stats=wide(tokens, LANE))
    scratch.update(rows3=wide(groups + 1, 2 * HEADS, tokens), rows=wide(2 * HEADS, clip), cols=wide(clip, LANE), csum=wide(1, 2 * PAIR),
                   columns=wide(D, LANE), acc=wide(2, D, LANE))
    scratch.update({name: wide(1, D) for name in ("gain1", "shift1", "gain2", "shift2", "obias", "dbias", "v_gain1", "v_shift1",
                                                  "v_gain2", "v_shift2", "v_out", "v_down")})
    scratch.update(qvbias=wide(1, 2 * D), bias3=wide(1, 3 * D), v_qv=wide(1, 2 * D), ubias=wide(1, FF), v_up=wide(1, FF))
    piece = max(m.quarter * m.tiles + 8 for m in MATS)
    scratch.update(pbuf=bf(3, 1, piece * LANE), fbuf=wide(piece, LANE), spbuf=bf(1, sum(c for _, c in SMALL) * LANE),
                   smb=wide(SROWS, LANE), sm=wide(groups, SROWS, LANE),
                   smacc=wide(steps + 1, groups, SROWS, LANE), smin=wide(steps, groups, SROWS, LANE))
    scratch.update(lsem=dma((3,)), ssem=dma((2,)), zs=dma((4,)), zfs=dma((2, groups - 1)), zr=dma((5, groups - 1)))
    scratch.update({name: dma((4, groups - 1)) for name in ("gs", "xr", "yr", "fr", "cr", "z2r")})
    scratch.update({name: dma((1,)) for name in ("ms", "mr", "rs", "rr")})
    scratch.update(shs=dma((2, groups - 1)), shr=dma((2,)), bks=dma((2,)), bkr=dma((1,)), zqr=dma((1,)))
    scratch.update({name: dma((4, groups)) for name in ("gone", "c1r", "ab1r", "ab2r")})
    if highs:
        scratch.update({name: dma((4, highs)) for name in ("fxs", "fxr")})
    scratch.update({name: dma((4,)) for name in ("os", "osent", "oxr", "oyr", "oar", "ocr")})
    scratch.update(sms=dma((steps,)), smr=dma((steps,)))
    vmem, hbm = pl.BlockSpec(memory_space=pltpu.VMEM), pl.BlockSpec(memory_space=pl.ANY)
    sds = jax.ShapeDtypeStruct
    names = tuple(scratch)
    flat, tree = jax.tree.flatten(list(scratch.values()))

    def body(*refs):
        fixed = 10
        layer_kernel(groups, highs, names, *refs[:fixed], *jax.tree.unflatten(tree, refs[fixed:]))

    return pl.pallas_call(
        body,
        out_shape=[sds((m.block, m.cols), BF) for m in WHOLES] + [sds((SROWS, LANE), F32), sds((tokens, D), BF), sds((tokens, D), BF)],
        in_specs=[vmem, vmem, hbm],
        out_specs=[hbm] * 4 + [vmem] * 3,
        scratch_shapes=flat,
        compiler_params=pltpu.CompilerParams(collective_id=0, has_side_effects=True, vmem_limit_bytes=67043328),
        name="layer",
    )(frames, cotangent, params)


BETA_ONE = 0.9
BETA_TWO = 0.98
ADAM_EPS = 1e-06
LEARN_RATE = 0.006
DECAY = 0.01
ADAM_STEP = 4
ROWS = 1792
CHUNKS = -(-FROWS // ROWS)
SUB = 224


def flatten(m, block, flat, late):
    def body(i):
        base = m.row0 + i * (48 * m.tiles)
        for c in range(m.tiles):
            at = (c % (m.tiles // 3)) if m is QKV else 0
            at = (at % 3 == 1) * 12 + (0, 0, 1, 2, 2, 3)[at] * 3 + c // (m.tiles // 3) if m is QKV else c
            tile = block[pl.ds(mo(i * 48, 16), 48), at * LANE:(at + 1) * LANE].astype(F32)
            if m.shifted:
                tile = pltpu.roll(tile, 64, 1)
                late[pl.ds(base + c + 1, 48, stride=m.tiles), :] = tile
            flat[pl.ds(base + c, 48, stride=m.tiles), :] = tile
    loop(m.block // 48, body)


def adam_kernel(scale, gq, go, gu, gd, sm, p_hbm, m_hbm, v_hbm, fo, fg, o_g, o_p, o_m, o_v, o_fo, o_fg,
                bq, bo, bu, bd, flat, late, pb, mb, vb, gb, nb, frames, bsem, isem, osem, fsem):
    blocks = (bq, bo, bu, bd)

    def view(ref, c):
        return ref.at[:, pl.ds(c * ROWS * LANE, min(ROWS, FROWS - c * ROWS) * LANE)]

    loads = [pltpu.make_async_copy(a, b, bsem.at[i]) for i, (a, b) in enumerate(zip((gq, go, gu, gd), blocks))]
    pairs = ((p_hbm, pb), (m_hbm, mb), (v_hbm, vb))
    ins = [[pltpu.make_async_copy(view(a, c), view(b, c), isem.at[c, i]) for i, (a, b) in enumerate(pairs)] for c in range(CHUNKS)]
    results = ((gb, o_g), (nb, o_p), (mb, o_m), (vb, o_v))
    puts = [[pltpu.make_async_copy(view(a, c), view(b, c), osem.at[c, i]) for i, (a, b) in enumerate(results)] for c in range(CHUNKS)]
    takes = [pltpu.make_async_copy(a, frames.at[i], fsem.at[i]) for i, a in enumerate((fo, fg))]
    gives = [pltpu.make_async_copy(frames.at[i], a, fsem.at[2 + i]) for i, a in enumerate((o_fo, o_fg))]
    def fetch(c):
        if c < CHUNKS:
            for cp in ins[c]:
                cp.start()

    loads[0].start()
    fetch(0)
    loads[1].start()
    fetch(1)
    loads[2].start()

    def update(c):
        for cp in ins[c]:
            cp.wait()

        def body(j):
            start = c * ROWS + j * SUB
            at = pl.ds(mo(start, 8), SUB)
            lanes = (slice(None), pl.ds(mo(start * LANE, LANE), SUB * LANE))
            number = start + lax.broadcasted_iota(jnp.int32, (SUB, LANE), 0)
            low = lax.broadcasted_iota(jnp.int32, (SUB, LANE), 1) < 64
            grad = jnp.where(jnp.logical_and(number > UP.row0, low), late[at, :], flat[at, :]).reshape(1, SUB * LANE) * scale
            first = BETA_ONE * mb[lanes] + (1.0 - BETA_ONE) * grad
            second = BETA_TWO * vb[lanes] + (1.0 - BETA_TWO) * grad * grad
            gb[lanes] = grad
            mb[lanes] = first
            vb[lanes] = second
            first_hat = first * (1.0 / (1.0 - BETA_ONE**ADAM_STEP))
            second_hat = second * (1.0 / (1.0 - BETA_TWO**ADAM_STEP))
            current = pb[lanes].astype(F32)
            nb[lanes] = current - LEARN_RATE * (first_hat / (jnp.sqrt(second_hat) + ADAM_EPS) + DECAY * current)
        loop(-(-min(ROWS, FROWS - c * ROWS) // SUB), body)
        fetch(c + 2)
        for cp in puts[c]:
            cp.start()

    loads[0].wait()
    flatten(QKV, bq, flat, late)
    flat[0:3, :] = sm[0:3, :]
    update(0)
    loads[1].wait()
    flatten(OUT, bo, flat, late)
    flat[3459:3462, :] = sm[3:6, :]
    update(1)
    loads[2].wait()
    flatten(UP, bu, flat, late)
    flat[4614:4618, :] = sm[6:10, :]
    flat[4618:4619, 0:64] = sm[10:11, 0:64]
    flat[9226:9227, 64:128] = sm[11:12, 64:128]
    update(2)
    loads[3].start()
    for cp in takes:
        cp.start()
    update(3)
    update(4)
    loads[3].wait()
    flatten(DOWN, bd, flat, late)
    for ref in (flat, late):
        ref[9227:9232, :] = sm[12:17, :]
        ref[9232:9233, 0:64] = sm[17:18, 0:64]
        ref[13841:13842, :] = sm[19:20, :]
    flat[13840:13841, 64:128] = sm[18:19, 64:128]
    update(5)
    for cp in takes:
        cp.wait()
    for cp in gives:
        cp.start()
    for c in range(6, CHUNKS):
        update(c)
    for cp in gives:
        cp.wait()
    for chunk in puts:
        for cp in chunk:
            cp.wait()


def adam(blocks, smalls, params, first, second, reps, *outputs):
    vmem, hbm = pl.BlockSpec(memory_space=pltpu.VMEM), pl.BlockSpec(memory_space=pl.ANY)
    dma = pltpu.SemaphoreType.DMA
    row = pltpu.VMEM((1, CHUNKS * ROWS * LANE), F32)
    return pl.pallas_call(
        functools.partial(adam_kernel, 1.0 / reps),
        out_shape=[jax.ShapeDtypeStruct((1, FLAT), F32)] * 4 + [jax.ShapeDtypeStruct(o.shape, o.dtype) for o in outputs],
        in_specs=[hbm] * 4 + [vmem] + [hbm] * 5,
        out_specs=[hbm] * 6,
        scratch_shapes=[pltpu.VMEM(b.shape, BF) for b in blocks] + [pltpu.VMEM((CHUNKS * ROWS, LANE), F32)] * 2
        + [pltpu.VMEM((1, CHUNKS * ROWS * LANE), BF)] + [row] * 4 + [pltpu.VMEM((2,) + outputs[0].shape, BF)]
        + [dma((4,)), dma((CHUNKS, 3)), dma((CHUNKS, 4)), dma((4,))],
        compiler_params=pltpu.CompilerParams(vmem_limit_bytes=67043328),
        name="adam",
    )(*blocks, smalls, params, first, second, *outputs)


def on_device(frames, cotangent, params, first_moment, second_moment):
    groups, reps = lax.axis_size("grp"), lax.axis_size("rep")
    *blocks, small, out_frames, frames_grad = layer(frames, cotangent, params, groups, reps)
    param_grad, new_params, new_first, new_second, out_frames, frames_grad = adam(
        blocks, small, params, first_moment, second_moment, reps, out_frames, frames_grad)
    return (out_frames, frames_grad, param_grad, new_params, new_first, new_second)


def solution(mesh):
    in_specs = (
        P(("rep", "grp"), None),
        P(("rep", "grp"), None),
        P("grp", None),
        P("grp", None),
        P("grp", None),
    )
    out_specs = (
        P(("rep", "grp"), None),
        P(("rep", "grp"), None),
        P("grp", None),
        P("grp", None),
        P("grp", None),
        P("grp", None),
    )
    return jax.shard_map(
        on_device, mesh=mesh, in_specs=in_specs, out_specs=out_specs, check_vma=False
    )
```

```python
import functools
import types

import jax
import jax.numpy as jnp
from jax import lax
from jax.sharding import PartitionSpec as P
from jax.experimental import pallas as pl
from jax.experimental.pallas import tpu as pltpu

MESH = pl.DeviceIdType.MESH
BF = jnp.bfloat16
F32 = jnp.float32
D = 768
FF = 3072
HDIM = 64
LANE = 128
FLAT = 1771776
FROWS = FLAT // LANE


class Mat:
    def __init__(self, offset, block, cols, suba, subb):
        self.offset, self.block, self.cols = offset, block, cols
        self.tiles = cols // LANE
        self.row0 = offset // LANE
        self.shifted = offset % LANE != 0
        self.quarter = block // 4
        self.half = cols // 2
        self.sub = (suba, subb)


QKV = Mat(384, 192, 2304, (0, 48, 0, 640), (0, 48, 640, 512))
OUT = Mat(443136, 192, 768, (0, 48, 0, 128), (0, 48, 128, 256))
UP = Mat(591168, 192, 3072, (0, 48, 0, 768), (0, 48, 768, 768))
DOWN = Mat(1181760, 768, 768, (0, 96, 0, 384), (96, 96, 0, 384))
MATS = (QKV, OUT, UP, DOWN)
SMALL = ((0, 3), (3459, 3), (4614, 5), (9226, 7), (13840, 2))
SROWS = 24


def flip(index, bit):
    return index + bit - 2 * bit * ((index // bit) % 2)


def mo(value, by):
    return pl.multiple_of(value, by)


def part(ref, m, r, k, h, sub=None):
    r0, rn, c0, cn = m.sub[sub] if sub is not None else (0, m.quarter, 0, m.half)
    row = mo(r * m.block + k * m.quarter + r0, 16)
    col = mo(h * m.half + c0, LANE)
    return ref.at[pl.ds(row, rn), pl.ds(col, cn)]


def slab(ref, m, r, h):
    return ref.at[pl.ds(mo(r * m.block, 16), m.block), pl.ds(mo(h * m.half, LANE), m.half)]


def remote(src, dst, send, recv, rep, grp):
    return pltpu.make_async_remote_copy(
        src_ref=src, dst_ref=dst, send_sem=send, recv_sem=recv,
        device_id={"rep": rep, "grp": grp}, device_id_type=MESH)


def greet(rep, g, groups):
    barrier = pltpu.get_barrier_semaphore()
    peers = [(flip(rep, b), g) for b in (1, 2, 4)]
    peers += [(rep, lax.rem(g + i, groups)) for i in range(1, groups)]
    return barrier, peers


def do_barrier(barrier, peers):
    for r, gg in peers:
        pl.semaphore_signal(barrier, inc=1, device_id={"rep": r, "grp": gg}, device_id_type=MESH)
    pl.semaphore_wait(barrier, len(peers))


def add_rows(dst, a, b, rows, step=16):
    def body(i, c):
        at = pl.ds(mo(i * step, 16), step)
        dst[at, :] = (a[at, :].astype(F32) + b[at, :].astype(F32)).astype(dst.dtype)
        return c
    lax.fori_loop(0, rows // step, body, 0)


EPS_NORM = 1e-05
ROOT_HALF = 0.7071067811865476
ROOT_TWO_PI = 0.3989422804014327
HEADS = D // HDIM
GAIN_ONE, SHIFT_ONE, QV_BIAS, OUT_BIAS, GAIN_TWO, SHIFT_TWO, UP_BIAS, DOWN_BIAS = (
    (0, 3), (3, 3), (6, 6), (12, 3), (15, 3), (18, 3), (23, 12), (37, 3))


def low_lanes():
    return lax.broadcasted_iota(jnp.int32, (1, LANE), 1) < 64


def assemble(sm, place, out):
    first, count = place
    halves = [(gi, first + i) for gi in range(sm.shape[0]) for i in range(count)]
    for t in range(len(halves) // 2):
        (g0, h0), (g1, h1) = halves[2 * t], halves[2 * t + 1]
        a = sm[g0, h0 // 2:h0 // 2 + 1, :]
        b = sm[g1, h1 // 2:h1 // 2 + 1, :]
        a = pltpu.roll(a, 64, 1) if h0 % 2 else a
        b = b if h1 % 2 else pltpu.roll(b, 64, 1)
        out[0:1, t * LANE:(t + 1) * LANE] = jnp.where(low_lanes(), a, b)


def fill_image(image, rows, vectors):
    where = {}
    for place, ref in vectors:
        for i in range(place[1]):
            where[place[0] + i] = (place[1], i, ref)
    for gi in range(image.shape[0]):
        for r in rows:
            parts = []
            for side in range(2):
                spot = where.get(2 * r + side)
                if spot is None:
                    parts.append(jnp.zeros((1, LANE), F32))
                    continue
                count, i, ref = spot
                q = gi * count + i
                v = ref[0:1, q // 2 * LANE:(q // 2 + 1) * LANE]
                parts.append(v if q % 2 == side else pltpu.roll(v, 64, 1))
            image[gi, r:r + 1, :] = jnp.where(low_lanes(), parts[0], parts[1])


def mean(v):
    return jnp.sum(v, axis=-1, keepdims=True) * (1.0 / D)


def normalize(v):
    centered = v - mean(v)
    inverse = lax.rsqrt(mean(centered * centered) + EPS_NORM)
    return centered * inverse, inverse


def norm_back(upstream, normal, inverse, gain):
    s = upstream * gain
    return inverse * (s - mean(s) - normal * mean(s * normal))


def nn(a, b):
    return lax.dot_general(a, b, (((1,), (0,)), ((), ())), preferred_element_type=F32)


def nt(a, b):
    return lax.dot_general(a, b, (((1,), (1,)), ((), ())), preferred_element_type=F32)


def loop(count, body):
    def step(i, c):
        body(i)
        return c
    lax.fori_loop(0, count, step, 0)


def head_mask(rows):
    return lax.broadcasted_iota(jnp.int32, (rows, LANE), 1) < HDIM


def third(p, n):
    return pl.ds(mo(n * D + p * LANE, LANE), LANE)


def project_block(j, fa, gain, shift, bias, wq, qkv, normed, turned, tokens):
    at = pl.ds(mo(j * tokens, 16), tokens)
    normal, _ = normalize(fa[at, :].astype(F32))
    normed[...] = (normal * gain[...] + shift[...]).astype(BF)
    turned[:, pl.ds(mo(j * tokens, LANE), tokens)] = normal.astype(BF).T

    def body(n):
        col = pl.ds(mo(n * 256, 256), 256)
        qkv[at, col] = (nn(normed[...], wq[:, col]) + bias[0:1, col]).astype(BF)
    loop(3 * D // 256, body)


def attend_pair(p, g, qkv, attended, stats, tokens):
    col = third(p, 0)
    query = qkv[pl.ds(mo(g * tokens, 16), tokens), col] * jnp.asarray(HDIM**-0.5, BF)
    keys, values = qkv[:, third(p, 1)], qkv[:, third(p, 2)]
    mask = head_mask(tokens)
    zero = jnp.zeros_like(query)
    lanes = lax.broadcasted_iota(jnp.int32, (tokens, LANE), 1)
    results = []
    for side in range(2):
        scores = nt(jnp.where(mask, query, zero) if side == 0 else jnp.where(mask, zero, query), keys)
        highest = jnp.max(scores, axis=-1, keepdims=True)
        shares = jnp.exp(scores - highest)
        total = jnp.sum(shares, axis=-1, keepdims=True)
        results.append(nn(shares.astype(BF), values) * (1.0 / total))
        stats[...] = jnp.where(lanes == 2 * p + side, highest + jnp.log(total), stats[...])
    attended[:, col] = jnp.where(mask, results[0], results[1]).astype(BF)


def query_back(w, p, j, qkv, upstream_all, cols, pgh, csum, tokens):
    own = pl.ds(mo(j * tokens, 16), tokens)
    scale = jnp.asarray(HDIM**-0.5, BF)
    query, upstream = qkv[own, third(p, 0)] * scale, upstream_all[w, own, :]
    keys, values = qkv[:, third(p, 1)], qkv[:, third(p, 2)]
    mask = head_mask(tokens)
    zero = jnp.zeros_like(query)
    lanes = lax.broadcasted_iota(jnp.int32, (tokens, LANE), 1)
    stats = cols[own, :]
    results = []
    for side in range(2):
        def pick(v):
            return jnp.where(mask, v, zero) if side == 0 else jnp.where(mask, zero, v)
        total = jnp.sum(jnp.where(lanes == 2 * p + side, stats, 0.0), axis=-1, keepdims=True)
        centre = jnp.sum(jnp.where(lanes == HEADS + 2 * p + side, stats, 0.0), axis=-1, keepdims=True)
        shares = jnp.exp(nt(pick(query), keys) - total)
        back = (shares * (nt(pick(upstream), values) - centre)).astype(BF) * scale
        results.append(nn(back, keys))
    store_grad(3 * w, own, jnp.where(mask, results[0], results[1]), pgh, csum)


def store_grad(n, own, grad, pgh, csum):
    col = pl.ds(mo(n * LANE, LANE), LANE)
    pgh[own, col] = grad.astype(BF)
    csum[0:1, col] = csum[0:1, col] + jnp.sum(grad, axis=0, keepdims=True)


def key_back(w, p, j, qkv, upstream_all, rows, pgh, csum, tokens):
    own = pl.ds(mo(j * tokens, 16), tokens)
    scale = jnp.asarray(HDIM**-0.5, BF)
    keys, values = qkv[own, third(p, 1)] * scale, qkv[own, third(p, 2)]
    queries, upstream = qkv[:, third(p, 0)], upstream_all[w]
    mask = head_mask(tokens)
    zero = jnp.zeros_like(keys)
    ks, vs = [], []
    for side in range(2):
        def pick(v):
            return jnp.where(mask, v, zero) if side == 0 else jnp.where(mask, zero, v)
        total = rows[pl.ds(2 * p + side, 1), :]
        centre = rows[pl.ds(HEADS + 2 * p + side, 1), :]
        shares = jnp.exp(nt(pick(keys), queries) - total)
        vs.append(nn(shares.astype(BF), upstream))
        back = (shares * (nt(pick(values), upstream) - centre)).astype(BF) * scale
        ks.append(nn(back, queries))
    store_grad(3 * w + 1, own, jnp.where(mask, ks[0], ks[1]), pgh, csum)
    store_grad(3 * w + 2, own, jnp.where(mask, vs[0], vs[1]), pgh, csum)


def cell(ref, m, row, sub=None):
    r0, rn, c0, cn = m.sub[sub] if sub is not None else (0, m.quarter, 0, m.half)
    return ref.at[pl.ds(mo(row + r0, 16), rn), pl.ds(c0, cn)]


ORDER = (3, 2, 1, 0)
SUMS = (OUT, OUT, UP, DOWN)
WHOLES = (UP, OUT, UP, DOWN)
PAIR = 3 * LANE


def layer_kernel(groups, highs, names, fr, ct, p_ref, oq, oo, ou, od, osm, out_frames, frames_grad, *scratch):
    s = types.SimpleNamespace(**dict(zip(names, scratch)))
    rep, g = lax.axis_index("rep"), lax.axis_index("grp")
    tokens = fr.shape[0]
    share_of = lax.rem(rep, 8)
    h = lax.rem(share_of, 2)
    k = share_of // 2
    x, y = lax.rem(k, 2), k // 2
    kx, ky, kd = flip(k, 1), flip(k, 2), 3 - k
    core, xn, yn = flip(rep, 1), flip(rep, 2), flip(rep, 4)
    full = (s.wq, s.wo, s.wu, s.wd)
    outs = (oq, oo, ou, od)
    grads = (s.wu, s.go, s.gu, s.gd)
    last = groups - 1

    def has_next(d):
        return g < last if d == 0 else g > 0

    def toward(d):
        return lax.rem(g + (1 if d == 0 else last), groups)

    def row_of(d, step):
        return g - 1 - step if d == 0 else g + 1 + step

    def valid(d, step):
        return row_of(d, step) >= 0 if d == 0 else row_of(d, step) <= last

    slots = [(d, step) for step in range(last) for d in range(2)]

    def slot_of(d, step):
        return step if d else last - 1 - step

    def sent(region, sem):
        remote(region, region, sem, s.smr.at[0], core, g).wait_send()

    def arrived(region, sem):
        pltpu.make_async_copy(region, region, sem).wait()

    def piece_load(t, i, slot):
        m = MATS[t]
        count = (m.quarter * m.tiles + (2 if m.shifted else 0)) * LANE
        start = mo((m.row0 + lax.rem(k + i, 4) * (m.quarter * m.tiles)) * LANE, LANE)
        return pltpu.make_async_copy(p_ref.at[:, pl.ds(start, count)], s.pbuf.at[slot, :, pl.ds(0, count)], s.lsem.at[slot])

    def relayout(t, i, slot):
        m = MATS[t]
        piece_load(t, i, slot).wait()
        count = m.quarter * m.tiles + (8 if m.shifted else 0)
        s.fbuf[0:count, :] = s.pbuf[slot, :, 0:count * LANE].astype(F32).reshape(count, LANE)
        at = pl.ds(mo(g * m.block + lax.rem(k + i, 4) * m.quarter, 16), m.quarter)
        low = lax.broadcasted_iota(jnp.int32, (m.quarter, LANE), 1) < 64
        for c in range(m.tiles):
            a = s.fbuf[pl.ds(c, m.quarter, stride=m.tiles), :]
            if m.shifted:
                b = s.fbuf[pl.ds(c + 1, m.quarter, stride=m.tiles), :]
                a = pltpu.roll(jnp.where(low, b, a), 64, 1)
            full[t][at, c * LANE:(c + 1) * LANE] = a.astype(BF)

    def rest_load(t):
        for i in range(3):
            piece_load(t, i + 1, i).start()

    def rest(t):
        loop(3, lambda i: relayout(t, i + 1, i))

    def small_loads():
        at, result = 0, []
        for first, count in SMALL:
            result.append(pltpu.make_async_copy(
                p_ref.at[:, pl.ds(first * LANE, count * LANE)], s.spbuf.at[:, pl.ds(at * LANE, count * LANE)], s.ssem.at[0]))
            at += count
        return result

    def zregion(t, r):
        if t == 4:
            return s.fa.at[pl.ds(mo(r * tokens, 16), tokens), :]
        return part(full[t], MATS[t], r, k, h)

    def zcopy(t, d, step, r):
        reg = zregion(t, r)
        send = s.zs.at[t] if t < 4 else s.zfs.at[d, step]
        return remote(reg, reg, send, s.zr.at[t, slot_of(d, step)], rep, toward(d))

    def own_send(t):
        for d in range(2):
            @pl.when(has_next(d))
            def _():
                zcopy(t, d, 0, g).start()

    def xcopy(t, i, r, kk):
        reg = part(full[t], MATS[t], r, kk, h)
        return remote(reg, reg, s.gs.at[t, i], s.xr.at[t, i], xn, g)

    def ycopy(t, i, r, kk):
        reg = part(full[t], MATS[t], r, kk, h)
        return remote(reg, reg, s.gs.at[t, i], s.yr.at[t, i], yn, g)

    def acopy(t, i, r, kk):
        reg = part(full[t], MATS[t], r, kk, h, 0)
        return remote(reg, reg, s.gs.at[t, i], s.fr.at[t, i], yn, g)

    def bcopy(t, i, r, kk):
        reg = part(full[t], MATS[t], r, kk, h, 1)
        return remote(reg, reg, s.gs.at[t, i], s.fr.at[t, i], xn, g)

    def ccopy(t, i, r, hh):
        reg = slab(full[t], MATS[t], r, hh)
        return remote(reg, reg, s.gs.at[t, i], s.cr.at[t, i], core, g)

    def stage(number, t, d, step):
        i = slot_of(d, step)

        @pl.when(valid(d, step))
        def _():
            r = row_of(d, step)
            if number == 0:
                zcopy(t, d, step, r).wait_recv()
                if step < last - 1:
                    @pl.when(has_next(d))
                    def _():
                        zcopy(t, d, step + 1, r).start()
                if t < 4:
                    xcopy(t, i, r, k).start()
                    ycopy(t, i, r, k).start()
            if number == 1:
                xcopy(t, i, r, kx).wait_recv()
                acopy(t, i, r, kx).start()
                ycopy(t, i, r, ky).wait_recv()
                bcopy(t, i, r, ky).start()
            if number == 2:
                arrived(part(full[t], MATS[t], r, kd, h), s.fr.at[t, i])
                ccopy(t, i, r, h).start()
            if number == 3:
                ccopy(t, i, r, 1 - h).wait_recv()

    def both(number, t, step):
        for d in range(2):
            stage(number, t, d, step)

    def gather_sent():
        inner = jnp.logical_and(g > 0, g < last)
        for t in range(4):
            m = MATS[t]

            @pl.when(inner)
            def _():
                sent(full[t].at[pl.ds(0, (2 + last) * m.quarter), pl.ds(0, m.half)], s.zs.at[t])

            @pl.when(jnp.logical_not(inner))
            def _():
                sent(full[t].at[pl.ds(0, m.quarter), pl.ds(0, m.half)], s.zs.at[t])
            for i in range(last):
                sent(full[t].at[pl.ds(0, 7 * m.quarter), pl.ds(0, m.half)], s.gs.at[t, i])
        for d in range(2):
            @pl.when(has_next(d))
            def _():
                zcopy(4, d, 0, g).wait_send()
            for step in range(last - 1):
                @pl.when(jnp.logical_and(valid(d, step), has_next(d)))
                def _():
                    zcopy(4, d, step + 1, g).wait_send()

    def vcopy(i, owner):
        return remote(s.smb, s.sm.at[owner], s.ms.at[0], s.mr.at[0], rep, lax.rem(g + i, groups))

    def pair(owner, w):
        return (3 * owner + 1) // 2 + w

    def second(owner):
        return lax.rem(owner, 2) == 0

    def rows_at(r):
        return pl.ds(mo(r * tokens, 16), tokens)

    def scopy(i, w):
        dest = lax.rem(g + i, groups)
        return remote(s.agrad.at[:, third(pair(dest, w), 0)], s.a_h.at[w, rows_at(g), :], s.shs.at[w, i - 1], s.shr.at[w],
                      rep, dest)

    def rcopy(i, owner):
        return remote(s.rows3.at[groups], s.rows3.at[owner], s.rs.at[0], s.rr.at[0], rep, lax.rem(g + i, groups))

    def share_start():
        for i in range(1, groups):
            scopy(i, 0).start()

            @pl.when(second(lax.rem(g + i, groups)))
            def _():
                scopy(i, 1).start()
            rcopy(i, g).start()
        s.a_h[0, rows_at(g), :] = s.agrad[:, third(pair(g, 0), 0)]

        @pl.when(second(g))
        def _():
            s.a_h[1, rows_at(g), :] = s.agrad[:, third(pair(g, 1), 0)]
        s.csum[...] = jnp.zeros_like(s.csum)

    def share_got():
        arrived(s.a_h.at[0, pl.ds(0, last * tokens), :], s.shr.at[0])

        @pl.when(second(g))
        def _():
            arrived(s.a_h.at[1, pl.ds(0, last * tokens), :], s.shr.at[1])
        arrived(s.rows3.at[pl.ds(0, last)], s.rr.at[0])
        for i in range(groups):
            s.rows[0:2 * HEADS, i * tokens:(i + 1) * tokens] = s.rows3[i]
        s.rows[0:2 * HEADS, pl.ds(mo(g * tokens, LANE), tokens)] = s.rows3[groups]
        s.cols[...] = jnp.concatenate([s.rows[...], jnp.zeros((LANE - 2 * HEADS, groups * tokens), F32)], axis=0).T

    def share_sent():
        for i in range(1, groups):
            scopy(i, 0).wait_send()

            @pl.when(second(lax.rem(g + i, groups)))
            def _():
                scopy(i, 1).wait_send()
        sent(s.rows3.at[pl.ds(0, last)], s.rs.at[0])

    def bcopy_back(i, w, n):
        dest = lax.rem(g + i, groups)
        return remote(s.pgh.at[rows_at(dest), pl.ds((3 * w + n) * LANE, LANE)], s.pgrad.at[:, third(pair(g, w), n)],
                      s.bks.at[w], s.bkr.at[0], rep, dest)

    def each_pair(body):
        body(0)

        @pl.when(second(g))
        def _():
            body(1)

    def return_queries():
        def body(w):
            for i in range(1, groups):
                bcopy_back(i, w, 0).start()
            s.pgrad[:, third(pair(g, w), 0)] = s.pgh[rows_at(g), 3 * w * LANE:(3 * w + 1) * LANE]
        each_pair(body)

    def return_keys(i):
        def body(w):
            for n in (1, 2):
                if i:
                    bcopy_back(i, w, n).start()
                else:
                    s.pgrad[:, third(pair(g, w), n)] = s.pgh[rows_at(g), (3 * w + n) * LANE:(3 * w + n + 1) * LANE]
        each_pair(body)

    def return_got():
        @pl.when(second(g))
        def _():
            arrived(s.pgrad.at[:, pl.ds(0, 3 * D - 2 * PAIR)], s.bkr.at[0])

        @pl.when(jnp.logical_not(second(g)))
        def _():
            arrived(s.pgrad.at[:, pl.ds(0, 3 * D - PAIR)], s.bkr.at[0])

    def return_sent():
        sent(s.pgh.at[pl.ds(0, last * tokens), pl.ds(0, PAIR)], s.bks.at[0])

        @pl.when(second(g))
        def _():
            sent(s.pgh.at[pl.ds(0, last * tokens), pl.ds(0, PAIR)], s.bks.at[1])

    def row(i):
        return lax.rem(g + 1 + i, groups)

    def first(t, i):
        m = SUMS[t]
        at = pl.ds(mo(row(i) * m.block, 16), m.block)
        return remote(grads[t].at[at, pl.ds(mo((1 - h) * m.half, LANE), m.half)], s.buf1[t].at[at, :],
                      s.gone.at[t, i], s.c1r.at[t, i], core, g)

    def cell1(t, i, kk, sub=None):
        return cell(s.buf1[t], SUMS[t], row(i) * SUMS[t].block + kk * SUMS[t].quarter, sub)

    def cell2(t, i, j, sub):
        return cell(s.buf2[t], SUMS[t], (row(i) * 2 + j) * SUMS[t].quarter, sub)

    def cell3(t, i, sub=None):
        return cell(s.buf3[t], SUMS[t], row(i) * SUMS[t].quarter, sub)

    def a1(t, i, j, kk):
        return remote(cell1(t, i, kk, 0), cell2(t, i, j, 0), s.gone.at[t, i], s.ab1r.at[t, i], xn, g)

    def b1(t, i, j, kk):
        return remote(cell1(t, i, kk, 1), cell2(t, i, j, 1), s.gone.at[t, i], s.ab1r.at[t, i], yn, g)

    def a2(t, i, j):
        return remote(cell2(t, i, j, 0), cell3(t, i, 0), s.gone.at[t, i], s.ab2r.at[t, i], yn, g)

    def b2(t, i, j):
        return remote(cell2(t, i, j, 1), cell3(t, i, 1), s.gone.at[t, i], s.ab2r.at[t, i], xn, g)

    def z2(t, i):
        slot = (1 - lax.rem(g, 2)) if i == 0 else lax.rem(g, 2)
        return remote(cell3(t, i), s.zbuf[t].at[slot], s.gone.at[t, i], s.z2r.at[t, slot], rep, flip(g, 1))

    def z2_got(t, slot):
        arrived(s.zbuf[t].at[slot], s.z2r.at[t, slot])

    def z3(t):
        return remote(cell3(t, 1), s.zbuf[t].at[2], s.gone.at[t, 1], s.z2r.at[t, 2], rep, flip(g, 2))

    def z4(i):
        return remote(cell3(0, i), s.fin[0].at[0, :, pl.ds(mo(g * PAIR, LANE), PAIR)], s.gone.at[0, i], s.zqr.at[0], rep, row(i))

    def r1(t, i):
        m = SUMS[t]
        first(t, i).wait_recv()
        at = pl.ds(mo(row(i) * m.block, 16), m.block)
        mine = grads[t].at[at, pl.ds(mo(h * m.half, LANE), m.half)]
        add_rows(s.buf1[t].at[at, :], mine, s.buf1[t].at[at, :], m.block)
        for j in range(2):
            a1(t, i, j, 2 * j + (1 - x)).start()
            b1(t, i, j, 2 * (1 - y) + j).start()

    def r2(t, i):
        m = SUMS[t]
        arrived(s.buf2[t].at[pl.ds(mo(row(i) * 2 * m.quarter, 16), 2 * m.quarter), :], s.ab1r.at[t, i])
        for j in range(2):
            add_rows(cell2(t, i, j, 0), cell1(t, i, 2 * j + x, 0), cell2(t, i, j, 0), m.sub[0][1])
        a2(t, i, 1 - y).start()
        for j in range(2):
            add_rows(cell2(t, i, j, 1), cell1(t, i, 2 * y + j, 1), cell2(t, i, j, 1), m.sub[1][1])
        b2(t, i, 1 - x).start()

    def r3(t, i):
        m = SUMS[t]
        arrived(cell3(t, i), s.ab2r.at[t, i])
        add_rows(cell3(t, i, 0), cell2(t, i, y, 0), cell3(t, i, 0), m.sub[0][1])
        add_rows(cell3(t, i, 1), cell2(t, i, x, 1), cell3(t, i, 1), m.sub[1][1])
        if t == 0:
            if i < last:
                z4(i).start()
            else:
                s.fin[0][0, :, pl.ds(mo(g * PAIR, LANE), PAIR)] = cell3(0, last)[...]
        elif i % 2 == 0:
            z2(t, i).start()

    def r3b(t):
        z2_got(t, 0)
        add_rows(cell3(t, 1), cell3(t, 1), s.zbuf[t].at[0], SUMS[t].quarter)
        z3(t).start()

    def fpart(t, kk, hh, sub=None):
        return part(outs[t], WHOLES[t], 0, kk, hh, sub)

    def keep(t):
        return pltpu.make_async_copy(s.fin[t].at[0], fpart(t, k, h), s.os.at[t])

    def xsend(t):
        return remote(s.fin[t].at[0], fpart(t, k, h), s.osent.at[t], s.oxr.at[t], xn, g)

    def ysend(t):
        return remote(s.fin[t].at[0], fpart(t, k, h), s.osent.at[t], s.oyr.at[t], yn, g)

    def xgot(t):
        return remote(fpart(t, kx, h), fpart(t, kx, h), s.osent.at[t], s.oxr.at[t], xn, g)

    def ygot(t):
        return remote(fpart(t, ky, h), fpart(t, ky, h), s.osent.at[t], s.oyr.at[t], yn, g)

    def fwd(t, sub, kk):
        reg = fpart(t, kk, h, sub)
        return remote(reg, reg, s.osent.at[t], s.oar.at[t], (yn, xn)[sub], g)

    def cross(t, hh):
        reg = slab(outs[t], WHOLES[t], 0, hh)
        return remote(reg, reg, s.osent.at[t], s.ocr.at[t], core, g)

    def r4(t):
        m = WHOLES[t]
        if t == 0:
            arrived(s.fin[0].at[0, :, pl.ds(0, last * PAIR)], s.zqr.at[0])
        else:
            z2_got(t, 1)
            z3(t).wait_recv()
        mine = cell3(t, last)

        def body(n):
            at = pl.ds(mo(n * 16, 16), 16)
            total = mine[at, :].astype(F32) + s.zbuf[t][1, at, :].astype(F32) + s.zbuf[t][2, at, :].astype(F32)
            s.fin[t][0, at, :] = total.astype(BF)
        if t:
            loop(m.quarter // 16, body)
        for b in range(highs):
            cp = remote(s.fin[t].at[0], s.fin[t].at[1 + b], s.fxs.at[t, b], s.fxr.at[t, b], flip(rep, 8 << b), g)
            cp.start()
            cp.wait()
            add_rows(s.fin[t].at[0], s.fin[t].at[0], s.fin[t].at[1 + b], m.quarter)
        keep(t).start()
        xsend(t).start()
        ysend(t).start()

    def r5(t):
        xgot(t).wait_recv()
        fwd(t, 0, kx).start()
        ygot(t).wait_recv()
        fwd(t, 1, ky).start()

    def r6(t):
        arrived(fpart(t, kd, h), s.oar.at[t])
        keep(t).wait()
        cross(t, h).start()

    partners = []
    bit = 1
    while bit < groups:
        partners.append((rep, flip(g, bit)))
        bit *= 2
    partners += [(core, g), (xn, g), (yn, g)] + [(flip(rep, 8 << b), g) for b in range(highs)]

    def smcopy(j):
        return remote(s.smacc.at[j], s.smin.at[j], s.sms.at[j], s.smr.at[j], *partners[j])

    def small(j):
        if j:
            smcopy(j - 1).wait_recv()
            s.smacc[j] = s.smacc[j - 1] + s.smin[j - 1]
        if j < len(partners):
            smcopy(j).start()
        else:
            osm[...] = s.smacc[j, g]

    def crossed():
        for t in ORDER:
            cross(t, 1 - h).wait_recv()

    def chunks_sent():
        for t in ORDER:
            m = SUMS[t]
            for i in range(groups):
                sent(grads[t].at[pl.ds(0, (8 if i < last else 7) * m.quarter), pl.ds(0, m.half)], s.gone.at[t, i])

    def outs_sent():
        sent(s.sm.at[pl.ds(0, last)], s.ms.at[0])
        for t in ORDER:
            m = WHOLES[t]
            sent(grads[t].at[pl.ds(0, 7 * m.quarter), pl.ds(0, m.half)], s.osent.at[t])
        for j in range(len(partners)):
            smcopy(j).wait_send()

    def project(j):
        project_block(j, s.fa, s.gain1, s.shift1, s.bias3, s.wq, s.qkv, s.normed, s.turned_all, tokens)

    def attention(p):
        loop(2, lambda i: attend_pair(p + i, g, s.qkv, s.attended, s.stats, tokens))

    def block(n):
        return pl.ds(mo(n * 256, 256), 256)

    def to_middle():
        def body(n):
            c = block(n)
            s.middle[:, c] = nn(s.attended[...], s.wo[:, c]) + s.obias[0:1, c] + fr[:, c].astype(F32)
        loop(D // 256, body)
        value, _ = normalize(s.middle[...])
        s.normed[...] = (value * s.gain2[...] + s.shift2[...]).astype(BF)

    def hidden(i):
        def body(j):
            n = row(i) * (FF // 256 // groups) + j
            c = block(n)
            u = nn(s.normed[...], s.wu[:, c]) + s.ubias[0:1, c]
            bell = 0.5 * (1.0 + lax.erf(u * ROOT_HALF))
            s.act[:, c] = (u * bell).astype(BF)
            slope = bell + u * jnp.exp(-0.5 * u * u) * ROOT_TWO_PI
            grad = nt(ct[...], s.wd[block(n), :]) * slope
            s.v_up[0:1, c] = jnp.sum(grad, axis=0, keepdims=True)
            s.pre[:, c] = grad.astype(BF)
        loop(FF // 256 // groups, body)

    def to_output():
        def body(n):
            c = block(n)
            out_frames[:, c] = (nn(s.act[...], s.wd[:, c]) + s.dbias[0:1, c] + s.middle[:, c]).astype(BF)
        loop(D // 256, body)

    def back_up():
        def body(n):
            s.wide[:, block(n)] = nt(s.pre[...], s.wu[block(n), :])
        loop(D // 256, body)

    def back_norm():
        upstream = s.wide[...]
        normal, inverse = normalize(s.middle[...])
        s.v_gain2[...] = jnp.sum(upstream * normal, axis=0, keepdims=True)
        s.v_shift2[...] = jnp.sum(upstream, axis=0, keepdims=True)
        total = ct[...].astype(F32) + norm_back(upstream, normal, inverse, s.gain2[...])
        s.mgrad[...] = total
        s.half[...] = total.astype(BF)
        s.v_out[...] = jnp.sum(total, axis=0, keepdims=True)
        s.v_down[...] = jnp.sum(ct[...].astype(F32), axis=0, keepdims=True)

        def body(n):
            s.agrad[:, block(n)] = nt(s.half[...], s.wo[block(n), :]).astype(BF)
        loop(D // 256, body)
        lanes = lax.broadcasted_iota(jnp.int32, (tokens, LANE), 1)
        mask = head_mask(tokens)
        stats = s.stats[...]
        for p in range(HEADS // 2):
            c = slice(p * LANE, (p + 1) * LANE)
            product = s.agrad[:, c].astype(F32) * s.attended[:, c].astype(F32)
            for side in range(2):
                mine = jnp.where(mask if side == 0 else jnp.logical_not(mask), product, 0.0)
                stats = jnp.where(lanes == HEADS + 2 * p + side, jnp.sum(mine, axis=-1, keepdims=True), stats)
        s.stats[...] = stats
        s.rows3[groups] = stats.T[0:2 * HEADS, :]

    def weight(t, i, left, right):
        m = MATS[t]
        s.turned[0:m.block, :] = left[:, pl.ds(mo(row(i) * m.block, LANE if m.block % LANE == 0 else 64), m.block)].T

        def body(n):
            c = block(n)
            grads[t][pl.ds(mo(row(i) * m.block, 16), m.block), c] = nn(s.turned[0:m.block, :], right[:, c]).astype(BF)
        loop(m.cols // 256, body)
        first(t, i).start()

    def turn(left, out):
        out[...] = left[...].T

    def weight_all(t, left, right):
        def body(n):
            c = block(n)
            grads[t][:, c] = nn(left[...], right[:, c]).astype(BF)
        loop(MATS[t].cols // 256, body)
        for i in (0, 2, 1, 3):
            first(t, i).start()

    pairs_here = 2 - lax.rem(g, 2)

    def queries(j):
        loop(pairs_here, lambda w: query_back(w, pair(g, w), j, s.qkv, s.a_h, s.cols, s.pgh, s.csum, tokens))

    def keys(i):
        j = lax.rem(g + i, groups)
        loop(pairs_here, lambda w: key_back(w, pair(g, w), j, s.qkv, s.a_h, s.rows, s.pgh, s.csum, tokens))

    def weight_pairs():
        s.acc[...] = jnp.zeros_like(s.acc)

        def body(w):
            product = nn(s.turned_all[...], s.pgh[:, pl.ds(mo(w * PAIR, LANE), PAIR)])
            sums = s.csum[0:1, pl.ds(mo(w * PAIR, LANE), PAIR)]
            s.wu[:, pl.ds(mo(w * PAIR, LANE), PAIR)] = (product * s.columns[:, 0:1] + s.columns[:, 1:2] * sums).astype(BF)
            for n in range(3):
                weights = s.wq[:, third(pair(g, w), n)].astype(F32)
                c = slice(n * LANE, (n + 1) * LANE)
                s.acc[0] = s.acc[0] + weights * product[:, c]
                s.acc[1] = s.acc[1] + weights * sums[:, c]
        loop(pairs_here, body)

        @pl.when(jnp.logical_not(second(g)))
        def _():
            s.wu[:, PAIR:2 * PAIR] = jnp.zeros((D, PAIR), BF)
        for i in (0, 2, 1, 3):
            first(0, i).start()

    def send_small():
        s.v_gain1[...] = jnp.sum(s.acc[0].T, axis=0, keepdims=True)
        s.v_shift1[...] = jnp.sum(s.acc[1].T, axis=0, keepdims=True)
        s.v_qv[...] = jnp.zeros_like(s.v_qv)

        def body(w):
            p = pair(g, w)
            s.v_qv[0:1, third(p, 0)] = s.csum[0:1, pl.ds(mo(w * PAIR, LANE), LANE)]
            s.v_qv[0:1, third(p, 1)] = s.csum[0:1, pl.ds(mo(w * PAIR + 2 * LANE, LANE), LANE)]
        loop(pairs_here, body)
        fill_image(s.smacc.at[0], range(SROWS), (
            (GAIN_ONE, s.v_gain1), (SHIFT_ONE, s.v_shift1), (QV_BIAS, s.v_qv), (OUT_BIAS, s.v_out), (GAIN_TWO, s.v_gain2),
            (SHIFT_TWO, s.v_shift2), (UP_BIAS, s.v_up), (DOWN_BIAS, s.v_down)))
        small(0)

    def input_grad():
        def body(n):
            s.wide[:, block(n)] = nt(s.pgrad[...], s.wq[block(n), :])
        loop(D // 256, body)
        normal, inverse = normalize(fr[...].astype(F32))
        frames_grad[...] = (s.mgrad[...] + norm_back(s.wide[...], normal, inverse, s.gain1[...])).astype(BF)

    barrier, peers = greet(rep, g, groups)
    peers += [(flip(rep, 8 << b), g) for b in range(highs)]
    for t in range(3):
        piece_load(t, 0, t).start()
    for cp in small_loads():
        cp.start()
    own_frames = pltpu.make_async_copy(fr, zregion(4, g), s.ssem.at[1])
    own_frames.start()
    do_barrier(barrier, peers)
    relayout(0, 0, 0)
    own_send(0)
    piece_load(3, 0, 0).start()
    relayout(1, 0, 1)
    own_send(1)
    relayout(2, 0, 2)
    own_send(2)
    pltpu.make_async_copy(s.spbuf, s.spbuf, s.ssem.at[0]).wait()
    s.smb[...] = jnp.zeros_like(s.smb)
    count = sum(c for _, c in SMALL)
    s.smb[0:count, :] = s.spbuf[...].astype(F32).reshape(count, LANE)
    for i in range(1, groups):
        vcopy(i, g).start()
    both(0, 0, 0)
    both(0, 0, 1)
    own_frames.wait()
    own_send(4)
    relayout(3, 0, 0)
    own_send(3)
    rest_load(0)
    rest(0)
    rest_load(1)
    both(0, 0, 2)
    both(1, 0, 0)
    both(1, 0, 1)
    both(0, 1, 0)
    both(0, 2, 0)
    both(1, 0, 2)
    both(2, 0, 0)
    both(2, 0, 1)
    rest(1)
    rest_load(2)
    both(2, 0, 2)
    arrived(s.sm.at[pl.ds(0, last)], s.mr.at[0])
    s.sm[g] = s.smb[...]
    for spot, ref in ((GAIN_ONE, s.gain1), (SHIFT_ONE, s.shift1), (QV_BIAS, s.qvbias), (GAIN_TWO, s.gain2), (SHIFT_TWO, s.shift2),
                      (OUT_BIAS, s.obias), (UP_BIAS, s.ubias), (DOWN_BIAS, s.dbias)):
        assemble(s.sm, spot, ref)
    lower = lax.broadcasted_iota(jnp.int32, (LANE, D), 0) == 0
    s.columns[...] = jnp.where(lower, s.gain1[...], s.shift1[...]).T
    s.bias3[...] = jnp.zeros_like(s.bias3)
    s.bias3[0:1, 0:D] = s.qvbias[0:1, 0:D]
    s.bias3[0:1, 2 * D:3 * D] = s.qvbias[0:1, D:2 * D]
    s.stats[...] = jnp.zeros_like(s.stats)
    both(0, 4, 0)
    rest(2)
    rest_load(3)
    both(1, 1, 0)
    both(1, 2, 0)
    for step in range(last):
        both(3, 0, step)
    project(g)
    both(0, 3, 0)

    def project_rows(step):
        def body(d):
            r = g + (2 * d - 1) * (1 + step)

            @pl.when(jnp.logical_and(r >= 0, r <= last))
            def _():
                project(r)
        loop(2, body)
    project_rows(0)
    both(0, 4, 1)
    rest(3)
    both(2, 1, 0)
    both(2, 2, 0)
    both(1, 3, 0)
    both(0, 1, 1)
    both(0, 2, 1)
    project_rows(1)
    both(0, 3, 1)
    both(2, 3, 0)
    both(1, 1, 1)
    both(1, 2, 1)
    both(0, 4, 2)
    project_rows(2)
    both(0, 1, 2)
    both(1, 3, 1)
    both(2, 1, 1)
    both(2, 2, 1)
    both(0, 2, 2)
    attention(0)
    both(0, 3, 2)
    both(1, 1, 2)
    both(2, 3, 1)
    attention(2)
    both(1, 2, 2)
    attention(4)
    both(1, 3, 2)
    both(2, 1, 2)
    both(2, 2, 2)
    both(2, 3, 2)
    rest = [(t, step) for step in range(last) for t in (1, 2, 3)]
    for t, step in rest:
        if t == 1:
            both(3, t, step)
    to_middle()
    for t, step in rest:
        if t > 1:
            both(3, t, step)
    hidden(0)
    weight(3, 0, s.act, ct)
    hidden(1)
    hidden(2)
    r1(3, 0)
    hidden(3)
    back_up()
    back_norm()
    share_start()
    weight(3, 2, s.act, ct)
    r2(3, 0)
    weight(3, 1, s.act, ct)
    r1(3, 2)
    weight(3, 3, s.act, ct)
    r1(3, 1)
    turn(s.normed, s.turned)
    r1(3, 3)
    r2(3, 2)
    weight_all(2, s.turned, s.pre)
    r2(3, 1)
    r1(2, 0)
    share_got()
    r1(2, 2)
    turn(s.attended, s.turned)
    weight_all(1, s.turned, s.half)
    r2(3, 3)
    queries(0)
    r3(3, 0)
    r3(3, 2)
    queries(1)
    r2(2, 0)
    r1(2, 1)
    queries(2)
    gather_sent()
    r3(3, 1)
    r3(3, 3)
    queries(3)
    r2(2, 2)
    r1(2, 3)
    keys(1)
    r3b(3)
    r2(2, 1)
    for i in (0, 2, 1, 3):
        r1(1, i)
    keys(2)
    r3(2, 0)
    r3(2, 2)
    r2(2, 3)
    keys(3)
    r2(1, 0)
    r2(1, 2)
    keys(0)
    r3(2, 1)
    r3(2, 3)
    r4(3)
    r3b(2)
    return_queries()
    weight_pairs()
    r2(1, 1)
    r2(1, 3)
    send_small()
    for i in (0, 2, 1, 3):
        r1(0, i)
    r5(3)
    r3(1, 0)
    r3(1, 2)
    for i in (0, 2, 1, 3):
        r2(0, i)
    r3(1, 1)
    r3(1, 3)
    r4(2)
    for i in (0, 2, 1, 3):
        r3(0, i)
    small(1)
    r3b(1)
    for i in (1, 2, 3, 0):
        return_keys(i)
    to_output()
    r6(3)
    r5(2)
    small(2)
    r4(0)
    r4(1)
    small(3)
    r5(0)
    r6(2)
    r5(1)
    small(4)
    r6(0)
    r6(1)
    return_got()
    input_grad()
    for j in range(5, len(partners) + 1):
        small(j)
    return_sent()
    crossed()
    share_sent()
    chunks_sent()
    outs_sent()


def layer(frames, cotangent, params, groups, reps):
    dma = pltpu.SemaphoreType.DMA
    tokens = frames.shape[0]
    clip = tokens * groups
    highs = (reps // 8).bit_length() - 1
    steps = 3 + highs + groups.bit_length() - 1
    n = 2 * (groups - 1)

    def bf(*shape):
        return pltpu.VMEM(shape, BF)

    def wide(*shape):
        return pltpu.VMEM(shape, F32)

    scratch = {name: bf(m.block * groups, m.cols) for name, m in zip(("wq", "wo", "wu", "wd"), MATS)}
    scratch.update(go=bf(D, D), gu=bf(D, FF), gd=bf(FF, D))
    scratch.update(buf1=[bf(m.block * groups, m.half) for m in SUMS], buf2=[bf(m.quarter * groups * 2, m.half) for m in SUMS],
                   buf3=[bf(m.quarter * groups, m.half) for m in SUMS], zbuf=[bf(groups - 1 if t else 1, m.quarter, m.half) for t, m in enumerate(SUMS)],
                   fin=[bf(highs + 1, m.quarter, m.half) for m in WHOLES])
    scratch.update(fa=bf(clip, D), qkv=bf(clip, 3 * D), a_h=bf(2, clip, LANE), agrad=bf(tokens, D), pgh=bf(clip, 2 * PAIR), turned_all=bf(D, clip))
    scratch.update(attended=bf(tokens, D), normed=bf(tokens, D), half=bf(tokens, D),
                   act=bf(tokens, FF), pre=bf(tokens, FF), pgrad=bf(tokens, 3 * D), turned=bf(D, tokens))
    scratch.update(middle=wide(tokens, D), mgrad=wide(tokens, D), wide=wide(tokens, D),
                   stats=wide(tokens, LANE))
    scratch.update(rows3=wide(groups + 1, 2 * HEADS, tokens), rows=wide(2 * HEADS, clip), cols=wide(clip, LANE), csum=wide(1, 2 * PAIR),
                   columns=wide(D, LANE), acc=wide(2, D, LANE))
    scratch.update({name: wide(1, D) for name in ("gain1", "shift1", "gain2", "shift2", "obias", "dbias", "v_gain1", "v_shift1",
                                                  "v_gain2", "v_shift2", "v_out", "v_down")})
    scratch.update(qvbias=wide(1, 2 * D), bias3=wide(1, 3 * D), v_qv=wide(1, 2 * D), ubias=wide(1, FF), v_up=wide(1, FF))
    piece = max(m.quarter * m.tiles + 8 for m in MATS)
    scratch.update(pbuf=bf(3, 1, piece * LANE), fbuf=wide(piece, LANE), spbuf=bf(1, sum(c for _, c in SMALL) * LANE),
                   smb=wide(SROWS, LANE), sm=wide(groups, SROWS, LANE),
                   smacc=wide(steps + 1, groups, SROWS, LANE), smin=wide(steps, groups, SROWS, LANE))
    scratch.update(lsem=dma((3,)), ssem=dma((2,)), zs=dma((4,)), zfs=dma((2, groups - 1)), zr=dma((5, groups - 1)))
    scratch.update({name: dma((4, groups - 1)) for name in ("gs", "xr", "yr", "fr", "cr", "z2r")})
    scratch.update({name: dma((1,)) for name in ("ms", "mr", "rs", "rr")})
    scratch.update(shs=dma((2, groups - 1)), shr=dma((2,)), bks=dma((2,)), bkr=dma((1,)), zqr=dma((1,)))
    scratch.update({name: dma((4, groups)) for name in ("gone", "c1r", "ab1r", "ab2r")})
    if highs:
        scratch.update({name: dma((4, highs)) for name in ("fxs", "fxr")})
    scratch.update({name: dma((4,)) for name in ("os", "osent", "oxr", "oyr", "oar", "ocr")})
    scratch.update(sms=dma((steps,)), smr=dma((steps,)))
    vmem, hbm = pl.BlockSpec(memory_space=pltpu.VMEM), pl.BlockSpec(memory_space=pl.ANY)
    sds = jax.ShapeDtypeStruct
    names = tuple(scratch)
    flat, tree = jax.tree.flatten(list(scratch.values()))

    def body(*refs):
        fixed = 10
        layer_kernel(groups, highs, names, *refs[:fixed], *jax.tree.unflatten(tree, refs[fixed:]))

    return pl.pallas_call(
        body,
        out_shape=[sds((m.block, m.cols), BF) for m in WHOLES] + [sds((SROWS, LANE), F32), sds((tokens, D), BF), sds((tokens, D), BF)],
        in_specs=[vmem, vmem, hbm],
        out_specs=[hbm] * 4 + [vmem] * 3,
        scratch_shapes=flat,
        compiler_params=pltpu.CompilerParams(collective_id=0, has_side_effects=True, vmem_limit_bytes=67043328),
        name="layer",
    )(frames, cotangent, params)


BETA_ONE = 0.9
BETA_TWO = 0.98
ADAM_EPS = 1e-06
LEARN_RATE = 0.006
DECAY = 0.01
ADAM_STEP = 4
ROWS = 1792
CHUNKS = -(-FROWS // ROWS)
SUB = 224


def flatten(m, block, flat, late):
    def body(i):
        base = m.row0 + i * (48 * m.tiles)
        for c in range(m.tiles):
            at = (c % (m.tiles // 3)) if m is QKV else 0
            at = (at % 3 == 1) * 12 + (0, 0, 1, 2, 2, 3)[at] * 3 + c // (m.tiles // 3) if m is QKV else c
            tile = block[pl.ds(mo(i * 48, 16), 48), at * LANE:(at + 1) * LANE].astype(F32)
            if m.shifted:
                tile = pltpu.roll(tile, 64, 1)
                late[pl.ds(base + c + 1, 48, stride=m.tiles), :] = tile
            flat[pl.ds(base + c, 48, stride=m.tiles), :] = tile
    loop(m.block // 48, body)


def adam_kernel(scale, gq, go, gu, gd, sm, p_hbm, m_hbm, v_hbm, fo, fg, o_g, o_p, o_m, o_v, o_fo, o_fg,
                bq, bo, bu, bd, flat, late, pb, mb, vb, gb, nb, frames, bsem, isem, osem, fsem):
    blocks = (bq, bo, bu, bd)

    def view(ref, c):
        return ref.at[:, pl.ds(c * ROWS * LANE, min(ROWS, FROWS - c * ROWS) * LANE)]

    loads = [pltpu.make_async_copy(a, b, bsem.at[i]) for i, (a, b) in enumerate(zip((gq, go, gu, gd), blocks))]
    pairs = ((p_hbm, pb), (m_hbm, mb), (v_hbm, vb))
    ins = [[pltpu.make_async_copy(view(a, c), view(b, c), isem.at[c, i]) for i, (a, b) in enumerate(pairs)] for c in range(CHUNKS)]
    results = ((gb, o_g), (nb, o_p), (mb, o_m), (vb, o_v))
    puts = [[pltpu.make_async_copy(view(a, c), view(b, c), osem.at[c, i]) for i, (a, b) in enumerate(results)] for c in range(CHUNKS)]
    takes = [pltpu.make_async_copy(a, frames.at[i], fsem.at[i]) for i, a in enumerate((fo, fg))]
    gives = [pltpu.make_async_copy(frames.at[i], a, fsem.at[2 + i]) for i, a in enumerate((o_fo, o_fg))]
    def fetch(c):
        if c < CHUNKS:
            for cp in ins[c]:
                cp.start()

    loads[0].start()
    fetch(0)
    loads[1].start()
    fetch(1)
    loads[2].start()
    fetch(2)
    loads[3].start()

    def update(c):
        for cp in ins[c]:
            cp.wait()

        def body(j):
            start = c * ROWS + j * SUB
            at = pl.ds(mo(start, 8), SUB)
            lanes = (slice(None), pl.ds(mo(start * LANE, LANE), SUB * LANE))
            number = start + lax.broadcasted_iota(jnp.int32, (SUB, LANE), 0)
            low = lax.broadcasted_iota(jnp.int32, (SUB, LANE), 1) < 64
            grad = jnp.where(jnp.logical_and(number > UP.row0, low), late[at, :], flat[at, :]).reshape(1, SUB * LANE) * scale
            first = BETA_ONE * mb[lanes] + (1.0 - BETA_ONE) * grad
            second = BETA_TWO * vb[lanes] + (1.0 - BETA_TWO) * grad * grad
            gb[lanes] = grad
            mb[lanes] = first
            vb[lanes] = second
            first_hat = first * (1.0 / (1.0 - BETA_ONE**ADAM_STEP))
            second_hat = second * (1.0 / (1.0 - BETA_TWO**ADAM_STEP))
            current = pb[lanes].astype(F32)
            nb[lanes] = current - LEARN_RATE * (first_hat / (jnp.sqrt(second_hat) + ADAM_EPS) + DECAY * current)
        loop(-(-min(ROWS, FROWS - c * ROWS) // SUB), body)
        fetch(c + 3)
        for cp in puts[c]:
            cp.start()

    loads[0].wait()
    flatten(QKV, bq, flat, late)
    flat[0:3, :] = sm[0:3, :]
    update(0)
    loads[1].wait()
    flatten(OUT, bo, flat, late)
    flat[3459:3462, :] = sm[3:6, :]
    update(1)
    loads[2].wait()
    flatten(UP, bu, flat, late)
    flat[4614:4618, :] = sm[6:10, :]
    flat[4618:4619, 0:64] = sm[10:11, 0:64]
    flat[9226:9227, 64:128] = sm[11:12, 64:128]
    update(2)
    update(3)
    for cp in takes:
        cp.start()
    update(4)
    loads[3].wait()
    flatten(DOWN, bd, flat, late)
    for ref in (flat, late):
        ref[9227:9232, :] = sm[12:17, :]
        ref[9232:9233, 0:64] = sm[17:18, 0:64]
        ref[13841:13842, :] = sm[19:20, :]
    flat[13840:13841, 64:128] = sm[18:19, 64:128]
    update(5)
    for cp in takes:
        cp.wait()
    for cp in gives:
        cp.start()
    for c in range(6, CHUNKS):
        update(c)
    for cp in gives:
        cp.wait()
    for chunk in puts:
        for cp in chunk:
            cp.wait()


def adam(blocks, smalls, params, first, second, reps, *outputs):
    vmem, hbm = pl.BlockSpec(memory_space=pltpu.VMEM), pl.BlockSpec(memory_space=pl.ANY)
    dma = pltpu.SemaphoreType.DMA
    row = pltpu.VMEM((1, CHUNKS * ROWS * LANE), F32)
    return pl.pallas_call(
        functools.partial(adam_kernel, 1.0 / reps),
        out_shape=[jax.ShapeDtypeStruct((1, FLAT), F32)] * 4 + [jax.ShapeDtypeStruct(o.shape, o.dtype) for o in outputs],
        in_specs=[hbm] * 4 + [vmem] + [hbm] * 5,
        out_specs=[hbm] * 6,
        scratch_shapes=[pltpu.VMEM(b.shape, BF) for b in blocks] + [pltpu.VMEM((CHUNKS * ROWS, LANE), F32)] * 2
        + [pltpu.VMEM((1, CHUNKS * ROWS * LANE), BF)] + [row] * 4 + [pltpu.VMEM((2,) + outputs[0].shape, BF)]
        + [dma((4,)), dma((CHUNKS, 3)), dma((CHUNKS, 4)), dma((4,))],
        compiler_params=pltpu.CompilerParams(vmem_limit_bytes=67043328),
        name="adam",
    )(*blocks, smalls, params, first, second, *outputs)


def on_device(frames, cotangent, params, first_moment, second_moment):
    groups, reps = lax.axis_size("grp"), lax.axis_size("rep")
    *blocks, small, out_frames, frames_grad = layer(frames, cotangent, params, groups, reps)
    param_grad, new_params, new_first, new_second, out_frames, frames_grad = adam(
        blocks, small, params, first_moment, second_moment, reps, out_frames, frames_grad)
    return (out_frames, frames_grad, param_grad, new_params, new_first, new_second)


def solution(mesh):
    in_specs = (
        P(("rep", "grp"), None),
        P(("rep", "grp"), None),
        P("grp", None),
        P("grp", None),
        P("grp", None),
    )
    out_specs = (
        P(("rep", "grp"), None),
        P(("rep", "grp"), None),
        P("grp", None),
        P("grp", None),
        P("grp", None),
        P("grp", None),
    )
    return jax.shard_map(
        on_device, mesh=mesh, in_specs=in_specs, out_specs=out_specs, check_vma=False
    )
```
